32 devices in a mesh: fsdp: 4 (over y, x), context: 2 (over core), tensor: 4 (over z).
Axes of the slice: x: 2, y: 2, z: 4, core: 2. Of those that a mesh axis runs over, the one named last changes fastest.
Arguments:
- tokens: bfloat16 [1024, 4, 1024], P('context', 'fsdp'), may hold values from -6 to 6
- out_grad: bfloat16 [1024, 4, 1024], P('context', 'fsdp'), may hold values from -6 to 6
- weight_stack: bfloat16 [4, 4, 1312, 1024], P('fsdp', 'tensor', 'context'), as said below
- muon_state: float32 [4, 4, 1312, 1024], P('fsdp', 'tensor', 'context'), as said below
- norm_gains: float32 [2, 1024], replicated, may hold values from 0.5 to 1.5
- adam_first: float32 [2, 1024], replicated, may hold values from -112 to 112
- adam_second: float32 [2, 1024], replicated, may hold values from 122.88 to 1228.8
- segment_ids: int32 [1024, 4], P(None, 'fsdp'), may hold values from 0 to 1024, as said below
- position_ids: int32 [1024, 4], P('context', 'fsdp'), may hold values from 0 to 1023, as said below
Outputs:
- layer_out: bfloat16 [1024, 4, 1024], P('context', 'fsdp')
- tokens_grad: bfloat16 [1024, 4, 1024], P('context', 'fsdp')
- weight_grads: float32 [4, 4, 1312, 1024], P('fsdp', 'tensor', 'context')
- muon_next: float32 [4, 4, 1312, 1024], P('fsdp', 'tensor', 'context')
- weight_update: float32 [4, 4, 1312, 1024], P('fsdp', 'tensor', 'context')
- direction_scale: float32 [4], P('fsdp')
- gain_grads: float32 [2, 1024], replicated
- adam_first_next: float32 [2, 1024], replicated
- adam_second_next: float32 [2, 1024], replicated
- gain_update: float32 [2, 1024], replicated
The draws below stay inside these ranges and needn't reach their ends.
Inputs may be any that keep to these rules, and one draw needn't show every extreme that they name: `segment_ids`: along a sequence the nonzero ids start at 1 and rise by at most one from one token to the next; id 0 marks padding, a possibly empty run of tokens at the end of a sequence. `position_ids`: A token's offset from the first token of its document, or of the padding run. `weight_stack`: rows of a block beyond its weight's row count (R_k of the steps) are zero. `muon_state`: rows of a block beyond its weight's row count are zero.
All inputs are finite; a program needn't handle non-finite values.
Results may differ from the reference program's by a relative error of at most 0.035.
Values may be sent and summed in bfloat16 or wider, within the bound.
A program may use at most 192 MiB of HBM per device.

```python
import math
import jax
import jax.numpy as jnp
from jax import lax

D = 1024
HEAD_DIM = 64
FF = 2624
LEN = 1024
ITERS = 5
STEP = 8
BATCH = 4
PAD = 1312
N_CONTEXT = 2
N_TENSOR = 4


def stack_mask(scales_list):
    n_tensor = 2 * FF // PAD
    row_counts = jnp.array([3 * D // n_tensor, D // n_tensor, 2 * FF // n_tensor, FF // n_tensor], jnp.int32)
    row_index = jnp.arange(PAD, dtype=jnp.int32)[None, None, :, None]
    live_rows = row_index < row_counts[:, None, None, None]
    scale_rows = jnp.array(scales_list, jnp.float32)[:, None, None, None]
    return (n_tensor, live_rows, scale_rows)


def draw_weight_stack(key, part):
    n_tensor, live_rows, scale_rows = stack_mask([D ** (-0.5), 4.0 * D ** (-0.5), D ** (-0.5), FF ** (-0.5)])
    normal_draw = jax.random.truncated_normal(jax.random.fold_in(key, 3), -4.0, 4.0, (4, n_tensor, PAD, D), jnp.float32)
    return jnp.where(live_rows, normal_draw * scale_rows, 0.0).astype(jnp.bfloat16)


def draw_muon_state(key, part):
    state_scale = 0.3 * (LEN * BATCH) ** 0.5
    n_tensor, live_rows, scale_rows = stack_mask([state_scale, state_scale, state_scale, state_scale])
    normal_draw = jax.random.truncated_normal(jax.random.fold_in(key, 5), -5.0, 5.0, (4, n_tensor, PAD, D), jnp.float32)
    block_rows = PAD // N_CONTEXT
    heavy_group = jax.random.randint(jax.random.fold_in(key, 7), (4, 1, 1, 1), 0, n_tensor)
    heavy_block = jax.random.randint(jax.random.fold_in(key, 9), (4, 1, 1, 1), 0, N_CONTEXT)
    group_index = jnp.arange(n_tensor, dtype=jnp.int32)[None, :, None, None]
    block_index = (jnp.arange(PAD, dtype=jnp.int32) // block_rows)[None, None, :, None]
    heavy = (group_index == heavy_group) & (block_index == heavy_block)
    boost = jnp.where(heavy, 10.0, 1.0)
    return jnp.where(live_rows, normal_draw * scale_rows * boost, 0.0).astype(jnp.float32)


def doc_layout(key):
    keyed = jax.random.fold_in(key, 11)
    first_key, second_key, third_key = jax.random.split(keyed, 3)
    level = jax.random.randint(first_key, (1, BATCH), 0, 6)
    chance = jnp.left_shift(jnp.ones_like(level), level)
    uniform_ints = jax.random.randint(second_key, (LEN, BATCH), 0, LEN)
    index = jnp.arange(LEN, dtype=jnp.int32)[:, None]
    column = jnp.arange(BATCH, dtype=jnp.int32)[None, :]
    starts = (uniform_ints < chance) | (index == 0)
    starts = jnp.where(column == 0, index == 0, starts)
    starts = jnp.where(column == 1, True, starts)
    ident = jnp.cumsum(starts.astype(jnp.int32), axis=0)
    padding = jax.random.randint(third_key, (1, BATCH), 0, LEN // 8 + 1)
    padding = jnp.where(column < 2, 0, padding)
    pad_start = LEN - padding
    in_pad = index >= pad_start
    begin = lax.cummax(jnp.where(starts, index, 0), axis=0)
    segment = jnp.where(in_pad, 0, ident)
    position = index - jnp.where(in_pad, pad_start, begin)
    return (segment.astype(jnp.int32), position.astype(jnp.int32))


def draw_segment_ids(key, part):
    return doc_layout(key)[0]


def draw_position_ids(key, part):
    return doc_layout(key)[1]


def steps_of(stream_key, dims, shards, smallest, top_value):
    loudness = 1.0
    for dim, blocks in shards:
        heights = jax.random.uniform(jax.random.fold_in(jax.random.fold_in(stream_key, 6), dim), (blocks,), jnp.float32, smallest / len(shards), top_value / len(shards))
        loudness = loudness * jnp.repeat(jnp.exp(heights), dims[dim] // blocks).reshape((-1,) + (1,) * (len(dims) - 1 - dim))
    return loudness


def gaussian(key, extent, deviation, most, cuts=(), kind=jnp.bfloat16):
    factor_of = steps_of(key, extent, cuts, -0.22, 0.18) if cuts else 1.0
    entries = jax.random.normal(key, extent, jnp.float32) * deviation * factor_of
    return jnp.minimum(jnp.maximum(entries, -most), most).astype(kind)


def setup_inputs(seed: int = 0) -> dict:
    arg_keys = jax.random.split(jax.random.key(seed), 10)
    return {
        "tokens": gaussian(arg_keys[0], (LEN, BATCH, D), 1.0, 6.0, ((0, 2), (1, 4))),
        "out_grad": gaussian(arg_keys[1], (LEN, BATCH, D), 1.0, 6.0, ((0, 2), (1, 4))),
        "weight_stack": draw_weight_stack(jax.random.fold_in(arg_keys[9], 71), 0),
        "muon_state": draw_muon_state(jax.random.fold_in(arg_keys[9], 71), 0),
        "norm_gains": jnp.clip(1.0 + 0.1 * jax.random.normal(arg_keys[4], (2, D), jnp.float32), 0.5, 1.5),
        "adam_first": gaussian(arg_keys[5], (2, D), (0.3 * (LEN * BATCH) ** 0.5), 112.0, (), jnp.float32),
        "adam_second": jnp.clip(jax.random.uniform(arg_keys[6], (2, D), jnp.float32, 122.88, 1228.8), 122.88, 1228.8),
        "segment_ids": draw_segment_ids(jax.random.fold_in(arg_keys[9], 71), 0),
        "position_ids": draw_position_ids(jax.random.fold_in(arg_keys[9], 71), 0),
    }


@jax.custom_vjp
def low(v):
    return lax.optimization_barrier(v.astype(jnp.bfloat16)).astype(jnp.float32)

@jax.custom_vjp
def low_back(v):
    return v

def low_keep(v):
    return (low(v), None)

def low_pass(kept, grad):
    return (grad,)

def back_keep(v):
    return (v, None)

def back_low(kept, grad):
    return (low(grad),)
low.defvjp(low_keep, low_pass)
low_back.defvjp(back_keep, back_low)
precision_highest = lax.Precision.HIGHEST
rope_base = 160000.0
norm_eps = 1e-05
ns_first = 3.4445
ns_second = -4.775
ns_third = 2.0315
muon_beta = 0.5
muon_rate = 0.15
decay_rate = 0.1
adam_beta = 0.5
adam_rate = 0.05
ortho_eps = 1e-07
adam_eps = 1e-08

def layer_norm(values, gain_row):
    centre = values - lax.optimization_barrier(jnp.mean(values, axis=-1, keepdims=True))
    spread = lax.optimization_barrier(jnp.mean(centre * centre, axis=-1, keepdims=True))
    return centre * lax.rsqrt(spread + norm_eps) * gain_row

def rope_tables(positions, head_width):
    half_width = head_width // 2
    freqs = rope_base ** (-(jnp.arange(half_width, dtype=jnp.float32) * 2.0 / head_width))
    angle = positions.astype(jnp.float32)[..., None] * freqs
    angle = jnp.concatenate([angle, angle], axis=-1)
    return (jnp.cos(angle), jnp.sin(angle))

def rotate(values, cosine, sine_table):
    half_width = values.shape[-1] // 2
    turned = jnp.concatenate([-values[..., half_width:], values[..., :half_width]], axis=-1)
    return values * cosine + turned * sine_table

def attend_one(query_matrix, key_matrix_rows, value_matrix_rows, segment):
    unscaled_score = jnp.einsum('prt,frt->rpf', query_matrix, key_matrix_rows, precision=precision_highest)
    unscaled_score = low_back(unscaled_score)
    same_doc = (segment[:, None] == segment[None, :])[None]
    scores = jnp.where(same_doc, unscaled_score * HEAD_DIM ** (-0.5), -jnp.inf)
    row_max = lax.optimization_barrier(jnp.max(scores, axis=-1, keepdims=True))
    log_total = row_max + jnp.log(lax.optimization_barrier(jnp.sum(jnp.exp(scores - row_max), axis=-1, keepdims=True)))
    attention_probabilities = jnp.exp(scores - log_total)
    return jnp.einsum('sxj,jsv->xsv', low(attention_probabilities), value_matrix_rows, precision=precision_highest)

def forward(inputs, w_qkv, w_out, w_in, w_down, gain_rows, segments, cosine, sine_table):
    length, batch_size, model_width = inputs.shape
    groups = w_qkv.shape[0]
    heads_dev = w_out.shape[1] // HEAD_DIM
    ff_dev = w_down.shape[1]
    act_in = low(layer_norm(inputs, gain_rows[0]))
    projected = low_back(jnp.einsum('lbd,trd->lbtr', act_in, w_qkv, precision=precision_highest))
    projected = projected.reshape(length, batch_size, groups, 3, heads_dev, HEAD_DIM)
    rot_cos = cosine[:, :, None, None, :]
    rot_sin = sine_table[:, :, None, None, :]
    all_heads = groups * heads_dev
    query_matrix = low(rotate(projected[:, :, :, 0], rot_cos, rot_sin)).reshape(length, batch_size, all_heads, HEAD_DIM)
    key_matrix_rows = low(rotate(projected[:, :, :, 1], rot_cos, rot_sin)).reshape(length, batch_size, all_heads, HEAD_DIM)
    value_matrix_rows = low(projected[:, :, :, 2]).reshape(length, batch_size, all_heads, HEAD_DIM)
    attend = jax.checkpoint(attend_one)

    def per_sequence(pieces):
        return attend(pieces[0], pieces[1], pieces[2], pieces[3])
    attended = lax.map(per_sequence, (jnp.swapaxes(query_matrix, 0, 1), jnp.swapaxes(key_matrix_rows, 0, 1), jnp.swapaxes(value_matrix_rows, 0, 1), jnp.swapaxes(segments, 0, 1)))
    attended = jnp.swapaxes(attended, 0, 1)
    keep_mask = (segments > 0).astype(jnp.float32)[:, :, None, None]
    attn_in = low_back(low(attended * keep_mask)).reshape(length, batch_size, groups, heads_dev * HEAD_DIM)
    branch_one = low_back(lax.optimization_barrier(jnp.sum(low(jnp.einsum('lbtr,trd->lbtd', attn_in, w_out, precision=precision_highest)), axis=2)))
    resid = inputs + branch_one
    mlp_in = low(layer_norm(resid, gain_rows[1]))
    mixed_rows = low_back(jnp.einsum('lbd,trd->lbtr', mlp_in, w_in, precision=precision_highest))
    hidden = low(jax.nn.gelu(mixed_rows[..., :ff_dev], approximate=False) * mixed_rows[..., ff_dev:])
    branch_two = low_back(lax.optimization_barrier(jnp.sum(low(jnp.einsum('lbtr,trd->lbtd', hidden, w_down, precision=precision_highest)), axis=2)))
    return resid + branch_two

def reference(tokens, out_grad, weight_stack, muon_state, norm_gains, adam_first, adam_second, segment_ids, position_ids):
    groups = N_TENSOR
    counts = (3 * D // groups, D // groups, 2 * FF // groups, FF // groups)
    stack_full = weight_stack.astype(jnp.float32)
    weights = tuple((stack_full[which, :, :counts[which], :] for which in range(4)))
    cosine, sine_table = rope_tables(position_ids, HEAD_DIM)

    def run(inputs, w_qkv, w_out, w_in, w_down, gain_rows):
        return forward(inputs, w_qkv, w_out, w_in, w_down, gain_rows, segment_ids, cosine, sine_table)
    layer_out, pull_back = jax.vjp(run, tokens.astype(jnp.float32), weights[0], weights[1], weights[2], weights[3], norm_gains)
    all_grads = pull_back(out_grad.astype(jnp.float32))
    tokens_grad = all_grads[0].astype(jnp.bfloat16)
    pad_rows = weight_stack.shape[2]
    weight_grads = jnp.stack([jnp.pad(all_grads[1 + which], ((0, 0), (0, pad_rows - counts[which]), (0, 0))) for which in range(4)])
    gain_grads = all_grads[5]
    muon_next = muon_beta * muon_state + (1.0 - muon_beta) * weight_grads
    direction = (1.0 - muon_beta) * weight_grads + muon_beta * muon_next
    norm_sizes = jnp.sqrt(lax.optimization_barrier(jnp.sum(direction * direction, axis=(1, 2, 3), keepdims=True)))
    direction_scale = jnp.log(norm_sizes).reshape(4)
    ortho_block = direction / (norm_sizes + ortho_eps)
    for sweep_index in range(ITERS):
        gram_sum = lax.optimization_barrier(jnp.sum(low(jnp.einsum('ktrd,ktre->ktde', ortho_block, ortho_block, precision=precision_highest)), axis=1))
        square = jnp.einsum('kde,kef->kdf', gram_sum, gram_sum, precision=precision_highest)
        mix_matrix = ns_second * gram_sum + ns_third * square
        ortho_block = ns_first * ortho_block + jnp.einsum('ktrd,kde->ktre', ortho_block, mix_matrix, precision=precision_highest)
    spreads = jnp.array([0.2 * math.sqrt(3 * D), 0.2 * math.sqrt(D), 0.2 * math.sqrt(2 * FF), 0.2 * math.sqrt(FF)], jnp.float32)
    weight_update = -muon_rate * (spreads[:, None, None, None] * ortho_block + decay_rate * stack_full)
    adam_first_next = adam_beta * adam_first + (1.0 - adam_beta) * gain_grads
    adam_second_next = adam_beta * adam_second + (1.0 - adam_beta) * gain_grads * gain_grads
    correction = 1.0 - adam_beta ** STEP
    gain_update = -adam_rate * (adam_first_next / correction / (jnp.sqrt(adam_second_next / correction) + adam_eps) + decay_rate * norm_gains)
    return (layer_out.astype(jnp.bfloat16), tokens_grad, weight_grads, muon_next, weight_update, direction_scale, gain_grads, adam_first_next, adam_second_next, gain_update)
```

```python
import math

import jax
import jax.numpy as jnp
from jax import lax
from jax.experimental import pallas as pl
from jax.experimental.pallas import tpu as pltpu
from jax.sharding import PartitionSpec as P

D = 1024
HEADS = 16
HEAD_DIM = 64
FF = 2624
ITERS = 5
STEP = 8


rope_base = 160000.0
norm_eps = 1e-05
ns_first = 3.4445
ns_second = -4.775
ns_third = 2.0315
muon_beta = 0.5
muon_rate = 0.15
decay_rate = 0.1
adam_beta = 0.5
adam_rate = 0.05
ortho_eps = 1e-07
adam_eps = 1e-08
precision_highest = lax.Precision.HIGHEST


def layer_norm(values, gain_row):
    centre = values - jnp.mean(values, axis=-1, keepdims=True)
    spread = jnp.mean(centre * centre, axis=-1, keepdims=True)
    return centre * lax.rsqrt(spread + norm_eps) * gain_row


def rope_tables(positions, head_width):
    half_width = head_width // 2
    freqs = rope_base ** (-(jnp.arange(half_width, dtype=jnp.float32) * 2.0 / head_width))
    angle = positions.astype(jnp.float32)[..., None] * freqs
    angle = jnp.concatenate([angle, angle], axis=-1)
    return (jnp.cos(angle), jnp.sin(angle))


def rotate(values, cosine, sine_table):
    half_width = values.shape[-1] // 2
    turned = jnp.concatenate([-values[..., half_width:], values[..., :half_width]], axis=-1)
    return values * cosine + turned * sine_table


def rotate_back(grads_in, cosine, sine_table):
    half_width = grads_in.shape[-1] // 2
    scaled = grads_in * sine_table
    turned = jnp.concatenate([scaled[..., half_width:], -scaled[..., :half_width]], axis=-1)
    return grads_in * cosine + turned


def project(left_rows, right_rows):
    return lax.dot_general(
        left_rows, right_rows, (((1,), (1,)), ((), ())), preferred_element_type=jnp.float32
    )


def contract_exact(left_rows, right_rows):
    return lax.dot_general(
        left_rows,
        right_rows,
        (((0,), (0,)), ((), ())),
        precision=precision_highest,
        preferred_element_type=jnp.float32,
    )


def geglu_gate(gate_part, up_part):
    return jax.nn.gelu(gate_part, approximate=False) * up_part


def per_device(
    tokens,
    out_grad,
    weight_stack,
    muon_state,
    norm_gains,
    adam_first,
    adam_second,
    segment_ids,
    position_ids,
):
    local_len, seq_count, model_width = tokens.shape
    token_count = local_len * seq_count
    groups = lax.axis_size("tensor")
    contexts = lax.axis_size("context")
    full_len = local_len * contexts
    local_rows = weight_stack.shape[2]
    pad_rows = local_rows * contexts
    heads_dev = HEADS // groups
    ff_dev = FF // groups
    inner_width = heads_dev * HEAD_DIM
    counts = (3 * inner_width, inner_width, 2 * ff_dev, ff_dev)
    score_scale = HEAD_DIM ** (-0.5)
    own_block = weight_stack.reshape(local_rows, model_width)
    gathered = lax.all_gather(own_block, ("fsdp", "context"), axis=0, tiled=True).reshape(
        4, pad_rows, model_width
    )
    w_qkv = gathered[0, : counts[0]]
    w_out = gathered[1, : counts[1]]
    w_in = gathered[2, : counts[2]]
    w_down = gathered[3, : counts[3]]
    inputs = tokens.astype(jnp.float32).reshape(token_count, model_width)
    act_in = layer_norm(inputs, norm_gains[0]).astype(jnp.bfloat16)
    projected = project(act_in, w_qkv).reshape(local_len, seq_count, 3, heads_dev, HEAD_DIM)
    cosine, sine_table = rope_tables(position_ids, HEAD_DIM)
    rot_cos = cosine[:, :, None, :]
    rot_sin = sine_table[:, :, None, :]
    query_matrix = rotate(projected[:, :, 0], rot_cos, rot_sin).astype(jnp.bfloat16)
    key_matrix_rows = rotate(projected[:, :, 1], rot_cos, rot_sin).astype(jnp.bfloat16)
    value_matrix_rows = projected[:, :, 2].astype(jnp.bfloat16)
    key_value = jnp.concatenate(
        [
            key_matrix_rows.reshape(local_len, seq_count, inner_width),
            value_matrix_rows.reshape(local_len, seq_count, inner_width),
        ],
        axis=-1,
    )
    key_value_all = lax.all_gather(key_value, "context", axis=0, tiled=True)
    keys_all = key_value_all[..., :inner_width].reshape(full_len, seq_count, heads_dev, HEAD_DIM)
    values_all = key_value_all[..., inner_width:].reshape(full_len, seq_count, heads_dev, HEAD_DIM)
    offset = lax.axis_index("context") * local_len
    seg_query = lax.dynamic_slice_in_dim(segment_ids, offset, local_len, 0)
    same_doc = seg_query.T[:, :, None] == segment_ids.T[:, None, :]
    keep_mask = (seg_query > 0).astype(jnp.float32)
    unscaled_score = jnp.einsum(
        "lshd,mshd->shlm", query_matrix, keys_all, preferred_element_type=jnp.float32
    )
    scores = jnp.where(same_doc[:, None], unscaled_score * score_scale, -jnp.inf)
    row_max = jnp.max(scores, axis=-1, keepdims=True)
    log_total = row_max + jnp.log(jnp.sum(jnp.exp(scores - row_max), axis=-1, keepdims=True))
    probs_low = jnp.exp(scores - log_total).astype(jnp.bfloat16)
    attended = jnp.einsum(
        "shlm,mshd->lshd", probs_low, values_all, preferred_element_type=jnp.float32
    )
    attn_in = (
        (attended * keep_mask[:, :, None, None])
        .astype(jnp.bfloat16)
        .reshape(token_count, inner_width)
    )
    branch_one = lax.psum(
        jnp.dot(attn_in, w_out, preferred_element_type=jnp.float32).astype(jnp.bfloat16), "tensor"
    ).astype(jnp.float32)
    resid = inputs + branch_one
    mlp_in = layer_norm(resid, norm_gains[1]).astype(jnp.bfloat16)
    mixed_rows = project(mlp_in, w_in)
    hidden_full, geglu_pull = jax.vjp(geglu_gate, mixed_rows[:, :ff_dev], mixed_rows[:, ff_dev:])
    hidden = hidden_full.astype(jnp.bfloat16)
    branch_two = lax.psum(
        jnp.dot(hidden, w_down, preferred_element_type=jnp.float32).astype(jnp.bfloat16), "tensor"
    ).astype(jnp.float32)
    layer_out = (resid + branch_two).astype(jnp.bfloat16).reshape(local_len, seq_count, model_width)
    out_cot = out_grad.astype(jnp.float32).reshape(token_count, model_width)
    dbranch_two = out_cot.astype(jnp.bfloat16)
    dhidden = project(dbranch_two, w_down)
    dgate, dup_part = geglu_pull(dhidden)
    dmixed = jnp.concatenate([dgate, dup_part], axis=1).astype(jnp.bfloat16)
    dnormed_two = lax.psum(
        jnp.dot(dmixed, w_in, preferred_element_type=jnp.float32).astype(jnp.bfloat16), "tensor"
    ).astype(jnp.float32)
    norm_two_out, norm_two_pull = jax.vjp(layer_norm, resid, norm_gains[1])
    dresid_norm, dgain_two = norm_two_pull(dnormed_two)
    dresid = out_cot + dresid_norm
    dbranch_one = dresid.astype(jnp.bfloat16)
    keep_low = keep_mask.reshape(token_count, 1).astype(jnp.bfloat16)
    dattended = project(dbranch_one, w_out).astype(jnp.bfloat16) * keep_low
    dattn = dattended.reshape(local_len, seq_count, heads_dev, HEAD_DIM)
    dquery_list = []
    dkey_list = []
    dvalue_list = []
    for head_index in range(heads_dev):
        query_head = query_matrix[:, :, head_index]
        key_head = keys_all[:, :, head_index]
        value_head = values_all[:, :, head_index]
        dout_head = dattn[:, :, head_index]
        raw_head = jnp.einsum(
            "lsd,msd->slm", query_head, key_head, preferred_element_type=jnp.float32
        )
        prob_head = jnp.exp(
            jnp.where(same_doc, raw_head * score_scale, -jnp.inf) - log_total[:, head_index]
        )
        dprob = jnp.einsum(
            "lsd,msd->slm", dout_head, value_head, preferred_element_type=jnp.float32
        )
        delta = jnp.sum(prob_head * dprob, axis=-1, keepdims=True)
        dscore = (prob_head * (dprob - delta) * score_scale).astype(jnp.bfloat16)
        dquery_list.append(
            jnp.einsum("slm,msd->lsd", dscore, key_head, preferred_element_type=jnp.float32)
        )
        dkey_head = jnp.einsum(
            "slm,lsd->msd", dscore, query_head, preferred_element_type=jnp.float32
        )
        dvalue_head = jnp.einsum(
            "slm,lsd->msd",
            prob_head.astype(jnp.bfloat16),
            dout_head,
            preferred_element_type=jnp.float32,
        )
        summed = lax.psum_scatter(
            jnp.concatenate([dkey_head, dvalue_head], axis=-1).astype(jnp.bfloat16),
            "context",
            scatter_dimension=0,
            tiled=True,
        ).astype(jnp.float32)
        dkey_list.append(summed[..., :HEAD_DIM])
        dvalue_list.append(summed[..., HEAD_DIM:])
    dqueries = jnp.stack(dquery_list, axis=2)
    dkeys = jnp.stack(dkey_list, axis=2)
    dvalues = jnp.stack(dvalue_list, axis=2)
    dprojected = (
        jnp.stack(
            [
                rotate_back(dqueries, rot_cos, rot_sin),
                rotate_back(dkeys, rot_cos, rot_sin),
                dvalues,
            ],
            axis=2,
        )
        .astype(jnp.bfloat16)
        .reshape(token_count, 3 * inner_width)
    )
    dnormed_one = lax.psum(
        jnp.dot(dprojected, w_qkv, preferred_element_type=jnp.float32).astype(jnp.bfloat16),
        "tensor",
    ).astype(jnp.float32)
    norm_one_out, norm_one_pull = jax.vjp(layer_norm, inputs, norm_gains[0])
    dinput_norm, dgain_one = norm_one_pull(dnormed_one)
    tokens_grad = (
        (dresid + dinput_norm).astype(jnp.bfloat16).reshape(local_len, seq_count, model_width)
    )
    gain_grads = lax.psum(jnp.stack([dgain_one, dgain_two]), ("fsdp", "context"))

    def padded(block, used_rows):
        return jnp.pad(block, ((0, 0), (0, pad_rows - used_rows)))

    left_rows = jnp.concatenate(
        [
            padded(dprojected, counts[0]),
            padded(attn_in, counts[1]),
            padded(dmixed, counts[2]),
            padded(hidden, counts[3]),
        ],
        axis=1,
    )
    right_rows = jnp.stack([act_in, dbranch_one, mlp_in, dbranch_two])
    blocks = local_rows * lax.axis_size(("fsdp", "context")) // pad_rows
    col_block = left_rows.reshape(token_count, blocks, pad_rows)
    grad_block = lax.psum_scatter(
        jnp.einsum(
            "nbp,bnd->bpd", col_block, right_rows, preferred_element_type=jnp.float32
        ).reshape(local_rows * lax.axis_size(("fsdp", "context")), model_width),
        ("fsdp", "context"),
        scatter_dimension=0,
        tiled=True,
    )
    momentum = muon_state.reshape(local_rows, model_width)
    muon_next = muon_beta * momentum + (1.0 - muon_beta) * grad_block
    direction = (1.0 - muon_beta) * grad_block + muon_beta * muon_next
    norm_total = lax.psum(jnp.sum(direction * direction), ("context", "tensor"))
    norm_size = jnp.sqrt(norm_total)
    direction_scale = jnp.log(norm_size).reshape(1)
    ortho_local = direction / (norm_size + ortho_eps)
    ortho_block = lax.all_gather(
        ortho_local.astype(jnp.bfloat16), "context", axis=0, tiled=True
    ).astype(ortho_local.dtype)
    for sweep_index in range(ITERS):
        gram_sum = lax.psum(
            contract_exact(ortho_block, ortho_block).astype(jnp.bfloat16), "tensor"
        ).astype(jnp.float32)
        square = jnp.dot(
            gram_sum, gram_sum, precision=precision_highest, preferred_element_type=jnp.float32
        )
        mix_matrix = ns_second * gram_sum + ns_third * square
        ortho_block = ns_first * ortho_block + jnp.dot(
            ortho_block, mix_matrix, precision=precision_highest, preferred_element_type=jnp.float32
        )
    own_rows = lax.dynamic_slice_in_dim(
        ortho_block, lax.axis_index("context") * local_rows, local_rows, 0
    )
    owner_index = lax.axis_index("fsdp")
    spreads = jnp.array(
        [0.2 * math.sqrt(3 * D), 0.2 * math.sqrt(D), 0.2 * math.sqrt(2 * FF), 0.2 * math.sqrt(FF)],
        jnp.float32,
    )
    spread = jnp.sum(jnp.where(jnp.arange(4) == owner_index, spreads, 0.0))
    old_weight = own_block.astype(jnp.float32)
    weight_update = -muon_rate * (spread * own_rows + decay_rate * old_weight)
    adam_first_next = adam_beta * adam_first + (1.0 - adam_beta) * gain_grads
    adam_second_next = adam_beta * adam_second + (1.0 - adam_beta) * gain_grads * gain_grads
    correction = 1.0 - adam_beta**STEP
    gain_update = -adam_rate * (
        adam_first_next / correction / (jnp.sqrt(adam_second_next / correction) + adam_eps)
        + decay_rate * norm_gains
    )
    block_shape = (1, 1, local_rows, model_width)
    return (
        layer_out,
        tokens_grad,
        grad_block.reshape(block_shape),
        muon_next.reshape(block_shape),
        weight_update.reshape(block_shape),
        direction_scale,
        gain_grads,
        adam_first_next,
        adam_second_next,
        gain_update,
    )


MESH_ID = pl.DeviceIdType.MESH
ANY = pl.ANY


def ring_place(index):
    return index + index // 2 - 2 * (index // 3)


def split_units(rows, parts, unit=16):
    units = rows // unit
    sizes = [(units // parts + (1 if i < units % parts else 0)) * unit for i in range(parts)]
    return [s for s in sizes if s]


def ring_chunks(counts, local_rows, which, core, target):
    first = core * local_rows
    rows = min(counts[which], first + local_rows) - first
    if rows <= 0:
        return [[], []]
    halves = split_units(rows, 2)
    if len(halves) == 1:
        halves = halves + [0]
    out, at = [], first
    for half in halves:
        pieces = []
        if half:
            for size in split_units(half, max(1, round(half / target))):
                pieces.append((at, size))
                at += size
        out.append(pieces)
    return out


class Place:
    def __init__(self):
        self.f = lax.axis_index("fsdp")
        self.c = lax.axis_index("context")
        self.t = lax.axis_index("tensor")
        self.pos = ring_place(self.f)
        self.next = ring_place((self.pos + 1) % 4)
        self.prev = ring_place((self.pos + 3) % 4)
        self.outer = jnp.logical_or(self.t == 0, self.t == 3)
        self.inner_mate = jnp.where(self.t == 0, 1, 2)
        self.outer_mate = jnp.where(self.t == 1, 0, 3)

    def ring(self, direction):
        return (self.next if direction == 0 else self.prev, self.c, self.t)

    def partner(self):
        return (self.f, 1 - self.c, self.t)

    def chip_z(self, z):
        return (self.f, self.c, z)

    def hop(self, which, direction):
        home = (0, 1, 3, 2)[which]
        if direction == 0:
            return (self.pos + 4 - home) % 4
        return (home + 4 - self.pos) % 4


def greet(place, ring, partner, line):
    barrier = pltpu.get_barrier_semaphore()

    def signal(device):
        pl.semaphore_signal(barrier, inc=1, device_id=device, device_id_type=MESH_ID)

    count = 0
    if ring:
        signal(place.ring(0))
        signal(place.ring(1))
        count += 2
    if partner:
        signal(place.partner())
        count += 1
    if line:
        @pl.when(place.outer)
        def _():
            signal(place.chip_z(place.inner_mate))
            pl.semaphore_wait(barrier, count + 1)

        @pl.when(jnp.logical_not(place.outer))
        def _():
            signal(place.chip_z(place.outer_mate))
            signal(place.chip_z(3 - place.t))
            pl.semaphore_wait(barrier, count + 2)
    else:
        pl.semaphore_wait(barrier, count)


def remote(src, dst, send, recv, device):
    return pltpu.make_async_remote_copy(
        src_ref=src, dst_ref=dst, send_sem=send, recv_sem=recv, device_id=device, device_id_type=MESH_ID
    )


def run_steps(*tracks):
    total = max(len(track) for track in tracks)
    done = [0] * len(tracks)
    for index in range(total):
        for number, track in enumerate(tracks):
            upto = -(-len(track) * (index + 1) // total)
            while done[number] < upto:
                track[done[number]]()
                done[number] += 1


def gather_plan(counts, local_rows, ks, target=96):
    plan = []
    for core in (0, 1):
        ident = 0
        for which in ks:
            for direction, pieces in enumerate(ring_chunks(counts, local_rows, which, core, target)):
                for order, (row, rows) in enumerate(pieces):
                    plan.append((ident, which, core, direction, order, row, rows))
                    ident += 1
    return plan, max(p[0] for p in plan) + 1


def gather_steps(place, plan, local_rows, base, own_ref, out_ref, sems):
    ss, rs, sp, rp = sems

    def dst(which, row, rows):
        return out_ref.at[pl.ds(base[which] + row, rows)]

    def src(core, row, rows):
        return own_ref.at[pl.ds(row - core * local_rows, rows)]

    def begin():
        for ident, which, core, direction, order, row, rows in plan:
            @pl.when(jnp.logical_and(place.c == core, place.f == which))
            def _():
                remote(src(core, row, rows), dst(which, row, rows), ss.at[ident], rs.at[ident],
                       place.ring(direction)).start()
        for ident, which, core, direction, order, row, rows in plan:
            @pl.when(jnp.logical_and(place.c == core, place.f == which))
            def _():
                remote(src(core, row, rows), dst(which, row, rows), sp.at[ident], rp.at[ident],
                       place.partner()).start()

    def step(item):
        ident, which, core, direction, order, row, rows = item

        def run():
            hop = place.hop(which, direction)
            mine = dst(which, row, rows)

            @pl.when(jnp.logical_and(place.c == core, hop >= 1))
            def _():
                remote(mine, mine, ss.at[ident], rs.at[ident], place.ring(direction)).wait_recv()

                @pl.when(hop <= 2)
                def _():
                    remote(mine, mine, ss.at[ident], rs.at[ident], place.ring(direction)).start()

                remote(mine, mine, sp.at[ident], rp.at[ident], place.partner()).start()
        return run

    def end():
        for ident, which, core, direction, order, row, rows in plan:
            hop = place.hop(which, direction)
            mine = dst(which, row, rows)

            @pl.when(jnp.logical_and(place.c == core, hop <= 2))
            def _():
                remote(mine, mine, ss.at[ident], rs.at[ident], place.ring(direction)).wait_send()

            @pl.when(place.c == core)
            def _():
                remote(mine, mine, sp.at[ident], rp.at[ident], place.partner()).wait_send()

            @pl.when(place.c == 1 - core)
            def _():
                remote(mine, mine, sp.at[ident], rp.at[ident], place.partner()).wait_recv()

    ordered = sorted(plan, key=lambda p: (p[4], p[1]))
    return begin, [step(item) for item in ordered], end


def line_steps(place, chunks, own, out, early, mid, low, sems, lag=1, back_lag=3, prep=None, done=None):
    s1, r1, s2, r2, s3, r3 = sems

    def from_end(i, device):
        return remote(own(i), early(i), s1.at[i], r1.at[i], device)

    def across(i):
        return remote(mid(i), low(i), s2.at[i], r2.at[i], place.chip_z(3 - place.t))

    def back(i, device):
        return remote(out(i), out(i), s3.at[i], r3.at[i], device)

    def step(i):
        def run():
            if i < chunks and prep is not None:
                prep(i)

            @pl.when(place.outer)
            def _():
                if i < chunks:
                    from_end(i, place.chip_z(place.inner_mate)).start()
                if 0 <= i - lag - back_lag < chunks:
                    back(i - lag - back_lag, place.chip_z(place.inner_mate)).wait_recv()

            @pl.when(jnp.logical_not(place.outer))
            def _():
                if i < chunks:
                    from_end(i, place.chip_z(place.outer_mate)).wait_recv()
                    pair = own(i)[...].astype(jnp.float32) + early(i)[...].astype(jnp.float32)
                    mid(i)[...] = pair.astype(mid(i).dtype)
                    across(i).start()
                j = i - lag
                if 0 <= j < chunks:
                    across(j).wait_recv()
                    total = mid(j)[...].astype(jnp.float32) + low(j)[...].astype(jnp.float32)
                    out(j)[...] = total.astype(out(j).dtype)
                    back(j, place.chip_z(place.outer_mate)).start()
            if done is not None:
                if 0 <= i - lag - back_lag < chunks:
                    done(i - lag - back_lag)
        return run

    def end():
        @pl.when(place.outer)
        def _():
            for i in range(chunks):
                from_end(i, place.chip_z(place.inner_mate)).wait_send()

        @pl.when(jnp.logical_not(place.outer))
        def _():
            for i in range(chunks):
                across(i).wait_send()
                back(i, place.chip_z(place.outer_mate)).wait_send()

    return [step(i) for i in range(chunks + lag + back_lag)], end


def scatter_steps(place, plan, local_rows, base, part_ref, grad_ref, prx, rrx, tx, sems):
    ss, rs, sp, rp = sems

    def rows_of(ref, which, row, rows):
        return ref.at[pl.ds(base[which] + row, rows)]

    def partner_copy(item):
        ident, which, core, direction, order, row, rows = item
        return remote(rows_of(part_ref, which, row, rows), rows_of(prx, which, row, rows),
                      sp.at[ident], rp.at[ident], place.partner())

    def ring_copy(item):
        ident, which, core, direction, order, row, rows = item
        return remote(rows_of(tx, which, row, rows), rows_of(rrx, which, row, rows),
                      ss.at[ident], rs.at[ident], place.ring(direction))

    ordered = sorted(plan, key=lambda p: (p[4], p[1]))
    last = max(p[4] for p in plan)

    def begin():
        for item in ordered:
            @pl.when(place.c == 1 - item[2])
            def _():
                partner_copy(item).start()

    def visit(item, late):
        ident, which, core, direction, order, row, rows = item
        hop = place.hop(which, direction)
        role = (late + 1) % 4

        @pl.when(jnp.logical_and(place.c == core, hop == role))
        def _():
            partner_copy(item).wait_recv()
            total = (rows_of(part_ref, which, row, rows)[...].astype(jnp.float32)
                     + rows_of(prx, which, row, rows)[...].astype(jnp.float32))
            if role != 1:
                ring_copy(item).wait_recv()
                total = total + rows_of(rrx, which, row, rows)[...].astype(jnp.float32)
            if role == 0:
                grad_ref[pl.ds(row - core * local_rows, rows)] = total
            else:
                rows_of(tx, which, row, rows)[...] = total.astype(tx.dtype)
                ring_copy(item).start()

    def step(j):
        def run():
            for late in range(4):
                for item in ordered:
                    if item[4] == j - late:
                        visit(item, late)
        return run

    def end():
        for item in plan:
            ident, which, core, direction, order, row, rows = item

            @pl.when(place.c == 1 - core)
            def _():
                partner_copy(item).wait_send()

            @pl.when(jnp.logical_and(place.c == core, place.hop(which, direction) != 0))
            def _():
                ring_copy(item).wait_send()

    return begin, [step(j) for j in range(last + 4)], end


VMEM_SPEC = pl.BlockSpec(memory_space=pltpu.VMEM)
ANY_SPEC = pl.BlockSpec(memory_space=pl.ANY)


def dma(count):
    return pltpu.SemaphoreType.DMA((count,))


def comm_call(kernel, outs, ins, in_specs, out_specs, scratch, ident):
    return pl.pallas_call(
        kernel,
        out_shape=outs,
        in_specs=in_specs,
        out_specs=out_specs,
        scratch_shapes=scratch,
        compiler_params=pltpu.CompilerParams(
            collective_id=ident, has_side_effects=True, vmem_limit_bytes=60 * 2**20
        ),
    )(*ins)


def base_rows(counts, ks):
    base, at = {}, 0
    for which in ks:
        base[which] = at
        at += counts[which]
    return base, at


def own_rows_copy(place, counts, local_rows, ks, base, own_ref, out_ref, sem, act):
    for which in ks:
        for core in (0, 1):
            rows = min(counts[which] - core * local_rows, local_rows)
            if rows > 0:
                @pl.when(jnp.logical_and(place.c == core, place.f == which))
                def _():
                    act(pltpu.make_async_copy(
                        own_ref.at[pl.ds(0, rows)],
                        out_ref.at[pl.ds(base[which] + core * local_rows, rows)],
                        sem.at[0],
                    ))


def gather_weights(own_block, counts, ks, ident):
    local_rows, width = own_block.shape
    plan, count = gather_plan(counts, local_rows, ks)
    base, total = base_rows(counts, ks)

    def kernel(own_ref, out_ref, ss, rs, sp, rp, local_sem):
        place = Place()
        greet(place, True, True, False)
        begin, steps, end = gather_steps(place, plan, local_rows, base, own_ref, out_ref, (ss, rs, sp, rp))
        begin()
        own_rows_copy(place, counts, local_rows, ks, base, own_ref, out_ref, local_sem, lambda d: d.start())
        run_steps(steps)
        own_rows_copy(place, counts, local_rows, ks, base, own_ref, out_ref, local_sem, lambda d: d.wait())
        end()

    return comm_call(kernel, jax.ShapeDtypeStruct((total, width), own_block.dtype), (own_block,),
                     [VMEM_SPEC], VMEM_SPEC, [dma(count)] * 4 + [dma(1)], ident), base


def line_sum_and_gather(term, own_block, counts, ks, ident, chunks=8):
    local_rows, width = own_block.shape
    plan, count = gather_plan(counts, local_rows, ks)
    base, total = base_rows(counts, ks)
    rows = term.shape[0] // chunks

    def kernel(term_ref, own_ref, sum_ref, out_ref, early, mid, low, *sems):
        place = Place()
        greet(place, True, True, True)
        cut = lambda ref: lambda i: ref.at[pl.ds(i * rows, rows)]
        line, line_end = line_steps(place, chunks, cut(term_ref), cut(sum_ref), cut(early), cut(mid), cut(low), sems[:6])
        begin, steps, end = gather_steps(place, plan, local_rows, base, own_ref, out_ref, sems[6:10])
        begin()
        own_rows_copy(place, counts, local_rows, ks, base, own_ref, out_ref, sems[10], lambda d: d.start())
        run_steps(line, steps)
        own_rows_copy(place, counts, local_rows, ks, base, own_ref, out_ref, sems[10], lambda d: d.wait())
        line_end()
        end()

    return comm_call(
        kernel,
        (jax.ShapeDtypeStruct(term.shape, term.dtype), jax.ShapeDtypeStruct((total, width), own_block.dtype)),
        (term, own_block), [VMEM_SPEC] * 2, (VMEM_SPEC, VMEM_SPEC),
        [pltpu.VMEM(term.shape, term.dtype)] * 3 + [dma(chunks)] * 6 + [dma(count)] * 4 + [dma(1)], ident,
    ), base


def scatter_grads(part, counts, ks, local_rows, ident, term=None, chunks=8):
    plan, count = gather_plan(counts, local_rows, ks)
    base, total = base_rows(counts, ks)
    width = part.shape[1]
    lined = term is not None
    rows = term.shape[0] // chunks if lined else 0

    def kernel(*refs):
        part_ref, refs = refs[0], refs[1:]
        if lined:
            term_ref, grad_ref, sum_ref, prx, rrx, tx, early, mid, low = refs[:9]
            sems = refs[9:]
        else:
            grad_ref, prx, rrx, tx = refs[:4]
            sems = refs[4:]
        place = Place()
        greet(place, True, True, lined)
        begin, steps, end = scatter_steps(place, plan, local_rows, base, part_ref, grad_ref, prx, rrx, tx, sems[:4])
        begin()
        grad_ref[...] = jnp.zeros_like(grad_ref)
        if lined:
            cut = lambda ref: lambda i: ref.at[pl.ds(i * rows, rows)]
            line, line_end = line_steps(place, chunks, cut(term_ref), cut(sum_ref), cut(early), cut(mid), cut(low), sems[4:10])
            run_steps(line, steps)
            line_end()
        else:
            run_steps(steps)
        end()

    ins = (part, term) if lined else (part,)
    outs = [jax.ShapeDtypeStruct((local_rows, width), jnp.float32)]
    scratch = [pltpu.VMEM(part.shape, part.dtype)] * 3
    sems = [dma(count)] * 4
    if lined:
        outs.append(jax.ShapeDtypeStruct(term.shape, term.dtype))
        scratch += [pltpu.VMEM(term.shape, term.dtype)] * 3
        sems += [dma(chunks)] * 6
    return comm_call(kernel, tuple(outs), ins, [VMEM_SPEC] * len(ins), tuple([VMEM_SPEC] * len(outs)), scratch + sems, ident)


def swap_cores(block, ident):
    def kernel(x_ref, o_ref, send, recv):
        place = Place()
        greet(place, False, True, False)
        copy = remote(x_ref, o_ref, send.at[0], recv.at[0], place.partner())
        copy.start()
        copy.wait()

    return comm_call(kernel, jax.ShapeDtypeStruct(block.shape, block.dtype), (block,), [VMEM_SPEC], VMEM_SPEC,
                     [dma(1), dma(1)], ident)


def plane_sum(block, ident):
    def kernel(x_ref, o_ref, held, send, recv):
        f, c, t = lax.axis_index("fsdp"), lax.axis_index("context"), lax.axis_index("tensor")
        me = f * 2 + c
        barrier = pltpu.get_barrier_semaphore()

        def device(shift):
            other = (me + shift) % 8
            return (other // 2, other % 2, t)

        for shift in range(1, 8):
            pl.semaphore_signal(barrier, inc=1, device_id=device(shift), device_id_type=MESH_ID)
        pl.semaphore_wait(barrier, 7)
        held[pl.ds(me, 1)] = x_ref[...][None]
        copies = []
        for shift in range(1, 8):
            copy = remote(x_ref, held.at[me], send.at[shift], recv.at[shift], device(shift))
            copy.start()
            copies.append(copy)
        for copy in copies:
            copy.wait()
        total = held[0]
        for k in range(1, 8):
            total = total + held[k]
        o_ref[...] = total

    return comm_call(kernel, jax.ShapeDtypeStruct(block.shape, block.dtype), (block,), [VMEM_SPEC], VMEM_SPEC,
                     [pltpu.VMEM((8,) + block.shape, block.dtype), dma(8), dma(8)], ident)


def gram_sum(rows_low, square, ident):
    rows, width = rows_low.shape
    tile = width // 4
    half = tile // 2
    chunks = 10

    def kernel(x_ref, q_ref, g_ref, norm_ref, mine, theirs, prx, tot, other, early, mid, low, *sems):
        place = Place()
        c = place.c
        sp, rp, st, rt = sems[6:10]

        def blocks(core):
            return [(3 * core, 3 * core), (2 * core, 2 * core + 1), (core + 1, core + 1), (core, core + 2), (core, 3 - core)]

        greet(place, False, True, True)

        def at(k):
            return pl.ds(pl.multiple_of(k * tile, tile), tile)

        def gram(i, j):
            return lax.dot_general(x_ref[:, at(i)], x_ref[:, at(j)], (((0,), (0,)), ((), ())),
                                   preferred_element_type=jnp.float32)

        def partner(n):
            sl = pl.ds(n * tile, tile)
            return remote(theirs.at[sl], prx.at[sl], sp.at[n], rp.at[n], place.partner())

        def norm_row(ref):
            return ref.at[pl.ds(5 * tile, 8)]

        for n, (i, j) in enumerate(blocks(1 - c)):
            theirs[pl.ds(n * tile, tile)] = gram(i, j)
            partner(n).start()
        norm_row(theirs)[...] = jnp.broadcast_to(q_ref[0:1, 0:1], (8, tile))
        pn = remote(norm_row(theirs), norm_row(prx), sp.at[5], rp.at[5], place.partner())
        pn.start()

        def span(i):
            return pl.ds(i * half, half) if i < chunks - 1 else pl.ds(i * half, half + 8)

        def cut(ref):
            return lambda i: ref.at[span(i)]

        def prep(i):
            if i % 2 == 0:
                n = i // 2
                sl = pl.ds(n * tile, tile)
                block = gram(*blocks(c)[n])
                partner(n).wait_recv()
                mine[sl] = block + prx[sl]
            if i == chunks - 1:
                pn.wait_recv()
                norm_row(mine)[...] = norm_row(prx)[...] + jnp.broadcast_to(q_ref[0:1, 0:1], (8, tile))

        def share(i):
            return remote(cut(tot)(i), cut(other)(i), st.at[i], rt.at[i], place.partner())

        def place_block(ref, n, core):
            i, j = blocks(core)[n]
            block = ref[pl.ds(n * tile, tile)]
            g_ref[at(i), at(j)] = block
            g_ref[at(j), at(i)] = block.T

        def done(i):
            share(i).start()
            if i % 2 == 1:
                place_block(tot, i // 2, c)
            if i >= 2:
                share(i - 2).wait_recv()
                if (i - 2) % 2 == 1:
                    place_block(other, (i - 2) // 2, 1 - c)

        steps, end = line_steps(place, chunks, cut(mine), cut(tot), cut(early), cut(mid), cut(low), sems[:6],
                                prep=prep, done=done)
        run_steps(steps)
        for i in (chunks - 2, chunks - 1):
            share(i).wait_recv()
        place_block(other, 4, 1 - c)
        norm_ref[...] = jnp.broadcast_to(tot[5 * tile:5 * tile + 8, 0:128], (8, 128))
        end()
        for n in range(5):
            partner(n).wait_send()
        pn.wait_send()
        for i in range(chunks):
            share(i).wait_send()

    packed = pltpu.VMEM((5 * tile + 8, tile), jnp.float32)
    return comm_call(
        kernel,
        (jax.ShapeDtypeStruct((width, width), jnp.float32), jax.ShapeDtypeStruct((8, 128), jnp.float32)),
        (rows_low, square), [VMEM_SPEC] * 2, (VMEM_SPEC, VMEM_SPEC),
        [packed] * 8 + [dma(chunks)] * 6 + [dma(6), dma(6), dma(chunks), dma(chunks)], ident,
    )


def per_device_block(tokens, out_grad, weight_stack, muon_state, norm_gains, adam_first, adam_second, segment_ids,
                     position_ids):
    token_count, _, model_width = tokens.shape
    groups, contexts = 4, 2
    full_len = token_count * contexts
    local_rows = weight_stack.shape[2]
    heads_dev = HEADS // groups
    ff_dev = FF // groups
    inner_width = heads_dev * HEAD_DIM
    counts = (3 * inner_width, inner_width, 2 * ff_dev, ff_dev)
    score_scale = HEAD_DIM ** (-0.5)
    own_block = weight_stack.reshape(local_rows, model_width)
    low = jnp.bfloat16
    context = lax.axis_index("context")

    first_weights, base = gather_weights(own_block, counts, (0, 1), 0)
    w_qkv = first_weights[: counts[0]]
    w_out = first_weights[counts[0]:]
    inputs = tokens.astype(jnp.float32).reshape(token_count, model_width)
    act_in = layer_norm(inputs, norm_gains[0]).astype(low)
    projected = project(act_in, w_qkv).reshape(token_count, 3, heads_dev, HEAD_DIM)
    cosine, sine_table = rope_tables(position_ids.reshape(token_count), HEAD_DIM)
    rot_cos = cosine[:, None, :]
    rot_sin = sine_table[:, None, :]
    queries = rotate(projected[:, 0], rot_cos, rot_sin).astype(low)
    keys = rotate(projected[:, 1], rot_cos, rot_sin).astype(low)
    values = projected[:, 2].astype(low)
    mine = jnp.concatenate([keys.reshape(token_count, inner_width), values.reshape(token_count, inner_width)], axis=1)
    theirs = swap_cores(mine, 1)
    key_value = jnp.concatenate([mine, theirs], axis=0)
    keys_all = key_value[:, :inner_width].reshape(full_len, heads_dev, HEAD_DIM)
    values_all = key_value[:, inner_width:].reshape(full_len, heads_dev, HEAD_DIM)
    segments = segment_ids.reshape(full_len)
    seg_query = lax.dynamic_slice_in_dim(segments, context * token_count, token_count, 0)
    seg_other = lax.dynamic_slice_in_dim(segments, (1 - context) * token_count, token_count, 0)
    seg_key = jnp.concatenate([seg_query, seg_other])
    same_doc = (seg_query[:, None] == seg_key[None, :])[None]
    keep_mask = (seg_query > 0).astype(jnp.float32)[:, None]
    raw = jnp.einsum("lhd,mhd->hlm", queries, keys_all, preferred_element_type=jnp.float32)
    scores = jnp.where(same_doc, raw * score_scale, -jnp.inf)
    row_max = jnp.max(scores, axis=-1, keepdims=True)
    log_total = row_max + jnp.log(jnp.sum(jnp.exp(scores - row_max), axis=-1, keepdims=True))
    probs = jnp.exp(scores - log_total)
    probs_low = probs.astype(low)
    attended = jnp.einsum("hlm,mhd->lhd", probs_low, values_all, preferred_element_type=jnp.float32)
    attn_in = (attended.reshape(token_count, inner_width) * keep_mask).astype(low)
    branch_term = jnp.dot(attn_in, w_out, preferred_element_type=jnp.float32).astype(low)
    (branch_one, last_weights), _ = line_sum_and_gather(branch_term, own_block, counts, (2, 3), 2)
    w_in = last_weights[: counts[2]]
    w_down = last_weights[counts[2]:]
    resid = inputs + branch_one.astype(jnp.float32)
    mlp_in = layer_norm(resid, norm_gains[1]).astype(low)
    mixed_rows = project(mlp_in, w_in)
    hidden_full, geglu_pull = jax.vjp(geglu_gate, mixed_rows[:, :ff_dev], mixed_rows[:, ff_dev:])
    hidden = hidden_full.astype(low)
    branch_two_term = jnp.dot(hidden, w_down, preferred_element_type=jnp.float32).astype(low)
    out_low = out_grad.reshape(token_count, model_width)
    out_cot = out_low.astype(jnp.float32)
    dgate, dup_part = geglu_pull(project(out_low, w_down))
    dmixed = jnp.concatenate([dgate, dup_part], axis=1).astype(low)
    dnormed_two_term = jnp.dot(dmixed, w_in, preferred_element_type=jnp.float32).astype(low)

    def grad_term(left, right):
        return lax.dot_general(left, right, (((0,), (0,)), ((), ())), preferred_element_type=jnp.float32).astype(low)

    late_terms = jnp.concatenate([grad_term(dmixed, mlp_in), grad_term(hidden, out_low)], axis=0)
    grad_late, dnormed_two = scatter_grads(late_terms, counts, (2, 3), local_rows, 3, dnormed_two_term)
    _, norm_two_pull = jax.vjp(layer_norm, resid, norm_gains[1])
    dresid_norm, dgain_two = norm_two_pull(dnormed_two.astype(jnp.float32))
    dresid = out_cot + dresid_norm
    dbranch_one = dresid.astype(low)
    dattended = project(dbranch_one, w_out).astype(low) * keep_mask.astype(low)
    dattn = dattended.reshape(token_count, heads_dev, HEAD_DIM)
    dprobs = jnp.einsum("lhd,mhd->hlm", dattn, values_all, preferred_element_type=jnp.float32)
    delta = jnp.sum(probs * dprobs, axis=-1, keepdims=True)
    dscores = (probs * (dprobs - delta) * score_scale).astype(low)
    dqueries = jnp.einsum("hlm,mhd->lhd", dscores, keys_all, preferred_element_type=jnp.float32)
    dkeys = jnp.einsum("hlm,lhd->mhd", dscores, queries, preferred_element_type=jnp.float32)
    dvalues = jnp.einsum("hlm,lhd->mhd", probs_low, dattn, preferred_element_type=jnp.float32)
    dkv = jnp.concatenate([dkeys.reshape(full_len, inner_width), dvalues.reshape(full_len, inner_width)], axis=1)
    dkv_other = swap_cores(dkv[token_count:].astype(low), 4)
    dkv_own = dkv[:token_count] + dkv_other.astype(jnp.float32)
    dkeys = dkv_own[:, :inner_width].reshape(token_count, heads_dev, HEAD_DIM)
    dprojected = jnp.concatenate(
        [
            rotate_back(dqueries, rot_cos, rot_sin).reshape(token_count, inner_width),
            rotate_back(dkeys, rot_cos, rot_sin).reshape(token_count, inner_width),
            dkv_own[:, inner_width:],
        ],
        axis=1,
    ).astype(low)
    early_terms = jnp.concatenate([grad_term(dprojected, act_in), grad_term(attn_in, dbranch_one)], axis=0)
    (grad_early,) = scatter_grads(early_terms, counts, (0, 1), local_rows, 5)
    dnormed_one_term = jnp.dot(dprojected, w_qkv, preferred_element_type=jnp.float32).astype(low)

    owner_index = lax.axis_index("fsdp")
    grad_block = jnp.where(owner_index >= 2, grad_late, grad_early)
    momentum = muon_state.reshape(local_rows, model_width)
    muon_next = muon_beta * momentum + (1.0 - muon_beta) * grad_block
    direction = (1.0 - muon_beta) * grad_block + muon_beta * muon_next
    direction_low = direction.astype(low)
    square = jnp.sum(direction * direction).reshape(1, 1)
    gram, norm_total = gram_sum(direction_low, jnp.broadcast_to(square, (8, 128)), 6)
    norm_size = jnp.sqrt(norm_total[0, 0])
    direction_scale = jnp.log(norm_size).reshape(1)
    inverse = 1.0 / (norm_size + ortho_eps)
    branch_two_term, dnormed_one_term, gram = lax.optimization_barrier((branch_two_term, dnormed_one_term, gram))
    branch_two = lax.psum(branch_two_term, "tensor").astype(jnp.float32)
    dnormed_one = lax.psum(dnormed_one_term, "tensor").astype(jnp.float32)

    power = gram * (inverse * inverse)
    ortho = direction_low.astype(jnp.float32) * inverse
    high = lax.Precision.HIGH

    def times(left, right):
        return jnp.dot(left, right, precision=high, preferred_element_type=jnp.float32)

    for sweep_index in range(ITERS):
        square_power = times(power, power)
        mix = ns_second * power + ns_third * square_power
        ortho = ns_first * ortho + jnp.dot(ortho.astype(low), mix.astype(low), preferred_element_type=jnp.float32)
        if sweep_index < ITERS - 1:
            cube = times(power, square_power)
            tail = (2.0 * ns_second * ns_third) * square_power + (ns_third * ns_third) * cube
            power = (
                (ns_first * ns_first) * power
                + (2.0 * ns_first * ns_second) * square_power
                + (ns_second * ns_second + 2.0 * ns_first * ns_third) * cube
                + times(square_power, tail)
            )

    layer_out = (resid + branch_two).astype(low).reshape(tokens.shape)
    _, norm_one_pull = jax.vjp(layer_norm, inputs, norm_gains[0])
    dinput_norm, dgain_one = norm_one_pull(dnormed_one)
    tokens_grad = (dresid + dinput_norm).astype(low).reshape(tokens.shape)
    gain_grads = plane_sum(jnp.concatenate([jnp.stack([dgain_one, dgain_two])] * 4, axis=0), 7)[:2]
    spreads = jnp.array(
        [0.2 * math.sqrt(3 * D), 0.2 * math.sqrt(D), 0.2 * math.sqrt(2 * FF), 0.2 * math.sqrt(FF)],
        jnp.float32,
    )
    spread = jnp.sum(jnp.where(jnp.arange(4) == owner_index, spreads, 0.0))
    weight_update = -muon_rate * (spread * ortho + decay_rate * own_block.astype(jnp.float32))
    adam_first_next = adam_beta * adam_first + (1.0 - adam_beta) * gain_grads
    adam_second_next = adam_beta * adam_second + (1.0 - adam_beta) * gain_grads * gain_grads
    correction = 1.0 - adam_beta**STEP
    gain_update = -adam_rate * (
        adam_first_next / correction / (jnp.sqrt(adam_second_next / correction) + adam_eps)
        + decay_rate * norm_gains
    )
    block_shape = (1, 1, local_rows, model_width)
    return (
        layer_out,
        tokens_grad,
        grad_block.reshape(block_shape),
        muon_next.reshape(block_shape),
        weight_update.reshape(block_shape),
        direction_scale,
        gain_grads,
        adam_first_next,
        adam_second_next,
        gain_update,
    )


def solution(mesh):
    sizes = dict(mesh.shape)
    block = (sizes["fsdp"], sizes["context"], sizes["tensor"]) == (4, 2, 4)
    return jax.shard_map(
        per_device_block if block else per_device,
        mesh=mesh,
        in_specs=(
            P("context", "fsdp", None),
            P("context", "fsdp", None),
            P("fsdp", "tensor", "context", None),
            P("fsdp", "tensor", "context", None),
            P(),
            P(),
            P(),
            P(None, "fsdp"),
            P("context", "fsdp"),
        ),
        out_specs=(
            P("context", "fsdp", None),
            P("context", "fsdp", None),
            P("fsdp", "tensor", "context", None),
            P("fsdp", "tensor", "context", None),
            P("fsdp", "tensor", "context", None),
            P("fsdp"),
            P(),
            P(),
            P(),
            P(),
        ),
        check_vma=False,
    )
```

```python
import math

import jax
import jax.numpy as jnp
from jax import lax
from jax.experimental import pallas as pl
from jax.experimental.pallas import tpu as pltpu
from jax.sharding import PartitionSpec as P

D = 1024
HEADS = 16
HEAD_DIM = 64
FF = 2624
ITERS = 5
STEP = 8


rope_base = 160000.0
norm_eps = 1e-05
ns_first = 3.4445
ns_second = -4.775
ns_third = 2.0315
muon_beta = 0.5
muon_rate = 0.15
decay_rate = 0.1
adam_beta = 0.5
adam_rate = 0.05
ortho_eps = 1e-07
adam_eps = 1e-08
precision_highest = lax.Precision.HIGHEST


def layer_norm(values, gain_row):
    centre = values - jnp.mean(values, axis=-1, keepdims=True)
    spread = jnp.mean(centre * centre, axis=-1, keepdims=True)
    return centre * lax.rsqrt(spread + norm_eps) * gain_row


def rope_tables(positions, head_width):
    half_width = head_width // 2
    freqs = rope_base ** (-(jnp.arange(half_width, dtype=jnp.float32) * 2.0 / head_width))
    angle = positions.astype(jnp.float32)[..., None] * freqs
    angle = jnp.concatenate([angle, angle], axis=-1)
    return (jnp.cos(angle), jnp.sin(angle))


def rotate(values, cosine, sine_table):
    half_width = values.shape[-1] // 2
    turned = jnp.concatenate([-values[..., half_width:], values[..., :half_width]], axis=-1)
    return values * cosine + turned * sine_table


def rotate_back(grads_in, cosine, sine_table):
    half_width = grads_in.shape[-1] // 2
    scaled = grads_in * sine_table
    turned = jnp.concatenate([scaled[..., half_width:], -scaled[..., :half_width]], axis=-1)
    return grads_in * cosine + turned


def project(left_rows, right_rows):
    return lax.dot_general(
        left_rows, right_rows, (((1,), (1,)), ((), ())), preferred_element_type=jnp.float32
    )


def contract_exact(left_rows, right_rows):
    return lax.dot_general(
        left_rows,
        right_rows,
        (((0,), (0,)), ((), ())),
        precision=precision_highest,
        preferred_element_type=jnp.float32,
    )


def geglu_gate(gate_part, up_part):
    return jax.nn.gelu(gate_part, approximate=False) * up_part


def per_device(
    tokens,
    out_grad,
    weight_stack,
    muon_state,
    norm_gains,
    adam_first,
    adam_second,
    segment_ids,
    position_ids,
):
    local_len, seq_count, model_width = tokens.shape
    token_count = local_len * seq_count
    groups = lax.axis_size("tensor")
    contexts = lax.axis_size("context")
    full_len = local_len * contexts
    local_rows = weight_stack.shape[2]
    pad_rows = local_rows * contexts
    heads_dev = HEADS // groups
    ff_dev = FF // groups
    inner_width = heads_dev * HEAD_DIM
    counts = (3 * inner_width, inner_width, 2 * ff_dev, ff_dev)
    score_scale = HEAD_DIM ** (-0.5)
    own_block = weight_stack.reshape(local_rows, model_width)
    gathered = lax.all_gather(own_block, ("fsdp", "context"), axis=0, tiled=True).reshape(
        4, pad_rows, model_width
    )
    w_qkv = gathered[0, : counts[0]]
    w_out = gathered[1, : counts[1]]
    w_in = gathered[2, : counts[2]]
    w_down = gathered[3, : counts[3]]
    inputs = tokens.astype(jnp.float32).reshape(token_count, model_width)
    act_in = layer_norm(inputs, norm_gains[0]).astype(jnp.bfloat16)
    projected = project(act_in, w_qkv).reshape(local_len, seq_count, 3, heads_dev, HEAD_DIM)
    cosine, sine_table = rope_tables(position_ids, HEAD_DIM)
    rot_cos = cosine[:, :, None, :]
    rot_sin = sine_table[:, :, None, :]
    query_matrix = rotate(projected[:, :, 0], rot_cos, rot_sin).astype(jnp.bfloat16)
    key_matrix_rows = rotate(projected[:, :, 1], rot_cos, rot_sin).astype(jnp.bfloat16)
    value_matrix_rows = projected[:, :, 2].astype(jnp.bfloat16)
    key_value = jnp.concatenate(
        [
            key_matrix_rows.reshape(local_len, seq_count, inner_width),
            value_matrix_rows.reshape(local_len, seq_count, inner_width),
        ],
        axis=-1,
    )
    key_value_all = lax.all_gather(key_value, "context", axis=0, tiled=True)
    keys_all = key_value_all[..., :inner_width].reshape(full_len, seq_count, heads_dev, HEAD_DIM)
    values_all = key_value_all[..., inner_width:].reshape(full_len, seq_count, heads_dev, HEAD_DIM)
    offset = lax.axis_index("context") * local_len
    seg_query = lax.dynamic_slice_in_dim(segment_ids, offset, local_len, 0)
    same_doc = seg_query.T[:, :, None] == segment_ids.T[:, None, :]
    keep_mask = (seg_query > 0).astype(jnp.float32)
    unscaled_score = jnp.einsum(
        "lshd,mshd->shlm", query_matrix, keys_all, preferred_element_type=jnp.float32
    )
    scores = jnp.where(same_doc[:, None], unscaled_score * score_scale, -jnp.inf)
    row_max = jnp.max(scores, axis=-1, keepdims=True)
    log_total = row_max + jnp.log(jnp.sum(jnp.exp(scores - row_max), axis=-1, keepdims=True))
    probs_low = jnp.exp(scores - log_total).astype(jnp.bfloat16)
    attended = jnp.einsum(
        "shlm,mshd->lshd", probs_low, values_all, preferred_element_type=jnp.float32
    )
    attn_in = (
        (attended * keep_mask[:, :, None, None])
        .astype(jnp.bfloat16)
        .reshape(token_count, inner_width)
    )
    branch_one = lax.psum(
        jnp.dot(attn_in, w_out, preferred_element_type=jnp.float32).astype(jnp.bfloat16), "tensor"
    ).astype(jnp.float32)
    resid = inputs + branch_one
    mlp_in = layer_norm(resid, norm_gains[1]).astype(jnp.bfloat16)
    mixed_rows = project(mlp_in, w_in)
    hidden_full, geglu_pull = jax.vjp(geglu_gate, mixed_rows[:, :ff_dev], mixed_rows[:, ff_dev:])
    hidden = hidden_full.astype(jnp.bfloat16)
    branch_two = lax.psum(
        jnp.dot(hidden, w_down, preferred_element_type=jnp.float32).astype(jnp.bfloat16), "tensor"
    ).astype(jnp.float32)
    layer_out = (resid + branch_two).astype(jnp.bfloat16).reshape(local_len, seq_count, model_width)
    out_cot = out_grad.astype(jnp.float32).reshape(token_count, model_width)
    dbranch_two = out_cot.astype(jnp.bfloat16)
    dhidden = project(dbranch_two, w_down)
    dgate, dup_part = geglu_pull(dhidden)
    dmixed = jnp.concatenate([dgate, dup_part], axis=1).astype(jnp.bfloat16)
    dnormed_two = lax.psum(
        jnp.dot(dmixed, w_in, preferred_element_type=jnp.float32).astype(jnp.bfloat16), "tensor"
    ).astype(jnp.float32)
    norm_two_out, norm_two_pull = jax.vjp(layer_norm, resid, norm_gains[1])
    dresid_norm, dgain_two = norm_two_pull(dnormed_two)
    dresid = out_cot + dresid_norm
    dbranch_one = dresid.astype(jnp.bfloat16)
    keep_low = keep_mask.reshape(token_count, 1).astype(jnp.bfloat16)
    dattended = project(dbranch_one, w_out).astype(jnp.bfloat16) * keep_low
    dattn = dattended.reshape(local_len, seq_count, heads_dev, HEAD_DIM)
    dquery_list = []
    dkey_list = []
    dvalue_list = []
    for head_index in range(heads_dev):
        query_head = query_matrix[:, :, head_index]
        key_head = keys_all[:, :, head_index]
        value_head = values_all[:, :, head_index]
        dout_head = dattn[:, :, head_index]
        raw_head = jnp.einsum(
            "lsd,msd->slm", query_head, key_head, preferred_element_type=jnp.float32
        )
        prob_head = jnp.exp(
            jnp.where(same_doc, raw_head * score_scale, -jnp.inf) - log_total[:, head_index]
        )
        dprob = jnp.einsum(
            "lsd,msd->slm", dout_head, value_head, preferred_element_type=jnp.float32
        )
        delta = jnp.sum(prob_head * dprob, axis=-1, keepdims=True)
        dscore = (prob_head * (dprob - delta) * score_scale).astype(jnp.bfloat16)
        dquery_list.append(
            jnp.einsum("slm,msd->lsd", dscore, key_head, preferred_element_type=jnp.float32)
        )
        dkey_head = jnp.einsum(
            "slm,lsd->msd", dscore, query_head, preferred_element_type=jnp.float32
        )
        dvalue_head = jnp.einsum(
            "slm,lsd->msd",
            prob_head.astype(jnp.bfloat16),
            dout_head,
            preferred_element_type=jnp.float32,
        )
        summed = lax.psum_scatter(
            jnp.concatenate([dkey_head, dvalue_head], axis=-1).astype(jnp.bfloat16),
            "context",
            scatter_dimension=0,
            tiled=True,
        ).astype(jnp.float32)
        dkey_list.append(summed[..., :HEAD_DIM])
        dvalue_list.append(summed[..., HEAD_DIM:])
    dqueries = jnp.stack(dquery_list, axis=2)
    dkeys = jnp.stack(dkey_list, axis=2)
    dvalues = jnp.stack(dvalue_list, axis=2)
    dprojected = (
        jnp.stack(
            [
                rotate_back(dqueries, rot_cos, rot_sin),
                rotate_back(dkeys, rot_cos, rot_sin),
                dvalues,
            ],
            axis=2,
        )
        .astype(jnp.bfloat16)
        .reshape(token_count, 3 * inner_width)
    )
    dnormed_one = lax.psum(
        jnp.dot(dprojected, w_qkv, preferred_element_type=jnp.float32).astype(jnp.bfloat16),
        "tensor",
    ).astype(jnp.float32)
    norm_one_out, norm_one_pull = jax.vjp(layer_norm, inputs, norm_gains[0])
    dinput_norm, dgain_one = norm_one_pull(dnormed_one)
    tokens_grad = (
        (dresid + dinput_norm).astype(jnp.bfloat16).reshape(local_len, seq_count, model_width)
    )
    gain_grads = lax.psum(jnp.stack([dgain_one, dgain_two]), ("fsdp", "context"))

    def padded(block, used_rows):
        return jnp.pad(block, ((0, 0), (0, pad_rows - used_rows)))

    left_rows = jnp.concatenate(
        [
            padded(dprojected, counts[0]),
            padded(attn_in, counts[1]),
            padded(dmixed, counts[2]),
            padded(hidden, counts[3]),
        ],
        axis=1,
    )
    right_rows = jnp.stack([act_in, dbranch_one, mlp_in, dbranch_two])
    blocks = local_rows * lax.axis_size(("fsdp", "context")) // pad_rows
    col_block = left_rows.reshape(token_count, blocks, pad_rows)
    grad_block = lax.psum_scatter(
        jnp.einsum(
            "nbp,bnd->bpd", col_block, right_rows, preferred_element_type=jnp.float32
        ).reshape(local_rows * lax.axis_size(("fsdp", "context")), model_width),
        ("fsdp", "context"),
        scatter_dimension=0,
        tiled=True,
    )
    momentum = muon_state.reshape(local_rows, model_width)
    muon_next = muon_beta * momentum + (1.0 - muon_beta) * grad_block
    direction = (1.0 - muon_beta) * grad_block + muon_beta * muon_next
    norm_total = lax.psum(jnp.sum(direction * direction), ("context", "tensor"))
    norm_size = jnp.sqrt(norm_total)
    direction_scale = jnp.log(norm_size).reshape(1)
    ortho_local = direction / (norm_size + ortho_eps)
    ortho_block = lax.all_gather(
        ortho_local.astype(jnp.bfloat16), "context", axis=0, tiled=True
    ).astype(ortho_local.dtype)
    for sweep_index in range(ITERS):
        gram_sum = lax.psum(
            contract_exact(ortho_block, ortho_block).astype(jnp.bfloat16), "tensor"
        ).astype(jnp.float32)
        square = jnp.dot(
            gram_sum, gram_sum, precision=precision_highest, preferred_element_type=jnp.float32
        )
        mix_matrix = ns_second * gram_sum + ns_third * square
        ortho_block = ns_first * ortho_block + jnp.dot(
            ortho_block, mix_matrix, precision=precision_highest, preferred_element_type=jnp.float32
        )
    own_rows = lax.dynamic_slice_in_dim(
        ortho_block, lax.axis_index("context") * local_rows, local_rows, 0
    )
    owner_index = lax.axis_index("fsdp")
    spreads = jnp.array(
        [0.2 * math.sqrt(3 * D), 0.2 * math.sqrt(D), 0.2 * math.sqrt(2 * FF), 0.2 * math.sqrt(FF)],
        jnp.float32,
    )
    spread = jnp.sum(jnp.where(jnp.arange(4) == owner_index, spreads, 0.0))
    old_weight = own_block.astype(jnp.float32)
    weight_update = -muon_rate * (spread * own_rows + decay_rate * old_weight)
    adam_first_next = adam_beta * adam_first + (1.0 - adam_beta) * gain_grads
    adam_second_next = adam_beta * adam_second + (1.0 - adam_beta) * gain_grads * gain_grads
    correction = 1.0 - adam_beta**STEP
    gain_update = -adam_rate * (
        adam_first_next / correction / (jnp.sqrt(adam_second_next / correction) + adam_eps)
        + decay_rate * norm_gains
    )
    block_shape = (1, 1, local_rows, model_width)
    return (
        layer_out,
        tokens_grad,
        grad_block.reshape(block_shape),
        muon_next.reshape(block_shape),
        weight_update.reshape(block_shape),
        direction_scale,
        gain_grads,
        adam_first_next,
        adam_second_next,
        gain_update,
    )


MESH_ID = pl.DeviceIdType.MESH
ANY = pl.ANY


def ring_place(index):
    return index + index // 2 - 2 * (index // 3)


def split_units(rows, parts, unit=16):
    units = rows // unit
    sizes = [(units // parts + (1 if i < units % parts else 0)) * unit for i in range(parts)]
    return [s for s in sizes if s]


def ring_chunks(counts, local_rows, which, core, target):
    first = core * local_rows
    rows = min(counts[which], first + local_rows) - first
    if rows <= 0:
        return [[], []]
    halves = split_units(rows, 2)
    if len(halves) == 1:
        halves = halves + [0]
    out, at = [], first
    for half in halves:
        pieces = []
        if half:
            for size in split_units(half, max(1, round(half / target))):
                pieces.append((at, size))
                at += size
        out.append(pieces)
    return out


class Place:
    def __init__(self):
        self.f = lax.axis_index("fsdp")
        self.c = lax.axis_index("context")
        self.t = lax.axis_index("tensor")
        self.pos = ring_place(self.f)
        self.next = ring_place((self.pos + 1) % 4)
        self.prev = ring_place((self.pos + 3) % 4)
        self.outer = jnp.logical_or(self.t == 0, self.t == 3)
        self.inner_mate = jnp.where(self.t == 0, 1, 2)
        self.outer_mate = jnp.where(self.t == 1, 0, 3)

    def ring(self, direction):
        return (self.next if direction == 0 else self.prev, self.c, self.t)

    def partner(self):
        return (self.f, 1 - self.c, self.t)

    def chip_z(self, z):
        return (self.f, self.c, z)

    def hop(self, which, direction):
        home = (0, 1, 3, 2)[which]
        if direction == 0:
            return (self.pos + 4 - home) % 4
        return (home + 4 - self.pos) % 4


def greet(place, ring, partner, line):
    barrier = pltpu.get_barrier_semaphore()

    def signal(device):
        pl.semaphore_signal(barrier, inc=1, device_id=device, device_id_type=MESH_ID)

    count = 0
    if ring:
        signal(place.ring(0))
        signal(place.ring(1))
        count += 2
    if partner:
        signal(place.partner())
        count += 1
    if line:
        @pl.when(place.outer)
        def _():
            signal(place.chip_z(place.inner_mate))
            pl.semaphore_wait(barrier, count + 1)

        @pl.when(jnp.logical_not(place.outer))
        def _():
            signal(place.chip_z(place.outer_mate))
            signal(place.chip_z(3 - place.t))
            pl.semaphore_wait(barrier, count + 2)
    else:
        pl.semaphore_wait(barrier, count)


def remote(src, dst, send, recv, device):
    return pltpu.make_async_remote_copy(
        src_ref=src, dst_ref=dst, send_sem=send, recv_sem=recv, device_id=device, device_id_type=MESH_ID
    )


def run_steps(*tracks):
    total = max(len(track) for track in tracks)
    done = [0] * len(tracks)
    for index in range(total):
        for number, track in enumerate(tracks):
            upto = -(-len(track) * (index + 1) // total)
            while done[number] < upto:
                track[done[number]]()
                done[number] += 1


def gather_plan(counts, local_rows, ks, target=96):
    plan = []
    for core in (0, 1):
        ident = 0
        for which in ks:
            for direction, pieces in enumerate(ring_chunks(counts, local_rows, which, core, target)):
                for order, (row, rows) in enumerate(pieces):
                    plan.append((ident, which, core, direction, order, row, rows))
                    ident += 1
    return plan, max(p[0] for p in plan) + 1


def gather_steps(place, plan, local_rows, base, own_ref, out_ref, sems):
    ss, rs, sp, rp = sems

    def dst(which, row, rows):
        return out_ref.at[pl.ds(base[which] + row, rows)]

    def src(core, row, rows):
        return own_ref.at[pl.ds(row - core * local_rows, rows)]

    def begin():
        for ident, which, core, direction, order, row, rows in plan:
            @pl.when(jnp.logical_and(place.c == core, place.f == which))
            def _():
                remote(src(core, row, rows), dst(which, row, rows), ss.at[ident], rs.at[ident],
                       place.ring(direction)).start()
        for ident, which, core, direction, order, row, rows in plan:
            @pl.when(jnp.logical_and(place.c == core, place.f == which))
            def _():
                remote(src(core, row, rows), dst(which, row, rows), sp.at[ident], rp.at[ident],
                       place.partner()).start()

    ordered = sorted(plan, key=lambda p: (p[4], p[1]))
    last = max(p[4] for p in plan)

    def visit(item, role):
        ident, which, core, direction, order, row, rows = item
        mine = dst(which, row, rows)

        @pl.when(jnp.logical_and(place.c == core, place.hop(which, direction) == role))
        def _():
            remote(mine, mine, ss.at[ident], rs.at[ident], place.ring(direction)).wait_recv()
            if role <= 2:
                remote(mine, mine, ss.at[ident], rs.at[ident], place.ring(direction)).start()
            remote(mine, mine, sp.at[ident], rp.at[ident], place.partner()).start()

    def step(j):
        def run():
            for role in (1, 2, 3):
                for item in ordered:
                    if item[4] == j - (role - 1):
                        visit(item, role)
        return run

    def end():
        for ident, which, core, direction, order, row, rows in plan:
            hop = place.hop(which, direction)
            mine = dst(which, row, rows)

            @pl.when(jnp.logical_and(place.c == core, hop <= 2))
            def _():
                remote(mine, mine, ss.at[ident], rs.at[ident], place.ring(direction)).wait_send()

            @pl.when(place.c == core)
            def _():
                remote(mine, mine, sp.at[ident], rp.at[ident], place.partner()).wait_send()

            @pl.when(place.c == 1 - core)
            def _():
                remote(mine, mine, sp.at[ident], rp.at[ident], place.partner()).wait_recv()

    return begin, [step(j) for j in range(last + 3)], end


def line_steps(place, chunks, own, out, early, mid, low, sems, lag=1, back_lag=3, prep=None, done=None):
    s1, r1, s2, r2, s3, r3 = sems

    def from_end(i, device):
        return remote(own(i), early(i), s1.at[i], r1.at[i], device)

    def across(i):
        return remote(mid(i), low(i), s2.at[i], r2.at[i], place.chip_z(3 - place.t))

    def back(i, device):
        return remote(out(i), out(i), s3.at[i], r3.at[i], device)

    def step(i):
        def run():
            if i < chunks and prep is not None:
                prep(i)

            @pl.when(place.outer)
            def _():
                if i < chunks:
                    from_end(i, place.chip_z(place.inner_mate)).start()
                if 0 <= i - lag - back_lag < chunks:
                    back(i - lag - back_lag, place.chip_z(place.inner_mate)).wait_recv()

            @pl.when(jnp.logical_not(place.outer))
            def _():
                if i < chunks:
                    from_end(i, place.chip_z(place.outer_mate)).wait_recv()
                    pair = own(i)[...].astype(jnp.float32) + early(i)[...].astype(jnp.float32)
                    mid(i)[...] = pair.astype(mid(i).dtype)
                    across(i).start()
                j = i - lag
                if 0 <= j < chunks:
                    across(j).wait_recv()
                    total = mid(j)[...].astype(jnp.float32) + low(j)[...].astype(jnp.float32)
                    out(j)[...] = total.astype(out(j).dtype)
                    back(j, place.chip_z(place.outer_mate)).start()
            if done is not None:
                if 0 <= i - lag - back_lag < chunks:
                    done(i - lag - back_lag)
        return run

    def end():
        @pl.when(place.outer)
        def _():
            for i in range(chunks):
                from_end(i, place.chip_z(place.inner_mate)).wait_send()

        @pl.when(jnp.logical_not(place.outer))
        def _():
            for i in range(chunks):
                across(i).wait_send()
                back(i, place.chip_z(place.outer_mate)).wait_send()

    return [step(i) for i in range(chunks + lag + back_lag)], end


def scatter_steps(place, plan, local_rows, base, part_ref, grad_ref, prx, rrx, tx, sems):
    ss, rs, sp, rp = sems

    def rows_of(ref, which, row, rows):
        return ref.at[pl.ds(base[which] + row, rows)]

    def partner_copy(item):
        ident, which, core, direction, order, row, rows = item
        return remote(rows_of(part_ref, which, row, rows), rows_of(prx, which, row, rows),
                      sp.at[ident], rp.at[ident], place.partner())

    def ring_copy(item):
        ident, which, core, direction, order, row, rows = item
        return remote(rows_of(tx, which, row, rows), rows_of(rrx, which, row, rows),
                      ss.at[ident], rs.at[ident], place.ring(direction))

    ordered = sorted(plan, key=lambda p: (p[4], p[1]))
    last = max(p[4] for p in plan)

    def begin():
        for item in ordered:
            @pl.when(place.c == 1 - item[2])
            def _():
                partner_copy(item).start()

    def visit(item, late):
        ident, which, core, direction, order, row, rows = item
        hop = place.hop(which, direction)
        role = (late + 1) % 4

        @pl.when(jnp.logical_and(place.c == core, hop == role))
        def _():
            partner_copy(item).wait_recv()
            total = (rows_of(part_ref, which, row, rows)[...].astype(jnp.float32)
                     + rows_of(prx, which, row, rows)[...].astype(jnp.float32))
            if role != 1:
                ring_copy(item).wait_recv()
                total = total + rows_of(rrx, which, row, rows)[...].astype(jnp.float32)
            if role == 0:
                grad_ref[pl.ds(row - core * local_rows, rows)] = total
            else:
                rows_of(tx, which, row, rows)[...] = total.astype(tx.dtype)
                ring_copy(item).start()

    def step(j):
        def run():
            for late in range(4):
                for item in ordered:
                    if item[4] == j - late:
                        visit(item, late)
        return run

    def end():
        for item in plan:
            ident, which, core, direction, order, row, rows = item

            @pl.when(place.c == 1 - core)
            def _():
                partner_copy(item).wait_send()

            @pl.when(jnp.logical_and(place.c == core, place.hop(which, direction) != 0))
            def _():
                ring_copy(item).wait_send()

    return begin, [step(j) for j in range(last + 4)], end


VMEM_SPEC = pl.BlockSpec(memory_space=pltpu.VMEM)
ANY_SPEC = pl.BlockSpec(memory_space=pl.ANY)


def dma(count):
    return pltpu.SemaphoreType.DMA((count,))


def comm_call(kernel, outs, ins, in_specs, out_specs, scratch, ident):
    return pl.pallas_call(
        kernel,
        out_shape=outs,
        in_specs=in_specs,
        out_specs=out_specs,
        scratch_shapes=scratch,
        compiler_params=pltpu.CompilerParams(
            collective_id=ident, has_side_effects=True, vmem_limit_bytes=60 * 2**20
        ),
    )(*ins)


def base_rows(counts, ks):
    base, at = {}, 0
    for which in ks:
        base[which] = at
        at += counts[which]
    return base, at


def own_rows_copy(place, counts, local_rows, ks, base, own_ref, out_ref, sem, act):
    for which in ks:
        for core in (0, 1):
            rows = min(counts[which] - core * local_rows, local_rows)
            if rows > 0:
                @pl.when(jnp.logical_and(place.c == core, place.f == which))
                def _():
                    act(pltpu.make_async_copy(
                        own_ref.at[pl.ds(0, rows)],
                        out_ref.at[pl.ds(base[which] + core * local_rows, rows)],
                        sem.at[0],
                    ))


def gather_weights(own_block, counts, ks, ident):
    local_rows, width = own_block.shape
    plan, count = gather_plan(counts, local_rows, ks)
    base, total = base_rows(counts, ks)

    def kernel(own_ref, out_ref, ss, rs, sp, rp, local_sem):
        place = Place()
        greet(place, True, True, False)
        begin, steps, end = gather_steps(place, plan, local_rows, base, own_ref, out_ref, (ss, rs, sp, rp))
        begin()
        own_rows_copy(place, counts, local_rows, ks, base, own_ref, out_ref, local_sem, lambda d: d.start())
        run_steps(steps)
        own_rows_copy(place, counts, local_rows, ks, base, own_ref, out_ref, local_sem, lambda d: d.wait())
        end()

    return comm_call(kernel, jax.ShapeDtypeStruct((total, width), own_block.dtype), (own_block,),
                     [VMEM_SPEC], VMEM_SPEC, [dma(count)] * 4 + [dma(1)], ident), base


def line_sum_and_gather(term, own_block, counts, ks, ident, chunks=8):
    local_rows, width = own_block.shape
    plan, count = gather_plan(counts, local_rows, ks)
    base, total = base_rows(counts, ks)
    rows = term.shape[0] // chunks

    def kernel(term_ref, own_ref, sum_ref, out_ref, early, mid, low, *sems):
        place = Place()
        greet(place, True, True, True)
        cut = lambda ref: lambda i: ref.at[pl.ds(i * rows, rows)]
        line, line_end = line_steps(place, chunks, cut(term_ref), cut(sum_ref), cut(early), cut(mid), cut(low), sems[:6])
        begin, steps, end = gather_steps(place, plan, local_rows, base, own_ref, out_ref, sems[6:10])
        begin()
        own_rows_copy(place, counts, local_rows, ks, base, own_ref, out_ref, sems[10], lambda d: d.start())
        run_steps(line, steps)
        own_rows_copy(place, counts, local_rows, ks, base, own_ref, out_ref, sems[10], lambda d: d.wait())
        line_end()
        end()

    return comm_call(
        kernel,
        (jax.ShapeDtypeStruct(term.shape, term.dtype), jax.ShapeDtypeStruct((total, width), own_block.dtype)),
        (term, own_block), [VMEM_SPEC] * 2, (VMEM_SPEC, VMEM_SPEC),
        [pltpu.VMEM(term.shape, term.dtype)] * 3 + [dma(chunks)] * 6 + [dma(count)] * 4 + [dma(1)], ident,
    ), base


def scatter_grads(part, counts, ks, local_rows, ident, term=None, chunks=8):
    plan, count = gather_plan(counts, local_rows, ks)
    base, total = base_rows(counts, ks)
    width = part.shape[1]
    lined = term is not None
    rows = term.shape[0] // chunks if lined else 0

    def kernel(*refs):
        part_ref, refs = refs[0], refs[1:]
        if lined:
            term_ref, grad_ref, sum_ref, prx, rrx, tx, early, mid, low = refs[:9]
            sems = refs[9:]
        else:
            grad_ref, prx, rrx, tx = refs[:4]
            sems = refs[4:]
        place = Place()
        greet(place, True, True, lined)
        begin, steps, end = scatter_steps(place, plan, local_rows, base, part_ref, grad_ref, prx, rrx, tx, sems[:4])
        begin()
        grad_ref[...] = jnp.zeros_like(grad_ref)
        if lined:
            cut = lambda ref: lambda i: ref.at[pl.ds(i * rows, rows)]
            line, line_end = line_steps(place, chunks, cut(term_ref), cut(sum_ref), cut(early), cut(mid), cut(low), sems[4:10])
            run_steps(line, steps)
            line_end()
        else:
            run_steps(steps)
        end()

    ins = (part, term) if lined else (part,)
    outs = [jax.ShapeDtypeStruct((local_rows, width), jnp.float32)]
    scratch = [pltpu.VMEM(part.shape, part.dtype)] * 3
    sems = [dma(count)] * 4
    if lined:
        outs.append(jax.ShapeDtypeStruct(term.shape, term.dtype))
        scratch += [pltpu.VMEM(term.shape, term.dtype)] * 3
        sems += [dma(chunks)] * 6
    return comm_call(kernel, tuple(outs), ins, [VMEM_SPEC] * len(ins), tuple([VMEM_SPEC] * len(outs)), scratch + sems, ident)


def swap_cores(block, ident):
    def kernel(x_ref, o_ref, send, recv):
        place = Place()
        greet(place, False, True, False)
        copy = remote(x_ref, o_ref, send.at[0], recv.at[0], place.partner())
        copy.start()
        copy.wait()

    return comm_call(kernel, jax.ShapeDtypeStruct(block.shape, block.dtype), (block,), [VMEM_SPEC], VMEM_SPEC,
                     [dma(1), dma(1)], ident)


def plane_sum(block, ident):
    def kernel(x_ref, o_ref, held, send, recv):
        f, c, t = lax.axis_index("fsdp"), lax.axis_index("context"), lax.axis_index("tensor")
        me = f * 2 + c
        barrier = pltpu.get_barrier_semaphore()

        def device(shift):
            other = (me + shift) % 8
            return (other // 2, other % 2, t)

        for shift in range(1, 8):
            pl.semaphore_signal(barrier, inc=1, device_id=device(shift), device_id_type=MESH_ID)
        pl.semaphore_wait(barrier, 7)
        held[pl.ds(me, 1)] = x_ref[...][None]
        copies = []
        for shift in range(1, 8):
            copy = remote(x_ref, held.at[me], send.at[shift], recv.at[shift], device(shift))
            copy.start()
            copies.append(copy)
        for copy in copies:
            copy.wait()
        total = held[0]
        for k in range(1, 8):
            total = total + held[k]
        o_ref[...] = total

    return comm_call(kernel, jax.ShapeDtypeStruct(block.shape, block.dtype), (block,), [VMEM_SPEC], VMEM_SPEC,
                     [pltpu.VMEM((8,) + block.shape, block.dtype), dma(8), dma(8)], ident)


def gram_sum(rows_low, square, ident):
    rows, width = rows_low.shape
    tile = width // 4
    half = tile // 2
    chunks = 10

    def kernel(x_ref, q_ref, g_ref, norm_ref, mine, theirs, prx, tot, other, early, mid, low, *sems):
        place = Place()
        c = place.c
        sp, rp, st, rt = sems[6:10]

        def blocks(core):
            return [(3 * core, 3 * core), (2 * core, 2 * core + 1), (core + 1, core + 1), (core, core + 2), (core, 3 - core)]

        greet(place, False, True, True)

        def at(k):
            return pl.ds(pl.multiple_of(k * tile, tile), tile)

        def gram(i, j):
            return lax.dot_general(x_ref[:, at(i)], x_ref[:, at(j)], (((0,), (0,)), ((), ())),
                                   preferred_element_type=jnp.float32)

        def partner(n):
            sl = pl.ds(n * tile, tile)
            return remote(theirs.at[sl], prx.at[sl], sp.at[n], rp.at[n], place.partner())

        def norm_row(ref):
            return ref.at[pl.ds(5 * tile, 8)]

        for n, (i, j) in enumerate(blocks(1 - c)):
            theirs[pl.ds(n * tile, tile)] = gram(i, j)
            partner(n).start()
        norm_row(theirs)[...] = jnp.broadcast_to(q_ref[0:1, 0:1], (8, tile))
        pn = remote(norm_row(theirs), norm_row(prx), sp.at[5], rp.at[5], place.partner())
        pn.start()

        def span(i):
            return pl.ds(i * half, half) if i < chunks - 1 else pl.ds(i * half, half + 8)

        def cut(ref):
            return lambda i: ref.at[span(i)]

        def prep(i):
            if i % 2 == 0:
                n = i // 2
                sl = pl.ds(n * tile, tile)
                block = gram(*blocks(c)[n])
                partner(n).wait_recv()
                mine[sl] = block + prx[sl]
            if i == chunks - 1:
                pn.wait_recv()
                norm_row(mine)[...] = norm_row(prx)[...] + jnp.broadcast_to(q_ref[0:1, 0:1], (8, tile))

        def share(i):
            return remote(cut(tot)(i), cut(other)(i), st.at[i], rt.at[i], place.partner())

        def place_block(ref, n, core):
            i, j = blocks(core)[n]
            block = ref[pl.ds(n * tile, tile)]
            g_ref[at(i), at(j)] = block
            g_ref[at(j), at(i)] = block.T

        def done(i):
            share(i).start()
            if i % 2 == 1:
                place_block(tot, i // 2, c)
            if i >= 2:
                share(i - 2).wait_recv()
                if (i - 2) % 2 == 1:
                    place_block(other, (i - 2) // 2, 1 - c)

        steps, end = line_steps(place, chunks, cut(mine), cut(tot), cut(early), cut(mid), cut(low), sems[:6],
                                prep=prep, done=done)
        run_steps(steps)
        for i in (chunks - 2, chunks - 1):
            share(i).wait_recv()
        place_block(other, 4, 1 - c)
        norm_ref[...] = jnp.broadcast_to(tot[5 * tile:5 * tile + 8, 0:128], (8, 128))
        end()
        for n in range(5):
            partner(n).wait_send()
        pn.wait_send()
        for i in range(chunks):
            share(i).wait_send()

    packed = pltpu.VMEM((5 * tile + 8, tile), jnp.float32)
    return comm_call(
        kernel,
        (jax.ShapeDtypeStruct((width, width), jnp.float32), jax.ShapeDtypeStruct((8, 128), jnp.float32)),
        (rows_low, square), [VMEM_SPEC] * 2, (VMEM_SPEC, VMEM_SPEC),
        [packed] * 8 + [dma(chunks)] * 6 + [dma(6), dma(6), dma(chunks), dma(chunks)], ident,
    )


def halves(value):
    high = value.astype(jnp.bfloat16)
    return high, (value - high.astype(jnp.float32)).astype(jnp.bfloat16)


def gaps(fixed, moved):
    return [(fixed * (index + 1)) // moved for index in range(moved)]


def iterate(gram, norm, direction_low, own_block, branch_term, resid, dgains, norm_gains, adam_first, adam_second, ident):
    rows, width = direction_low.shape
    tile = 256
    parts = width // tile
    tokens = branch_term.shape[0]
    chunks = 8
    step_rows = tokens // chunks
    aa = ns_first * ns_first
    ab = 2.0 * ns_first * ns_second
    bbac = ns_second * ns_second + 2.0 * ns_first * ns_third
    bc = 2.0 * ns_second * ns_third
    cc = ns_third * ns_third
    correction = 1.0 - adam_beta**STEP

    def kernel(g_ref, n_ref, d_ref, w_ref, t_ref, r_ref, dg_ref, gain_ref, af_ref, as_ref,
               u_ref, lo_ref, gg_ref, afn_ref, asn_ref, gu_ref,
               p_ref, ph, pl_, hh, hl, uh, ul, mx, x_ref, early, mid, low, total, held, *sems):
        place = Place()
        s1, r1, s2, r2, s3, r3, sg, rg = sems
        me = place.f * 2 + place.c
        barrier = pltpu.get_barrier_semaphore()

        def plane(shift):
            other = (me + shift) % 8
            return (other // 2, other % 2, place.t)

        for shift in range(1, 8):
            pl.semaphore_signal(barrier, inc=1, device_id=plane(shift), device_id_type=MESH_ID)

        @pl.when(place.outer)
        def _():
            pl.semaphore_signal(barrier, inc=1, device_id=place.chip_z(place.inner_mate), device_id_type=MESH_ID)
            pl.semaphore_wait(barrier, 8)

        @pl.when(jnp.logical_not(place.outer))
        def _():
            pl.semaphore_signal(barrier, inc=1, device_id=place.chip_z(place.outer_mate), device_id_type=MESH_ID)
            pl.semaphore_signal(barrier, inc=1, device_id=place.chip_z(3 - place.t), device_id_type=MESH_ID)
            pl.semaphore_wait(barrier, 9)

        def cut(ref, i):
            if isinstance(i, int):
                return ref.at[pl.ds(i * step_rows, step_rows)]
            return ref.at[pl.ds(pl.multiple_of(i * step_rows, step_rows), step_rows)]

        def from_end(i, device):
            return remote(cut(t_ref, i), cut(early, i), s1.at[i], r1.at[i], device)

        def across(i):
            return remote(cut(mid, i), cut(low, i), s2.at[i], r2.at[i], place.chip_z(3 - place.t))

        def back(i, device):
            return remote(cut(total, i), cut(total, i), s3.at[i], r3.at[i], device)

        held[pl.ds(me, 1)] = dg_ref[...][None]
        for shift in range(1, 8):
            remote(dg_ref, held.at[me], sg.at[shift], rg.at[shift], plane(shift)).start()

        @pl.when(place.outer)
        def _():
            for i in range(chunks):
                from_end(i, place.chip_z(place.inner_mate)).start()

        def pair_up(i):
            @pl.when(jnp.logical_not(place.outer))
            def _():
                from_end(i, place.chip_z(place.outer_mate)).wait_recv()
                pair = cut(t_ref, i)[...].astype(jnp.float32) + cut(early, i)[...].astype(jnp.float32)
                cut(mid, i)[...] = pair.astype(mid.dtype)
                across(i).start()

        def join(i):
            @pl.when(jnp.logical_not(place.outer))
            def _():
                across(i).wait_recv()
                whole = cut(mid, i)[...].astype(jnp.float32) + cut(low, i)[...].astype(jnp.float32)
                cut(total, i)[...] = whole.astype(total.dtype)
                back(i, place.chip_z(place.outer_mate)).start()

        norm_size = jnp.sqrt(n_ref[0:1, 0:1])
        inverse = 1.0 / (norm_size + ortho_eps)
        scale = inverse * inverse

        for k in range(parts):
            sl = pl.ds(k * tile, tile)
            value = g_ref[sl] * scale
            p_ref[sl] = value
            high, rest = halves(value)
            ph[sl] = high
            pl_[sl] = rest
        x_ref[...] = d_ref[...].astype(jnp.float32) * inverse

        def product(lh, ll, rh, rl, k):
            sl, cols = pl.ds(k * tile, tile), pl.ds(k * tile, width - k * tile)

            def dot(left, right):
                return jnp.dot(left[sl], right[:, cols], preferred_element_type=jnp.float32)

            return dot(lh, rh) + dot(ll, rh) + dot(lh, rl)

        def spread_out(value, high_ref, low_ref, k):
            sl, cols = pl.ds(k * tile, tile), pl.ds(k * tile, width - k * tile)
            high, rest = halves(value)
            high_ref[sl, cols] = high
            low_ref[sl, cols] = rest
            for j in range(k + 1, parts):
                at = (j - k) * tile
                high_ref[pl.ds(j * tile, tile), sl] = high[:, at:at + tile].T
                low_ref[pl.ds(j * tile, tile), sl] = rest[:, at:at + tile].T

        def squares():
            for k in range(parts):
                sl, cols = pl.ds(k * tile, tile), pl.ds(k * tile, width - k * tile)
                value = product(ph, pl_, ph, pl_, k)
                spread_out(value, hh, hl, k)
                mix = (ns_second * p_ref[sl, cols] + ns_third * value).astype(mx.dtype)
                mx[sl, cols] = mix
                for j in range(k + 1, parts):
                    at = (j - k) * tile
                    mx[pl.ds(j * tile, tile), sl] = mix[:, at:at + tile].T

        def rotate_rows():
            for at, size in ((0, 336), (336, 320)):
                sl = pl.ds(at, size)
                old = x_ref[sl]
                x_ref[sl] = ns_first * old + jnp.dot(old.astype(jnp.bfloat16), mx[...], preferred_element_type=jnp.float32)

        def body(sweep, carry):
            pair_up(2 * sweep)
            squares()
            pair_up(2 * sweep + 1)

            @pl.when(sweep >= 1)
            def _():
                join(2 * sweep - 2)
            rotate_rows()
            for k in range(parts):
                sl, cols = pl.ds(k * tile, tile), pl.ds(k * tile, width - k * tile)
                cube = product(ph, pl_, hh, hl, k)
                square = hh[sl, cols].astype(jnp.float32) + hl[sl, cols].astype(jnp.float32)
                spread_out(bc * square + cc * cube, uh, ul, k)
                p_ref[sl, cols] = aa * p_ref[sl, cols] + ab * square + bbac * cube

            @pl.when(sweep >= 1)
            def _():
                join(2 * sweep - 1)
            for k in range(parts):
                sl, cols = pl.ds(k * tile, tile), pl.ds(k * tile, width - k * tile)
                value = p_ref[sl, cols] + product(hh, hl, uh, ul, k)
                p_ref[sl, cols] = value
                spread_out(value, ph, pl_, k)
            return carry

        lax.fori_loop(0, ITERS - 1, body, 0)
        join(chunks - 2)
        join(chunks - 1)
        squares()
        rotate_rows()
        spread = jnp.where(place.f == 0, 0.2 * math.sqrt(3 * D), jnp.where(place.f == 1, 0.2 * math.sqrt(D), jnp.where(
            place.f == 2, 0.2 * math.sqrt(2 * FF), 0.2 * math.sqrt(FF)))).astype(jnp.float32)
        u_ref[...] = -muon_rate * (spread * x_ref[...] + decay_rate * w_ref[...].astype(jnp.float32))

        for shift in range(1, 8):
            remote(dg_ref, held.at[me], sg.at[shift], rg.at[shift], plane(shift)).wait()
        grads = held[0]
        for k in range(1, 8):
            grads = grads + held[k]
        gg_ref[...] = grads
        first = adam_beta * af_ref[...] + (1.0 - adam_beta) * grads
        second = adam_beta * as_ref[...] + (1.0 - adam_beta) * grads * grads
        afn_ref[...] = first
        asn_ref[...] = second
        gu_ref[...] = -adam_rate * (
            first / correction / (jnp.sqrt(second / correction) + adam_eps) + decay_rate * gain_ref[...]
        )

        @pl.when(place.outer)
        def _():
            for i in range(chunks):
                back(i, place.chip_z(place.inner_mate)).wait_recv()
                from_end(i, place.chip_z(place.inner_mate)).wait_send()
        lo_ref[...] = (r_ref[...] + total[...].astype(jnp.float32)).astype(lo_ref.dtype)

        @pl.when(jnp.logical_not(place.outer))
        def _():
            for i in range(chunks):
                across(i).wait_send()
                back(i, place.chip_z(place.outer_mate)).wait_send()

    f32, low16 = jnp.float32, jnp.bfloat16
    small = jax.ShapeDtypeStruct(dgains.shape, f32)
    outs = (jax.ShapeDtypeStruct((rows, width), f32), jax.ShapeDtypeStruct((tokens, width), low16), small, small, small, small)
    full = pltpu.VMEM((width, width), low16)
    line = pltpu.VMEM((tokens, width), low16)
    scratch = [pltpu.VMEM((width, width), f32)] + [full] * 7 + [pltpu.VMEM((rows, width), f32)] + [line] * 4
    scratch += [pltpu.VMEM((8,) + dgains.shape, f32)] + [dma(chunks)] * 6 + [dma(8)] * 2
    ins = (gram, norm, direction_low, own_block, branch_term, resid, dgains, norm_gains, adam_first, adam_second)
    return comm_call(kernel, outs, ins, [VMEM_SPEC] * len(ins), (VMEM_SPEC,) * len(outs), scratch, ident)


def per_device_block(tokens, out_grad, weight_stack, muon_state, norm_gains, adam_first, adam_second, segment_ids,
                     position_ids):
    token_count, _, model_width = tokens.shape
    groups, contexts = 4, 2
    full_len = token_count * contexts
    local_rows = weight_stack.shape[2]
    heads_dev = HEADS // groups
    ff_dev = FF // groups
    inner_width = heads_dev * HEAD_DIM
    counts = (3 * inner_width, inner_width, 2 * ff_dev, ff_dev)
    score_scale = HEAD_DIM ** (-0.5)
    own_block = weight_stack.reshape(local_rows, model_width)
    low = jnp.bfloat16
    context = lax.axis_index("context")

    first_weights, base = gather_weights(own_block, counts, (0, 1), 0)
    w_qkv = first_weights[: counts[0]]
    w_out = first_weights[counts[0]:]
    inputs = tokens.astype(jnp.float32).reshape(token_count, model_width)
    act_in = layer_norm(inputs, norm_gains[0]).astype(low)
    projected = project(act_in, w_qkv).reshape(token_count, 3, heads_dev, HEAD_DIM)
    cosine, sine_table = rope_tables(position_ids.reshape(token_count), HEAD_DIM)
    rot_cos = cosine[:, None, :]
    rot_sin = sine_table[:, None, :]
    queries = rotate(projected[:, 0], rot_cos, rot_sin).astype(low)
    keys = rotate(projected[:, 1], rot_cos, rot_sin).astype(low)
    values = projected[:, 2].astype(low)
    mine = jnp.concatenate([keys.reshape(token_count, inner_width), values.reshape(token_count, inner_width)], axis=1)
    theirs = swap_cores(mine, 1)
    key_value = jnp.concatenate([mine, theirs], axis=0)
    keys_all = key_value[:, :inner_width].reshape(full_len, heads_dev, HEAD_DIM)
    values_all = key_value[:, inner_width:].reshape(full_len, heads_dev, HEAD_DIM)
    segments = segment_ids.reshape(full_len)
    seg_query = lax.dynamic_slice_in_dim(segments, context * token_count, token_count, 0)
    seg_other = lax.dynamic_slice_in_dim(segments, (1 - context) * token_count, token_count, 0)
    seg_key = jnp.concatenate([seg_query, seg_other])
    same_doc = (seg_query[:, None] == seg_key[None, :])[None]
    keep_mask = (seg_query > 0).astype(jnp.float32)[:, None]
    raw = jnp.einsum("lhd,mhd->hlm", queries, keys_all, preferred_element_type=jnp.float32)
    scores = jnp.where(same_doc, raw * score_scale, -jnp.inf)
    row_max = jnp.max(scores, axis=-1, keepdims=True)
    log_total = row_max + jnp.log(jnp.sum(jnp.exp(scores - row_max), axis=-1, keepdims=True))
    probs = jnp.exp(scores - log_total)
    probs_low = probs.astype(low)
    attended = jnp.einsum("hlm,mhd->lhd", probs_low, values_all, preferred_element_type=jnp.float32)
    attn_in = (attended.reshape(token_count, inner_width) * keep_mask).astype(low)
    branch_term = jnp.dot(attn_in, w_out, preferred_element_type=jnp.float32).astype(low)
    (branch_one, last_weights), _ = line_sum_and_gather(branch_term, own_block, counts, (2, 3), 2)
    w_in = last_weights[: counts[2]]
    w_down = last_weights[counts[2]:]
    resid = inputs + branch_one.astype(jnp.float32)
    mlp_in = layer_norm(resid, norm_gains[1]).astype(low)
    mixed_rows = project(mlp_in, w_in)
    hidden_full, geglu_pull = jax.vjp(geglu_gate, mixed_rows[:, :ff_dev], mixed_rows[:, ff_dev:])
    hidden = hidden_full.astype(low)
    branch_two_term = jnp.dot(hidden, w_down, preferred_element_type=jnp.float32).astype(low)
    out_low = out_grad.reshape(token_count, model_width)
    out_cot = out_low.astype(jnp.float32)
    dgate, dup_part = geglu_pull(project(out_low, w_down))
    dmixed = jnp.concatenate([dgate, dup_part], axis=1).astype(low)
    dnormed_two_term = jnp.dot(dmixed, w_in, preferred_element_type=jnp.float32).astype(low)

    def grad_term(left, right):
        return lax.dot_general(left, right, (((0,), (0,)), ((), ())), preferred_element_type=jnp.float32).astype(low)

    late_terms = jnp.concatenate([grad_term(dmixed, mlp_in), grad_term(hidden, out_low)], axis=0)
    grad_late, dnormed_two = scatter_grads(late_terms, counts, (2, 3), local_rows, 3, dnormed_two_term)
    _, norm_two_pull = jax.vjp(layer_norm, resid, norm_gains[1])
    dresid_norm, dgain_two = norm_two_pull(dnormed_two.astype(jnp.float32))
    dresid = out_cot + dresid_norm
    dbranch_one = dresid.astype(low)
    dattended = project(dbranch_one, w_out).astype(low) * keep_mask.astype(low)
    dattn = dattended.reshape(token_count, heads_dev, HEAD_DIM)
    dprobs = jnp.einsum("lhd,mhd->hlm", dattn, values_all, preferred_element_type=jnp.float32)
    delta = jnp.sum(probs * dprobs, axis=-1, keepdims=True)
    dscores = (probs * (dprobs - delta) * score_scale).astype(low)
    dqueries = jnp.einsum("hlm,mhd->lhd", dscores, keys_all, preferred_element_type=jnp.float32)
    dkeys = jnp.einsum("hlm,lhd->mhd", dscores, queries, preferred_element_type=jnp.float32)
    dvalues = jnp.einsum("hlm,lhd->mhd", probs_low, dattn, preferred_element_type=jnp.float32)
    dkv = jnp.concatenate([dkeys.reshape(full_len, inner_width), dvalues.reshape(full_len, inner_width)], axis=1)
    dkv_other = swap_cores(dkv[token_count:].astype(low), 4)
    dkv_own = dkv[:token_count] + dkv_other.astype(jnp.float32)
    dkeys = dkv_own[:, :inner_width].reshape(token_count, heads_dev, HEAD_DIM)
    dprojected = jnp.concatenate(
        [
            rotate_back(dqueries, rot_cos, rot_sin).reshape(token_count, inner_width),
            rotate_back(dkeys, rot_cos, rot_sin).reshape(token_count, inner_width),
            dkv_own[:, inner_width:],
        ],
        axis=1,
    ).astype(low)
    early_terms = jnp.concatenate([grad_term(dprojected, act_in), grad_term(attn_in, dbranch_one)], axis=0)
    dnormed_one_term = jnp.dot(dprojected, w_qkv, preferred_element_type=jnp.float32).astype(low)
    grad_early, dnormed_one = scatter_grads(early_terms, counts, (0, 1), local_rows, 5, dnormed_one_term)
    _, norm_one_pull = jax.vjp(layer_norm, inputs, norm_gains[0])
    dinput_norm, dgain_one = norm_one_pull(dnormed_one.astype(jnp.float32))
    tokens_grad = (dresid + dinput_norm).astype(low).reshape(tokens.shape)

    owner_index = lax.axis_index("fsdp")
    grad_block = jnp.where(owner_index >= 2, grad_late, grad_early)
    momentum = muon_state.reshape(local_rows, model_width)
    muon_next = muon_beta * momentum + (1.0 - muon_beta) * grad_block
    direction = (1.0 - muon_beta) * grad_block + muon_beta * muon_next
    direction_low = direction.astype(low)
    square = jnp.sum(direction * direction).reshape(1, 1)
    gram, norm_total = gram_sum(direction_low, jnp.broadcast_to(square, (8, 128)), 6)
    direction_scale = jnp.log(jnp.sqrt(norm_total[0, 0])).reshape(1)
    weight_update, layer_out, gain_grads, adam_first_next, adam_second_next, gain_update = iterate(
        gram, norm_total, direction_low, own_block, branch_two_term, resid, jnp.stack([dgain_one, dgain_two]),
        norm_gains, adam_first, adam_second, 7,
    )
    layer_out = layer_out.reshape(tokens.shape)
    block_shape = (1, 1, local_rows, model_width)
    return (
        layer_out,
        tokens_grad,
        grad_block.reshape(block_shape),
        muon_next.reshape(block_shape),
        weight_update.reshape(block_shape),
        direction_scale,
        gain_grads,
        adam_first_next,
        adam_second_next,
        gain_update,
    )


def solution(mesh):
    sizes = dict(mesh.shape)
    block = (sizes["fsdp"], sizes["context"], sizes["tensor"]) == (4, 2, 4)
    return jax.shard_map(
        per_device_block if block else per_device,
        mesh=mesh,
        in_specs=(
            P("context", "fsdp", None),
            P("context", "fsdp", None),
            P("fsdp", "tensor", "context", None),
            P("fsdp", "tensor", "context", None),
            P(),
            P(),
            P(),
            P(None, "fsdp"),
            P("context", "fsdp"),
        ),
        out_specs=(
            P("context", "fsdp", None),
            P("context", "fsdp", None),
            P("fsdp", "tensor", "context", None),
            P("fsdp", "tensor", "context", None),
            P("fsdp", "tensor", "context", None),
            P("fsdp"),
            P(),
            P(),
            P(),
            P(),
        ),
        check_vma=False,
    )
```

```python
import math

import jax
import jax.numpy as jnp
from jax import lax
from jax.experimental import pallas as pl
from jax.experimental.pallas import tpu as pltpu
from jax.sharding import PartitionSpec as P

D = 1024
HEADS = 16
HEAD_DIM = 64
FF = 2624
ITERS = 5
STEP = 8


rope_base = 160000.0
norm_eps = 1e-05
ns_first = 3.4445
ns_second = -4.775
ns_third = 2.0315
muon_beta = 0.5
muon_rate = 0.15
decay_rate = 0.1
adam_beta = 0.5
adam_rate = 0.05
ortho_eps = 1e-07
adam_eps = 1e-08
precision_highest = lax.Precision.HIGHEST


def layer_norm(values, gain_row):
    centre = values - jnp.mean(values, axis=-1, keepdims=True)
    spread = jnp.mean(centre * centre, axis=-1, keepdims=True)
    return centre * lax.rsqrt(spread + norm_eps) * gain_row


def rope_tables(positions, head_width):
    half_width = head_width // 2
    freqs = rope_base ** (-(jnp.arange(half_width, dtype=jnp.float32) * 2.0 / head_width))
    angle = positions.astype(jnp.float32)[..., None] * freqs
    angle = jnp.concatenate([angle, angle], axis=-1)
    return (jnp.cos(angle), jnp.sin(angle))


def rotate(values, cosine, sine_table):
    half_width = values.shape[-1] // 2
    turned = jnp.concatenate([-values[..., half_width:], values[..., :half_width]], axis=-1)
    return values * cosine + turned * sine_table


def rotate_back(grads_in, cosine, sine_table):
    half_width = grads_in.shape[-1] // 2
    scaled = grads_in * sine_table
    turned = jnp.concatenate([scaled[..., half_width:], -scaled[..., :half_width]], axis=-1)
    return grads_in * cosine + turned


def project(left_rows, right_rows):
    return lax.dot_general(
        left_rows, right_rows, (((1,), (1,)), ((), ())), preferred_element_type=jnp.float32
    )


def contract_exact(left_rows, right_rows):
    return lax.dot_general(
        left_rows,
        right_rows,
        (((0,), (0,)), ((), ())),
        precision=precision_highest,
        preferred_element_type=jnp.float32,
    )


def geglu_gate(gate_part, up_part):
    return jax.nn.gelu(gate_part, approximate=False) * up_part


def per_device(
    tokens,
    out_grad,
    weight_stack,
    muon_state,
    norm_gains,
    adam_first,
    adam_second,
    segment_ids,
    position_ids,
):
    local_len, seq_count, model_width = tokens.shape
    token_count = local_len * seq_count
    groups = lax.axis_size("tensor")
    contexts = lax.axis_size("context")
    full_len = local_len * contexts
    local_rows = weight_stack.shape[2]
    pad_rows = local_rows * contexts
    heads_dev = HEADS // groups
    ff_dev = FF // groups
    inner_width = heads_dev * HEAD_DIM
    counts = (3 * inner_width, inner_width, 2 * ff_dev, ff_dev)
    score_scale = HEAD_DIM ** (-0.5)
    own_block = weight_stack.reshape(local_rows, model_width)
    gathered = lax.all_gather(own_block, ("fsdp", "context"), axis=0, tiled=True).reshape(
        4, pad_rows, model_width
    )
    w_qkv = gathered[0, : counts[0]]
    w_out = gathered[1, : counts[1]]
    w_in = gathered[2, : counts[2]]
    w_down = gathered[3, : counts[3]]
    inputs = tokens.astype(jnp.float32).reshape(token_count, model_width)
    act_in = layer_norm(inputs, norm_gains[0]).astype(jnp.bfloat16)
    projected = project(act_in, w_qkv).reshape(local_len, seq_count, 3, heads_dev, HEAD_DIM)
    cosine, sine_table = rope_tables(position_ids, HEAD_DIM)
    rot_cos = cosine[:, :, None, :]
    rot_sin = sine_table[:, :, None, :]
    query_matrix = rotate(projected[:, :, 0], rot_cos, rot_sin).astype(jnp.bfloat16)
    key_matrix_rows = rotate(projected[:, :, 1], rot_cos, rot_sin).astype(jnp.bfloat16)
    value_matrix_rows = projected[:, :, 2].astype(jnp.bfloat16)
    key_value = jnp.concatenate(
        [
            key_matrix_rows.reshape(local_len, seq_count, inner_width),
            value_matrix_rows.reshape(local_len, seq_count, inner_width),
        ],
        axis=-1,
    )
    key_value_all = lax.all_gather(key_value, "context", axis=0, tiled=True)
    keys_all = key_value_all[..., :inner_width].reshape(full_len, seq_count, heads_dev, HEAD_DIM)
    values_all = key_value_all[..., inner_width:].reshape(full_len, seq_count, heads_dev, HEAD_DIM)
    offset = lax.axis_index("context") * local_len
    seg_query = lax.dynamic_slice_in_dim(segment_ids, offset, local_len, 0)
    same_doc = seg_query.T[:, :, None] == segment_ids.T[:, None, :]
    keep_mask = (seg_query > 0).astype(jnp.float32)
    unscaled_score = jnp.einsum(
        "lshd,mshd->shlm", query_matrix, keys_all, preferred_element_type=jnp.float32
    )
    scores = jnp.where(same_doc[:, None], unscaled_score * score_scale, -jnp.inf)
    row_max = jnp.max(scores, axis=-1, keepdims=True)
    log_total = row_max + jnp.log(jnp.sum(jnp.exp(scores - row_max), axis=-1, keepdims=True))
    probs_low = jnp.exp(scores - log_total).astype(jnp.bfloat16)
    attended = jnp.einsum(
        "shlm,mshd->lshd", probs_low, values_all, preferred_element_type=jnp.float32
    )
    attn_in = (
        (attended * keep_mask[:, :, None, None])
        .astype(jnp.bfloat16)
        .reshape(token_count, inner_width)
    )
    branch_one = lax.psum(
        jnp.dot(attn_in, w_out, preferred_element_type=jnp.float32).astype(jnp.bfloat16), "tensor"
    ).astype(jnp.float32)
    resid = inputs + branch_one
    mlp_in = layer_norm(resid, norm_gains[1]).astype(jnp.bfloat16)
    mixed_rows = project(mlp_in, w_in)
    hidden_full, geglu_pull = jax.vjp(geglu_gate, mixed_rows[:, :ff_dev], mixed_rows[:, ff_dev:])
    hidden = hidden_full.astype(jnp.bfloat16)
    branch_two = lax.psum(
        jnp.dot(hidden, w_down, preferred_element_type=jnp.float32).astype(jnp.bfloat16), "tensor"
    ).astype(jnp.float32)
    layer_out = (resid + branch_two).astype(jnp.bfloat16).reshape(local_len, seq_count, model_width)
    out_cot = out_grad.astype(jnp.float32).reshape(token_count, model_width)
    dbranch_two = out_cot.astype(jnp.bfloat16)
    dhidden = project(dbranch_two, w_down)
    dgate, dup_part = geglu_pull(dhidden)
    dmixed = jnp.concatenate([dgate, dup_part], axis=1).astype(jnp.bfloat16)
    dnormed_two = lax.psum(
        jnp.dot(dmixed, w_in, preferred_element_type=jnp.float32).astype(jnp.bfloat16), "tensor"
    ).astype(jnp.float32)
    norm_two_out, norm_two_pull = jax.vjp(layer_norm, resid, norm_gains[1])
    dresid_norm, dgain_two = norm_two_pull(dnormed_two)
    dresid = out_cot + dresid_norm
    dbranch_one = dresid.astype(jnp.bfloat16)
    keep_low = keep_mask.reshape(token_count, 1).astype(jnp.bfloat16)
    dattended = project(dbranch_one, w_out).astype(jnp.bfloat16) * keep_low
    dattn = dattended.reshape(local_len, seq_count, heads_dev, HEAD_DIM)
    dquery_list = []
    dkey_list = []
    dvalue_list = []
    for head_index in range(heads_dev):
        query_head = query_matrix[:, :, head_index]
        key_head = keys_all[:, :, head_index]
        value_head = values_all[:, :, head_index]
        dout_head = dattn[:, :, head_index]
        raw_head = jnp.einsum(
            "lsd,msd->slm", query_head, key_head, preferred_element_type=jnp.float32
        )
        prob_head = jnp.exp(
            jnp.where(same_doc, raw_head * score_scale, -jnp.inf) - log_total[:, head_index]
        )
        dprob = jnp.einsum(
            "lsd,msd->slm", dout_head, value_head, preferred_element_type=jnp.float32
        )
        delta = jnp.sum(prob_head * dprob, axis=-1, keepdims=True)
        dscore = (prob_head * (dprob - delta) * score_scale).astype(jnp.bfloat16)
        dquery_list.append(
            jnp.einsum("slm,msd->lsd", dscore, key_head, preferred_element_type=jnp.float32)
        )
        dkey_head = jnp.einsum(
            "slm,lsd->msd", dscore, query_head, preferred_element_type=jnp.float32
        )
        dvalue_head = jnp.einsum(
            "slm,lsd->msd",
            prob_head.astype(jnp.bfloat16),
            dout_head,
            preferred_element_type=jnp.float32,
        )
        summed = lax.psum_scatter(
            jnp.concatenate([dkey_head, dvalue_head], axis=-1).astype(jnp.bfloat16),
            "context",
            scatter_dimension=0,
            tiled=True,
        ).astype(jnp.float32)
        dkey_list.append(summed[..., :HEAD_DIM])
        dvalue_list.append(summed[..., HEAD_DIM:])
    dqueries = jnp.stack(dquery_list, axis=2)
    dkeys = jnp.stack(dkey_list, axis=2)
    dvalues = jnp.stack(dvalue_list, axis=2)
    dprojected = (
        jnp.stack(
            [
                rotate_back(dqueries, rot_cos, rot_sin),
                rotate_back(dkeys, rot_cos, rot_sin),
                dvalues,
            ],
            axis=2,
        )
        .astype(jnp.bfloat16)
        .reshape(token_count, 3 * inner_width)
    )
    dnormed_one = lax.psum(
        jnp.dot(dprojected, w_qkv, preferred_element_type=jnp.float32).astype(jnp.bfloat16),
        "tensor",
    ).astype(jnp.float32)
    norm_one_out, norm_one_pull = jax.vjp(layer_norm, inputs, norm_gains[0])
    dinput_norm, dgain_one = norm_one_pull(dnormed_one)
    tokens_grad = (
        (dresid + dinput_norm).astype(jnp.bfloat16).reshape(local_len, seq_count, model_width)
    )
    gain_grads = lax.psum(jnp.stack([dgain_one, dgain_two]), ("fsdp", "context"))

    def padded(block, used_rows):
        return jnp.pad(block, ((0, 0), (0, pad_rows - used_rows)))

    left_rows = jnp.concatenate(
        [
            padded(dprojected, counts[0]),
            padded(attn_in, counts[1]),
            padded(dmixed, counts[2]),
            padded(hidden, counts[3]),
        ],
        axis=1,
    )
    right_rows = jnp.stack([act_in, dbranch_one, mlp_in, dbranch_two])
    blocks = local_rows * lax.axis_size(("fsdp", "context")) // pad_rows
    col_block = left_rows.reshape(token_count, blocks, pad_rows)
    grad_block = lax.psum_scatter(
        jnp.einsum(
            "nbp,bnd->bpd", col_block, right_rows, preferred_element_type=jnp.float32
        ).reshape(local_rows * lax.axis_size(("fsdp", "context")), model_width),
        ("fsdp", "context"),
        scatter_dimension=0,
        tiled=True,
    )
    momentum = muon_state.reshape(local_rows, model_width)
    muon_next = muon_beta * momentum + (1.0 - muon_beta) * grad_block
    direction = (1.0 - muon_beta) * grad_block + muon_beta * muon_next
    norm_total = lax.psum(jnp.sum(direction * direction), ("context", "tensor"))
    norm_size = jnp.sqrt(norm_total)
    direction_scale = jnp.log(norm_size).reshape(1)
    ortho_local = direction / (norm_size + ortho_eps)
    ortho_block = lax.all_gather(
        ortho_local.astype(jnp.bfloat16), "context", axis=0, tiled=True
    ).astype(ortho_local.dtype)
    for sweep_index in range(ITERS):
        gram_sum = lax.psum(
            contract_exact(ortho_block, ortho_block).astype(jnp.bfloat16), "tensor"
        ).astype(jnp.float32)
        square = jnp.dot(
            gram_sum, gram_sum, precision=precision_highest, preferred_element_type=jnp.float32
        )
        mix_matrix = ns_second * gram_sum + ns_third * square
        ortho_block = ns_first * ortho_block + jnp.dot(
            ortho_block, mix_matrix, precision=precision_highest, preferred_element_type=jnp.float32
        )
    own_rows = lax.dynamic_slice_in_dim(
        ortho_block, lax.axis_index("context") * local_rows, local_rows, 0
    )
    owner_index = lax.axis_index("fsdp")
    spreads = jnp.array(
        [0.2 * math.sqrt(3 * D), 0.2 * math.sqrt(D), 0.2 * math.sqrt(2 * FF), 0.2 * math.sqrt(FF)],
        jnp.float32,
    )
    spread = jnp.sum(jnp.where(jnp.arange(4) == owner_index, spreads, 0.0))
    old_weight = own_block.astype(jnp.float32)
    weight_update = -muon_rate * (spread * own_rows + decay_rate * old_weight)
    adam_first_next = adam_beta * adam_first + (1.0 - adam_beta) * gain_grads
    adam_second_next = adam_beta * adam_second + (1.0 - adam_beta) * gain_grads * gain_grads
    correction = 1.0 - adam_beta**STEP
    gain_update = -adam_rate * (
        adam_first_next / correction / (jnp.sqrt(adam_second_next / correction) + adam_eps)
        + decay_rate * norm_gains
    )
    block_shape = (1, 1, local_rows, model_width)
    return (
        layer_out,
        tokens_grad,
        grad_block.reshape(block_shape),
        muon_next.reshape(block_shape),
        weight_update.reshape(block_shape),
        direction_scale,
        gain_grads,
        adam_first_next,
        adam_second_next,
        gain_update,
    )


MESH_ID = pl.DeviceIdType.MESH
ANY = pl.ANY


def ring_place(index):
    return index + index // 2 - 2 * (index // 3)


def split_units(rows, parts, unit=16):
    units = rows // unit
    sizes = [(units // parts + (1 if i < units % parts else 0)) * unit for i in range(parts)]
    return [s for s in sizes if s]


def ring_chunks(counts, local_rows, which, core, target):
    first = core * local_rows
    rows = min(counts[which], first + local_rows) - first
    if rows <= 0:
        return [[], []]
    halves = split_units(rows, 2)
    if len(halves) == 1:
        halves = halves + [0]
    out, at = [], first
    for half in halves:
        pieces = []
        if half:
            for size in split_units(half, max(1, round(half / target))):
                pieces.append((at, size))
                at += size
        out.append(pieces)
    return out


class Place:
    def __init__(self):
        self.f = lax.axis_index("fsdp")
        self.c = lax.axis_index("context")
        self.t = lax.axis_index("tensor")
        self.pos = ring_place(self.f)
        self.next = ring_place((self.pos + 1) % 4)
        self.prev = ring_place((self.pos + 3) % 4)
        self.outer = jnp.logical_or(self.t == 0, self.t == 3)
        self.inner_mate = jnp.where(self.t == 0, 1, 2)
        self.outer_mate = jnp.where(self.t == 1, 0, 3)

    def ring(self, direction):
        return (self.next if direction == 0 else self.prev, self.c, self.t)

    def partner(self):
        return (self.f, 1 - self.c, self.t)

    def chip_z(self, z):
        return (self.f, self.c, z)

    def hop(self, which, direction):
        home = (0, 1, 3, 2)[which]
        if direction == 0:
            return (self.pos + 4 - home) % 4
        return (home + 4 - self.pos) % 4


def greet(place, ring, partner, line):
    barrier = pltpu.get_barrier_semaphore()

    def signal(device):
        pl.semaphore_signal(barrier, inc=1, device_id=device, device_id_type=MESH_ID)

    count = 0
    if ring:
        signal(place.ring(0))
        signal(place.ring(1))
        count += 2
    if partner:
        signal(place.partner())
        count += 1
    if line:
        @pl.when(place.outer)
        def _():
            signal(place.chip_z(place.inner_mate))
            pl.semaphore_wait(barrier, count + 1)

        @pl.when(jnp.logical_not(place.outer))
        def _():
            signal(place.chip_z(place.outer_mate))
            signal(place.chip_z(3 - place.t))
            pl.semaphore_wait(barrier, count + 2)
    else:
        pl.semaphore_wait(barrier, count)


def remote(src, dst, send, recv, device):
    return pltpu.make_async_remote_copy(
        src_ref=src, dst_ref=dst, send_sem=send, recv_sem=recv, device_id=device, device_id_type=MESH_ID
    )


def run_steps(*tracks):
    total = max(len(track) for track in tracks)
    done = [0] * len(tracks)
    for index in range(total):
        for number, track in enumerate(tracks):
            upto = -(-len(track) * (index + 1) // total)
            while done[number] < upto:
                track[done[number]]()
                done[number] += 1


def gather_plan(counts, local_rows, ks, target=96):
    plan = []
    for core in (0, 1):
        ident = 0
        for which in ks:
            for direction, pieces in enumerate(ring_chunks(counts, local_rows, which, core, target)):
                for order, (row, rows) in enumerate(pieces):
                    plan.append((ident, which, core, direction, order, row, rows))
                    ident += 1
    return plan, max(p[0] for p in plan) + 1


def gather_steps(place, plan, local_rows, base, own_ref, out_ref, sems):
    ss, rs, sp, rp = sems

    def dst(which, row, rows):
        return out_ref.at[pl.ds(base[which] + row, rows)]

    def src(core, row, rows):
        return own_ref.at[pl.ds(row - core * local_rows, rows)]

    def begin():
        for ident, which, core, direction, order, row, rows in plan:
            @pl.when(jnp.logical_and(place.c == core, place.f == which))
            def _():
                remote(src(core, row, rows), dst(which, row, rows), ss.at[ident], rs.at[ident],
                       place.ring(direction)).start()
        for ident, which, core, direction, order, row, rows in plan:
            @pl.when(jnp.logical_and(place.c == core, place.f == which))
            def _():
                remote(src(core, row, rows), dst(which, row, rows), sp.at[ident], rp.at[ident],
                       place.partner()).start()

    ordered = sorted(plan, key=lambda p: (p[4], p[1]))
    last = max(p[4] for p in plan)

    def visit(item, role):
        ident, which, core, direction, order, row, rows = item
        mine = dst(which, row, rows)

        @pl.when(jnp.logical_and(place.c == core, place.hop(which, direction) == role))
        def _():
            remote(mine, mine, ss.at[ident], rs.at[ident], place.ring(direction)).wait_recv()
            if role <= 2:
                remote(mine, mine, ss.at[ident], rs.at[ident], place.ring(direction)).start()
            remote(mine, mine, sp.at[ident], rp.at[ident], place.partner()).start()

    def step(j):
        def run():
            for role in (1, 2, 3):
                for item in ordered:
                    if item[4] == j - (role - 1):
                        visit(item, role)
        return run

    def end():
        for ident, which, core, direction, order, row, rows in plan:
            hop = place.hop(which, direction)
            mine = dst(which, row, rows)

            @pl.when(jnp.logical_and(place.c == core, hop <= 2))
            def _():
                remote(mine, mine, ss.at[ident], rs.at[ident], place.ring(direction)).wait_send()

            @pl.when(place.c == core)
            def _():
                remote(mine, mine, sp.at[ident], rp.at[ident], place.partner()).wait_send()

            @pl.when(place.c == 1 - core)
            def _():
                remote(mine, mine, sp.at[ident], rp.at[ident], place.partner()).wait_recv()

    return begin, [step(j) for j in range(last + 3)], end


def line_steps(place, chunks, own, out, early, mid, low, sems, lag=2, back_lag=3, prep=None, done=None):
    s1, r1, s2, r2, s3, r3 = sems

    def from_end(i, device):
        return remote(own(i), early(i), s1.at[i], r1.at[i], device)

    def across(i):
        return remote(mid(i), low(i), s2.at[i], r2.at[i], place.chip_z(3 - place.t))

    def back(i, device):
        return remote(out(i), out(i), s3.at[i], r3.at[i], device)

    def step(i):
        def run():
            if i < chunks and prep is not None:
                prep(i)

            @pl.when(place.outer)
            def _():
                if i < chunks:
                    from_end(i, place.chip_z(place.inner_mate)).start()
                if 0 <= i - lag - back_lag < chunks:
                    back(i - lag - back_lag, place.chip_z(place.inner_mate)).wait_recv()

            @pl.when(jnp.logical_not(place.outer))
            def _():
                if i < chunks:
                    from_end(i, place.chip_z(place.outer_mate)).wait_recv()
                    pair = own(i)[...].astype(jnp.float32) + early(i)[...].astype(jnp.float32)
                    mid(i)[...] = pair.astype(mid(i).dtype)
                    across(i).start()
                j = i - lag
                if 0 <= j < chunks:
                    across(j).wait_recv()
                    total = mid(j)[...].astype(jnp.float32) + low(j)[...].astype(jnp.float32)
                    out(j)[...] = total.astype(out(j).dtype)
                    back(j, place.chip_z(place.outer_mate)).start()
            if done is not None:
                if 0 <= i - lag - back_lag < chunks:
                    done(i - lag - back_lag)
        return run

    def end():
        @pl.when(place.outer)
        def _():
            for i in range(chunks):
                from_end(i, place.chip_z(place.inner_mate)).wait_send()

        @pl.when(jnp.logical_not(place.outer))
        def _():
            for i in range(chunks):
                across(i).wait_send()
                back(i, place.chip_z(place.outer_mate)).wait_send()

    return [step(i) for i in range(chunks + lag + back_lag)], end


def scatter_steps(place, plan, local_rows, base, part_ref, grad_ref, prx, rrx, tx, sems):
    ss, rs, sp, rp = sems

    def rows_of(ref, which, row, rows):
        return ref.at[pl.ds(base[which] + row, rows)]

    def partner_copy(item):
        ident, which, core, direction, order, row, rows = item
        return remote(rows_of(part_ref, which, row, rows), rows_of(prx, which, row, rows),
                      sp.at[ident], rp.at[ident], place.partner())

    def ring_copy(item):
        ident, which, core, direction, order, row, rows = item
        return remote(rows_of(tx, which, row, rows), rows_of(rrx, which, row, rows),
                      ss.at[ident], rs.at[ident], place.ring(direction))

    ordered = sorted(plan, key=lambda p: (p[4], p[1]))
    last = max(p[4] for p in plan)

    def begin():
        for item in ordered:
            @pl.when(place.c == 1 - item[2])
            def _():
                partner_copy(item).start()

    def visit(item, late):
        ident, which, core, direction, order, row, rows = item
        hop = place.hop(which, direction)
        role = (late + 1) % 4

        @pl.when(jnp.logical_and(place.c == core, hop == role))
        def _():
            partner_copy(item).wait_recv()
            total = (rows_of(part_ref, which, row, rows)[...].astype(jnp.float32)
                     + rows_of(prx, which, row, rows)[...].astype(jnp.float32))
            if role != 1:
                ring_copy(item).wait_recv()
                total = total + rows_of(rrx, which, row, rows)[...].astype(jnp.float32)
            if role == 0:
                grad_ref[pl.ds(row - core * local_rows, rows)] = total
            else:
                rows_of(tx, which, row, rows)[...] = total.astype(tx.dtype)
                ring_copy(item).start()

    def step(j):
        def run():
            for late in range(4):
                for item in ordered:
                    if item[4] == j - late:
                        visit(item, late)
        return run

    def end():
        for item in plan:
            ident, which, core, direction, order, row, rows = item

            @pl.when(place.c == 1 - core)
            def _():
                partner_copy(item).wait_send()

            @pl.when(jnp.logical_and(place.c == core, place.hop(which, direction) != 0))
            def _():
                ring_copy(item).wait_send()

    return begin, [step(j) for j in range(last + 4)], end


VMEM_SPEC = pl.BlockSpec(memory_space=pltpu.VMEM)
ANY_SPEC = pl.BlockSpec(memory_space=pl.ANY)


def dma(count):
    return pltpu.SemaphoreType.DMA((count,))


def comm_call(kernel, outs, ins, in_specs, out_specs, scratch, ident):
    return pl.pallas_call(
        kernel,
        out_shape=outs,
        in_specs=in_specs,
        out_specs=out_specs,
        scratch_shapes=scratch,
        compiler_params=pltpu.CompilerParams(
            collective_id=ident, has_side_effects=True, vmem_limit_bytes=60 * 2**20
        ),
    )(*ins)


def base_rows(counts, ks):
    base, at = {}, 0
    for which in ks:
        base[which] = at
        at += counts[which]
    return base, at


def own_rows_copy(place, counts, local_rows, ks, base, own_ref, out_ref, sem, act):
    for which in ks:
        for core in (0, 1):
            rows = min(counts[which] - core * local_rows, local_rows)
            if rows > 0:
                @pl.when(jnp.logical_and(place.c == core, place.f == which))
                def _():
                    act(pltpu.make_async_copy(
                        own_ref.at[pl.ds(0, rows)],
                        out_ref.at[pl.ds(base[which] + core * local_rows, rows)],
                        sem.at[0],
                    ))


def gather_weights(own_block, counts, ks, ident):
    local_rows, width = own_block.shape
    plan, count = gather_plan(counts, local_rows, ks)
    base, total = base_rows(counts, ks)

    def kernel(own_ref, out_ref, ss, rs, sp, rp, local_sem):
        place = Place()
        greet(place, True, True, False)
        begin, steps, end = gather_steps(place, plan, local_rows, base, own_ref, out_ref, (ss, rs, sp, rp))
        begin()
        own_rows_copy(place, counts, local_rows, ks, base, own_ref, out_ref, local_sem, lambda d: d.start())
        run_steps(steps)
        own_rows_copy(place, counts, local_rows, ks, base, own_ref, out_ref, local_sem, lambda d: d.wait())
        end()

    return comm_call(kernel, jax.ShapeDtypeStruct((total, width), own_block.dtype), (own_block,),
                     [VMEM_SPEC], VMEM_SPEC, [dma(count)] * 4 + [dma(1)], ident), base


def line_sum_and_gather(term, own_block, counts, ks, ident, chunks=8):
    local_rows, width = own_block.shape
    plan, count = gather_plan(counts, local_rows, ks)
    base, total = base_rows(counts, ks)
    rows = term.shape[0] // chunks

    def kernel(term_ref, own_ref, sum_ref, out_ref, early, mid, low, *sems):
        place = Place()
        greet(place, True, True, True)
        cut = lambda ref: lambda i: ref.at[pl.ds(i * rows, rows)]
        line, line_end = line_steps(place, chunks, cut(term_ref), cut(sum_ref), cut(early), cut(mid), cut(low), sems[:6])
        begin, steps, end = gather_steps(place, plan, local_rows, base, own_ref, out_ref, sems[6:10])
        begin()
        own_rows_copy(place, counts, local_rows, ks, base, own_ref, out_ref, sems[10], lambda d: d.start())
        run_steps(line, steps)
        own_rows_copy(place, counts, local_rows, ks, base, own_ref, out_ref, sems[10], lambda d: d.wait())
        line_end()
        end()

    return comm_call(
        kernel,
        (jax.ShapeDtypeStruct(term.shape, term.dtype), jax.ShapeDtypeStruct((total, width), own_block.dtype)),
        (term, own_block), [VMEM_SPEC] * 2, (VMEM_SPEC, VMEM_SPEC),
        [pltpu.VMEM(term.shape, term.dtype)] * 3 + [dma(chunks)] * 6 + [dma(count)] * 4 + [dma(1)], ident,
    ), base


def scatter_grads(part, counts, ks, local_rows, ident, term=None, chunks=8):
    plan, count = gather_plan(counts, local_rows, ks)
    base, total = base_rows(counts, ks)
    width = part.shape[1]
    lined = term is not None
    rows = term.shape[0] // chunks if lined else 0

    def kernel(*refs):
        part_ref, refs = refs[0], refs[1:]
        if lined:
            term_ref, grad_ref, sum_ref, prx, rrx, tx, early, mid, low = refs[:9]
            sems = refs[9:]
        else:
            grad_ref, prx, rrx, tx = refs[:4]
            sems = refs[4:]
        place = Place()
        greet(place, True, True, lined)
        begin, steps, end = scatter_steps(place, plan, local_rows, base, part_ref, grad_ref, prx, rrx, tx, sems[:4])
        begin()
        grad_ref[...] = jnp.zeros_like(grad_ref)
        if lined:
            cut = lambda ref: lambda i: ref.at[pl.ds(i * rows, rows)]
            line, line_end = line_steps(place, chunks, cut(term_ref), cut(sum_ref), cut(early), cut(mid), cut(low), sems[4:10])
            run_steps(line, steps)
            line_end()
        else:
            run_steps(steps)
        end()

    ins = (part, term) if lined else (part,)
    outs = [jax.ShapeDtypeStruct((local_rows, width), jnp.float32)]
    scratch = [pltpu.VMEM(part.shape, part.dtype)] * 3
    sems = [dma(count)] * 4
    if lined:
        outs.append(jax.ShapeDtypeStruct(term.shape, term.dtype))
        scratch += [pltpu.VMEM(term.shape, term.dtype)] * 3
        sems += [dma(chunks)] * 6
    return comm_call(kernel, tuple(outs), ins, [VMEM_SPEC] * len(ins), tuple([VMEM_SPEC] * len(outs)), scratch + sems, ident)


def swap_cores(block, ident):
    def kernel(x_ref, o_ref, send, recv):
        place = Place()
        greet(place, False, True, False)
        copy = remote(x_ref, o_ref, send.at[0], recv.at[0], place.partner())
        copy.start()
        copy.wait()

    return comm_call(kernel, jax.ShapeDtypeStruct(block.shape, block.dtype), (block,), [VMEM_SPEC], VMEM_SPEC,
                     [dma(1), dma(1)], ident)


def plane_sum(block, ident):
    def kernel(x_ref, o_ref, held, send, recv):
        f, c, t = lax.axis_index("fsdp"), lax.axis_index("context"), lax.axis_index("tensor")
        me = f * 2 + c
        barrier = pltpu.get_barrier_semaphore()

        def device(shift):
            other = (me + shift) % 8
            return (other // 2, other % 2, t)

        for shift in range(1, 8):
            pl.semaphore_signal(barrier, inc=1, device_id=device(shift), device_id_type=MESH_ID)
        pl.semaphore_wait(barrier, 7)
        held[pl.ds(me, 1)] = x_ref[...][None]
        copies = []
        for shift in range(1, 8):
            copy = remote(x_ref, held.at[me], send.at[shift], recv.at[shift], device(shift))
            copy.start()
            copies.append(copy)
        for copy in copies:
            copy.wait()
        total = held[0]
        for k in range(1, 8):
            total = total + held[k]
        o_ref[...] = total

    return comm_call(kernel, jax.ShapeDtypeStruct(block.shape, block.dtype), (block,), [VMEM_SPEC], VMEM_SPEC,
                     [pltpu.VMEM((8,) + block.shape, block.dtype), dma(8), dma(8)], ident)


def gram_sum(rows_low, square, ident):
    rows, width = rows_low.shape
    tile = width // 4
    half = tile // 2
    chunks = 10

    def kernel(x_ref, q_ref, g_ref, norm_ref, mine, theirs, prx, tot, other, early, mid, low, *sems):
        place = Place()
        c = place.c
        sp, rp, st, rt = sems[6:10]

        def blocks(core):
            return [(3 * core, 3 * core), (2 * core, 2 * core + 1), (core + 1, core + 1), (core, core + 2), (core, 3 - core)]

        greet(place, False, True, True)

        def at(k):
            return pl.ds(pl.multiple_of(k * tile, tile), tile)

        def gram(i, j):
            return lax.dot_general(x_ref[:, at(i)], x_ref[:, at(j)], (((0,), (0,)), ((), ())),
                                   preferred_element_type=jnp.float32)

        def partner(n):
            sl = pl.ds(n * tile, tile)
            return remote(theirs.at[sl], prx.at[sl], sp.at[n], rp.at[n], place.partner())

        def norm_row(ref):
            return ref.at[pl.ds(5 * tile, 8)]

        for n, (i, j) in enumerate(blocks(1 - c)):
            theirs[pl.ds(n * tile, tile)] = gram(i, j)
            partner(n).start()
        norm_row(theirs)[...] = jnp.broadcast_to(q_ref[0:1, 0:1], (8, tile))
        pn = remote(norm_row(theirs), norm_row(prx), sp.at[5], rp.at[5], place.partner())
        pn.start()

        def span(i):
            return pl.ds(i * half, half) if i < chunks - 1 else pl.ds(i * half, half + 8)

        def cut(ref):
            return lambda i: ref.at[span(i)]

        def prep(i):
            if i % 2 == 0:
                n = i // 2
                sl = pl.ds(n * tile, tile)
                block = gram(*blocks(c)[n])
                partner(n).wait_recv()
                mine[sl] = block + prx[sl]
            if i == chunks - 1:
                pn.wait_recv()
                norm_row(mine)[...] = norm_row(prx)[...] + jnp.broadcast_to(q_ref[0:1, 0:1], (8, tile))

        def share(i):
            return remote(cut(tot)(i), cut(other)(i), st.at[i], rt.at[i], place.partner())

        def place_block(ref, n, core):
            i, j = blocks(core)[n]
            block = ref[pl.ds(n * tile, tile)]
            g_ref[at(i), at(j)] = block
            g_ref[at(j), at(i)] = block.T

        def done(i):
            share(i).start()
            if i % 2 == 1:
                place_block(tot, i // 2, c)
            if i >= 2:
                share(i - 2).wait_recv()
                if (i - 2) % 2 == 1:
                    place_block(other, (i - 2) // 2, 1 - c)

        steps, end = line_steps(place, chunks, cut(mine), cut(tot), cut(early), cut(mid), cut(low), sems[:6],
                                prep=prep, done=done)
        run_steps(steps)
        for i in (chunks - 2, chunks - 1):
            share(i).wait_recv()
        place_block(other, 4, 1 - c)
        norm_ref[...] = jnp.broadcast_to(tot[5 * tile:5 * tile + 8, 0:128], (8, 128))
        end()
        for n in range(5):
            partner(n).wait_send()
        pn.wait_send()
        for i in range(chunks):
            share(i).wait_send()

    packed = pltpu.VMEM((5 * tile + 8, tile), jnp.float32)
    return comm_call(
        kernel,
        (jax.ShapeDtypeStruct((width, width), jnp.float32), jax.ShapeDtypeStruct((8, 128), jnp.float32)),
        (rows_low, square), [VMEM_SPEC] * 2, (VMEM_SPEC, VMEM_SPEC),
        [packed] * 8 + [dma(chunks)] * 6 + [dma(6), dma(6), dma(chunks), dma(chunks)], ident,
    )


class LineSum:
    def __init__(self, place, rows, own, early, mid, low, total, sems):
        self.place, self.rows = place, rows
        self.own, self.early, self.mid, self.low, self.total = own, early, mid, low, total
        self.sems = sems

    def cut(self, ref, i):
        return ref.at[pl.ds(pl.multiple_of(i * self.rows, self.rows), self.rows)]

    def from_end(self, i, mate):
        s1, r1 = self.sems[:2]
        return remote(self.cut(self.own, i), self.cut(self.early, i), s1.at[i], r1.at[i], self.place.chip_z(mate))

    def across(self, i):
        s2, r2 = self.sems[2:4]
        return remote(self.cut(self.mid, i), self.cut(self.low, i), s2.at[i], r2.at[i], self.place.chip_z(3 - self.place.t))

    def back(self, i, mate):
        s3, r3 = self.sems[4:6]
        return remote(self.cut(self.total, i), self.cut(self.total, i), s3.at[i], r3.at[i], self.place.chip_z(mate))

    def send(self, i):
        @pl.when(self.place.outer)
        def _():
            self.from_end(i, self.place.inner_mate).start()

    def pair_up(self, i):
        @pl.when(jnp.logical_not(self.place.outer))
        def _():
            self.from_end(i, self.place.outer_mate).wait_recv()
            pair = self.cut(self.own, i)[...].astype(jnp.float32) + self.cut(self.early, i)[...].astype(jnp.float32)
            self.cut(self.mid, i)[...] = pair.astype(self.mid.dtype)
            self.across(i).start()

    def join(self, i):
        @pl.when(jnp.logical_not(self.place.outer))
        def _():
            self.across(i).wait_recv()
            whole = self.cut(self.mid, i)[...].astype(jnp.float32) + self.cut(self.low, i)[...].astype(jnp.float32)
            self.cut(self.total, i)[...] = whole.astype(self.total.dtype)
            self.back(i, self.place.outer_mate).start()

    def receive(self, i):
        @pl.when(self.place.outer)
        def _():
            self.back(i, self.place.inner_mate).wait_recv()

    def finish(self, pieces):
        @pl.when(self.place.outer)
        def _():
            for i in range(pieces):
                self.from_end(i, self.place.inner_mate).wait_send()

        @pl.when(jnp.logical_not(self.place.outer))
        def _():
            for i in range(pieces):
                self.across(i).wait_send()
                self.back(i, self.place.outer_mate).wait_send()


def nt_dot(left, right):
    return lax.dot_general(left, right, (((1,), (1,)), ((), ())), preferred_element_type=jnp.float32)


def nn_dot(left, right):
    return jnp.dot(left, right, preferred_element_type=jnp.float32)


def tn_dot(left, right):
    return lax.dot_general(left, right, (((0,), (0,)), ((), ())), preferred_element_type=jnp.float32)


def centred(values):
    centre = values - jnp.mean(values, axis=-1, keepdims=True)
    spread = jnp.mean(centre * centre, axis=-1, keepdims=True)
    return centre, lax.rsqrt(spread + norm_eps)


def norm_back(values, gain_row, grads):
    centre, scale = centred(values)
    xhat = centre * scale
    e = grads * gain_row
    moved = scale * (e - jnp.mean(e, axis=-1, keepdims=True) - xhat * jnp.mean(e * xhat, axis=-1, keepdims=True))
    return moved, jnp.sum(grads * xhat, axis=0, keepdims=True)


def layer_both_ways(tokens, out_grad, own_block, norm_gains, cosine, sine, seg_column, seg_row, counts, ident):
    count, width = tokens.shape
    local_rows = own_block.shape[0]
    inner = counts[1]
    ff = counts[3]
    heads = inner // HEAD_DIM
    full = 2 * count
    rows = count // 4
    sub = rows // 2
    stack = heads * rows
    piece = 64
    score_scale = HEAD_DIM ** (-0.5)
    f32, low = jnp.float32, jnp.bfloat16
    first_plan, first_count = gather_plan(counts, local_rows, (0, 1), 64)
    last_plan, last_count = gather_plan(counts, local_rows, (2, 3), 96)
    first_base, first_rows = base_rows(counts, (0, 1))
    last_base, last_rows = base_rows(counts, (2, 3))

    def kernel(tok_ref, og_ref, own_ref, gain_ref, cos_ref, sin_ref, sc_ref, sr_ref,
               act_ref, attn_ref, resid_ref, mlp_ref, hid_ref, dm_ref, b2_ref, dres_ref, db_ref, dproj_ref, t3_ref, dg_ref,
               w1st, wlast, q_ref, kv_ref, kq_ref, p_ref, s_ref, pl_ref, do_ref, dp_ref, ds_ref,
               t1_ref, e1, m1, l1, sum1, t2_ref, e2, m2, l2, sum2, dq_ref, dkv_ref, dkv_tx, dkv_rx, *sems):
        place = Place()
        greet(place, True, True, True)
        begin1, steps1, end1 = gather_steps(place, first_plan, local_rows, first_base, own_ref, w1st, sems[0:4])
        begin2, steps2, end2 = gather_steps(place, last_plan, local_rows, last_base, own_ref, wlast, sems[4:8])
        line1 = LineSum(place, sub, t1_ref, e1, m1, l1, sum1, sems[8:14])
        line2 = LineSum(place, sub, t2_ref, e2, m2, l2, sum2, sems[14:20])
        swap, local_sem = sems[20], sems[21]

        begin1()
        own_rows_copy(place, counts, local_rows, (0, 1), first_base, own_ref, w1st, local_sem, lambda d: d.start())

        def at(i, size=rows):
            return pl.ds(pl.multiple_of(i * size, size), size)

        def norm_one(i, carry):
            centre, scale = centred(tok_ref[at(i)].astype(f32))
            act_ref[at(i)] = (centre * scale * gain_ref[0:1]).astype(low)
            return carry

        lax.fori_loop(0, 4, norm_one, 0)
        dg_ref[...] = jnp.zeros_like(dg_ref)
        run_steps(steps1)
        own_rows_copy(place, counts, local_rows, (0, 1), first_base, own_ref, w1st, local_sem, lambda d: d.wait())
        begin2()
        own_rows_copy(place, counts, local_rows, (2, 3), last_base, own_ref, wlast, local_sem, lambda d: d.start())
        end1()

        lane = lax.broadcasted_iota(jnp.int32, (1, inner), 1)
        front = (lane % HEAD_DIM) < HEAD_DIM // 2

        def half_turn(value):
            return jnp.where(front, pltpu.roll(value, inner - HEAD_DIM // 2, 1), pltpu.roll(value, HEAD_DIM // 2, 1))

        sign = jnp.where(front, -1.0, 1.0).astype(f32)

        def rotated(value, i):
            return value * cos_ref[at(i)] + half_turn(value) * (sin_ref[at(i)] * sign)

        def rotated_back(value, i):
            return value * cos_ref[at(i)] - half_turn(value * sin_ref[at(i)]) * sign

        def project_rows(i, carry):
            value = nt_dot(act_ref[at(i)], w1st[0:3 * inner])
            q_ref[at(i)] = rotated(value[:, 0:inner], i).astype(low)
            kv_ref[at(i), 0:inner] = rotated(value[:, inner:2 * inner], i).astype(low)
            kv_ref[at(i), inner:2 * inner] = value[:, 2 * inner:3 * inner].astype(low)
            return carry

        lax.fori_loop(0, 4, project_rows, 0)
        kv_copy = remote(kv_ref.at[pl.ds(0, count)], kv_ref.at[pl.ds(count, count)], swap.at[0], swap.at[1], place.partner())
        kv_copy.start()
        for step in steps2[:2]:
            step()
        kv_copy.wait()

        def head_mask(h):
            return jnp.logical_and(lane >= h * HEAD_DIM, lane < (h + 1) * HEAD_DIM)

        def stacked(value):
            return jnp.concatenate([jnp.where(head_mask(h), value, jnp.zeros_like(value)) for h in range(heads)], axis=0)

        def unstacked(value):
            total = jnp.where(head_mask(0), value[0:rows], 0.0)
            for h in range(1, heads):
                total = total + jnp.where(head_mask(h), value[h * rows:(h + 1) * rows], 0.0)
            return total

        per = rows // piece

        def attend(i, carry):
            kq_ref[...] = stacked(q_ref[at(i)])
            s_ref[...] = nt_dot(kq_ref[...], kv_ref[:, 0:inner])

            def soft(r, inside):
                seg = sc_ref[pl.ds(pl.multiple_of(i * rows + (r % per) * piece, piece), piece)]
                score = jnp.where(seg == sr_ref[...], s_ref[at(r, piece)] * score_scale, -jnp.inf)
                score = jnp.exp(score - jnp.max(score, axis=-1, keepdims=True))
                prob = score * (1.0 / jnp.sum(score, axis=-1, keepdims=True))
                p_ref[i, at(r, piece)] = prob
                pl_ref[at(r, piece)] = prob.astype(low)
                return inside

            lax.fori_loop(0, stack // piece, soft, 0)
            mixed = unstacked(nn_dot(pl_ref[...], kv_ref[:, inner:2 * inner]))
            keep = (sc_ref[at(i)] > 0).astype(f32)
            attn = (mixed * keep).astype(low)
            attn_ref[at(i)] = attn
            t1_ref[at(i)] = nn_dot(attn, w1st[3 * inner:4 * inner]).astype(low)
            for part in range(2):
                line1.send(2 * i + part)

            @pl.when(i >= 1)
            def _():
                line1.pair_up(2 * i - 2)
                line1.pair_up(2 * i - 1)

            @pl.when(i >= 2)
            def _():
                line1.join(2 * i - 4)
                line1.join(2 * i - 3)
            return carry

        attend(0, 0)
        for step in steps2[2:]:
            step()
        lax.fori_loop(1, 4, attend, 0)
        own_rows_copy(place, counts, local_rows, (2, 3), last_base, own_ref, wlast, local_sem, lambda d: d.wait())
        end2()

        def feed(i, carry):
            for part in range(2):
                line1.receive(2 * i + part)
            resid = tok_ref[at(i)].astype(f32) + sum1[at(i)].astype(f32)
            resid_ref[at(i)] = resid
            centre, scale = centred(resid)
            mlp = (centre * scale * gain_ref[1:2]).astype(low)
            mlp_ref[at(i)] = mlp
            gate = nt_dot(mlp, wlast[0:ff])
            up = nt_dot(mlp, wlast[ff:2 * ff])
            cdf = 0.5 * (1.0 + lax.erf(gate * (0.5 ** 0.5)))
            bell = jnp.exp(gate * gate * -0.5) * (1.0 / math.sqrt(2.0 * math.pi))
            gelu = gate * cdf
            hidden = (gelu * up).astype(low)
            hid_ref[at(i)] = hidden
            dhidden = nt_dot(og_ref[at(i)], wlast[2 * ff:3 * ff])
            dgate = (dhidden * up * (cdf + gate * bell)).astype(low)
            dup = (dhidden * gelu).astype(low)
            dm_ref[0, at(i)] = dgate
            dm_ref[1, at(i)] = dup
            t2_ref[at(i)] = (nn_dot(dgate, wlast[0:ff]) + nn_dot(dup, wlast[ff:2 * ff])).astype(low)
            for part in range(2):
                line2.send(2 * i + part)
            b2_ref[at(i)] = nn_dot(hidden, wlast[2 * ff:3 * ff]).astype(low)

            @pl.when(i == 0)
            def _():
                line1.pair_up(6)
                line1.pair_up(7)

            @pl.when(i <= 1)
            def _():
                line1.join(2 * i + 4)
                line1.join(2 * i + 5)

            @pl.when(i >= 1)
            def _():
                line2.pair_up(2 * i - 2)
                line2.pair_up(2 * i - 1)

            @pl.when(i >= 2)
            def _():
                line2.join(2 * i - 4)
                line2.join(2 * i - 3)
            return carry

        lax.fori_loop(0, 4, feed, 0)
        dkv_ref[...] = jnp.zeros_like(dkv_ref)

        def turn_back(i, carry):
            @pl.when(i == 0)
            def _():
                line2.pair_up(6)
                line2.pair_up(7)
            for part in range(2):
                line2.receive(2 * i + part)
            moved, gain_part = norm_back(resid_ref[at(i)], gain_ref[1:2], sum2[at(i)].astype(f32))
            dg_ref[1:2] = dg_ref[1:2] + gain_part
            dresid = og_ref[at(i)].astype(f32) + moved
            dres_ref[at(i)] = dresid
            dbranch = dresid.astype(low)
            db_ref[at(i)] = dbranch
            keep = (sc_ref[at(i)] > 0).astype(low)
            dattn = nt_dot(dbranch, w1st[3 * inner:4 * inner]).astype(low) * keep
            do_ref[...] = stacked(dattn)
            kq_ref[...] = stacked(q_ref[at(i)])
            dp_ref[...] = nt_dot(do_ref[...], kv_ref[:, inner:2 * inner])

            def soft_back(r, inside):
                prob = p_ref[i, at(r, piece)]
                dprob = dp_ref[at(r, piece)]
                delta = jnp.sum(prob * dprob, axis=-1, keepdims=True)
                ds_ref[at(r, piece)] = (prob * (dprob - delta) * score_scale).astype(low)
                pl_ref[at(r, piece)] = prob.astype(low)
                return inside

            lax.fori_loop(0, stack // piece, soft_back, 0)
            dq_ref[at(i)] = unstacked(nn_dot(ds_ref[...], kv_ref[:, 0:inner]))
            dkv_ref[:, 0:inner] = dkv_ref[:, 0:inner] + tn_dot(ds_ref[...], kq_ref[...])
            dkv_ref[:, inner:2 * inner] = dkv_ref[:, inner:2 * inner] + tn_dot(pl_ref[...], do_ref[...])

            @pl.when(i <= 1)
            def _():
                line2.join(2 * i + 4)
                line2.join(2 * i + 5)
            return carry

        lax.fori_loop(0, 4, turn_back, 0)
        dkv_tx[...] = dkv_ref[count:full].astype(low)
        dkv_copy = remote(dkv_tx, dkv_rx, swap.at[2], swap.at[3], place.partner())
        dkv_copy.start()

        def unproject_query(i, carry):
            dproj_ref[at(i), 0:inner] = rotated_back(dq_ref[at(i)], i).astype(low)
            return carry

        lax.fori_loop(0, 4, unproject_query, 0)
        dkv_copy.wait()

        def unproject(i, carry):
            both = dkv_ref[at(i)] + dkv_rx[at(i)].astype(f32)
            dproj_ref[at(i), inner:2 * inner] = rotated_back(both[:, 0:inner], i).astype(low)
            dproj_ref[at(i), 2 * inner:3 * inner] = both[:, inner:2 * inner].astype(low)
            t3_ref[at(i)] = nn_dot(dproj_ref[at(i)], w1st[0:3 * inner]).astype(low)
            return carry

        lax.fori_loop(0, 4, unproject, 0)
        line1.finish(8)
        line2.finish(8)

    def shape(*dims, dtype=low):
        return jax.ShapeDtypeStruct(dims, dtype)

    outs = (
        shape(count, width), shape(count, inner), shape(count, width, dtype=f32), shape(count, width), shape(count, ff),
        shape(2, count, ff), shape(count, width), shape(count, width, dtype=f32), shape(count, width),
        shape(count, 3 * inner), shape(count, width), shape(8, width, dtype=f32),
    )
    line = pltpu.VMEM((count, width), low)
    scratch = [
        pltpu.VMEM((first_rows, width), low), pltpu.VMEM((last_rows, width), low), pltpu.VMEM((count, inner), low),
        pltpu.VMEM((full, 2 * inner), low), pltpu.VMEM((stack, inner), low), pltpu.VMEM((4, stack, full), f32),
        pltpu.VMEM((stack, full), f32), pltpu.VMEM((stack, full), low), pltpu.VMEM((stack, inner), low),
        pltpu.VMEM((stack, full), f32), pltpu.VMEM((stack, full), low),
    ]
    scratch += [line] * 10
    scratch += [
        pltpu.VMEM((count, inner), f32), pltpu.VMEM((full, 2 * inner), f32),
        pltpu.VMEM((count, 2 * inner), low), pltpu.VMEM((count, 2 * inner), low),
    ]
    scratch += [dma(first_count)] * 4 + [dma(last_count)] * 4 + [dma(8)] * 12 + [dma(4), dma(1)]
    ins = (tokens, out_grad, own_block, norm_gains, cosine, sine, seg_column, seg_row)
    return pl.pallas_call(
        kernel,
        out_shape=outs,
        in_specs=[VMEM_SPEC] * len(ins),
        out_specs=(VMEM_SPEC,) * len(outs),
        scratch_shapes=scratch,
        compiler_params=pltpu.CompilerParams(
            collective_id=ident, has_side_effects=True, vmem_limit_bytes=67043328
        ),
    )(*ins)


def halves(value):
    high = value.astype(jnp.bfloat16)
    return high, (value - high.astype(jnp.float32)).astype(jnp.bfloat16)


def gaps(fixed, moved):
    return [(fixed * (index + 1)) // moved for index in range(moved)]


def iterate(gram, norm, direction_low, own_block, branch_term, resid, dgains, norm_gains, adam_first, adam_second, ident):
    rows, width = direction_low.shape
    tile = 256
    parts = width // tile
    tokens = branch_term.shape[0]
    chunks = 8
    step_rows = tokens // chunks
    aa = ns_first * ns_first
    ab = 2.0 * ns_first * ns_second
    bbac = ns_second * ns_second + 2.0 * ns_first * ns_third
    bc = 2.0 * ns_second * ns_third
    cc = ns_third * ns_third
    correction = 1.0 - adam_beta**STEP

    def kernel(g_ref, n_ref, d_ref, w_ref, t_ref, r_ref, dg_ref, gain_ref, af_ref, as_ref,
               u_ref, lo_ref, gg_ref, afn_ref, asn_ref, gu_ref,
               p_ref, ph, pl_, hh, hl, uh, ul, mx, x_ref, early, mid, low, total, held, *sems):
        place = Place()
        s1, r1, s2, r2, s3, r3, sg, rg = sems
        me = place.f * 2 + place.c
        barrier = pltpu.get_barrier_semaphore()

        def plane(shift):
            other = (me + shift) % 8
            return (other // 2, other % 2, place.t)

        for shift in range(1, 8):
            pl.semaphore_signal(barrier, inc=1, device_id=plane(shift), device_id_type=MESH_ID)

        @pl.when(place.outer)
        def _():
            pl.semaphore_signal(barrier, inc=1, device_id=place.chip_z(place.inner_mate), device_id_type=MESH_ID)
            pl.semaphore_wait(barrier, 8)

        @pl.when(jnp.logical_not(place.outer))
        def _():
            pl.semaphore_signal(barrier, inc=1, device_id=place.chip_z(place.outer_mate), device_id_type=MESH_ID)
            pl.semaphore_signal(barrier, inc=1, device_id=place.chip_z(3 - place.t), device_id_type=MESH_ID)
            pl.semaphore_wait(barrier, 9)

        def cut(ref, i):
            if isinstance(i, int):
                return ref.at[pl.ds(i * step_rows, step_rows)]
            return ref.at[pl.ds(pl.multiple_of(i * step_rows, step_rows), step_rows)]

        def from_end(i, device):
            return remote(cut(t_ref, i), cut(early, i), s1.at[i], r1.at[i], device)

        def across(i):
            return remote(cut(mid, i), cut(low, i), s2.at[i], r2.at[i], place.chip_z(3 - place.t))

        def back(i, device):
            return remote(cut(total, i), cut(total, i), s3.at[i], r3.at[i], device)

        held[pl.ds(me, 1)] = dg_ref[...][None]
        for shift in range(1, 8):
            remote(dg_ref, held.at[me], sg.at[shift], rg.at[shift], plane(shift)).start()

        @pl.when(place.outer)
        def _():
            for i in range(chunks):
                from_end(i, place.chip_z(place.inner_mate)).start()

        def pair_up(i):
            @pl.when(jnp.logical_not(place.outer))
            def _():
                from_end(i, place.chip_z(place.outer_mate)).wait_recv()
                pair = cut(t_ref, i)[...].astype(jnp.float32) + cut(early, i)[...].astype(jnp.float32)
                cut(mid, i)[...] = pair.astype(mid.dtype)
                across(i).start()

        def join(i):
            @pl.when(jnp.logical_not(place.outer))
            def _():
                across(i).wait_recv()
                whole = cut(mid, i)[...].astype(jnp.float32) + cut(low, i)[...].astype(jnp.float32)
                cut(total, i)[...] = whole.astype(total.dtype)
                back(i, place.chip_z(place.outer_mate)).start()

        norm_size = jnp.sqrt(n_ref[0:1, 0:1])
        inverse = 1.0 / (norm_size + ortho_eps)
        scale = inverse * inverse

        for k in range(parts):
            sl = pl.ds(k * tile, tile)
            value = g_ref[sl] * scale
            p_ref[sl] = value
            high, rest = halves(value)
            ph[sl] = high
            pl_[sl] = rest
        x_ref[...] = d_ref[...].astype(jnp.float32) * inverse

        def product(lh, ll, rh, rl, k):
            sl, cols = pl.ds(k * tile, tile), pl.ds(k * tile, width - k * tile)

            def dot(left, right):
                return jnp.dot(left[sl], right[:, cols], preferred_element_type=jnp.float32)

            return dot(lh, rh) + dot(ll, rh) + dot(lh, rl)

        def spread_out(value, high_ref, low_ref, k):
            sl, cols = pl.ds(k * tile, tile), pl.ds(k * tile, width - k * tile)
            high, rest = halves(value)
            high_ref[sl, cols] = high
            low_ref[sl, cols] = rest
            for j in range(k + 1, parts):
                at = (j - k) * tile
                high_ref[pl.ds(j * tile, tile), sl] = high[:, at:at + tile].T
                low_ref[pl.ds(j * tile, tile), sl] = rest[:, at:at + tile].T

        def squares():
            for k in range(parts):
                sl, cols = pl.ds(k * tile, tile), pl.ds(k * tile, width - k * tile)
                value = product(ph, pl_, ph, pl_, k)
                spread_out(value, hh, hl, k)
                mix = (ns_second * p_ref[sl, cols] + ns_third * value).astype(mx.dtype)
                mx[sl, cols] = mix
                for j in range(k + 1, parts):
                    at = (j - k) * tile
                    mx[pl.ds(j * tile, tile), sl] = mix[:, at:at + tile].T

        def rotate_rows():
            for at, size in ((0, 336), (336, 320)):
                sl = pl.ds(at, size)
                old = x_ref[sl]
                x_ref[sl] = ns_first * old + jnp.dot(old.astype(jnp.bfloat16), mx[...], preferred_element_type=jnp.float32)

        def body(sweep, carry):
            pair_up(2 * sweep)
            squares()
            pair_up(2 * sweep + 1)

            @pl.when(sweep >= 1)
            def _():
                join(2 * sweep - 2)
            rotate_rows()
            for k in range(parts):
                sl, cols = pl.ds(k * tile, tile), pl.ds(k * tile, width - k * tile)
                cube = product(ph, pl_, hh, hl, k)
                square = hh[sl, cols].astype(jnp.float32) + hl[sl, cols].astype(jnp.float32)
                spread_out(bc * square + cc * cube, uh, ul, k)
                p_ref[sl, cols] = aa * p_ref[sl, cols] + ab * square + bbac * cube

            @pl.when(sweep >= 1)
            def _():
                join(2 * sweep - 1)
            for k in range(parts):
                sl, cols = pl.ds(k * tile, tile), pl.ds(k * tile, width - k * tile)
                value = p_ref[sl, cols] + product(hh, hl, uh, ul, k)
                p_ref[sl, cols] = value
                spread_out(value, ph, pl_, k)
            return carry

        lax.fori_loop(0, ITERS - 1, body, 0)
        join(chunks - 2)
        join(chunks - 1)
        squares()
        rotate_rows()
        spread = jnp.where(place.f == 0, 0.2 * math.sqrt(3 * D), jnp.where(place.f == 1, 0.2 * math.sqrt(D), jnp.where(
            place.f == 2, 0.2 * math.sqrt(2 * FF), 0.2 * math.sqrt(FF)))).astype(jnp.float32)
        u_ref[...] = -muon_rate * (spread * x_ref[...] + decay_rate * w_ref[...].astype(jnp.float32))

        for shift in range(1, 8):
            remote(dg_ref, held.at[me], sg.at[shift], rg.at[shift], plane(shift)).wait()
        grads = held[0]
        for k in range(1, 8):
            grads = grads + held[k]
        gg_ref[...] = grads
        first = adam_beta * af_ref[...] + (1.0 - adam_beta) * grads
        second = adam_beta * as_ref[...] + (1.0 - adam_beta) * grads * grads
        afn_ref[...] = first
        asn_ref[...] = second
        gu_ref[...] = -adam_rate * (
            first / correction / (jnp.sqrt(second / correction) + adam_eps) + decay_rate * gain_ref[...]
        )

        @pl.when(place.outer)
        def _():
            for i in range(chunks):
                back(i, place.chip_z(place.inner_mate)).wait_recv()
                from_end(i, place.chip_z(place.inner_mate)).wait_send()
        lo_ref[...] = (r_ref[...] + total[...].astype(jnp.float32)).astype(lo_ref.dtype)

        @pl.when(jnp.logical_not(place.outer))
        def _():
            for i in range(chunks):
                across(i).wait_send()
                back(i, place.chip_z(place.outer_mate)).wait_send()

    f32, low16 = jnp.float32, jnp.bfloat16
    small = jax.ShapeDtypeStruct(dgains.shape, f32)
    outs = (jax.ShapeDtypeStruct((rows, width), f32), jax.ShapeDtypeStruct((tokens, width), low16), small, small, small, small)
    full = pltpu.VMEM((width, width), low16)
    line = pltpu.VMEM((tokens, width), low16)
    scratch = [pltpu.VMEM((width, width), f32)] + [full] * 7 + [pltpu.VMEM((rows, width), f32)] + [line] * 4
    scratch += [pltpu.VMEM((8,) + dgains.shape, f32)] + [dma(chunks)] * 6 + [dma(8)] * 2
    ins = (gram, norm, direction_low, own_block, branch_term, resid, dgains, norm_gains, adam_first, adam_second)
    return comm_call(kernel, outs, ins, [VMEM_SPEC] * len(ins), (VMEM_SPEC,) * len(outs), scratch, ident)


def per_device_block(tokens, out_grad, weight_stack, muon_state, norm_gains, adam_first, adam_second, segment_ids,
                     position_ids):
    token_count, _, model_width = tokens.shape
    groups, contexts = 4, 2
    full_len = token_count * contexts
    local_rows = weight_stack.shape[2]
    heads_dev = HEADS // groups
    ff_dev = FF // groups
    inner_width = heads_dev * HEAD_DIM
    counts = (3 * inner_width, inner_width, 2 * ff_dev, ff_dev)
    score_scale = HEAD_DIM ** (-0.5)
    own_block = weight_stack.reshape(local_rows, model_width)
    low = jnp.bfloat16
    context = lax.axis_index("context")

    inputs = tokens.astype(jnp.float32).reshape(token_count, model_width)
    cosine, sine_table = rope_tables(position_ids.reshape(token_count), HEAD_DIM)
    segments = segment_ids.reshape(full_len)
    seg_query = lax.dynamic_slice_in_dim(segments, context * token_count, token_count, 0)
    seg_other = lax.dynamic_slice_in_dim(segments, (1 - context) * token_count, token_count, 0)
    (act_in, attn_in, resid, mlp_in, hidden, dmixed, branch_two_term, dresid, dbranch_one, dprojected, dnormed_one_term,
     dgain_rows) = layer_both_ways(
        tokens.reshape(token_count, model_width), out_grad.reshape(token_count, model_width), own_block, norm_gains,
        jnp.tile(cosine, (1, heads_dev)), jnp.tile(sine_table, (1, heads_dev)),
        seg_query.reshape(token_count, 1), jnp.concatenate([seg_query, seg_other]).reshape(1, full_len), counts, 0,
    )
    dgain_two = dgain_rows[1]
    out_low = out_grad.reshape(token_count, model_width)

    def grad_term(left, right):
        return lax.dot_general(left, right, (((0,), (0,)), ((), ())), preferred_element_type=jnp.float32).astype(low)

    terms = jnp.concatenate(
        [
            grad_term(dprojected, act_in), grad_term(attn_in, dbranch_one), grad_term(dmixed[0], mlp_in),
            grad_term(dmixed[1], mlp_in), grad_term(hidden, out_low),
        ],
        axis=0,
    )
    grad_block, dnormed_one = scatter_grads(terms, counts, (0, 1, 2, 3), local_rows, 5, dnormed_one_term)
    _, norm_one_pull = jax.vjp(layer_norm, inputs, norm_gains[0])
    dinput_norm, dgain_one = norm_one_pull(dnormed_one.astype(jnp.float32))
    tokens_grad = (dresid + dinput_norm).astype(low).reshape(tokens.shape)

    momentum = muon_state.reshape(local_rows, model_width)
    muon_next = muon_beta * momentum + (1.0 - muon_beta) * grad_block
    direction = (1.0 - muon_beta) * grad_block + muon_beta * muon_next
    direction_low = direction.astype(low)
    square = jnp.sum(direction * direction).reshape(1, 1)
    gram, norm_total = gram_sum(direction_low, jnp.broadcast_to(square, (8, 128)), 6)
    direction_scale = jnp.log(jnp.sqrt(norm_total[0, 0])).reshape(1)
    weight_update, layer_out, gain_grads, adam_first_next, adam_second_next, gain_update = iterate(
        gram, norm_total, direction_low, own_block, branch_two_term, resid, jnp.stack([dgain_one, dgain_two]),
        norm_gains, adam_first, adam_second, 7,
    )
    layer_out = layer_out.reshape(tokens.shape)
    block_shape = (1, 1, local_rows, model_width)
    return (
        layer_out,
        tokens_grad,
        grad_block.reshape(block_shape),
        muon_next.reshape(block_shape),
        weight_update.reshape(block_shape),
        direction_scale,
        gain_grads,
        adam_first_next,
        adam_second_next,
        gain_update,
    )


def solution(mesh):
    sizes = dict(mesh.shape)
    block = (sizes["fsdp"], sizes["context"], sizes["tensor"]) == (4, 2, 4)
    return jax.shard_map(
        per_device_block if block else per_device,
        mesh=mesh,
        in_specs=(
            P("context", "fsdp", None),
            P("context", "fsdp", None),
            P("fsdp", "tensor", "context", None),
            P("fsdp", "tensor", "context", None),
            P(),
            P(),
            P(),
            P(None, "fsdp"),
            P("context", "fsdp"),
        ),
        out_specs=(
            P("context", "fsdp", None),
            P("context", "fsdp", None),
            P("fsdp", "tensor", "context", None),
            P("fsdp", "tensor", "context", None),
            P("fsdp", "tensor", "context", None),
            P("fsdp"),
            P(),
            P(),
            P(),
            P(),
        ),
        check_vma=False,
    )
```

```python
import math

import jax
import jax.numpy as jnp
from jax import lax
from jax.experimental import pallas as pl
from jax.experimental.pallas import tpu as pltpu
from jax.sharding import PartitionSpec as P

D = 1024
HEADS = 16
HEAD_DIM = 64
FF = 2624
ITERS = 5
STEP = 8


rope_base = 160000.0
norm_eps = 1e-05
ns_first = 3.4445
ns_second = -4.775
ns_third = 2.0315
muon_beta = 0.5
muon_rate = 0.15
decay_rate = 0.1
adam_beta = 0.5
adam_rate = 0.05
ortho_eps = 1e-07
adam_eps = 1e-08
precision_highest = lax.Precision.HIGHEST


def layer_norm(values, gain_row):
    centre = values - jnp.mean(values, axis=-1, keepdims=True)
    spread = jnp.mean(centre * centre, axis=-1, keepdims=True)
    return centre * lax.rsqrt(spread + norm_eps) * gain_row


def rope_tables(positions, head_width):
    half_width = head_width // 2
    freqs = rope_base ** (-(jnp.arange(half_width, dtype=jnp.float32) * 2.0 / head_width))
    angle = positions.astype(jnp.float32)[..., None] * freqs
    angle = jnp.concatenate([angle, angle], axis=-1)
    return (jnp.cos(angle), jnp.sin(angle))


def rotate(values, cosine, sine_table):
    half_width = values.shape[-1] // 2
    turned = jnp.concatenate([-values[..., half_width:], values[..., :half_width]], axis=-1)
    return values * cosine + turned * sine_table


def rotate_back(grads_in, cosine, sine_table):
    half_width = grads_in.shape[-1] // 2
    scaled = grads_in * sine_table
    turned = jnp.concatenate([scaled[..., half_width:], -scaled[..., :half_width]], axis=-1)
    return grads_in * cosine + turned


def project(left_rows, right_rows):
    return lax.dot_general(
        left_rows, right_rows, (((1,), (1,)), ((), ())), preferred_element_type=jnp.float32
    )


def contract_exact(left_rows, right_rows):
    return lax.dot_general(
        left_rows,
        right_rows,
        (((0,), (0,)), ((), ())),
        precision=precision_highest,
        preferred_element_type=jnp.float32,
    )


def geglu_gate(gate_part, up_part):
    return jax.nn.gelu(gate_part, approximate=False) * up_part


def per_device(
    tokens,
    out_grad,
    weight_stack,
    muon_state,
    norm_gains,
    adam_first,
    adam_second,
    segment_ids,
    position_ids,
):
    local_len, seq_count, model_width = tokens.shape
    token_count = local_len * seq_count
    groups = lax.axis_size("tensor")
    contexts = lax.axis_size("context")
    full_len = local_len * contexts
    local_rows = weight_stack.shape[2]
    pad_rows = local_rows * contexts
    heads_dev = HEADS // groups
    ff_dev = FF // groups
    inner_width = heads_dev * HEAD_DIM
    counts = (3 * inner_width, inner_width, 2 * ff_dev, ff_dev)
    score_scale = HEAD_DIM ** (-0.5)
    own_block = weight_stack.reshape(local_rows, model_width)
    gathered = lax.all_gather(own_block, ("fsdp", "context"), axis=0, tiled=True).reshape(
        4, pad_rows, model_width
    )
    w_qkv = gathered[0, : counts[0]]
    w_out = gathered[1, : counts[1]]
    w_in = gathered[2, : counts[2]]
    w_down = gathered[3, : counts[3]]
    inputs = tokens.astype(jnp.float32).reshape(token_count, model_width)
    act_in = layer_norm(inputs, norm_gains[0]).astype(jnp.bfloat16)
    projected = project(act_in, w_qkv).reshape(local_len, seq_count, 3, heads_dev, HEAD_DIM)
    cosine, sine_table = rope_tables(position_ids, HEAD_DIM)
    rot_cos = cosine[:, :, None, :]
    rot_sin = sine_table[:, :, None, :]
    query_matrix = rotate(projected[:, :, 0], rot_cos, rot_sin).astype(jnp.bfloat16)
    key_matrix_rows = rotate(projected[:, :, 1], rot_cos, rot_sin).astype(jnp.bfloat16)
    value_matrix_rows = projected[:, :, 2].astype(jnp.bfloat16)
    key_value = jnp.concatenate(
        [
            key_matrix_rows.reshape(local_len, seq_count, inner_width),
            value_matrix_rows.reshape(local_len, seq_count, inner_width),
        ],
        axis=-1,
    )
    key_value_all = lax.all_gather(key_value, "context", axis=0, tiled=True)
    keys_all = key_value_all[..., :inner_width].reshape(full_len, seq_count, heads_dev, HEAD_DIM)
    values_all = key_value_all[..., inner_width:].reshape(full_len, seq_count, heads_dev, HEAD_DIM)
    offset = lax.axis_index("context") * local_len
    seg_query = lax.dynamic_slice_in_dim(segment_ids, offset, local_len, 0)
    same_doc = seg_query.T[:, :, None] == segment_ids.T[:, None, :]
    keep_mask = (seg_query > 0).astype(jnp.float32)
    unscaled_score = jnp.einsum(
        "lshd,mshd->shlm", query_matrix, keys_all, preferred_element_type=jnp.float32
    )
    scores = jnp.where(same_doc[:, None], unscaled_score * score_scale, -jnp.inf)
    row_max = jnp.max(scores, axis=-1, keepdims=True)
    log_total = row_max + jnp.log(jnp.sum(jnp.exp(scores - row_max), axis=-1, keepdims=True))
    probs_low = jnp.exp(scores - log_total).astype(jnp.bfloat16)
    attended = jnp.einsum(
        "shlm,mshd->lshd", probs_low, values_all, preferred_element_type=jnp.float32
    )
    attn_in = (
        (attended * keep_mask[:, :, None, None])
        .astype(jnp.bfloat16)
        .reshape(token_count, inner_width)
    )
    branch_one = lax.psum(
        jnp.dot(attn_in, w_out, preferred_element_type=jnp.float32).astype(jnp.bfloat16), "tensor"
    ).astype(jnp.float32)
    resid = inputs + branch_one
    mlp_in = layer_norm(resid, norm_gains[1]).astype(jnp.bfloat16)
    mixed_rows = project(mlp_in, w_in)
    hidden_full, geglu_pull = jax.vjp(geglu_gate, mixed_rows[:, :ff_dev], mixed_rows[:, ff_dev:])
    hidden = hidden_full.astype(jnp.bfloat16)
    branch_two = lax.psum(
        jnp.dot(hidden, w_down, preferred_element_type=jnp.float32).astype(jnp.bfloat16), "tensor"
    ).astype(jnp.float32)
    layer_out = (resid + branch_two).astype(jnp.bfloat16).reshape(local_len, seq_count, model_width)
    out_cot = out_grad.astype(jnp.float32).reshape(token_count, model_width)
    dbranch_two = out_cot.astype(jnp.bfloat16)
    dhidden = project(dbranch_two, w_down)
    dgate, dup_part = geglu_pull(dhidden)
    dmixed = jnp.concatenate([dgate, dup_part], axis=1).astype(jnp.bfloat16)
    dnormed_two = lax.psum(
        jnp.dot(dmixed, w_in, preferred_element_type=jnp.float32).astype(jnp.bfloat16), "tensor"
    ).astype(jnp.float32)
    norm_two_out, norm_two_pull = jax.vjp(layer_norm, resid, norm_gains[1])
    dresid_norm, dgain_two = norm_two_pull(dnormed_two)
    dresid = out_cot + dresid_norm
    dbranch_one = dresid.astype(jnp.bfloat16)
    keep_low = keep_mask.reshape(token_count, 1).astype(jnp.bfloat16)
    dattended = project(dbranch_one, w_out).astype(jnp.bfloat16) * keep_low
    dattn = dattended.reshape(local_len, seq_count, heads_dev, HEAD_DIM)
    dquery_list = []
    dkey_list = []
    dvalue_list = []
    for head_index in range(heads_dev):
        query_head = query_matrix[:, :, head_index]
        key_head = keys_all[:, :, head_index]
        value_head = values_all[:, :, head_index]
        dout_head = dattn[:, :, head_index]
        raw_head = jnp.einsum(
            "lsd,msd->slm", query_head, key_head, preferred_element_type=jnp.float32
        )
        prob_head = jnp.exp(
            jnp.where(same_doc, raw_head * score_scale, -jnp.inf) - log_total[:, head_index]
        )
        dprob = jnp.einsum(
            "lsd,msd->slm", dout_head, value_head, preferred_element_type=jnp.float32
        )
        delta = jnp.sum(prob_head * dprob, axis=-1, keepdims=True)
        dscore = (prob_head * (dprob - delta) * score_scale).astype(jnp.bfloat16)
        dquery_list.append(
            jnp.einsum("slm,msd->lsd", dscore, key_head, preferred_element_type=jnp.float32)
        )
        dkey_head = jnp.einsum(
            "slm,lsd->msd", dscore, query_head, preferred_element_type=jnp.float32
        )
        dvalue_head = jnp.einsum(
            "slm,lsd->msd",
            prob_head.astype(jnp.bfloat16),
            dout_head,
            preferred_element_type=jnp.float32,
        )
        summed = lax.psum_scatter(
            jnp.concatenate([dkey_head, dvalue_head], axis=-1).astype(jnp.bfloat16),
            "context",
            scatter_dimension=0,
            tiled=True,
        ).astype(jnp.float32)
        dkey_list.append(summed[..., :HEAD_DIM])
        dvalue_list.append(summed[..., HEAD_DIM:])
    dqueries = jnp.stack(dquery_list, axis=2)
    dkeys = jnp.stack(dkey_list, axis=2)
    dvalues = jnp.stack(dvalue_list, axis=2)
    dprojected = (
        jnp.stack(
            [
                rotate_back(dqueries, rot_cos, rot_sin),
                rotate_back(dkeys, rot_cos, rot_sin),
                dvalues,
            ],
            axis=2,
        )
        .astype(jnp.bfloat16)
        .reshape(token_count, 3 * inner_width)
    )
    dnormed_one = lax.psum(
        jnp.dot(dprojected, w_qkv, preferred_element_type=jnp.float32).astype(jnp.bfloat16),
        "tensor",
    ).astype(jnp.float32)
    norm_one_out, norm_one_pull = jax.vjp(layer_norm, inputs, norm_gains[0])
    dinput_norm, dgain_one = norm_one_pull(dnormed_one)
    tokens_grad = (
        (dresid + dinput_norm).astype(jnp.bfloat16).reshape(local_len, seq_count, model_width)
    )
    gain_grads = lax.psum(jnp.stack([dgain_one, dgain_two]), ("fsdp", "context"))

    def padded(block, used_rows):
        return jnp.pad(block, ((0, 0), (0, pad_rows - used_rows)))

    left_rows = jnp.concatenate(
        [
            padded(dprojected, counts[0]),
            padded(attn_in, counts[1]),
            padded(dmixed, counts[2]),
            padded(hidden, counts[3]),
        ],
        axis=1,
    )
    right_rows = jnp.stack([act_in, dbranch_one, mlp_in, dbranch_two])
    blocks = local_rows * lax.axis_size(("fsdp", "context")) // pad_rows
    col_block = left_rows.reshape(token_count, blocks, pad_rows)
    grad_block = lax.psum_scatter(
        jnp.einsum(
            "nbp,bnd->bpd", col_block, right_rows, preferred_element_type=jnp.float32
        ).reshape(local_rows * lax.axis_size(("fsdp", "context")), model_width),
        ("fsdp", "context"),
        scatter_dimension=0,
        tiled=True,
    )
    momentum = muon_state.reshape(local_rows, model_width)
    muon_next = muon_beta * momentum + (1.0 - muon_beta) * grad_block
    direction = (1.0 - muon_beta) * grad_block + muon_beta * muon_next
    norm_total = lax.psum(jnp.sum(direction * direction), ("context", "tensor"))
    norm_size = jnp.sqrt(norm_total)
    direction_scale = jnp.log(norm_size).reshape(1)
    ortho_local = direction / (norm_size + ortho_eps)
    ortho_block = lax.all_gather(
        ortho_local.astype(jnp.bfloat16), "context", axis=0, tiled=True
    ).astype(ortho_local.dtype)
    for sweep_index in range(ITERS):
        gram_sum = lax.psum(
            contract_exact(ortho_block, ortho_block).astype(jnp.bfloat16), "tensor"
        ).astype(jnp.float32)
        square = jnp.dot(
            gram_sum, gram_sum, precision=precision_highest, preferred_element_type=jnp.float32
        )
        mix_matrix = ns_second * gram_sum + ns_third * square
        ortho_block = ns_first * ortho_block + jnp.dot(
            ortho_block, mix_matrix, precision=precision_highest, preferred_element_type=jnp.float32
        )
    own_rows = lax.dynamic_slice_in_dim(
        ortho_block, lax.axis_index("context") * local_rows, local_rows, 0
    )
    owner_index = lax.axis_index("fsdp")
    spreads = jnp.array(
        [0.2 * math.sqrt(3 * D), 0.2 * math.sqrt(D), 0.2 * math.sqrt(2 * FF), 0.2 * math.sqrt(FF)],
        jnp.float32,
    )
    spread = jnp.sum(jnp.where(jnp.arange(4) == owner_index, spreads, 0.0))
    old_weight = own_block.astype(jnp.float32)
    weight_update = -muon_rate * (spread * own_rows + decay_rate * old_weight)
    adam_first_next = adam_beta * adam_first + (1.0 - adam_beta) * gain_grads
    adam_second_next = adam_beta * adam_second + (1.0 - adam_beta) * gain_grads * gain_grads
    correction = 1.0 - adam_beta**STEP
    gain_update = -adam_rate * (
        adam_first_next / correction / (jnp.sqrt(adam_second_next / correction) + adam_eps)
        + decay_rate * norm_gains
    )
    block_shape = (1, 1, local_rows, model_width)
    return (
        layer_out,
        tokens_grad,
        grad_block.reshape(block_shape),
        muon_next.reshape(block_shape),
        weight_update.reshape(block_shape),
        direction_scale,
        gain_grads,
        adam_first_next,
        adam_second_next,
        gain_update,
    )


MESH_ID = pl.DeviceIdType.MESH
ANY = pl.ANY


def ring_place(index):
    return index + index // 2 - 2 * (index // 3)


def split_units(rows, parts, unit=16):
    units = rows // unit
    sizes = [(units // parts + (1 if i < units % parts else 0)) * unit for i in range(parts)]
    return [s for s in sizes if s]


def ring_chunks(counts, local_rows, which, core, target):
    first = core * local_rows
    rows = min(counts[which], first + local_rows) - first
    if rows <= 0:
        return [[], []]
    halves = split_units(rows, 2)
    if len(halves) == 1:
        halves = halves + [0]
    out, at = [], first
    for half in halves:
        pieces = []
        if half:
            for size in split_units(half, max(1, round(half / target))):
                pieces.append((at, size))
                at += size
        out.append(pieces)
    return out


class Place:
    def __init__(self):
        self.f = lax.axis_index("fsdp")
        self.c = lax.axis_index("context")
        self.t = lax.axis_index("tensor")
        self.pos = ring_place(self.f)
        self.next = ring_place((self.pos + 1) % 4)
        self.prev = ring_place((self.pos + 3) % 4)
        homes = (0, 1, 3, 2)
        self.hops = [[(self.pos + 4 - home) % 4, (home + 4 - self.pos) % 4] for home in homes]
        self.outer = jnp.logical_or(self.t == 0, self.t == 3)
        self.inner_mate = jnp.where(self.t == 0, 1, 2)
        self.outer_mate = jnp.where(self.t == 1, 0, 3)

    def ring(self, direction):
        return (self.next if direction == 0 else self.prev, self.c, self.t)

    def partner(self):
        return (self.f, 1 - self.c, self.t)

    def chip_z(self, z):
        return (self.f, self.c, z)

    def hop(self, which, direction):
        return self.hops[which][direction]


def greet(place, ring, partner, line):
    barrier = pltpu.get_barrier_semaphore()

    def signal(device):
        pl.semaphore_signal(barrier, inc=1, device_id=device, device_id_type=MESH_ID)

    count = 0
    if ring:
        signal(place.ring(0))
        signal(place.ring(1))
        count += 2
    if partner:
        signal(place.partner())
        count += 1
    if line:
        @pl.when(place.outer)
        def _():
            signal(place.chip_z(place.inner_mate))
            pl.semaphore_wait(barrier, count + 1)

        @pl.when(jnp.logical_not(place.outer))
        def _():
            signal(place.chip_z(place.outer_mate))
            signal(place.chip_z(3 - place.t))
            pl.semaphore_wait(barrier, count + 2)
    else:
        pl.semaphore_wait(barrier, count)


def remote(src, dst, send, recv, device):
    return pltpu.make_async_remote_copy(
        src_ref=src, dst_ref=dst, send_sem=send, recv_sem=recv, device_id=device, device_id_type=MESH_ID
    )


def run_steps(*tracks):
    total = max(len(track) for track in tracks)
    done = [0] * len(tracks)
    for index in range(total):
        for number, track in enumerate(tracks):
            upto = -(-len(track) * (index + 1) // total)
            while done[number] < upto:
                track[done[number]]()
                done[number] += 1


def gather_plan(counts, local_rows, ks, target=96):
    plan = []
    for core in (0, 1):
        ident = 0
        for which in ks:
            for direction, pieces in enumerate(ring_chunks(counts, local_rows, which, core, target)):
                for order, (row, rows) in enumerate(pieces):
                    plan.append((ident, which, core, direction, order, row, rows))
                    ident += 1
    return plan, max(p[0] for p in plan) + 1


def gather_steps(place, plan, local_rows, base, own_ref, out_ref, sems, skew=2):
    ss, rs, sp, rp = sems

    def dst(which, row, rows):
        return out_ref.at[pl.ds(base[which] + row, rows)]

    def src(core, row, rows):
        return own_ref.at[pl.ds(row - core * local_rows, rows)]

    def begin():
        for ident, which, core, direction, order, row, rows in plan:
            @pl.when(jnp.logical_and(place.c == core, place.f == which))
            def _():
                remote(src(core, row, rows), dst(which, row, rows), ss.at[ident], rs.at[ident],
                       place.ring(direction)).start()
        for ident, which, core, direction, order, row, rows in plan:
            @pl.when(jnp.logical_and(place.c == core, place.f == which))
            def _():
                remote(src(core, row, rows), dst(which, row, rows), sp.at[ident], rp.at[ident],
                       place.partner()).start()

    ordered = sorted(plan, key=lambda p: (p[4], p[1]))
    last = max(p[4] for p in plan)

    def visit(item, role):
        ident, which, core, direction, order, row, rows = item
        mine = dst(which, row, rows)

        @pl.when(jnp.logical_and(place.c == core, place.hop(which, direction) == role))
        def _():
            remote(mine, mine, ss.at[ident], rs.at[ident], place.ring(direction)).wait_recv()
            if role <= 2:
                remote(mine, mine, ss.at[ident], rs.at[ident], place.ring(direction)).start()
            remote(mine, mine, sp.at[ident], rp.at[ident], place.partner()).start()

    def step(j):
        def run():
            for role in (1, 2, 3):
                for item in ordered:
                    if item[4] == j - skew * (role - 1):
                        visit(item, role)
        return run

    def ready():
        for ident, which, core, direction, order, row, rows in plan:
            mine = dst(which, row, rows)

            @pl.when(place.c == 1 - core)
            def _():
                remote(mine, mine, sp.at[ident], rp.at[ident], place.partner()).wait_recv()

    def end():
        for ident, which, core, direction, order, row, rows in plan:
            hop = place.hop(which, direction)
            mine = dst(which, row, rows)

            @pl.when(jnp.logical_and(place.c == core, hop <= 2))
            def _():
                remote(mine, mine, ss.at[ident], rs.at[ident], place.ring(direction)).wait_send()

            @pl.when(place.c == core)
            def _():
                remote(mine, mine, sp.at[ident], rp.at[ident], place.partner()).wait_send()

    return begin, [step(j) for j in range(last + 1 + 2 * skew)], ready, end


def line_steps(place, chunks, own, out, early, mid, low, sems, lag=2, back_lag=3, prep=None, done=None):
    s1, r1, s2, r2, s3, r3 = sems

    def from_end(i, device):
        return remote(own(i), early(i), s1.at[i], r1.at[i], device)

    def across(i):
        return remote(mid(i), low(i), s2.at[i], r2.at[i], place.chip_z(3 - place.t))

    def back(i, device):
        return remote(out(i), out(i), s3.at[i], r3.at[i], device)

    def step(i):
        def run():
            if i < chunks and prep is not None:
                prep(i)

            @pl.when(place.outer)
            def _():
                if i < chunks:
                    from_end(i, place.chip_z(place.inner_mate)).start()
                if 0 <= i - lag - back_lag < chunks:
                    back(i - lag - back_lag, place.chip_z(place.inner_mate)).wait_recv()

            @pl.when(jnp.logical_not(place.outer))
            def _():
                if i < chunks:
                    from_end(i, place.chip_z(place.outer_mate)).wait_recv()
                    pair = own(i)[...].astype(jnp.float32) + early(i)[...].astype(jnp.float32)
                    mid(i)[...] = pair.astype(mid(i).dtype)
                    across(i).start()
                j = i - lag
                if 0 <= j < chunks:
                    across(j).wait_recv()
                    total = mid(j)[...].astype(jnp.float32) + low(j)[...].astype(jnp.float32)
                    out(j)[...] = total.astype(out(j).dtype)
                    back(j, place.chip_z(place.outer_mate)).start()
            if done is not None:
                if 0 <= i - lag - back_lag < chunks:
                    done(i - lag - back_lag)
        return run

    def end():
        @pl.when(place.outer)
        def _():
            for i in range(chunks):
                from_end(i, place.chip_z(place.inner_mate)).wait_send()

        @pl.when(jnp.logical_not(place.outer))
        def _():
            for i in range(chunks):
                across(i).wait_send()
                back(i, place.chip_z(place.outer_mate)).wait_send()

    return [step(i) for i in range(chunks + lag + back_lag)], end


def scatter_steps(place, plan, local_rows, base, part_ref, grad_ref, prx, rrx, tx, sems, skew=2):
    ss, rs, sp, rp = sems

    def rows_of(ref, which, row, rows):
        return ref.at[pl.ds(base[which] + row, rows)]

    def partner_copy(item):
        ident, which, core, direction, order, row, rows = item
        return remote(rows_of(part_ref, which, row, rows), rows_of(prx, which, row, rows),
                      sp.at[ident], rp.at[ident], place.partner())

    def ring_copy(item):
        ident, which, core, direction, order, row, rows = item
        return remote(rows_of(tx, which, row, rows), rows_of(rrx, which, row, rows),
                      ss.at[ident], rs.at[ident], place.ring(direction))

    ordered = sorted(plan, key=lambda p: (p[4], p[1]))
    last = max(p[4] for p in plan)

    def begin(ks):
        for item in ordered:
            if item[1] in ks:
                @pl.when(place.c == 1 - item[2])
                def _():
                    partner_copy(item).start()

    def visit(item, late):
        ident, which, core, direction, order, row, rows = item
        hop = place.hop(which, direction)
        role = (late + 1) % 4

        @pl.when(jnp.logical_and(place.c == core, hop == role))
        def _():
            partner_copy(item).wait_recv()
            total = (rows_of(part_ref, which, row, rows)[...].astype(jnp.float32)
                     + rows_of(prx, which, row, rows)[...].astype(jnp.float32))
            if role != 1:
                ring_copy(item).wait_recv()
                total = total + rows_of(rrx, which, row, rows)[...].astype(jnp.float32)
            if role == 0:
                grad_ref[pl.ds(row - core * local_rows, rows)] = total
            else:
                rows_of(tx, which, row, rows)[...] = total.astype(tx.dtype)
                ring_copy(item).start()

    def step(j):
        def run():
            for late in range(4):
                for item in ordered:
                    if item[4] == j - skew * late:
                        visit(item, late)
        return run

    def end():
        for item in plan:
            ident, which, core, direction, order, row, rows = item

            @pl.when(place.c == 1 - core)
            def _():
                partner_copy(item).wait_send()

            @pl.when(jnp.logical_and(place.c == core, place.hop(which, direction) != 0))
            def _():
                ring_copy(item).wait_send()

    return begin, [step(j) for j in range(last + 1 + 3 * skew)], end


VMEM_SPEC = pl.BlockSpec(memory_space=pltpu.VMEM)
ANY_SPEC = pl.BlockSpec(memory_space=pl.ANY)


def dma(count):
    return pltpu.SemaphoreType.DMA((count,))


def comm_call(kernel, outs, ins, in_specs, out_specs, scratch, ident):
    return pl.pallas_call(
        kernel,
        out_shape=outs,
        in_specs=in_specs,
        out_specs=out_specs,
        scratch_shapes=scratch,
        compiler_params=pltpu.CompilerParams(
            collective_id=ident, has_side_effects=True, vmem_limit_bytes=60 * 2**20
        ),
    )(*ins)


def base_rows(counts, ks):
    base, at = {}, 0
    for which in ks:
        base[which] = at
        at += counts[which]
    return base, at


def own_rows_copy(place, counts, local_rows, ks, base, own_ref, out_ref, sem, act):
    for which in ks:
        for core in (0, 1):
            rows = min(counts[which] - core * local_rows, local_rows)
            if rows > 0:
                @pl.when(jnp.logical_and(place.c == core, place.f == which))
                def _():
                    act(pltpu.make_async_copy(
                        own_ref.at[pl.ds(0, rows)],
                        out_ref.at[pl.ds(base[which] + core * local_rows, rows)],
                        sem.at[0],
                    ))


class LineSum:
    def __init__(self, place, rows, own, early, mid, low, total, sems):
        self.place, self.rows = place, rows
        self.own, self.early, self.mid, self.low, self.total = own, early, mid, low, total
        self.sems = sems

    def cut(self, ref, i):
        return ref.at[pl.ds(pl.multiple_of(i * self.rows, self.rows), self.rows)]

    def from_end(self, i, mate):
        s1, r1 = self.sems[:2]
        return remote(self.cut(self.own, i), self.cut(self.early, i), s1.at[i], r1.at[i], self.place.chip_z(mate))

    def across(self, i):
        s2, r2 = self.sems[2:4]
        return remote(self.cut(self.mid, i), self.cut(self.low, i), s2.at[i], r2.at[i], self.place.chip_z(3 - self.place.t))

    def back(self, i, mate):
        s3, r3 = self.sems[4:6]
        return remote(self.cut(self.total, i), self.cut(self.total, i), s3.at[i], r3.at[i], self.place.chip_z(mate))

    def send(self, i):
        @pl.when(self.place.outer)
        def _():
            self.from_end(i, self.place.inner_mate).start()

    def pair_up(self, i):
        @pl.when(jnp.logical_not(self.place.outer))
        def _():
            self.from_end(i, self.place.outer_mate).wait_recv()
            pair = self.cut(self.own, i)[...].astype(jnp.float32) + self.cut(self.early, i)[...].astype(jnp.float32)
            self.cut(self.mid, i)[...] = pair.astype(self.mid.dtype)
            self.across(i).start()

    def join(self, i):
        @pl.when(jnp.logical_not(self.place.outer))
        def _():
            self.across(i).wait_recv()
            whole = self.cut(self.mid, i)[...].astype(jnp.float32) + self.cut(self.low, i)[...].astype(jnp.float32)
            self.cut(self.total, i)[...] = whole.astype(self.total.dtype)
            self.back(i, self.place.outer_mate).start()

    def receive(self, i):
        @pl.when(self.place.outer)
        def _():
            self.back(i, self.place.inner_mate).wait_recv()

    def finish(self, pieces):
        @pl.when(self.place.outer)
        def _():
            for i in range(pieces):
                self.from_end(i, self.place.inner_mate).wait_send()

        @pl.when(jnp.logical_not(self.place.outer))
        def _():
            for i in range(pieces):
                self.across(i).wait_send()
                self.back(i, self.place.outer_mate).wait_send()


def nt_dot(left, right):
    return lax.dot_general(left, right, (((1,), (1,)), ((), ())), preferred_element_type=jnp.float32)


def nn_dot(left, right):
    return jnp.dot(left, right, preferred_element_type=jnp.float32)


def tn_dot(left, right):
    return lax.dot_general(left, right, (((0,), (0,)), ((), ())), preferred_element_type=jnp.float32)


def centred(values):
    centre = values - jnp.mean(values, axis=-1, keepdims=True)
    spread = jnp.mean(centre * centre, axis=-1, keepdims=True)
    return centre, lax.rsqrt(spread + norm_eps)


def norm_back(values, gain_row, grads):
    centre, scale = centred(values)
    xhat = centre * scale
    e = grads * gain_row
    moved = scale * (e - jnp.mean(e, axis=-1, keepdims=True) - xhat * jnp.mean(e * xhat, axis=-1, keepdims=True))
    return moved, jnp.sum(grads * xhat, axis=0, keepdims=True)


def layer_both_ways(tokens, out_grad, own_block, norm_gains, cosine, sine, seg_column, seg_row, counts, ident):
    count, width = tokens.shape
    local_rows = own_block.shape[0]
    inner = counts[1]
    ff = counts[3]
    heads = inner // HEAD_DIM
    full = 2 * count
    rows = count // 4
    sub = rows // 2
    stack = heads * rows
    piece = 64
    score_scale = HEAD_DIM ** (-0.5)
    f32, low = jnp.float32, jnp.bfloat16
    first_plan, first_count = gather_plan(counts, local_rows, (0, 1), 64)
    last_plan, last_count = gather_plan(counts, local_rows, (2, 3), 64)
    first_base, first_rows = base_rows(counts, (0, 1))
    last_base, last_rows = base_rows(counts, (2, 3))

    def kernel(tok_ref, og_ref, own_ref, gain_ref, cos_ref, sin_ref, sc_ref, sr_ref,
               act_ref, attn_ref, resid_ref, mlp_ref, hid_ref, dm_ref, b2_ref, dres_ref, db_ref, dproj_ref, t3_ref, dg_ref,
               w1st, wlast, q_ref, kv_ref, kq_ref, p_ref, s_ref, pl_ref, do_ref, dp_ref, ds_ref,
               t1_ref, e1, m1, l1, sum1, t2_ref, e2, m2, l2, sum2, dq_ref, dkv_ref, dkv_tx, dkv_rx, *sems):
        place = Place()
        greet(place, True, True, True)
        begin1, steps1, ready1, end1 = gather_steps(place, first_plan, local_rows, first_base, own_ref, w1st, sems[0:4], 1)
        begin2, steps2, ready2, end2 = gather_steps(place, last_plan, local_rows, last_base, own_ref, wlast, sems[4:8])
        line1 = LineSum(place, sub, t1_ref, e1, m1, l1, sum1, sems[8:14])
        line2 = LineSum(place, sub, t2_ref, e2, m2, l2, sum2, sems[14:20])
        swap, local_sem = sems[20], sems[21]

        begin1()
        own_rows_copy(place, counts, local_rows, (0, 1), first_base, own_ref, w1st, local_sem, lambda d: d.start())

        def at(i, size=rows):
            return pl.ds(pl.multiple_of(i * size, size), size)

        def norm_one(i, carry):
            centre, scale = centred(tok_ref[at(i)].astype(f32))
            act_ref[at(i)] = (centre * scale * gain_ref[0:1]).astype(low)
            return carry

        lax.fori_loop(0, 4, norm_one, 0)
        dg_ref[...] = jnp.zeros_like(dg_ref)
        begin2()
        run_steps(steps1)
        own_rows_copy(place, counts, local_rows, (0, 1), first_base, own_ref, w1st, local_sem, lambda d: d.wait())
        own_rows_copy(place, counts, local_rows, (2, 3), last_base, own_ref, wlast, local_sem, lambda d: d.start())
        ready1()
        waiting = list(steps2)

        def forward(number):
            for step in waiting[:number]:
                step()
            del waiting[:number]

        forward(1)

        lane = lax.broadcasted_iota(jnp.int32, (1, inner), 1)
        front = (lane % HEAD_DIM) < HEAD_DIM // 2

        def half_turn(value):
            return jnp.where(front, pltpu.roll(value, inner - HEAD_DIM // 2, 1), pltpu.roll(value, HEAD_DIM // 2, 1))

        sign = jnp.where(front, -1.0, 1.0).astype(f32)

        def rotated(value, i):
            return value * cos_ref[at(i)] + half_turn(value) * (sin_ref[at(i)] * sign)

        def rotated_back(value, i):
            return value * cos_ref[at(i)] - half_turn(value * sin_ref[at(i)]) * sign

        def project_rows(i, carry):
            value = nt_dot(act_ref[at(i)], w1st[0:3 * inner])
            q_ref[at(i)] = rotated(value[:, 0:inner], i).astype(low)
            kv_ref[at(i), 0:inner] = rotated(value[:, inner:2 * inner], i).astype(low)
            kv_ref[at(i), inner:2 * inner] = value[:, 2 * inner:3 * inner].astype(low)
            return carry

        lax.fori_loop(0, 4, project_rows, 0)
        kv_copy = remote(kv_ref.at[pl.ds(0, count)], kv_ref.at[pl.ds(count, count)], swap.at[0], swap.at[1], place.partner())
        kv_copy.start()
        forward(2)
        kv_copy.wait()

        def head_mask(h):
            return jnp.logical_and(lane >= h * HEAD_DIM, lane < (h + 1) * HEAD_DIM)

        def stacked(value):
            return jnp.concatenate([jnp.where(head_mask(h), value, jnp.zeros_like(value)) for h in range(heads)], axis=0)

        def unstacked(value):
            total = jnp.where(head_mask(0), value[0:rows], 0.0)
            for h in range(1, heads):
                total = total + jnp.where(head_mask(h), value[h * rows:(h + 1) * rows], 0.0)
            return total

        per = rows // piece

        def attend(i):
            kq_ref[...] = stacked(q_ref[at(i)])
            s_ref[...] = nt_dot(kq_ref[...], kv_ref[:, 0:inner])

            def soft(r, inside):
                seg = sc_ref[pl.ds(pl.multiple_of(i * rows + (r % per) * piece, piece), piece)]
                score = jnp.where(seg == sr_ref[...], s_ref[at(r, piece)] * score_scale, -jnp.inf)
                score = jnp.exp(score - jnp.max(score, axis=-1, keepdims=True))
                prob = score * (1.0 / jnp.sum(score, axis=-1, keepdims=True))
                p_ref[i, at(r, piece)] = prob
                pl_ref[at(r, piece)] = prob.astype(low)
                return inside

            lax.fori_loop(0, stack // piece, soft, 0)
            mixed = unstacked(nn_dot(pl_ref[...], kv_ref[:, inner:2 * inner]))
            keep = (sc_ref[at(i)] > 0).astype(f32)
            attn = (mixed * keep).astype(low)
            attn_ref[at(i)] = attn
            t1_ref[at(i)] = nn_dot(attn, w1st[3 * inner:4 * inner]).astype(low)
            for part in range(2):
                line1.send(2 * i + part)

            if i >= 1:
                line1.pair_up(2 * i - 2)
                line1.pair_up(2 * i - 1)
            if i >= 2:
                line1.join(2 * i - 4)
                line1.join(2 * i - 3)

        for i in range(4):
            attend(i)
            forward(2)
        forward(len(waiting))
        own_rows_copy(place, counts, local_rows, (2, 3), last_base, own_ref, wlast, local_sem, lambda d: d.wait())
        ready2()

        def feed(i, carry):
            for part in range(2):
                line1.receive(2 * i + part)
            resid = tok_ref[at(i)].astype(f32) + sum1[at(i)].astype(f32)
            resid_ref[at(i)] = resid
            centre, scale = centred(resid)
            mlp = (centre * scale * gain_ref[1:2]).astype(low)
            mlp_ref[at(i)] = mlp
            gate = nt_dot(mlp, wlast[0:ff])
            up = nt_dot(mlp, wlast[ff:2 * ff])
            cdf = 0.5 * (1.0 + lax.erf(gate * (0.5 ** 0.5)))
            bell = jnp.exp(gate * gate * -0.5) * (1.0 / math.sqrt(2.0 * math.pi))
            gelu = gate * cdf
            hidden = (gelu * up).astype(low)
            hid_ref[at(i)] = hidden
            dhidden = nt_dot(og_ref[at(i)], wlast[2 * ff:3 * ff])
            dgate = (dhidden * up * (cdf + gate * bell)).astype(low)
            dup = (dhidden * gelu).astype(low)
            dm_ref[0, at(i)] = dgate
            dm_ref[1, at(i)] = dup
            t2_ref[at(i)] = (nn_dot(dgate, wlast[0:ff]) + nn_dot(dup, wlast[ff:2 * ff])).astype(low)
            for part in range(2):
                line2.send(2 * i + part)
            b2_ref[at(i)] = nn_dot(hidden, wlast[2 * ff:3 * ff]).astype(low)

            @pl.when(i == 0)
            def _():
                line1.pair_up(6)
                line1.pair_up(7)

            @pl.when(i <= 1)
            def _():
                line1.join(2 * i + 4)
                line1.join(2 * i + 5)

            @pl.when(i >= 1)
            def _():
                line2.pair_up(2 * i - 2)
                line2.pair_up(2 * i - 1)

            @pl.when(i >= 2)
            def _():
                line2.join(2 * i - 4)
                line2.join(2 * i - 3)
            return carry

        lax.fori_loop(0, 4, feed, 0)
        dkv_ref[...] = jnp.zeros_like(dkv_ref)

        def turn_back(i, carry):
            @pl.when(i == 0)
            def _():
                line2.pair_up(6)
                line2.pair_up(7)
            for part in range(2):
                line2.receive(2 * i + part)
            moved, gain_part = norm_back(resid_ref[at(i)], gain_ref[1:2], sum2[at(i)].astype(f32))
            dg_ref[1:2] = dg_ref[1:2] + gain_part
            dresid = og_ref[at(i)].astype(f32) + moved
            dres_ref[at(i)] = dresid
            dbranch = dresid.astype(low)
            db_ref[at(i)] = dbranch
            keep = (sc_ref[at(i)] > 0).astype(low)
            dattn = nt_dot(dbranch, w1st[3 * inner:4 * inner]).astype(low) * keep
            do_ref[...] = stacked(dattn)
            kq_ref[...] = stacked(q_ref[at(i)])
            dp_ref[...] = nt_dot(do_ref[...], kv_ref[:, inner:2 * inner])

            def soft_back(r, inside):
                prob = p_ref[i, at(r, piece)]
                dprob = dp_ref[at(r, piece)]
                delta = jnp.sum(prob * dprob, axis=-1, keepdims=True)
                ds_ref[at(r, piece)] = (prob * (dprob - delta) * score_scale).astype(low)
                pl_ref[at(r, piece)] = prob.astype(low)
                return inside

            lax.fori_loop(0, stack // piece, soft_back, 0)
            dq_ref[at(i)] = unstacked(nn_dot(ds_ref[...], kv_ref[:, 0:inner]))
            dkv_ref[:, 0:inner] = dkv_ref[:, 0:inner] + tn_dot(ds_ref[...], kq_ref[...])
            dkv_ref[:, inner:2 * inner] = dkv_ref[:, inner:2 * inner] + tn_dot(pl_ref[...], do_ref[...])

            @pl.when(i <= 1)
            def _():
                line2.join(2 * i + 4)
                line2.join(2 * i + 5)
            return carry

        lax.fori_loop(0, 4, turn_back, 0)
        dkv_tx[...] = dkv_ref[count:full].astype(low)
        dkv_copy = remote(dkv_tx, dkv_rx, swap.at[2], swap.at[3], place.partner())
        dkv_copy.start()

        def unproject_query(i, carry):
            dproj_ref[at(i), 0:inner] = rotated_back(dq_ref[at(i)], i).astype(low)
            return carry

        lax.fori_loop(0, 4, unproject_query, 0)
        dkv_copy.wait()

        def unproject(i, carry):
            both = dkv_ref[at(i)] + dkv_rx[at(i)].astype(f32)
            dproj_ref[at(i), inner:2 * inner] = rotated_back(both[:, 0:inner], i).astype(low)
            dproj_ref[at(i), 2 * inner:3 * inner] = both[:, inner:2 * inner].astype(low)
            t3_ref[at(i)] = nn_dot(dproj_ref[at(i)], w1st[0:3 * inner]).astype(low)
            return carry

        lax.fori_loop(0, 4, unproject, 0)
        line1.finish(8)
        line2.finish(8)
        end1()
        end2()

    def shape(*dims, dtype=low):
        return jax.ShapeDtypeStruct(dims, dtype)

    outs = (
        shape(count, width), shape(count, inner), shape(count, width, dtype=f32), shape(count, width), shape(count, ff),
        shape(2, count, ff), shape(count, width), shape(count, width, dtype=f32), shape(count, width),
        shape(count, 3 * inner), shape(count, width), shape(8, width, dtype=f32),
    )
    line = pltpu.VMEM((count, width), low)
    scratch = [
        pltpu.VMEM((first_rows, width), low), pltpu.VMEM((last_rows, width), low), pltpu.VMEM((count, inner), low),
        pltpu.VMEM((full, 2 * inner), low), pltpu.VMEM((stack, inner), low), pltpu.VMEM((4, stack, full), f32),
        pltpu.VMEM((stack, full), f32), pltpu.VMEM((stack, full), low), pltpu.VMEM((stack, inner), low),
        pltpu.VMEM((stack, full), f32), pltpu.VMEM((stack, full), low),
    ]
    scratch += [line] * 10
    scratch += [
        pltpu.VMEM((count, inner), f32), pltpu.VMEM((full, 2 * inner), f32),
        pltpu.VMEM((count, 2 * inner), low), pltpu.VMEM((count, 2 * inner), low),
    ]
    scratch += [dma(first_count)] * 4 + [dma(last_count)] * 4 + [dma(8)] * 12 + [dma(4), dma(1)]
    ins = (tokens, out_grad, own_block, norm_gains, cosine, sine, seg_column, seg_row)
    return pl.pallas_call(
        kernel,
        out_shape=outs,
        in_specs=[VMEM_SPEC] * len(ins),
        out_specs=(VMEM_SPEC,) * len(outs),
        scratch_shapes=scratch,
        compiler_params=pltpu.CompilerParams(
            collective_id=ident, has_side_effects=True, vmem_limit_bytes=67043328
        ),
    )(*ins)


def tail_grams(left_right, muon_rows, counts, ident):
    dproj, act_in, attn_in, dbranch, dmixed, mlp_in, hidden, out_low = left_right
    local_rows, width = muon_rows.shape
    ks = (0, 1, 2, 3)
    plan, count = gather_plan(counts, local_rows, ks, 96)
    base, total_rows = base_rows(counts, ks)
    ff = counts[3]
    tile = width // 4
    half = tile // 2
    chunks = 10
    f32, low16 = jnp.float32, jnp.bfloat16

    def kernel(dp_ref, act_ref, at_ref, db_ref, dm_ref, mlp_ref, hid_ref, og_ref, mu_ref,
               grad_ref, next_ref, x_ref, g_ref, norm_ref,
               part, prx, rrx, mine, theirs, gprx, tot, other, early, mid, low, norm_own, *sems):
        place = Place()
        c = place.c
        greet(place, True, True, True)
        begin, steps, end = scatter_steps(place, plan, local_rows, base, part, grad_ref, prx, rrx, part, sems[:4])

        def terms(row, left, right):
            span = left.shape[1]

            def columns(j, carry):
                cols = pl.ds(pl.multiple_of(j * tile, tile), tile)
                part[pl.ds(row, span), cols] = tn_dot(left[...], right[:, cols]).astype(low16)
                return carry

            lax.fori_loop(0, 4, columns, 0)

        terms(base[2], dm_ref.at[0], mlp_ref)
        terms(base[2] + ff, dm_ref.at[1], mlp_ref)
        begin((2,))
        terms(base[3], hid_ref, og_ref)
        begin((3,))
        terms(base[0], dp_ref, act_ref)
        begin((0,))
        terms(base[1], at_ref, db_ref)
        begin((1,))
        grad_ref[...] = jnp.zeros_like(grad_ref)
        run_steps(steps)
        end()

        def momentum(i, carry):
            sl = pl.ds(pl.multiple_of(i * 16, 16), 16)
            grad = grad_ref[sl]
            after = muon_beta * mu_ref[sl] + (1.0 - muon_beta) * grad
            next_ref[sl] = after
            direction = (1.0 - muon_beta) * grad + muon_beta * after
            x_ref[sl] = direction.astype(low16)
            square = direction * direction
            return carry + square[0:8] + square[8:16]

        square = lax.fori_loop(0, local_rows // 16, momentum, jnp.zeros((8, width), f32))
        own_square = jnp.broadcast_to(jnp.sum(jnp.sum(square, axis=1, keepdims=True), axis=0, keepdims=True), (8, tile))
        norm_own[...] = own_square

        sp, rp, st, rt = sems[10:14]

        def blocks(core):
            return [(3 * core, 3 * core), (2 * core, 2 * core + 1), (core + 1, core + 1), (core, core + 2), (core, 3 - core)]

        def at(k):
            return pl.ds(pl.multiple_of(k * tile, tile), tile)

        def gram(i, j):
            return tn_dot(x_ref[:, at(i)], x_ref[:, at(j)])

        def partner(n):
            sl = pl.ds(n * tile, tile)
            return remote(theirs.at[sl], gprx.at[sl], sp.at[n], rp.at[n], place.partner())

        def norm_row(ref):
            return ref.at[pl.ds(5 * tile, 8)]

        for n, (i, j) in enumerate(blocks(1 - c)):
            theirs[pl.ds(n * tile, tile)] = gram(i, j)
            partner(n).start()
        norm_row(theirs)[...] = norm_own[...]
        pn = remote(norm_row(theirs), norm_row(gprx), sp.at[5], rp.at[5], place.partner())
        pn.start()

        def span(i):
            return pl.ds(i * half, half) if i < chunks - 1 else pl.ds(i * half, half + 8)

        def cut(ref):
            return lambda i: ref.at[span(i)]

        def prep(i):
            if i % 2 == 0:
                n = i // 2
                sl = pl.ds(n * tile, tile)
                block = gram(*blocks(c)[n])
                partner(n).wait_recv()
                mine[sl] = block + gprx[sl]
            if i == chunks - 1:
                pn.wait_recv()
                norm_row(mine)[...] = norm_row(gprx)[...] + norm_own[...]

        def share(i):
            return remote(cut(tot)(i), cut(other)(i), st.at[i], rt.at[i], place.partner())

        def place_block(ref, n, core):
            i, j = blocks(core)[n]
            block = ref[pl.ds(n * tile, tile)]
            g_ref[at(i), at(j)] = block
            g_ref[at(j), at(i)] = block.T

        def done(i):
            share(i).start()
            if i % 2 == 1:
                place_block(tot, i // 2, c)
            if i >= 2:
                share(i - 2).wait_recv()
                if (i - 2) % 2 == 1:
                    place_block(other, (i - 2) // 2, 1 - c)

        line, line_end = line_steps(place, chunks, cut(mine), cut(tot), cut(early), cut(mid), cut(low), sems[4:10],
                                    prep=prep, done=done)
        run_steps(line)
        for i in (chunks - 2, chunks - 1):
            share(i).wait_recv()
        place_block(other, 4, 1 - c)
        norm_ref[...] = jnp.broadcast_to(tot[5 * tile:5 * tile + 8, 0:128], (8, 128))
        line_end()
        for n in range(5):
            partner(n).wait_send()
        pn.wait_send()
        for i in range(chunks):
            share(i).wait_send()

    rows_low = pltpu.VMEM((total_rows, width), low16)
    packed = pltpu.VMEM((5 * tile + 8, tile), f32)
    outs = (
        jax.ShapeDtypeStruct((local_rows, width), f32), jax.ShapeDtypeStruct((local_rows, width), f32),
        jax.ShapeDtypeStruct((local_rows, width), low16), jax.ShapeDtypeStruct((width, width), f32),
        jax.ShapeDtypeStruct((8, 128), f32),
    )
    scratch = [rows_low] * 3 + [packed] * 8 + [pltpu.VMEM((8, tile), f32)]
    scratch += [dma(count)] * 4 + [dma(chunks)] * 6 + [dma(6), dma(6), dma(chunks), dma(chunks)]
    ins = tuple(left_right) + (muon_rows,)
    return comm_call(kernel, outs, ins, [VMEM_SPEC] * len(ins), (VMEM_SPEC,) * len(outs), scratch, ident)


def halves(value):
    high = value.astype(jnp.bfloat16)
    return high, (value - high.astype(jnp.float32)).astype(jnp.bfloat16)


def iterate(gram, norm, direction_low, own_block, normed_term, branch_term, tokens_in, resid, dresid, dgain_rows, norm_gains, adam_first,
            adam_second, ident):
    rows, width = direction_low.shape
    tile = 256
    parts = width // tile
    tokens = branch_term.shape[0]
    each = 8
    chunks = 2 * each
    step_rows = tokens // each
    aa = ns_first * ns_first
    ab = 2.0 * ns_first * ns_second
    bbac = ns_second * ns_second + 2.0 * ns_first * ns_third
    bc = 2.0 * ns_second * ns_third
    cc = ns_third * ns_third
    correction = 1.0 - adam_beta**STEP

    def kernel(g_ref, n_ref, d_ref, w_ref, t3_ref, b2_ref, tok_ref, r_ref, dres_ref, dgr_ref, gain_ref, af_ref, as_ref,
               u_ref, lo_ref, tg_ref, gg_ref, afn_ref, asn_ref, gu_ref,
               p_ref, ph, pl_, hh, hl, uh, ul, mx, x_ref, early, mid, low, total, held, dg_ref, *sems):
        place = Place()
        s1, r1, s2, r2, s3, r3, sg, rg = sems
        me = place.f * 2 + place.c
        barrier = pltpu.get_barrier_semaphore()

        def plane(shift):
            other = (me + shift) % 8
            return (other // 2, other % 2, place.t)

        for shift in range(1, 8):
            pl.semaphore_signal(barrier, inc=1, device_id=plane(shift), device_id_type=MESH_ID)

        @pl.when(place.outer)
        def _():
            pl.semaphore_signal(barrier, inc=1, device_id=place.chip_z(place.inner_mate), device_id_type=MESH_ID)
            pl.semaphore_wait(barrier, 8)

        @pl.when(jnp.logical_not(place.outer))
        def _():
            pl.semaphore_signal(barrier, inc=1, device_id=place.chip_z(place.outer_mate), device_id_type=MESH_ID)
            pl.semaphore_signal(barrier, inc=1, device_id=place.chip_z(3 - place.t), device_id_type=MESH_ID)
            pl.semaphore_wait(barrier, 9)

        def cut(ref, i):
            if isinstance(i, int):
                return ref.at[pl.ds(i * step_rows, step_rows)]
            return ref.at[pl.ds(pl.multiple_of(i * step_rows, step_rows), step_rows)]

        def from_end(i, device, own):
            local = i % each
            return remote(cut(own, local), cut(early, i), s1.at[i], r1.at[i], device)

        def across(i):
            return remote(cut(mid, i), cut(low, i), s2.at[i], r2.at[i], place.chip_z(3 - place.t))

        def back(i, device):
            return remote(cut(total, i), cut(total, i), s3.at[i], r3.at[i], device)

        dg_ref[...] = jnp.zeros_like(dg_ref)

        @pl.when(place.outer)
        def _():
            for i in range(each):
                from_end(i, place.chip_z(place.inner_mate), t3_ref).start()
            for i in range(each):
                from_end(each + i, place.chip_z(place.inner_mate), b2_ref).start()

        def pair_up(i, own):
            @pl.when(jnp.logical_not(place.outer))
            def _():
                from_end(i, place.chip_z(place.outer_mate), own).wait_recv()
                pair = cut(own, i % each)[...].astype(jnp.float32) + cut(early, i)[...].astype(jnp.float32)
                cut(mid, i)[...] = pair.astype(mid.dtype)
                across(i).start()

        def pair_some(first):
            for part in range(4):
                @pl.when(first + part < each)
                def _():
                    pair_up(first + part, t3_ref)

                @pl.when(first + part >= each)
                def _():
                    pair_up(first + part, b2_ref)

        def join_some(first):
            for part in range(2):
                join(first + part)

        def join(i):
            @pl.when(jnp.logical_not(place.outer))
            def _():
                across(i).wait_recv()
                whole = cut(mid, i)[...].astype(jnp.float32) + cut(low, i)[...].astype(jnp.float32)
                cut(total, i)[...] = whole.astype(total.dtype)
                back(i, place.chip_z(place.outer_mate)).start()

        norm_size = jnp.sqrt(n_ref[0:1, 0:1])
        inverse = 1.0 / (norm_size + ortho_eps)
        scale = inverse * inverse

        for k in range(parts):
            sl = pl.ds(k * tile, tile)
            value = g_ref[sl] * scale
            p_ref[sl] = value
            high, rest = halves(value)
            ph[sl] = high
            pl_[sl] = rest
        x_ref[...] = d_ref[...].astype(jnp.float32) * inverse

        def product(lh, ll, rh, rl, k):
            sl, cols = pl.ds(k * tile, tile), pl.ds(k * tile, width - k * tile)

            def dot(left, right):
                return jnp.dot(left[sl], right[:, cols], preferred_element_type=jnp.float32)

            return dot(lh, rh) + dot(ll, rh) + dot(lh, rl)

        def spread_out(value, high_ref, low_ref, k):
            sl, cols = pl.ds(k * tile, tile), pl.ds(k * tile, width - k * tile)
            high, rest = halves(value)
            high_ref[sl, cols] = high
            low_ref[sl, cols] = rest
            for j in range(k + 1, parts):
                at = (j - k) * tile
                high_ref[pl.ds(j * tile, tile), sl] = high[:, at:at + tile].T
                low_ref[pl.ds(j * tile, tile), sl] = rest[:, at:at + tile].T

        def squares():
            for k in range(parts):
                sl, cols = pl.ds(k * tile, tile), pl.ds(k * tile, width - k * tile)
                value = product(ph, pl_, ph, pl_, k)
                spread_out(value, hh, hl, k)
                mix = (ns_second * p_ref[sl, cols] + ns_third * value).astype(mx.dtype)
                mx[sl, cols] = mix
                for j in range(k + 1, parts):
                    at = (j - k) * tile
                    mx[pl.ds(j * tile, tile), sl] = mix[:, at:at + tile].T

        def rotate_rows():
            for at, size in ((0, 336), (336, 320)):
                sl = pl.ds(at, size)
                old = x_ref[sl]
                x_ref[sl] = ns_first * old + jnp.dot(old.astype(jnp.bfloat16), mx[...], preferred_element_type=jnp.float32)

        def gains_copy(shift):
            return remote(dg_ref, held.at[me], sg.at[shift], rg.at[shift], plane(shift))

        def first_norm_back():
            @pl.when(place.outer)
            def _():
                for i in range(each):
                    back(i, place.chip_z(place.inner_mate)).wait_recv()

            def some(i, inside):
                sl = pl.ds(pl.multiple_of(i * 64, 64), 64)
                moved, gain_part = norm_back(tok_ref[sl].astype(jnp.float32), gain_ref[0:1], total[sl].astype(jnp.float32))
                dg_ref[0:1] = dg_ref[0:1] + gain_part
                tg_ref[sl] = (dres_ref[sl] + moved).astype(tg_ref.dtype)
                return inside

            lax.fori_loop(0, tokens // 64, some, 0)
            dg_ref[1:2] = dgr_ref[1:2]
            held[pl.ds(me, 1)] = dg_ref[...][None]
            for shift in range(1, 8):
                gains_copy(shift).start()

        def body(sweep, carry):
            @pl.when(sweep >= 1)
            def _():
                join_some(4 * sweep - 4)
            squares()

            @pl.when(sweep >= 1)
            def _():
                join_some(4 * sweep - 2)
            rotate_rows()

            @pl.when(sweep < ITERS - 1)
            def _():
                for k in range(parts):
                    sl, cols = pl.ds(k * tile, tile), pl.ds(k * tile, width - k * tile)
                    cube = product(ph, pl_, hh, hl, k)
                    square = hh[sl, cols].astype(jnp.float32) + hl[sl, cols].astype(jnp.float32)
                    spread_out(bc * square + cc * cube, uh, ul, k)
                    p_ref[sl, cols] = aa * p_ref[sl, cols] + ab * square + bbac * cube

                pair_some(4 * sweep)
                for k in range(parts):
                    sl, cols = pl.ds(k * tile, tile), pl.ds(k * tile, width - k * tile)
                    value = p_ref[sl, cols] + product(hh, hl, uh, ul, k)
                    p_ref[sl, cols] = value
                    spread_out(value, ph, pl_, k)

            @pl.when(sweep == ITERS - 2)
            def _():
                first_norm_back()
            return carry

        lax.fori_loop(0, ITERS, body, 0)
        spread = jnp.where(place.f == 0, 0.2 * math.sqrt(3 * D), jnp.where(place.f == 1, 0.2 * math.sqrt(D), jnp.where(
            place.f == 2, 0.2 * math.sqrt(2 * FF), 0.2 * math.sqrt(FF)))).astype(jnp.float32)
        u_ref[...] = -muon_rate * (spread * x_ref[...] + decay_rate * w_ref[...].astype(jnp.float32))

        for shift in range(1, 8):
            gains_copy(shift).wait()
        grads = held[0]
        for k in range(1, 8):
            grads = grads + held[k]
        grads = grads[0:2]
        gg_ref[...] = grads
        first = adam_beta * af_ref[...] + (1.0 - adam_beta) * grads
        second = adam_beta * as_ref[...] + (1.0 - adam_beta) * grads * grads
        afn_ref[...] = first
        asn_ref[...] = second
        gu_ref[...] = -adam_rate * (
            first / correction / (jnp.sqrt(second / correction) + adam_eps) + decay_rate * gain_ref[...]
        )

        @pl.when(place.outer)
        def _():
            for i in range(each, chunks):
                back(i, place.chip_z(place.inner_mate)).wait_recv()
            for i in range(each):
                from_end(i, place.chip_z(place.inner_mate), t3_ref).wait_send()
                from_end(each + i, place.chip_z(place.inner_mate), b2_ref).wait_send()
        lo_ref[...] = (r_ref[...] + total[tokens:2 * tokens].astype(jnp.float32)).astype(lo_ref.dtype)

        @pl.when(jnp.logical_not(place.outer))
        def _():
            for i in range(chunks):
                across(i).wait_send()
                back(i, place.chip_z(place.outer_mate)).wait_send()

    f32, low16 = jnp.float32, jnp.bfloat16
    small = jax.ShapeDtypeStruct(norm_gains.shape, f32)
    narrow = jax.ShapeDtypeStruct((tokens, width), low16)
    outs = (jax.ShapeDtypeStruct((rows, width), f32), narrow, narrow, small, small, small, small)
    full = pltpu.VMEM((width, width), low16)
    line = pltpu.VMEM((2 * tokens, width), low16)
    scratch = [pltpu.VMEM((width, width), f32)] + [full] * 7 + [pltpu.VMEM((rows, width), f32)] + [line] * 4
    scratch += [pltpu.VMEM((8, 8, width), f32), pltpu.VMEM((8, width), f32)] + [dma(chunks)] * 6 + [dma(8)] * 2
    ins = (gram, norm, direction_low, own_block, normed_term, branch_term, tokens_in, resid, dresid, dgain_rows, norm_gains,
           adam_first, adam_second)
    return comm_call(kernel, outs, ins, [VMEM_SPEC] * len(ins), (VMEM_SPEC,) * len(outs), scratch, ident)


def per_device_block(tokens, out_grad, weight_stack, muon_state, norm_gains, adam_first, adam_second, segment_ids,
                     position_ids):
    token_count, _, model_width = tokens.shape
    groups, contexts = 4, 2
    full_len = token_count * contexts
    local_rows = weight_stack.shape[2]
    heads_dev = HEADS // groups
    ff_dev = FF // groups
    inner_width = heads_dev * HEAD_DIM
    counts = (3 * inner_width, inner_width, 2 * ff_dev, ff_dev)
    own_block = weight_stack.reshape(local_rows, model_width)
    context = lax.axis_index("context")

    cosine, sine_table = rope_tables(position_ids.reshape(token_count), HEAD_DIM)
    segments = segment_ids.reshape(full_len)
    seg_query = lax.dynamic_slice_in_dim(segments, context * token_count, token_count, 0)
    seg_other = lax.dynamic_slice_in_dim(segments, (1 - context) * token_count, token_count, 0)
    (act_in, attn_in, resid, mlp_in, hidden, dmixed, branch_two_term, dresid, dbranch_one, dprojected, dnormed_one_term,
     dgain_rows) = layer_both_ways(
        tokens.reshape(token_count, model_width), out_grad.reshape(token_count, model_width), own_block, norm_gains,
        jnp.tile(cosine, (1, heads_dev)), jnp.tile(sine_table, (1, heads_dev)),
        seg_query.reshape(token_count, 1), jnp.concatenate([seg_query, seg_other]).reshape(1, full_len), counts, 0,
    )
    grad_block, muon_next, direction_low, gram, norm_total = tail_grams(
        (dprojected, act_in, attn_in, dbranch_one, dmixed, mlp_in, hidden, out_grad.reshape(token_count, model_width)),
        muon_state.reshape(local_rows, model_width), counts, 1,
    )
    direction_scale = jnp.log(jnp.sqrt(norm_total[0, 0])).reshape(1)
    weight_update, layer_out, tokens_grad, gain_grads, adam_first_next, adam_second_next, gain_update = iterate(
        gram, norm_total, direction_low, own_block, dnormed_one_term, branch_two_term,
        tokens.reshape(token_count, model_width), resid, dresid, dgain_rows, norm_gains, adam_first, adam_second, 2,
    )
    layer_out = layer_out.reshape(tokens.shape)
    tokens_grad = tokens_grad.reshape(tokens.shape)
    block_shape = (1, 1, local_rows, model_width)
    return (
        layer_out,
        tokens_grad,
        grad_block.reshape(block_shape),
        muon_next.reshape(block_shape),
        weight_update.reshape(block_shape),
        direction_scale,
        gain_grads,
        adam_first_next,
        adam_second_next,
        gain_update,
    )


def solution(mesh):
    sizes = dict(mesh.shape)
    block = (sizes["fsdp"], sizes["context"], sizes["tensor"]) == (4, 2, 4)
    return jax.shard_map(
        per_device_block if block else per_device,
        mesh=mesh,
        in_specs=(
            P("context", "fsdp", None),
            P("context", "fsdp", None),
            P("fsdp", "tensor", "context", None),
            P("fsdp", "tensor", "context", None),
            P(),
            P(),
            P(),
            P(None, "fsdp"),
            P("context", "fsdp"),
        ),
        out_specs=(
            P("context", "fsdp", None),
            P("context", "fsdp", None),
            P("fsdp", "tensor", "context", None),
            P("fsdp", "tensor", "context", None),
            P("fsdp", "tensor", "context", None),
            P("fsdp"),
            P(),
            P(),
            P(),
            P(),
        ),
        check_vma=False,
    )
```

```python
import math

import jax
import jax.numpy as jnp
from jax import lax
from jax.experimental import pallas as pl
from jax.experimental.pallas import tpu as pltpu
from jax.sharding import PartitionSpec as P

D = 1024
HEADS = 16
HEAD_DIM = 64
FF = 2624
ITERS = 5
STEP = 8


rope_base = 160000.0
norm_eps = 1e-05
ns_first = 3.4445
ns_second = -4.775
ns_third = 2.0315
muon_beta = 0.5
muon_rate = 0.15
decay_rate = 0.1
adam_beta = 0.5
adam_rate = 0.05
ortho_eps = 1e-07
adam_eps = 1e-08
precision_highest = lax.Precision.HIGHEST


def layer_norm(values, gain_row):
    centre = values - jnp.mean(values, axis=-1, keepdims=True)
    spread = jnp.mean(centre * centre, axis=-1, keepdims=True)
    return centre * lax.rsqrt(spread + norm_eps) * gain_row


def rope_tables(positions, head_width):
    half_width = head_width // 2
    freqs = rope_base ** (-(jnp.arange(half_width, dtype=jnp.float32) * 2.0 / head_width))
    angle = positions.astype(jnp.float32)[..., None] * freqs
    angle = jnp.concatenate([angle, angle], axis=-1)
    return (jnp.cos(angle), jnp.sin(angle))


def rotate(values, cosine, sine_table):
    half_width = values.shape[-1] // 2
    turned = jnp.concatenate([-values[..., half_width:], values[..., :half_width]], axis=-1)
    return values * cosine + turned * sine_table


def rotate_back(grads_in, cosine, sine_table):
    half_width = grads_in.shape[-1] // 2
    scaled = grads_in * sine_table
    turned = jnp.concatenate([scaled[..., half_width:], -scaled[..., :half_width]], axis=-1)
    return grads_in * cosine + turned


def project(left_rows, right_rows):
    return lax.dot_general(
        left_rows, right_rows, (((1,), (1,)), ((), ())), preferred_element_type=jnp.float32
    )


def contract_exact(left_rows, right_rows):
    return lax.dot_general(
        left_rows,
        right_rows,
        (((0,), (0,)), ((), ())),
        precision=precision_highest,
        preferred_element_type=jnp.float32,
    )


def geglu_gate(gate_part, up_part):
    return jax.nn.gelu(gate_part, approximate=False) * up_part


def per_device(
    tokens,
    out_grad,
    weight_stack,
    muon_state,
    norm_gains,
    adam_first,
    adam_second,
    segment_ids,
    position_ids,
):
    local_len, seq_count, model_width = tokens.shape
    token_count = local_len * seq_count
    groups = lax.axis_size("tensor")
    contexts = lax.axis_size("context")
    full_len = local_len * contexts
    local_rows = weight_stack.shape[2]
    pad_rows = local_rows * contexts
    heads_dev = HEADS // groups
    ff_dev = FF // groups
    inner_width = heads_dev * HEAD_DIM
    counts = (3 * inner_width, inner_width, 2 * ff_dev, ff_dev)
    score_scale = HEAD_DIM ** (-0.5)
    own_block = weight_stack.reshape(local_rows, model_width)
    gathered = lax.all_gather(own_block, ("fsdp", "context"), axis=0, tiled=True).reshape(
        4, pad_rows, model_width
    )
    w_qkv = gathered[0, : counts[0]]
    w_out = gathered[1, : counts[1]]
    w_in = gathered[2, : counts[2]]
    w_down = gathered[3, : counts[3]]
    inputs = tokens.astype(jnp.float32).reshape(token_count, model_width)
    act_in = layer_norm(inputs, norm_gains[0]).astype(jnp.bfloat16)
    projected = project(act_in, w_qkv).reshape(local_len, seq_count, 3, heads_dev, HEAD_DIM)
    cosine, sine_table = rope_tables(position_ids, HEAD_DIM)
    rot_cos = cosine[:, :, None, :]
    rot_sin = sine_table[:, :, None, :]
    query_matrix = rotate(projected[:, :, 0], rot_cos, rot_sin).astype(jnp.bfloat16)
    key_matrix_rows = rotate(projected[:, :, 1], rot_cos, rot_sin).astype(jnp.bfloat16)
    value_matrix_rows = projected[:, :, 2].astype(jnp.bfloat16)
    key_value = jnp.concatenate(
        [
            key_matrix_rows.reshape(local_len, seq_count, inner_width),
            value_matrix_rows.reshape(local_len, seq_count, inner_width),
        ],
        axis=-1,
    )
    key_value_all = lax.all_gather(key_value, "context", axis=0, tiled=True)
    keys_all = key_value_all[..., :inner_width].reshape(full_len, seq_count, heads_dev, HEAD_DIM)
    values_all = key_value_all[..., inner_width:].reshape(full_len, seq_count, heads_dev, HEAD_DIM)
    offset = lax.axis_index("context") * local_len
    seg_query = lax.dynamic_slice_in_dim(segment_ids, offset, local_len, 0)
    same_doc = seg_query.T[:, :, None] == segment_ids.T[:, None, :]
    keep_mask = (seg_query > 0).astype(jnp.float32)
    unscaled_score = jnp.einsum(
        "lshd,mshd->shlm", query_matrix, keys_all, preferred_element_type=jnp.float32
    )
    scores = jnp.where(same_doc[:, None], unscaled_score * score_scale, -jnp.inf)
    row_max = jnp.max(scores, axis=-1, keepdims=True)
    log_total = row_max + jnp.log(jnp.sum(jnp.exp(scores - row_max), axis=-1, keepdims=True))
    probs_low = jnp.exp(scores - log_total).astype(jnp.bfloat16)
    attended = jnp.einsum(
        "shlm,mshd->lshd", probs_low, values_all, preferred_element_type=jnp.float32
    )
    attn_in = (
        (attended * keep_mask[:, :, None, None])
        .astype(jnp.bfloat16)
        .reshape(token_count, inner_width)
    )
    branch_one = lax.psum(
        jnp.dot(attn_in, w_out, preferred_element_type=jnp.float32).astype(jnp.bfloat16), "tensor"
    ).astype(jnp.float32)
    resid = inputs + branch_one
    mlp_in = layer_norm(resid, norm_gains[1]).astype(jnp.bfloat16)
    mixed_rows = project(mlp_in, w_in)
    hidden_full, geglu_pull = jax.vjp(geglu_gate, mixed_rows[:, :ff_dev], mixed_rows[:, ff_dev:])
    hidden = hidden_full.astype(jnp.bfloat16)
    branch_two = lax.psum(
        jnp.dot(hidden, w_down, preferred_element_type=jnp.float32).astype(jnp.bfloat16), "tensor"
    ).astype(jnp.float32)
    layer_out = (resid + branch_two).astype(jnp.bfloat16).reshape(local_len, seq_count, model_width)
    out_cot = out_grad.astype(jnp.float32).reshape(token_count, model_width)
    dbranch_two = out_cot.astype(jnp.bfloat16)
    dhidden = project(dbranch_two, w_down)
    dgate, dup_part = geglu_pull(dhidden)
    dmixed = jnp.concatenate([dgate, dup_part], axis=1).astype(jnp.bfloat16)
    dnormed_two = lax.psum(
        jnp.dot(dmixed, w_in, preferred_element_type=jnp.float32).astype(jnp.bfloat16), "tensor"
    ).astype(jnp.float32)
    norm_two_out, norm_two_pull = jax.vjp(layer_norm, resid, norm_gains[1])
    dresid_norm, dgain_two = norm_two_pull(dnormed_two)
    dresid = out_cot + dresid_norm
    dbranch_one = dresid.astype(jnp.bfloat16)
    keep_low = keep_mask.reshape(token_count, 1).astype(jnp.bfloat16)
    dattended = project(dbranch_one, w_out).astype(jnp.bfloat16) * keep_low
    dattn = dattended.reshape(local_len, seq_count, heads_dev, HEAD_DIM)
    dquery_list = []
    dkey_list = []
    dvalue_list = []
    for head_index in range(heads_dev):
        query_head = query_matrix[:, :, head_index]
        key_head = keys_all[:, :, head_index]
        value_head = values_all[:, :, head_index]
        dout_head = dattn[:, :, head_index]
        raw_head = jnp.einsum(
            "lsd,msd->slm", query_head, key_head, preferred_element_type=jnp.float32
        )
        prob_head = jnp.exp(
            jnp.where(same_doc, raw_head * score_scale, -jnp.inf) - log_total[:, head_index]
        )
        dprob = jnp.einsum(
            "lsd,msd->slm", dout_head, value_head, preferred_element_type=jnp.float32
        )
        delta = jnp.sum(prob_head * dprob, axis=-1, keepdims=True)
        dscore = (prob_head * (dprob - delta) * score_scale).astype(jnp.bfloat16)
        dquery_list.append(
            jnp.einsum("slm,msd->lsd", dscore, key_head, preferred_element_type=jnp.float32)
        )
        dkey_head = jnp.einsum(
            "slm,lsd->msd", dscore, query_head, preferred_element_type=jnp.float32
        )
        dvalue_head = jnp.einsum(
            "slm,lsd->msd",
            prob_head.astype(jnp.bfloat16),
            dout_head,
            preferred_element_type=jnp.float32,
        )
        summed = lax.psum_scatter(
            jnp.concatenate([dkey_head, dvalue_head], axis=-1).astype(jnp.bfloat16),
            "context",
            scatter_dimension=0,
            tiled=True,
        ).astype(jnp.float32)
        dkey_list.append(summed[..., :HEAD_DIM])
        dvalue_list.append(summed[..., HEAD_DIM:])
    dqueries = jnp.stack(dquery_list, axis=2)
    dkeys = jnp.stack(dkey_list, axis=2)
    dvalues = jnp.stack(dvalue_list, axis=2)
    dprojected = (
        jnp.stack(
            [
                rotate_back(dqueries, rot_cos, rot_sin),
                rotate_back(dkeys, rot_cos, rot_sin),
                dvalues,
            ],
            axis=2,
        )
        .astype(jnp.bfloat16)
        .reshape(token_count, 3 * inner_width)
    )
    dnormed_one = lax.psum(
        jnp.dot(dprojected, w_qkv, preferred_element_type=jnp.float32).astype(jnp.bfloat16),
        "tensor",
    ).astype(jnp.float32)
    norm_one_out, norm_one_pull = jax.vjp(layer_norm, inputs, norm_gains[0])
    dinput_norm, dgain_one = norm_one_pull(dnormed_one)
    tokens_grad = (
        (dresid + dinput_norm).astype(jnp.bfloat16).reshape(local_len, seq_count, model_width)
    )
    gain_grads = lax.psum(jnp.stack([dgain_one, dgain_two]), ("fsdp", "context"))

    def padded(block, used_rows):
        return jnp.pad(block, ((0, 0), (0, pad_rows - used_rows)))

    left_rows = jnp.concatenate(
        [
            padded(dprojected, counts[0]),
            padded(attn_in, counts[1]),
            padded(dmixed, counts[2]),
            padded(hidden, counts[3]),
        ],
        axis=1,
    )
    right_rows = jnp.stack([act_in, dbranch_one, mlp_in, dbranch_two])
    blocks = local_rows * lax.axis_size(("fsdp", "context")) // pad_rows
    col_block = left_rows.reshape(token_count, blocks, pad_rows)
    grad_block = lax.psum_scatter(
        jnp.einsum(
            "nbp,bnd->bpd", col_block, right_rows, preferred_element_type=jnp.float32
        ).reshape(local_rows * lax.axis_size(("fsdp", "context")), model_width),
        ("fsdp", "context"),
        scatter_dimension=0,
        tiled=True,
    )
    momentum = muon_state.reshape(local_rows, model_width)
    muon_next = muon_beta * momentum + (1.0 - muon_beta) * grad_block
    direction = (1.0 - muon_beta) * grad_block + muon_beta * muon_next
    norm_total = lax.psum(jnp.sum(direction * direction), ("context", "tensor"))
    norm_size = jnp.sqrt(norm_total)
    direction_scale = jnp.log(norm_size).reshape(1)
    ortho_local = direction / (norm_size + ortho_eps)
    ortho_block = lax.all_gather(
        ortho_local.astype(jnp.bfloat16), "context", axis=0, tiled=True
    ).astype(ortho_local.dtype)
    for sweep_index in range(ITERS):
        gram_sum = lax.psum(
            contract_exact(ortho_block, ortho_block).astype(jnp.bfloat16), "tensor"
        ).astype(jnp.float32)
        square = jnp.dot(
            gram_sum, gram_sum, precision=precision_highest, preferred_element_type=jnp.float32
        )
        mix_matrix = ns_second * gram_sum + ns_third * square
        ortho_block = ns_first * ortho_block + jnp.dot(
            ortho_block, mix_matrix, precision=precision_highest, preferred_element_type=jnp.float32
        )
    own_rows = lax.dynamic_slice_in_dim(
        ortho_block, lax.axis_index("context") * local_rows, local_rows, 0
    )
    owner_index = lax.axis_index("fsdp")
    spreads = jnp.array(
        [0.2 * math.sqrt(3 * D), 0.2 * math.sqrt(D), 0.2 * math.sqrt(2 * FF), 0.2 * math.sqrt(FF)],
        jnp.float32,
    )
    spread = jnp.sum(jnp.where(jnp.arange(4) == owner_index, spreads, 0.0))
    old_weight = own_block.astype(jnp.float32)
    weight_update = -muon_rate * (spread * own_rows + decay_rate * old_weight)
    adam_first_next = adam_beta * adam_first + (1.0 - adam_beta) * gain_grads
    adam_second_next = adam_beta * adam_second + (1.0 - adam_beta) * gain_grads * gain_grads
    correction = 1.0 - adam_beta**STEP
    gain_update = -adam_rate * (
        adam_first_next / correction / (jnp.sqrt(adam_second_next / correction) + adam_eps)
        + decay_rate * norm_gains
    )
    block_shape = (1, 1, local_rows, model_width)
    return (
        layer_out,
        tokens_grad,
        grad_block.reshape(block_shape),
        muon_next.reshape(block_shape),
        weight_update.reshape(block_shape),
        direction_scale,
        gain_grads,
        adam_first_next,
        adam_second_next,
        gain_update,
    )


MESH_ID = pl.DeviceIdType.MESH
ANY = pl.ANY


def ring_place(index):
    return index + index // 2 - 2 * (index // 3)


def split_units(rows, parts, unit=16):
    units = rows // unit
    sizes = [(units // parts + (1 if i < units % parts else 0)) * unit for i in range(parts)]
    return [s for s in sizes if s]


def ring_chunks(counts, local_rows, which, core, target):
    first = core * local_rows
    rows = min(counts[which], first + local_rows) - first
    if rows <= 0:
        return [[], []]
    halves = split_units(rows, 2)
    if len(halves) == 1:
        halves = halves + [0]
    out, at = [], first
    for half in halves:
        pieces = []
        if half:
            for size in split_units(half, max(1, round(half / target))):
                pieces.append((at, size))
                at += size
        out.append(pieces)
    return out


class Place:
    def __init__(self):
        self.f = lax.axis_index("fsdp")
        self.c = lax.axis_index("context")
        self.t = lax.axis_index("tensor")
        self.pos = ring_place(self.f)
        self.next = ring_place((self.pos + 1) % 4)
        self.prev = ring_place((self.pos + 3) % 4)
        homes = (0, 1, 3, 2)
        self.hops = [[(self.pos + 4 - home) % 4, (home + 4 - self.pos) % 4] for home in homes]
        self.outer = jnp.logical_or(self.t == 0, self.t == 3)
        self.inner_mate = jnp.where(self.t == 0, 1, 2)
        self.outer_mate = jnp.where(self.t == 1, 0, 3)

    def ring(self, direction):
        return (self.next if direction == 0 else self.prev, self.c, self.t)

    def partner(self):
        return (self.f, 1 - self.c, self.t)

    def chip_z(self, z):
        return (self.f, self.c, z)

    def hop(self, which, direction):
        return self.hops[which][direction]


def greet(place, ring, partner, line):
    barrier = pltpu.get_barrier_semaphore()

    def signal(device):
        pl.semaphore_signal(barrier, inc=1, device_id=device, device_id_type=MESH_ID)

    count = 0
    if ring:
        signal(place.ring(0))
        signal(place.ring(1))
        count += 2
    if partner:
        signal(place.partner())
        count += 1
    if line:
        @pl.when(place.outer)
        def _():
            signal(place.chip_z(place.inner_mate))
            pl.semaphore_wait(barrier, count + 1)

        @pl.when(jnp.logical_not(place.outer))
        def _():
            signal(place.chip_z(place.outer_mate))
            signal(place.chip_z(3 - place.t))
            pl.semaphore_wait(barrier, count + 2)
    else:
        pl.semaphore_wait(barrier, count)


def remote(src, dst, send, recv, device):
    return pltpu.make_async_remote_copy(
        src_ref=src, dst_ref=dst, send_sem=send, recv_sem=recv, device_id=device, device_id_type=MESH_ID
    )


def run_steps(*tracks):
    total = max(len(track) for track in tracks)
    done = [0] * len(tracks)
    for index in range(total):
        for number, track in enumerate(tracks):
            upto = -(-len(track) * (index + 1) // total)
            while done[number] < upto:
                track[done[number]]()
                done[number] += 1


def gather_plan(counts, local_rows, ks, target=96):
    plan = []
    for core in (0, 1):
        ident = 0
        for which in ks:
            for direction, pieces in enumerate(ring_chunks(counts, local_rows, which, core, target)):
                for order, (row, rows) in enumerate(pieces):
                    plan.append((ident, which, core, direction, order, row, rows))
                    ident += 1
    return plan, max(p[0] for p in plan) + 1


def gather_steps(place, plan, local_rows, base, own_ref, out_ref, sems, skew=2):
    ss, rs, sp, rp = sems

    def dst(which, row, rows):
        return out_ref.at[pl.ds(base[which] + row, rows)]

    def src(core, row, rows):
        return own_ref.at[pl.ds(row - core * local_rows, rows)]

    def begin():
        for ident, which, core, direction, order, row, rows in plan:
            @pl.when(jnp.logical_and(place.c == core, place.f == which))
            def _():
                remote(src(core, row, rows), dst(which, row, rows), ss.at[ident], rs.at[ident],
                       place.ring(direction)).start()
        for ident, which, core, direction, order, row, rows in plan:
            @pl.when(jnp.logical_and(place.c == core, place.f == which))
            def _():
                remote(src(core, row, rows), dst(which, row, rows), sp.at[ident], rp.at[ident],
                       place.partner()).start()

    ordered = sorted(plan, key=lambda p: (p[4], p[1]))
    last = max(p[4] for p in plan)

    def visit(item, role):
        ident, which, core, direction, order, row, rows = item
        mine = dst(which, row, rows)

        @pl.when(jnp.logical_and(place.c == core, place.hop(which, direction) == role))
        def _():
            remote(mine, mine, ss.at[ident], rs.at[ident], place.ring(direction)).wait_recv()
            if role <= 2:
                remote(mine, mine, ss.at[ident], rs.at[ident], place.ring(direction)).start()
            remote(mine, mine, sp.at[ident], rp.at[ident], place.partner()).start()

    def step(j):
        def run():
            for role in (1, 2, 3):
                for item in ordered:
                    if item[4] == j - skew * (role - 1):
                        visit(item, role)
        return run

    def ready():
        for ident, which, core, direction, order, row, rows in plan:
            mine = dst(which, row, rows)

            @pl.when(place.c == 1 - core)
            def _():
                remote(mine, mine, sp.at[ident], rp.at[ident], place.partner()).wait_recv()

    def end():
        for ident, which, core, direction, order, row, rows in plan:
            hop = place.hop(which, direction)
            mine = dst(which, row, rows)

            @pl.when(jnp.logical_and(place.c == core, hop <= 2))
            def _():
                remote(mine, mine, ss.at[ident], rs.at[ident], place.ring(direction)).wait_send()

            @pl.when(place.c == core)
            def _():
                remote(mine, mine, sp.at[ident], rp.at[ident], place.partner()).wait_send()

    return begin, [step(j) for j in range(last + 1 + 2 * skew)], ready, end


def line_steps(place, chunks, own, out, early, mid, low, sems, lag=2, back_lag=3, prep=None, done=None):
    s1, r1, s2, r2, s3, r3 = sems

    def from_end(i, device):
        return remote(own(i), early(i), s1.at[i], r1.at[i], device)

    def across(i):
        return remote(mid(i), low(i), s2.at[i], r2.at[i], place.chip_z(3 - place.t))

    def back(i, device):
        return remote(out(i), out(i), s3.at[i], r3.at[i], device)

    def step(i):
        def run():
            if i < chunks and prep is not None:
                prep(i)

            @pl.when(place.outer)
            def _():
                if i < chunks:
                    from_end(i, place.chip_z(place.inner_mate)).start()
                if 0 <= i - lag - back_lag < chunks:
                    back(i - lag - back_lag, place.chip_z(place.inner_mate)).wait_recv()

            @pl.when(jnp.logical_not(place.outer))
            def _():
                if i < chunks:
                    from_end(i, place.chip_z(place.outer_mate)).wait_recv()
                    pair = own(i)[...].astype(jnp.float32) + early(i)[...].astype(jnp.float32)
                    mid(i)[...] = pair.astype(mid(i).dtype)
                    across(i).start()
                j = i - lag
                if 0 <= j < chunks:
                    across(j).wait_recv()
                    total = mid(j)[...].astype(jnp.float32) + low(j)[...].astype(jnp.float32)
                    out(j)[...] = total.astype(out(j).dtype)
                    back(j, place.chip_z(place.outer_mate)).start()
            if done is not None:
                if 0 <= i - lag - back_lag < chunks:
                    done(i - lag - back_lag)
        return run

    def end():
        @pl.when(place.outer)
        def _():
            for i in range(chunks):
                from_end(i, place.chip_z(place.inner_mate)).wait_send()

        @pl.when(jnp.logical_not(place.outer))
        def _():
            for i in range(chunks):
                across(i).wait_send()
                back(i, place.chip_z(place.outer_mate)).wait_send()

    return [step(i) for i in range(chunks + lag + back_lag)], end


def scatter_steps(place, plan, local_rows, base, part_ref, grad_ref, prx, rrx, tx, sems, skew=2):
    ss, rs, sp, rp = sems

    def rows_of(ref, which, row, rows):
        return ref.at[pl.ds(base[which] + row, rows)]

    def partner_copy(item):
        ident, which, core, direction, order, row, rows = item
        return remote(rows_of(part_ref, which, row, rows), rows_of(prx, which, row, rows),
                      sp.at[ident], rp.at[ident], place.partner())

    def ring_copy(item):
        ident, which, core, direction, order, row, rows = item
        return remote(rows_of(tx, which, row, rows), rows_of(rrx, which, row, rows),
                      ss.at[ident], rs.at[ident], place.ring(direction))

    ordered = sorted(plan, key=lambda p: (p[4], p[1]))
    last = max(p[4] for p in plan)

    def begin(ks):
        for item in ordered:
            if item[1] in ks:
                @pl.when(place.c == 1 - item[2])
                def _():
                    partner_copy(item).start()

    def visit(item, late):
        ident, which, core, direction, order, row, rows = item
        hop = place.hop(which, direction)
        role = (late + 1) % 4

        @pl.when(jnp.logical_and(place.c == core, hop == role))
        def _():
            partner_copy(item).wait_recv()
            total = (rows_of(part_ref, which, row, rows)[...].astype(jnp.float32)
                     + rows_of(prx, which, row, rows)[...].astype(jnp.float32))
            if role != 1:
                ring_copy(item).wait_recv()
                total = total + rows_of(rrx, which, row, rows)[...].astype(jnp.float32)
            if role == 0:
                grad_ref[pl.ds(row - core * local_rows, rows)] = total
            else:
                rows_of(tx, which, row, rows)[...] = total.astype(tx.dtype)
                ring_copy(item).start()

    def step(j):
        def run():
            for late in range(4):
                for item in ordered:
                    if item[4] == j - skew * late:
                        visit(item, late)
        return run

    def end():
        for item in plan:
            ident, which, core, direction, order, row, rows = item

            @pl.when(place.c == 1 - core)
            def _():
                partner_copy(item).wait_send()

            @pl.when(jnp.logical_and(place.c == core, place.hop(which, direction) != 0))
            def _():
                ring_copy(item).wait_send()

    return begin, [step(j) for j in range(last + 1 + 3 * skew)], end


VMEM_SPEC = pl.BlockSpec(memory_space=pltpu.VMEM)
ANY_SPEC = pl.BlockSpec(memory_space=pl.ANY)


def dma(count):
    return pltpu.SemaphoreType.DMA((count,))


def comm_call(kernel, outs, ins, in_specs, out_specs, scratch, ident):
    return pl.pallas_call(
        kernel,
        out_shape=outs,
        in_specs=in_specs,
        out_specs=out_specs,
        scratch_shapes=scratch,
        compiler_params=pltpu.CompilerParams(
            collective_id=ident, has_side_effects=True, vmem_limit_bytes=60 * 2**20
        ),
    )(*ins)


def base_rows(counts, ks):
    base, at = {}, 0
    for which in ks:
        base[which] = at
        at += counts[which]
    return base, at


def own_rows_copy(place, counts, local_rows, ks, base, own_ref, out_ref, sem, act):
    for which in ks:
        for core in (0, 1):
            rows = min(counts[which] - core * local_rows, local_rows)
            if rows > 0:
                @pl.when(jnp.logical_and(place.c == core, place.f == which))
                def _():
                    act(pltpu.make_async_copy(
                        own_ref.at[pl.ds(0, rows)],
                        out_ref.at[pl.ds(base[which] + core * local_rows, rows)],
                        sem.at[0],
                    ))


class LineSum:
    def __init__(self, place, rows, own, early, mid, low, total, sems):
        self.place, self.rows = place, rows
        self.own, self.early, self.mid, self.low, self.total = own, early, mid, low, total
        self.sems = sems

    def cut(self, ref, i):
        return ref.at[pl.ds(pl.multiple_of(i * self.rows, self.rows), self.rows)]

    def from_end(self, i, mate):
        s1, r1 = self.sems[:2]
        return remote(self.cut(self.own, i), self.cut(self.early, i), s1.at[i], r1.at[i], self.place.chip_z(mate))

    def across(self, i):
        s2, r2 = self.sems[2:4]
        return remote(self.cut(self.mid, i), self.cut(self.low, i), s2.at[i], r2.at[i], self.place.chip_z(3 - self.place.t))

    def back(self, i, mate):
        s3, r3 = self.sems[4:6]
        return remote(self.cut(self.total, i), self.cut(self.total, i), s3.at[i], r3.at[i], self.place.chip_z(mate))

    def send(self, i):
        @pl.when(self.place.outer)
        def _():
            self.from_end(i, self.place.inner_mate).start()

    def pair_up(self, i):
        @pl.when(jnp.logical_not(self.place.outer))
        def _():
            self.from_end(i, self.place.outer_mate).wait_recv()
            pair = self.cut(self.own, i)[...].astype(jnp.float32) + self.cut(self.early, i)[...].astype(jnp.float32)
            self.cut(self.mid, i)[...] = pair.astype(self.mid.dtype)
            self.across(i).start()

    def join(self, i):
        @pl.when(jnp.logical_not(self.place.outer))
        def _():
            self.across(i).wait_recv()
            whole = self.cut(self.mid, i)[...].astype(jnp.float32) + self.cut(self.low, i)[...].astype(jnp.float32)
            self.cut(self.total, i)[...] = whole.astype(self.total.dtype)
            self.back(i, self.place.outer_mate).start()

    def receive(self, i):
        @pl.when(self.place.outer)
        def _():
            self.back(i, self.place.inner_mate).wait_recv()

    def finish(self, pieces):
        @pl.when(self.place.outer)
        def _():
            for i in range(pieces):
                self.from_end(i, self.place.inner_mate).wait_send()

        @pl.when(jnp.logical_not(self.place.outer))
        def _():
            for i in range(pieces):
                self.across(i).wait_send()
                self.back(i, self.place.outer_mate).wait_send()


def nt_dot(left, right):
    return lax.dot_general(left, right, (((1,), (1,)), ((), ())), preferred_element_type=jnp.float32)


def nn_dot(left, right):
    return jnp.dot(left, right, preferred_element_type=jnp.float32)


def tn_dot(left, right):
    return lax.dot_general(left, right, (((0,), (0,)), ((), ())), preferred_element_type=jnp.float32)


def centred(values):
    centre = values - jnp.mean(values, axis=-1, keepdims=True)
    spread = jnp.mean(centre * centre, axis=-1, keepdims=True)
    return centre, lax.rsqrt(spread + norm_eps)


def norm_back(values, gain_row, grads):
    centre, scale = centred(values)
    xhat = centre * scale
    e = grads * gain_row
    moved = scale * (e - jnp.mean(e, axis=-1, keepdims=True) - xhat * jnp.mean(e * xhat, axis=-1, keepdims=True))
    return moved, jnp.sum(grads * xhat, axis=0, keepdims=True)


def layer_both_ways(tokens, out_grad, own_block, norm_gains, cosine, sine, seg_column, seg_row, counts, ident):
    count, width = tokens.shape
    local_rows = own_block.shape[0]
    inner = counts[1]
    ff = counts[3]
    heads = inner // HEAD_DIM
    full = 2 * count
    rows = count // 4
    sub = rows // 2
    stack = heads * rows
    piece = 64
    score_scale = HEAD_DIM ** (-0.5)
    f32, low = jnp.float32, jnp.bfloat16
    first_plan, first_count = gather_plan(counts, local_rows, (0, 1), 64)
    last_plan, last_count = gather_plan(counts, local_rows, (2, 3), 64)
    first_base, first_rows = base_rows(counts, (0, 1))
    last_base, last_rows = base_rows(counts, (2, 3))

    def kernel(tok_ref, og_ref, own_ref, gain_ref, cos_ref, sin_ref, sc_ref, sr_ref,
               act_ref, attn_ref, resid_ref, mlp_ref, hid_ref, dm_ref, b2_ref, dres_ref, db_ref, dproj_ref, t3_ref, dg_ref,
               w1st, wlast, q_ref, kv_ref, kq_ref, p_ref, s_ref, pl_ref, do_ref, dp_ref, ds_ref,
               t1_ref, e1, m1, l1, sum1, t2_ref, e2, m2, l2, sum2, dq_ref, dkv_ref, dkv_tx, dkv_rx, *sems):
        place = Place()
        greet(place, True, True, True)
        begin1, steps1, ready1, end1 = gather_steps(place, first_plan, local_rows, first_base, own_ref, w1st, sems[0:4], 1)
        begin2, steps2, ready2, end2 = gather_steps(place, last_plan, local_rows, last_base, own_ref, wlast, sems[4:8])
        line1 = LineSum(place, sub, t1_ref, e1, m1, l1, sum1, sems[8:14])
        line2 = LineSum(place, sub, t2_ref, e2, m2, l2, sum2, sems[14:20])
        swap, local_sem = sems[20], sems[21]

        begin1()
        own_rows_copy(place, counts, local_rows, (0, 1), first_base, own_ref, w1st, local_sem, lambda d: d.start())

        def at(i, size=rows):
            return pl.ds(pl.multiple_of(i * size, size), size)

        def norm_one(i, carry):
            centre, scale = centred(tok_ref[at(i)].astype(f32))
            act_ref[at(i)] = (centre * scale * gain_ref[0:1]).astype(low)
            return carry

        lax.fori_loop(0, 4, norm_one, 0)
        dg_ref[...] = jnp.zeros_like(dg_ref)
        begin2()
        run_steps(steps1)
        own_rows_copy(place, counts, local_rows, (0, 1), first_base, own_ref, w1st, local_sem, lambda d: d.wait())
        own_rows_copy(place, counts, local_rows, (2, 3), last_base, own_ref, wlast, local_sem, lambda d: d.start())
        ready1()
        waiting = list(steps2)

        def forward(number):
            for step in waiting[:number]:
                step()
            del waiting[:number]

        forward(1)

        lane = lax.broadcasted_iota(jnp.int32, (1, inner), 1)
        front = (lane % HEAD_DIM) < HEAD_DIM // 2

        def half_turn(value):
            return jnp.where(front, pltpu.roll(value, inner - HEAD_DIM // 2, 1), pltpu.roll(value, HEAD_DIM // 2, 1))

        sign = jnp.where(front, -1.0, 1.0).astype(f32)

        def rotated(value, i):
            return value * cos_ref[at(i)] + half_turn(value) * (sin_ref[at(i)] * sign)

        def rotated_back(value, i):
            return value * cos_ref[at(i)] - half_turn(value * sin_ref[at(i)]) * sign

        def project_rows(i, carry):
            value = nt_dot(act_ref[at(i)], w1st[0:3 * inner])
            q_ref[at(i)] = rotated(value[:, 0:inner], i).astype(low)
            kv_ref[at(i), 0:inner] = rotated(value[:, inner:2 * inner], i).astype(low)
            kv_ref[at(i), inner:2 * inner] = value[:, 2 * inner:3 * inner].astype(low)
            return carry

        lax.fori_loop(0, 4, project_rows, 0)
        kv_copy = remote(kv_ref.at[pl.ds(0, count)], kv_ref.at[pl.ds(count, count)], swap.at[0], swap.at[1], place.partner())
        kv_copy.start()
        forward(2)
        kv_copy.wait()

        def head_mask(h):
            return jnp.logical_and(lane >= h * HEAD_DIM, lane < (h + 1) * HEAD_DIM)

        def stacked(value):
            return jnp.concatenate([jnp.where(head_mask(h), value, jnp.zeros_like(value)) for h in range(heads)], axis=0)

        def unstacked(value):
            total = jnp.where(head_mask(0), value[0:rows], 0.0)
            for h in range(1, heads):
                total = total + jnp.where(head_mask(h), value[h * rows:(h + 1) * rows], 0.0)
            return total

        per = rows // piece

        def attend(i):
            kq_ref[...] = stacked(q_ref[at(i)])
            s_ref[...] = nt_dot(kq_ref[...], kv_ref[:, 0:inner])

            def soft(r, inside):
                seg = sc_ref[pl.ds(pl.multiple_of(i * rows + (r % per) * piece, piece), piece)]
                score = jnp.where(seg == sr_ref[...], s_ref[at(r, piece)] * score_scale, -jnp.inf)
                score = jnp.exp(score - jnp.max(score, axis=-1, keepdims=True))
                prob = score * (1.0 / jnp.sum(score, axis=-1, keepdims=True))
                p_ref[i, at(r, piece)] = prob
                pl_ref[at(r, piece)] = prob.astype(low)
                return inside

            lax.fori_loop(0, stack // piece, soft, 0)
            mixed = unstacked(nn_dot(pl_ref[...], kv_ref[:, inner:2 * inner]))
            keep = (sc_ref[at(i)] > 0).astype(f32)
            attn = (mixed * keep).astype(low)
            attn_ref[at(i)] = attn
            t1_ref[at(i)] = nn_dot(attn, w1st[3 * inner:4 * inner]).astype(low)
            for part in range(2):
                line1.send(2 * i + part)

            if i >= 1:
                line1.pair_up(2 * i - 2)
                line1.pair_up(2 * i - 1)
            if i >= 2:
                line1.join(2 * i - 4)
                line1.join(2 * i - 3)

        for i in range(4):
            attend(i)
            forward(2)
        forward(len(waiting))
        own_rows_copy(place, counts, local_rows, (2, 3), last_base, own_ref, wlast, local_sem, lambda d: d.wait())
        ready2()

        def feed(i, carry):
            for part in range(2):
                line1.receive(2 * i + part)
            resid = tok_ref[at(i)].astype(f32) + sum1[at(i)].astype(f32)
            resid_ref[at(i)] = resid
            centre, scale = centred(resid)
            mlp = (centre * scale * gain_ref[1:2]).astype(low)
            mlp_ref[at(i)] = mlp
            gate = nt_dot(mlp, wlast[0:ff])
            up = nt_dot(mlp, wlast[ff:2 * ff])
            cdf = 0.5 * (1.0 + lax.erf(gate * (0.5 ** 0.5)))
            bell = jnp.exp(gate * gate * -0.5) * (1.0 / math.sqrt(2.0 * math.pi))
            gelu = gate * cdf
            hidden = (gelu * up).astype(low)
            hid_ref[at(i)] = hidden
            dhidden = nt_dot(og_ref[at(i)], wlast[2 * ff:3 * ff])
            dgate = (dhidden * up * (cdf + gate * bell)).astype(low)
            dup = (dhidden * gelu).astype(low)
            dm_ref[0, at(i)] = dgate
            dm_ref[1, at(i)] = dup
            t2_ref[at(i)] = (nn_dot(dgate, wlast[0:ff]) + nn_dot(dup, wlast[ff:2 * ff])).astype(low)
            for part in range(2):
                line2.send(2 * i + part)
            b2_ref[at(i)] = nn_dot(hidden, wlast[2 * ff:3 * ff]).astype(low)

            @pl.when(i == 0)
            def _():
                line1.pair_up(6)
                line1.pair_up(7)

            @pl.when(i <= 1)
            def _():
                line1.join(2 * i + 4)
                line1.join(2 * i + 5)

            @pl.when(i >= 1)
            def _():
                line2.pair_up(2 * i - 2)
                line2.pair_up(2 * i - 1)

            @pl.when(i >= 2)
            def _():
                line2.join(2 * i - 4)
                line2.join(2 * i - 3)
            return carry

        lax.fori_loop(0, 4, feed, 0)
        dkv_ref[...] = jnp.zeros_like(dkv_ref)

        def turn_back(i, carry):
            for part in range(2):
                line2.receive(2 * i + part)
            moved, gain_part = norm_back(resid_ref[at(i)], gain_ref[1:2], sum2[at(i)].astype(f32))
            dg_ref[1:2] = dg_ref[1:2] + gain_part
            dresid = og_ref[at(i)].astype(f32) + moved
            dres_ref[at(i)] = dresid
            dbranch = dresid.astype(low)
            db_ref[at(i)] = dbranch
            keep = (sc_ref[at(i)] > 0).astype(low)
            dattn = nt_dot(dbranch, w1st[3 * inner:4 * inner]).astype(low) * keep
            do_ref[...] = stacked(dattn)
            kq_ref[...] = stacked(q_ref[at(i)])
            dp_ref[...] = nt_dot(do_ref[...], kv_ref[:, inner:2 * inner])

            def soft_back(r, inside):
                prob = p_ref[i, at(r, piece)]
                dprob = dp_ref[at(r, piece)]
                delta = jnp.sum(prob * dprob, axis=-1, keepdims=True)
                ds_ref[at(r, piece)] = (prob * (dprob - delta) * score_scale).astype(low)
                pl_ref[at(r, piece)] = prob.astype(low)
                return inside

            lax.fori_loop(0, stack // piece, soft_back, 0)
            dq_ref[at(i)] = unstacked(nn_dot(ds_ref[...], kv_ref[:, 0:inner]))
            dkv_ref[:, 0:inner] = dkv_ref[:, 0:inner] + tn_dot(ds_ref[...], kq_ref[...])
            dkv_ref[:, inner:2 * inner] = dkv_ref[:, inner:2 * inner] + tn_dot(pl_ref[...], do_ref[...])

            @pl.when(i == 0)
            def _():
                line2.pair_up(6)
                line2.pair_up(7)

            @pl.when(i <= 1)
            def _():
                line2.join(2 * i + 4)
                line2.join(2 * i + 5)
            return carry

        lax.fori_loop(0, 4, turn_back, 0)
        dkv_tx[...] = dkv_ref[count:full].astype(low)
        dkv_copy = remote(dkv_tx, dkv_rx, swap.at[2], swap.at[3], place.partner())
        dkv_copy.start()

        def unproject_query(i, carry):
            dproj_ref[at(i), 0:inner] = rotated_back(dq_ref[at(i)], i).astype(low)
            return carry

        lax.fori_loop(0, 4, unproject_query, 0)
        dkv_copy.wait()

        def unproject(i, carry):
            both = dkv_ref[at(i)] + dkv_rx[at(i)].astype(f32)
            dproj_ref[at(i), inner:2 * inner] = rotated_back(both[:, 0:inner], i).astype(low)
            dproj_ref[at(i), 2 * inner:3 * inner] = both[:, inner:2 * inner].astype(low)
            t3_ref[at(i)] = nn_dot(dproj_ref[at(i)], w1st[0:3 * inner]).astype(low)
            return carry

        lax.fori_loop(0, 4, unproject, 0)
        line1.finish(8)
        line2.finish(8)
        end1()
        end2()

    def shape(*dims, dtype=low):
        return jax.ShapeDtypeStruct(dims, dtype)

    outs = (
        shape(count, width), shape(count, inner), shape(count, width, dtype=f32), shape(count, width), shape(count, ff),
        shape(2, count, ff), shape(count, width), shape(count, width, dtype=f32), shape(count, width),
        shape(count, 3 * inner), shape(count, width), shape(8, width, dtype=f32),
    )
    line = pltpu.VMEM((count, width), low)
    scratch = [
        pltpu.VMEM((first_rows, width), low), pltpu.VMEM((last_rows, width), low), pltpu.VMEM((count, inner), low),
        pltpu.VMEM((full, 2 * inner), low), pltpu.VMEM((stack, inner), low), pltpu.VMEM((4, stack, full), f32),
        pltpu.VMEM((stack, full), f32), pltpu.VMEM((stack, full), low), pltpu.VMEM((stack, inner), low),
        pltpu.VMEM((stack, full), f32), pltpu.VMEM((stack, full), low),
    ]
    scratch += [line] * 10
    scratch += [
        pltpu.VMEM((count, inner), f32), pltpu.VMEM((full, 2 * inner), f32),
        pltpu.VMEM((count, 2 * inner), low), pltpu.VMEM((count, 2 * inner), low),
    ]
    scratch += [dma(first_count)] * 4 + [dma(last_count)] * 4 + [dma(8)] * 12 + [dma(4), dma(1)]
    ins = (tokens, out_grad, own_block, norm_gains, cosine, sine, seg_column, seg_row)
    return pl.pallas_call(
        kernel,
        out_shape=outs,
        in_specs=[VMEM_SPEC] * len(ins),
        out_specs=(VMEM_SPEC,) * len(outs),
        scratch_shapes=scratch,
        compiler_params=pltpu.CompilerParams(
            collective_id=ident, has_side_effects=True, vmem_limit_bytes=67043328
        ),
    )(*ins)


def tail_grams(left_right, muon_rows, counts, ident):
    dproj, act_in, attn_in, dbranch, dmixed, mlp_in, hidden, out_low = left_right
    local_rows, width = muon_rows.shape
    ks = (0, 1, 2, 3)
    plan, count = gather_plan(counts, local_rows, ks, 96)
    base, total_rows = base_rows(counts, ks)
    ff = counts[3]
    tile = width // 4
    half = tile // 2
    chunks = 10
    f32, low16 = jnp.float32, jnp.bfloat16

    def kernel(dp_ref, act_ref, at_ref, db_ref, dm_ref, mlp_ref, hid_ref, og_ref, mu_ref,
               grad_ref, x_ref, g_ref, norm_ref,
               part, prx, rrx, mine, theirs, gprx, tot, other, early, mid, low, norm_own, *sems):
        place = Place()
        c = place.c
        greet(place, True, True, True)
        begin, steps, end = scatter_steps(place, plan, local_rows, base, part, grad_ref, prx, rrx, part, sems[:4])

        def terms(row, left, right):
            span = left.shape[1]

            def columns(j, carry):
                cols = pl.ds(pl.multiple_of(j * tile, tile), tile)
                part[pl.ds(row, span), cols] = tn_dot(left[...], right[:, cols]).astype(low16)
                return carry

            lax.fori_loop(0, 4, columns, 0)

        terms(base[2], dm_ref.at[0], mlp_ref)
        terms(base[2] + ff, dm_ref.at[1], mlp_ref)
        begin((2,))
        terms(base[3], hid_ref, og_ref)
        begin((3,))
        terms(base[0], dp_ref, act_ref)
        begin((0,))
        terms(base[1], at_ref, db_ref)
        begin((1,))
        grad_ref[...] = jnp.zeros_like(grad_ref)
        run_steps(steps)
        end()

        def momentum(i, carry):
            sl = pl.ds(pl.multiple_of(i * 16, 16), 16)
            grad = grad_ref[sl]
            after = muon_beta * mu_ref[sl] + (1.0 - muon_beta) * grad
            direction = (1.0 - muon_beta) * grad + muon_beta * after
            x_ref[sl] = direction.astype(low16)
            square = direction * direction
            return carry + square[0:8] + square[8:16]

        square = lax.fori_loop(0, local_rows // 16, momentum, jnp.zeros((8, width), f32))
        own_square = jnp.broadcast_to(jnp.sum(jnp.sum(square, axis=1, keepdims=True), axis=0, keepdims=True), (8, tile))
        norm_own[...] = own_square

        sp, rp, st, rt = sems[10:14]

        def blocks(core):
            return [(3 * core, 3 * core), (2 * core, 2 * core + 1), (core + 1, core + 1), (core, core + 2), (core, 3 - core)]

        def at(k):
            return pl.ds(pl.multiple_of(k * tile, tile), tile)

        def gram(i, j):
            return tn_dot(x_ref[:, at(i)], x_ref[:, at(j)])

        def partner(n):
            sl = pl.ds(n * tile, tile)
            return remote(theirs.at[sl], gprx.at[sl], sp.at[n], rp.at[n], place.partner())

        def norm_row(ref):
            return ref.at[pl.ds(5 * tile, 8)]

        for n, (i, j) in enumerate(blocks(1 - c)):
            theirs[pl.ds(n * tile, tile)] = gram(i, j)
            partner(n).start()
        norm_row(theirs)[...] = norm_own[...]
        pn = remote(norm_row(theirs), norm_row(gprx), sp.at[5], rp.at[5], place.partner())
        pn.start()

        def span(i):
            return pl.ds(i * half, half) if i < chunks - 1 else pl.ds(i * half, half + 8)

        def cut(ref):
            return lambda i: ref.at[span(i)]

        def prep(i):
            if i % 2 == 0:
                n = i // 2
                sl = pl.ds(n * tile, tile)
                block = gram(*blocks(c)[n])
                partner(n).wait_recv()
                mine[sl] = block + gprx[sl]
            if i == chunks - 1:
                pn.wait_recv()
                norm_row(mine)[...] = norm_row(gprx)[...] + norm_own[...]

        def share(i):
            return remote(cut(tot)(i), cut(other)(i), st.at[i], rt.at[i], place.partner())

        def place_block(ref, n, core):
            i, j = blocks(core)[n]
            block = ref[pl.ds(n * tile, tile)]
            g_ref[at(i), at(j)] = block
            g_ref[at(j), at(i)] = block.T

        def done(i):
            share(i).start()
            if i % 2 == 1:
                place_block(tot, i // 2, c)
            if i >= 2:
                share(i - 2).wait_recv()
                if (i - 2) % 2 == 1:
                    place_block(other, (i - 2) // 2, 1 - c)

        line, line_end = line_steps(place, chunks, cut(mine), cut(tot), cut(early), cut(mid), cut(low), sems[4:10],
                                    prep=prep, done=done)
        run_steps(line)
        for i in (chunks - 2, chunks - 1):
            share(i).wait_recv()
        place_block(other, 4, 1 - c)
        norm_ref[...] = jnp.broadcast_to(tot[5 * tile:5 * tile + 8, 0:128], (8, 128))
        line_end()
        for n in range(5):
            partner(n).wait_send()
        pn.wait_send()
        for i in range(chunks):
            share(i).wait_send()

    rows_low = pltpu.VMEM((total_rows, width), low16)
    packed = pltpu.VMEM((5 * tile + 8, tile), f32)
    outs = (
        jax.ShapeDtypeStruct((local_rows, width), f32),
        jax.ShapeDtypeStruct((local_rows, width), low16), jax.ShapeDtypeStruct((width, width), f32),
        jax.ShapeDtypeStruct((8, 128), f32),
    )
    scratch = [rows_low] * 3 + [packed] * 8 + [pltpu.VMEM((8, tile), f32)]
    scratch += [dma(count)] * 4 + [dma(chunks)] * 6 + [dma(6), dma(6), dma(chunks), dma(chunks)]
    ins = tuple(left_right) + (muon_rows,)
    return comm_call(kernel, outs, ins, [VMEM_SPEC] * len(ins), (VMEM_SPEC,) * len(outs), scratch, ident)


def halves(value):
    high = value.astype(jnp.bfloat16)
    return high, (value - high.astype(jnp.float32)).astype(jnp.bfloat16)


def iterate(gram, norm, direction_low, normed_term, branch_term, tokens_in, resid, dresid, dgain_rows, norm_gains, adam_first,
            adam_second, ident):
    rows, width = direction_low.shape
    tile = 256
    parts = width // tile
    tokens = branch_term.shape[0]
    each = 8
    chunks = 2 * each
    step_rows = tokens // each
    aa = ns_first * ns_first
    ab = 2.0 * ns_first * ns_second
    bbac = ns_second * ns_second + 2.0 * ns_first * ns_third
    bc = 2.0 * ns_second * ns_third
    cc = ns_third * ns_third
    correction = 1.0 - adam_beta**STEP

    def kernel(g_ref, n_ref, d_ref, t3_ref, b2_ref, tok_ref, r_ref, dres_ref, dgr_ref, gain_ref, af_ref, as_ref,
               x_ref, lo_ref, tg_ref, gg_ref, afn_ref, asn_ref, gu_ref,
               p_ref, ph, pl_, hh, hl, uh, ul, mx, early, mid, low, total, held, dg_ref, *sems):
        place = Place()
        s1, r1, s2, r2, s3, r3, sg, rg = sems
        me = place.f * 2 + place.c
        barrier = pltpu.get_barrier_semaphore()

        def plane(shift):
            other = (me + shift) % 8
            return (other // 2, other % 2, place.t)

        for shift in range(1, 8):
            pl.semaphore_signal(barrier, inc=1, device_id=plane(shift), device_id_type=MESH_ID)

        @pl.when(place.outer)
        def _():
            pl.semaphore_signal(barrier, inc=1, device_id=place.chip_z(place.inner_mate), device_id_type=MESH_ID)
            pl.semaphore_wait(barrier, 8)

        @pl.when(jnp.logical_not(place.outer))
        def _():
            pl.semaphore_signal(barrier, inc=1, device_id=place.chip_z(place.outer_mate), device_id_type=MESH_ID)
            pl.semaphore_signal(barrier, inc=1, device_id=place.chip_z(3 - place.t), device_id_type=MESH_ID)
            pl.semaphore_wait(barrier, 9)

        def cut(ref, i):
            if isinstance(i, int):
                return ref.at[pl.ds(i * step_rows, step_rows)]
            return ref.at[pl.ds(pl.multiple_of(i * step_rows, step_rows), step_rows)]

        def from_end(i, device, own):
            local = i % each
            return remote(cut(own, local), cut(early, i), s1.at[i], r1.at[i], device)

        def across(i):
            return remote(cut(mid, i), cut(low, i), s2.at[i], r2.at[i], place.chip_z(3 - place.t))

        def back(i, device):
            return remote(cut(total, i), cut(total, i), s3.at[i], r3.at[i], device)

        dg_ref[...] = jnp.zeros_like(dg_ref)

        @pl.when(place.outer)
        def _():
            for i in range(each):
                from_end(i, place.chip_z(place.inner_mate), t3_ref).start()
            for i in range(each):
                from_end(each + i, place.chip_z(place.inner_mate), b2_ref).start()

        def pair_up(i, own):
            @pl.when(jnp.logical_not(place.outer))
            def _():
                from_end(i, place.chip_z(place.outer_mate), own).wait_recv()
                pair = cut(own, i % each)[...].astype(jnp.float32) + cut(early, i)[...].astype(jnp.float32)
                cut(mid, i)[...] = pair.astype(mid.dtype)
                across(i).start()

        def pair_some(first):
            for part in range(4):
                @pl.when(first + part < each)
                def _():
                    pair_up(first + part, t3_ref)

                @pl.when(first + part >= each)
                def _():
                    pair_up(first + part, b2_ref)

        def join_some(first):
            for part in range(2):
                join(first + part)

        def join(i):
            @pl.when(jnp.logical_not(place.outer))
            def _():
                across(i).wait_recv()
                whole = cut(mid, i)[...].astype(jnp.float32) + cut(low, i)[...].astype(jnp.float32)
                cut(total, i)[...] = whole.astype(total.dtype)
                back(i, place.chip_z(place.outer_mate)).start()

        norm_size = jnp.sqrt(n_ref[0:1, 0:1])
        inverse = 1.0 / (norm_size + ortho_eps)
        scale = inverse * inverse

        for k in range(parts):
            sl = pl.ds(k * tile, tile)
            value = g_ref[sl] * scale
            p_ref[sl] = value
            high, rest = halves(value)
            ph[sl] = high
            pl_[sl] = rest
        x_ref[...] = d_ref[...].astype(jnp.float32) * inverse

        def product(lh, ll, rh, rl, k):
            sl, cols = pl.ds(k * tile, tile), pl.ds(k * tile, width - k * tile)

            def dot(left, right):
                return jnp.dot(left[sl], right[:, cols], preferred_element_type=jnp.float32)

            return dot(lh, rh) + dot(ll, rh) + dot(lh, rl)

        def spread_out(value, high_ref, low_ref, k):
            sl, cols = pl.ds(k * tile, tile), pl.ds(k * tile, width - k * tile)
            high, rest = halves(value)
            high_ref[sl, cols] = high
            low_ref[sl, cols] = rest
            for j in range(k + 1, parts):
                at = (j - k) * tile
                high_ref[pl.ds(j * tile, tile), sl] = high[:, at:at + tile].T
                low_ref[pl.ds(j * tile, tile), sl] = rest[:, at:at + tile].T

        def squares():
            for k in range(parts):
                sl, cols = pl.ds(k * tile, tile), pl.ds(k * tile, width - k * tile)
                value = product(ph, pl_, ph, pl_, k)
                spread_out(value, hh, hl, k)
                mix = (ns_second * p_ref[sl, cols] + ns_third * value).astype(mx.dtype)
                mx[sl, cols] = mix
                for j in range(k + 1, parts):
                    at = (j - k) * tile
                    mx[pl.ds(j * tile, tile), sl] = mix[:, at:at + tile].T

        def rotate_rows():
            for at, size in ((0, 336), (336, 320)):
                sl = pl.ds(at, size)
                old = x_ref[sl]
                x_ref[sl] = ns_first * old + jnp.dot(old.astype(jnp.bfloat16), mx[...], preferred_element_type=jnp.float32)

        def gains_copy(shift):
            return remote(dg_ref, held.at[me], sg.at[shift], rg.at[shift], plane(shift))

        def first_norm_back():
            @pl.when(place.outer)
            def _():
                for i in range(each):
                    back(i, place.chip_z(place.inner_mate)).wait_recv()

            def some(i, inside):
                sl = pl.ds(pl.multiple_of(i * 64, 64), 64)
                moved, gain_part = norm_back(tok_ref[sl].astype(jnp.float32), gain_ref[0:1], total[sl].astype(jnp.float32))
                dg_ref[0:1] = dg_ref[0:1] + gain_part
                tg_ref[sl] = (dres_ref[sl] + moved).astype(tg_ref.dtype)
                return inside

            lax.fori_loop(0, tokens // 64, some, 0)
            dg_ref[1:2] = dgr_ref[1:2]
            held[pl.ds(me, 1)] = dg_ref[...][None]
            for shift in range(1, 8):
                gains_copy(shift).start()

        def body(sweep, carry):
            middle = jnp.logical_and(sweep >= 1, sweep < ITERS - 1)

            @pl.when(sweep == ITERS - 1)
            def _():
                join_some(4 * sweep - 4)
            squares()

            @pl.when(middle)
            def _():
                join_some(4 * sweep - 4)

            @pl.when(sweep == ITERS - 1)
            def _():
                join_some(4 * sweep - 2)
            rotate_rows()

            @pl.when(middle)
            def _():
                pair_some(4 * sweep)

            @pl.when(sweep < ITERS - 1)
            def _():
                for k in range(parts):
                    sl, cols = pl.ds(k * tile, tile), pl.ds(k * tile, width - k * tile)
                    cube = product(ph, pl_, hh, hl, k)
                    square = hh[sl, cols].astype(jnp.float32) + hl[sl, cols].astype(jnp.float32)
                    spread_out(bc * square + cc * cube, uh, ul, k)
                    p_ref[sl, cols] = aa * p_ref[sl, cols] + ab * square + bbac * cube

                @pl.when(sweep >= 1)
                def _():
                    join_some(4 * sweep - 2)

                @pl.when(sweep == 0)
                def _():
                    pair_some(0)
                for k in range(parts):
                    sl, cols = pl.ds(k * tile, tile), pl.ds(k * tile, width - k * tile)
                    value = p_ref[sl, cols] + product(hh, hl, uh, ul, k)
                    p_ref[sl, cols] = value
                    spread_out(value, ph, pl_, k)

            @pl.when(sweep == ITERS - 2)
            def _():
                first_norm_back()
            return carry

        lax.fori_loop(0, ITERS, body, 0)
        for shift in range(1, 8):
            gains_copy(shift).wait()
        grads = held[0]
        for k in range(1, 8):
            grads = grads + held[k]
        grads = grads[0:2]
        gg_ref[...] = grads
        first = adam_beta * af_ref[...] + (1.0 - adam_beta) * grads
        second = adam_beta * as_ref[...] + (1.0 - adam_beta) * grads * grads
        afn_ref[...] = first
        asn_ref[...] = second
        gu_ref[...] = -adam_rate * (
            first / correction / (jnp.sqrt(second / correction) + adam_eps) + decay_rate * gain_ref[...]
        )

        @pl.when(place.outer)
        def _():
            for i in range(each, chunks):
                back(i, place.chip_z(place.inner_mate)).wait_recv()
            for i in range(each):
                from_end(i, place.chip_z(place.inner_mate), t3_ref).wait_send()
                from_end(each + i, place.chip_z(place.inner_mate), b2_ref).wait_send()
        lo_ref[...] = (r_ref[...] + total[tokens:2 * tokens].astype(jnp.float32)).astype(lo_ref.dtype)

        @pl.when(jnp.logical_not(place.outer))
        def _():
            for i in range(chunks):
                across(i).wait_send()
                back(i, place.chip_z(place.outer_mate)).wait_send()

    f32, low16 = jnp.float32, jnp.bfloat16
    small = jax.ShapeDtypeStruct(norm_gains.shape, f32)
    narrow = jax.ShapeDtypeStruct((tokens, width), low16)
    outs = (jax.ShapeDtypeStruct((rows, width), f32), narrow, narrow, small, small, small, small)
    full = pltpu.VMEM((width, width), low16)
    line = pltpu.VMEM((2 * tokens, width), low16)
    scratch = [pltpu.VMEM((width, width), f32)] + [full] * 7 + [line] * 4
    scratch += [pltpu.VMEM((8, 8, width), f32), pltpu.VMEM((8, width), f32)] + [dma(chunks)] * 6 + [dma(8)] * 2
    ins = (gram, norm, direction_low, normed_term, branch_term, tokens_in, resid, dresid, dgain_rows, norm_gains,
           adam_first, adam_second)
    return comm_call(kernel, outs, ins, [VMEM_SPEC] * len(ins), (VMEM_SPEC,) * len(outs), scratch, ident)


def per_device_block(tokens, out_grad, weight_stack, muon_state, norm_gains, adam_first, adam_second, segment_ids,
                     position_ids):
    token_count, _, model_width = tokens.shape
    groups, contexts = 4, 2
    full_len = token_count * contexts
    local_rows = weight_stack.shape[2]
    heads_dev = HEADS // groups
    ff_dev = FF // groups
    inner_width = heads_dev * HEAD_DIM
    counts = (3 * inner_width, inner_width, 2 * ff_dev, ff_dev)
    own_block = weight_stack.reshape(local_rows, model_width)
    context = lax.axis_index("context")

    cosine, sine_table = rope_tables(position_ids.reshape(token_count), HEAD_DIM)
    segments = segment_ids.reshape(full_len)
    seg_query = lax.dynamic_slice_in_dim(segments, context * token_count, token_count, 0)
    seg_other = lax.dynamic_slice_in_dim(segments, (1 - context) * token_count, token_count, 0)
    (act_in, attn_in, resid, mlp_in, hidden, dmixed, branch_two_term, dresid, dbranch_one, dprojected, dnormed_one_term,
     dgain_rows) = layer_both_ways(
        tokens.reshape(token_count, model_width), out_grad.reshape(token_count, model_width), own_block, norm_gains,
        jnp.tile(cosine, (1, heads_dev)), jnp.tile(sine_table, (1, heads_dev)),
        seg_query.reshape(token_count, 1), jnp.concatenate([seg_query, seg_other]).reshape(1, full_len), counts, 0,
    )
    momentum = muon_state.reshape(local_rows, model_width)
    grad_block, direction_low, gram, norm_total = tail_grams(
        (dprojected, act_in, attn_in, dbranch_one, dmixed, mlp_in, hidden, out_grad.reshape(token_count, model_width)),
        momentum, counts, 1,
    )
    direction_scale = jnp.log(jnp.sqrt(norm_total[0, 0])).reshape(1)
    ortho, layer_out, tokens_grad, gain_grads, adam_first_next, adam_second_next, gain_update = iterate(
        gram, norm_total, direction_low, dnormed_one_term, branch_two_term,
        tokens.reshape(token_count, model_width), resid, dresid, dgain_rows, norm_gains, adam_first, adam_second, 2,
    )
    muon_next = muon_beta * momentum + (1.0 - muon_beta) * grad_block
    owner_index = lax.axis_index("fsdp")
    spreads = [0.2 * math.sqrt(3 * D), 0.2 * math.sqrt(D), 0.2 * math.sqrt(2 * FF), 0.2 * math.sqrt(FF)]
    spread = jnp.sum(jnp.where(jnp.arange(4) == owner_index, jnp.array(spreads, jnp.float32), 0.0))
    weight_update = -muon_rate * (spread * ortho + decay_rate * own_block.astype(jnp.float32))
    layer_out = layer_out.reshape(tokens.shape)
    tokens_grad = tokens_grad.reshape(tokens.shape)
    block_shape = (1, 1, local_rows, model_width)
    return (
        layer_out,
        tokens_grad,
        grad_block.reshape(block_shape),
        muon_next.reshape(block_shape),
        weight_update.reshape(block_shape),
        direction_scale,
        gain_grads,
        adam_first_next,
        adam_second_next,
        gain_update,
    )


def solution(mesh):
    sizes = dict(mesh.shape)
    block = (sizes["fsdp"], sizes["context"], sizes["tensor"]) == (4, 2, 4)
    return jax.shard_map(
        per_device_block if block else per_device,
        mesh=mesh,
        in_specs=(
            P("context", "fsdp", None),
            P("context", "fsdp", None),
            P("fsdp", "tensor", "context", None),
            P("fsdp", "tensor", "context", None),
            P(),
            P(),
            P(),
            P(None, "fsdp"),
            P("context", "fsdp"),
        ),
        out_specs=(
            P("context", "fsdp", None),
            P("context", "fsdp", None),
            P("fsdp", "tensor", "context", None),
            P("fsdp", "tensor", "context", None),
            P("fsdp", "tensor", "context", None),
            P("fsdp"),
            P(),
            P(),
            P(),
            P(),
        ),
        check_vma=False,
    )
```

```python
import math

import jax
import jax.numpy as jnp
from jax import lax
from jax.experimental import pallas as pl
from jax.experimental.pallas import tpu as pltpu
from jax.sharding import PartitionSpec as P

D = 1024
HEADS = 16
HEAD_DIM = 64
FF = 2624
ITERS = 5
STEP = 8


rope_base = 160000.0
norm_eps = 1e-05
ns_first = 3.4445
ns_second = -4.775
ns_third = 2.0315
muon_beta = 0.5
muon_rate = 0.15
decay_rate = 0.1
adam_beta = 0.5
adam_rate = 0.05
ortho_eps = 1e-07
adam_eps = 1e-08
precision_highest = lax.Precision.HIGHEST


def layer_norm(values, gain_row):
    centre = values - jnp.mean(values, axis=-1, keepdims=True)
    spread = jnp.mean(centre * centre, axis=-1, keepdims=True)
    return centre * lax.rsqrt(spread + norm_eps) * gain_row


def rope_tables(positions, head_width):
    half_width = head_width // 2
    freqs = rope_base ** (-(jnp.arange(half_width, dtype=jnp.float32) * 2.0 / head_width))
    angle = positions.astype(jnp.float32)[..., None] * freqs
    angle = jnp.concatenate([angle, angle], axis=-1)
    return (jnp.cos(angle), jnp.sin(angle))


def rotate(values, cosine, sine_table):
    half_width = values.shape[-1] // 2
    turned = jnp.concatenate([-values[..., half_width:], values[..., :half_width]], axis=-1)
    return values * cosine + turned * sine_table


def rotate_back(grads_in, cosine, sine_table):
    half_width = grads_in.shape[-1] // 2
    scaled = grads_in * sine_table
    turned = jnp.concatenate([scaled[..., half_width:], -scaled[..., :half_width]], axis=-1)
    return grads_in * cosine + turned


def project(left_rows, right_rows):
    return lax.dot_general(
        left_rows, right_rows, (((1,), (1,)), ((), ())), preferred_element_type=jnp.float32
    )


def contract_exact(left_rows, right_rows):
    return lax.dot_general(
        left_rows,
        right_rows,
        (((0,), (0,)), ((), ())),
        precision=precision_highest,
        preferred_element_type=jnp.float32,
    )


def geglu_gate(gate_part, up_part):
    return jax.nn.gelu(gate_part, approximate=False) * up_part


def per_device(
    tokens,
    out_grad,
    weight_stack,
    muon_state,
    norm_gains,
    adam_first,
    adam_second,
    segment_ids,
    position_ids,
):
    local_len, seq_count, model_width = tokens.shape
    token_count = local_len * seq_count
    groups = lax.axis_size("tensor")
    contexts = lax.axis_size("context")
    full_len = local_len * contexts
    local_rows = weight_stack.shape[2]
    pad_rows = local_rows * contexts
    heads_dev = HEADS // groups
    ff_dev = FF // groups
    inner_width = heads_dev * HEAD_DIM
    counts = (3 * inner_width, inner_width, 2 * ff_dev, ff_dev)
    score_scale = HEAD_DIM ** (-0.5)
    own_block = weight_stack.reshape(local_rows, model_width)
    gathered = lax.all_gather(own_block, ("fsdp", "context"), axis=0, tiled=True).reshape(
        4, pad_rows, model_width
    )
    w_qkv = gathered[0, : counts[0]]
    w_out = gathered[1, : counts[1]]
    w_in = gathered[2, : counts[2]]
    w_down = gathered[3, : counts[3]]
    inputs = tokens.astype(jnp.float32).reshape(token_count, model_width)
    act_in = layer_norm(inputs, norm_gains[0]).astype(jnp.bfloat16)
    projected = project(act_in, w_qkv).reshape(local_len, seq_count, 3, heads_dev, HEAD_DIM)
    cosine, sine_table = rope_tables(position_ids, HEAD_DIM)
    rot_cos = cosine[:, :, None, :]
    rot_sin = sine_table[:, :, None, :]
    query_matrix = rotate(projected[:, :, 0], rot_cos, rot_sin).astype(jnp.bfloat16)
    key_matrix_rows = rotate(projected[:, :, 1], rot_cos, rot_sin).astype(jnp.bfloat16)
    value_matrix_rows = projected[:, :, 2].astype(jnp.bfloat16)
    key_value = jnp.concatenate(
        [
            key_matrix_rows.reshape(local_len, seq_count, inner_width),
            value_matrix_rows.reshape(local_len, seq_count, inner_width),
        ],
        axis=-1,
    )
    key_value_all = lax.all_gather(key_value, "context", axis=0, tiled=True)
    keys_all = key_value_all[..., :inner_width].reshape(full_len, seq_count, heads_dev, HEAD_DIM)
    values_all = key_value_all[..., inner_width:].reshape(full_len, seq_count, heads_dev, HEAD_DIM)
    offset = lax.axis_index("context") * local_len
    seg_query = lax.dynamic_slice_in_dim(segment_ids, offset, local_len, 0)
    same_doc = seg_query.T[:, :, None] == segment_ids.T[:, None, :]
    keep_mask = (seg_query > 0).astype(jnp.float32)
    unscaled_score = jnp.einsum(
        "lshd,mshd->shlm", query_matrix, keys_all, preferred_element_type=jnp.float32
    )
    scores = jnp.where(same_doc[:, None], unscaled_score * score_scale, -jnp.inf)
    row_max = jnp.max(scores, axis=-1, keepdims=True)
    log_total = row_max + jnp.log(jnp.sum(jnp.exp(scores - row_max), axis=-1, keepdims=True))
    probs_low = jnp.exp(scores - log_total).astype(jnp.bfloat16)
    attended = jnp.einsum(
        "shlm,mshd->lshd", probs_low, values_all, preferred_element_type=jnp.float32
    )
    attn_in = (
        (attended * keep_mask[:, :, None, None])
        .astype(jnp.bfloat16)
        .reshape(token_count, inner_width)
    )
    branch_one = lax.psum(
        jnp.dot(attn_in, w_out, preferred_element_type=jnp.float32).astype(jnp.bfloat16), "tensor"
    ).astype(jnp.float32)
    resid = inputs + branch_one
    mlp_in = layer_norm(resid, norm_gains[1]).astype(jnp.bfloat16)
    mixed_rows = project(mlp_in, w_in)
    hidden_full, geglu_pull = jax.vjp(geglu_gate, mixed_rows[:, :ff_dev], mixed_rows[:, ff_dev:])
    hidden = hidden_full.astype(jnp.bfloat16)
    branch_two = lax.psum(
        jnp.dot(hidden, w_down, preferred_element_type=jnp.float32).astype(jnp.bfloat16), "tensor"
    ).astype(jnp.float32)
    layer_out = (resid + branch_two).astype(jnp.bfloat16).reshape(local_len, seq_count, model_width)
    out_cot = out_grad.astype(jnp.float32).reshape(token_count, model_width)
    dbranch_two = out_cot.astype(jnp.bfloat16)
    dhidden = project(dbranch_two, w_down)
    dgate, dup_part = geglu_pull(dhidden)
    dmixed = jnp.concatenate([dgate, dup_part], axis=1).astype(jnp.bfloat16)
    dnormed_two = lax.psum(
        jnp.dot(dmixed, w_in, preferred_element_type=jnp.float32).astype(jnp.bfloat16), "tensor"
    ).astype(jnp.float32)
    norm_two_out, norm_two_pull = jax.vjp(layer_norm, resid, norm_gains[1])
    dresid_norm, dgain_two = norm_two_pull(dnormed_two)
    dresid = out_cot + dresid_norm
    dbranch_one = dresid.astype(jnp.bfloat16)
    keep_low = keep_mask.reshape(token_count, 1).astype(jnp.bfloat16)
    dattended = project(dbranch_one, w_out).astype(jnp.bfloat16) * keep_low
    dattn = dattended.reshape(local_len, seq_count, heads_dev, HEAD_DIM)
    dquery_list = []
    dkey_list = []
    dvalue_list = []
    for head_index in range(heads_dev):
        query_head = query_matrix[:, :, head_index]
        key_head = keys_all[:, :, head_index]
        value_head = values_all[:, :, head_index]
        dout_head = dattn[:, :, head_index]
        raw_head = jnp.einsum(
            "lsd,msd->slm", query_head, key_head, preferred_element_type=jnp.float32
        )
        prob_head = jnp.exp(
            jnp.where(same_doc, raw_head * score_scale, -jnp.inf) - log_total[:, head_index]
        )
        dprob = jnp.einsum(
            "lsd,msd->slm", dout_head, value_head, preferred_element_type=jnp.float32
        )
        delta = jnp.sum(prob_head * dprob, axis=-1, keepdims=True)
        dscore = (prob_head * (dprob - delta) * score_scale).astype(jnp.bfloat16)
        dquery_list.append(
            jnp.einsum("slm,msd->lsd", dscore, key_head, preferred_element_type=jnp.float32)
        )
        dkey_head = jnp.einsum(
            "slm,lsd->msd", dscore, query_head, preferred_element_type=jnp.float32
        )
        dvalue_head = jnp.einsum(
            "slm,lsd->msd",
            prob_head.astype(jnp.bfloat16),
            dout_head,
            preferred_element_type=jnp.float32,
        )
        summed = lax.psum_scatter(
            jnp.concatenate([dkey_head, dvalue_head], axis=-1).astype(jnp.bfloat16),
            "context",
            scatter_dimension=0,
            tiled=True,
        ).astype(jnp.float32)
        dkey_list.append(summed[..., :HEAD_DIM])
        dvalue_list.append(summed[..., HEAD_DIM:])
    dqueries = jnp.stack(dquery_list, axis=2)
    dkeys = jnp.stack(dkey_list, axis=2)
    dvalues = jnp.stack(dvalue_list, axis=2)
    dprojected = (
        jnp.stack(
            [
                rotate_back(dqueries, rot_cos, rot_sin),
                rotate_back(dkeys, rot_cos, rot_sin),
                dvalues,
            ],
            axis=2,
        )
        .astype(jnp.bfloat16)
        .reshape(token_count, 3 * inner_width)
    )
    dnormed_one = lax.psum(
        jnp.dot(dprojected, w_qkv, preferred_element_type=jnp.float32).astype(jnp.bfloat16),
        "tensor",
    ).astype(jnp.float32)
    norm_one_out, norm_one_pull = jax.vjp(layer_norm, inputs, norm_gains[0])
    dinput_norm, dgain_one = norm_one_pull(dnormed_one)
    tokens_grad = (
        (dresid + dinput_norm).astype(jnp.bfloat16).reshape(local_len, seq_count, model_width)
    )
    gain_grads = lax.psum(jnp.stack([dgain_one, dgain_two]), ("fsdp", "context"))

    def padded(block, used_rows):
        return jnp.pad(block, ((0, 0), (0, pad_rows - used_rows)))

    left_rows = jnp.concatenate(
        [
            padded(dprojected, counts[0]),
            padded(attn_in, counts[1]),
            padded(dmixed, counts[2]),
            padded(hidden, counts[3]),
        ],
        axis=1,
    )
    right_rows = jnp.stack([act_in, dbranch_one, mlp_in, dbranch_two])
    blocks = local_rows * lax.axis_size(("fsdp", "context")) // pad_rows
    col_block = left_rows.reshape(token_count, blocks, pad_rows)
    grad_block = lax.psum_scatter(
        jnp.einsum(
            "nbp,bnd->bpd", col_block, right_rows, preferred_element_type=jnp.float32
        ).reshape(local_rows * lax.axis_size(("fsdp", "context")), model_width),
        ("fsdp", "context"),
        scatter_dimension=0,
        tiled=True,
    )
    momentum = muon_state.reshape(local_rows, model_width)
    muon_next = muon_beta * momentum + (1.0 - muon_beta) * grad_block
    direction = (1.0 - muon_beta) * grad_block + muon_beta * muon_next
    norm_total = lax.psum(jnp.sum(direction * direction), ("context", "tensor"))
    norm_size = jnp.sqrt(norm_total)
    direction_scale = jnp.log(norm_size).reshape(1)
    ortho_local = direction / (norm_size + ortho_eps)
    ortho_block = lax.all_gather(
        ortho_local.astype(jnp.bfloat16), "context", axis=0, tiled=True
    ).astype(ortho_local.dtype)
    for sweep_index in range(ITERS):
        gram_sum = lax.psum(
            contract_exact(ortho_block, ortho_block).astype(jnp.bfloat16), "tensor"
        ).astype(jnp.float32)
        square = jnp.dot(
            gram_sum, gram_sum, precision=precision_highest, preferred_element_type=jnp.float32
        )
        mix_matrix = ns_second * gram_sum + ns_third * square
        ortho_block = ns_first * ortho_block + jnp.dot(
            ortho_block, mix_matrix, precision=precision_highest, preferred_element_type=jnp.float32
        )
    own_rows = lax.dynamic_slice_in_dim(
        ortho_block, lax.axis_index("context") * local_rows, local_rows, 0
    )
    owner_index = lax.axis_index("fsdp")
    spreads = jnp.array(
        [0.2 * math.sqrt(3 * D), 0.2 * math.sqrt(D), 0.2 * math.sqrt(2 * FF), 0.2 * math.sqrt(FF)],
        jnp.float32,
    )
    spread = jnp.sum(jnp.where(jnp.arange(4) == owner_index, spreads, 0.0))
    old_weight = own_block.astype(jnp.float32)
    weight_update = -muon_rate * (spread * own_rows + decay_rate * old_weight)
    adam_first_next = adam_beta * adam_first + (1.0 - adam_beta) * gain_grads
    adam_second_next = adam_beta * adam_second + (1.0 - adam_beta) * gain_grads * gain_grads
    correction = 1.0 - adam_beta**STEP
    gain_update = -adam_rate * (
        adam_first_next / correction / (jnp.sqrt(adam_second_next / correction) + adam_eps)
        + decay_rate * norm_gains
    )
    block_shape = (1, 1, local_rows, model_width)
    return (
        layer_out,
        tokens_grad,
        grad_block.reshape(block_shape),
        muon_next.reshape(block_shape),
        weight_update.reshape(block_shape),
        direction_scale,
        gain_grads,
        adam_first_next,
        adam_second_next,
        gain_update,
    )


MESH_ID = pl.DeviceIdType.MESH
ANY = pl.ANY


def ring_place(index):
    return index + index // 2 - 2 * (index // 3)


def split_units(rows, parts, unit=16):
    units = rows // unit
    sizes = [(units // parts + (1 if i < units % parts else 0)) * unit for i in range(parts)]
    return [s for s in sizes if s]


def ring_chunks(counts, local_rows, which, core, target):
    first = core * local_rows
    rows = min(counts[which], first + local_rows) - first
    if rows <= 0:
        return [[], []]
    halves = split_units(rows, 2)
    if len(halves) == 1:
        halves = halves + [0]
    out, at = [], first
    for half in halves:
        pieces = []
        if half:
            for size in split_units(half, max(1, round(half / target))):
                pieces.append((at, size))
                at += size
        out.append(pieces)
    return out


class Place:
    def __init__(self):
        self.f = lax.axis_index("fsdp")
        self.c = lax.axis_index("context")
        self.t = lax.axis_index("tensor")
        self.pos = ring_place(self.f)
        self.next = ring_place((self.pos + 1) % 4)
        self.prev = ring_place((self.pos + 3) % 4)
        homes = (0, 1, 3, 2)
        self.hops = [[(self.pos + 4 - home) % 4, (home + 4 - self.pos) % 4] for home in homes]
        self.outer = jnp.logical_or(self.t == 0, self.t == 3)
        self.inner_mate = jnp.where(self.t == 0, 1, 2)
        self.outer_mate = jnp.where(self.t == 1, 0, 3)

    def ring(self, direction):
        return (self.next if direction == 0 else self.prev, self.c, self.t)

    def partner(self):
        return (self.f, 1 - self.c, self.t)

    def chip_z(self, z):
        return (self.f, self.c, z)

    def hop(self, which, direction):
        return self.hops[which][direction]


def greet(place, ring, partner, line):
    barrier = pltpu.get_barrier_semaphore()

    def signal(device):
        pl.semaphore_signal(barrier, inc=1, device_id=device, device_id_type=MESH_ID)

    count = 0
    if ring:
        signal(place.ring(0))
        signal(place.ring(1))
        count += 2
    if partner:
        signal(place.partner())
        count += 1
    if line:
        @pl.when(place.outer)
        def _():
            signal(place.chip_z(place.inner_mate))
            pl.semaphore_wait(barrier, count + 1)

        @pl.when(jnp.logical_not(place.outer))
        def _():
            signal(place.chip_z(place.outer_mate))
            signal(place.chip_z(3 - place.t))
            pl.semaphore_wait(barrier, count + 2)
    else:
        pl.semaphore_wait(barrier, count)


def remote(src, dst, send, recv, device):
    return pltpu.make_async_remote_copy(
        src_ref=src, dst_ref=dst, send_sem=send, recv_sem=recv, device_id=device, device_id_type=MESH_ID
    )


def run_steps(*tracks):
    total = max(len(track) for track in tracks)
    done = [0] * len(tracks)
    for index in range(total):
        for number, track in enumerate(tracks):
            upto = -(-len(track) * (index + 1) // total)
            while done[number] < upto:
                track[done[number]]()
                done[number] += 1


def gather_plan(counts, local_rows, ks, target=96):
    plan = []
    for core in (0, 1):
        ident = 0
        for which in ks:
            for direction, pieces in enumerate(ring_chunks(counts, local_rows, which, core, target)):
                for order, (row, rows) in enumerate(pieces):
                    plan.append((ident, which, core, direction, order, row, rows))
                    ident += 1
    return plan, max(p[0] for p in plan) + 1


def gather_steps(place, plan, local_rows, base, own_ref, out_ref, sems, skew=2):
    ss, rs, sp, rp = sems

    def dst(which, row, rows):
        return out_ref.at[pl.ds(base[which] + row, rows)]

    def src(core, row, rows):
        return own_ref.at[pl.ds(row - core * local_rows, rows)]

    def begin():
        for ident, which, core, direction, order, row, rows in plan:
            @pl.when(jnp.logical_and(place.c == core, place.f == which))
            def _():
                remote(src(core, row, rows), dst(which, row, rows), ss.at[ident], rs.at[ident],
                       place.ring(direction)).start()
        for ident, which, core, direction, order, row, rows in plan:
            @pl.when(jnp.logical_and(place.c == core, place.f == which))
            def _():
                remote(src(core, row, rows), dst(which, row, rows), sp.at[ident], rp.at[ident],
                       place.partner()).start()

    ordered = sorted(plan, key=lambda p: (p[4], p[1]))
    last = max(p[4] for p in plan)

    def visit(item, role):
        ident, which, core, direction, order, row, rows = item
        mine = dst(which, row, rows)

        @pl.when(jnp.logical_and(place.c == core, place.hop(which, direction) == role))
        def _():
            remote(mine, mine, ss.at[ident], rs.at[ident], place.ring(direction)).wait_recv()
            if role <= 2:
                remote(mine, mine, ss.at[ident], rs.at[ident], place.ring(direction)).start()
            remote(mine, mine, sp.at[ident], rp.at[ident], place.partner()).start()

    def step(j):
        def run():
            for role in (1, 2, 3):
                for item in ordered:
                    if item[4] == j - skew * (role - 1):
                        visit(item, role)
        return run

    def ready():
        for ident, which, core, direction, order, row, rows in plan:
            mine = dst(which, row, rows)

            @pl.when(place.c == 1 - core)
            def _():
                remote(mine, mine, sp.at[ident], rp.at[ident], place.partner()).wait_recv()

    def end():
        for ident, which, core, direction, order, row, rows in plan:
            hop = place.hop(which, direction)
            mine = dst(which, row, rows)

            @pl.when(jnp.logical_and(place.c == core, hop <= 2))
            def _():
                remote(mine, mine, ss.at[ident], rs.at[ident], place.ring(direction)).wait_send()

            @pl.when(place.c == core)
            def _():
                remote(mine, mine, sp.at[ident], rp.at[ident], place.partner()).wait_send()

    return begin, [step(j) for j in range(last + 1 + 2 * skew)], ready, end


def line_steps(place, chunks, own, out, early, mid, low, sems, lag=2, back_lag=3, prep=None, done=None):
    s1, r1, s2, r2, s3, r3 = sems

    def from_end(i, device):
        return remote(own(i), early(i), s1.at[i], r1.at[i], device)

    def across(i):
        return remote(mid(i), low(i), s2.at[i], r2.at[i], place.chip_z(3 - place.t))

    def back(i, device):
        return remote(out(i), out(i), s3.at[i], r3.at[i], device)

    def step(i):
        def run():
            if i < chunks and prep is not None:
                prep(i)

            @pl.when(place.outer)
            def _():
                if i < chunks:
                    from_end(i, place.chip_z(place.inner_mate)).start()
                if 0 <= i - lag - back_lag < chunks:
                    back(i - lag - back_lag, place.chip_z(place.inner_mate)).wait_recv()

            @pl.when(jnp.logical_not(place.outer))
            def _():
                if i < chunks:
                    from_end(i, place.chip_z(place.outer_mate)).wait_recv()
                    pair = own(i)[...].astype(jnp.float32) + early(i)[...].astype(jnp.float32)
                    mid(i)[...] = pair.astype(mid(i).dtype)
                    across(i).start()
                j = i - lag
                if 0 <= j < chunks:
                    across(j).wait_recv()
                    total = mid(j)[...].astype(jnp.float32) + low(j)[...].astype(jnp.float32)
                    out(j)[...] = total.astype(out(j).dtype)
                    back(j, place.chip_z(place.outer_mate)).start()
            if done is not None:
                if 0 <= i - lag - back_lag < chunks:
                    done(i - lag - back_lag)
        return run

    def end():
        @pl.when(place.outer)
        def _():
            for i in range(chunks):
                from_end(i, place.chip_z(place.inner_mate)).wait_send()

        @pl.when(jnp.logical_not(place.outer))
        def _():
            for i in range(chunks):
                across(i).wait_send()
                back(i, place.chip_z(place.outer_mate)).wait_send()

    return [step(i) for i in range(chunks + lag + back_lag)], end


def scatter_steps(place, plan, local_rows, base, part_ref, grad_ref, prx, rrx, tx, sems, skew=2):
    ss, rs, sp, rp = sems

    def rows_of(ref, which, row, rows):
        return ref.at[pl.ds(base[which] + row, rows)]

    def partner_copy(item):
        ident, which, core, direction, order, row, rows = item
        return remote(rows_of(part_ref, which, row, rows), rows_of(prx, which, row, rows),
                      sp.at[ident], rp.at[ident], place.partner())

    def ring_copy(item):
        ident, which, core, direction, order, row, rows = item
        return remote(rows_of(tx, which, row, rows), rows_of(rrx, which, row, rows),
                      ss.at[ident], rs.at[ident], place.ring(direction))

    ordered = sorted(plan, key=lambda p: (p[4], p[1]))
    last = max(p[4] for p in plan)

    def begin(ks):
        for item in ordered:
            if item[1] in ks:
                @pl.when(place.c == 1 - item[2])
                def _():
                    partner_copy(item).start()

    def visit(item, late):
        ident, which, core, direction, order, row, rows = item
        hop = place.hop(which, direction)
        role = (late + 1) % 4

        @pl.when(jnp.logical_and(place.c == core, hop == role))
        def _():
            partner_copy(item).wait_recv()
            total = (rows_of(part_ref, which, row, rows)[...].astype(jnp.float32)
                     + rows_of(prx, which, row, rows)[...].astype(jnp.float32))
            if role != 1:
                ring_copy(item).wait_recv()
                total = total + rows_of(rrx, which, row, rows)[...].astype(jnp.float32)
            if role == 0:
                grad_ref[pl.ds(row - core * local_rows, rows)] = total
            else:
                rows_of(tx, which, row, rows)[...] = total.astype(tx.dtype)
                ring_copy(item).start()

    def step(j):
        def run():
            for late in range(4):
                for item in ordered:
                    if item[4] == j - skew * late:
                        visit(item, late)
        return run

    def end():
        for item in plan:
            ident, which, core, direction, order, row, rows = item

            @pl.when(place.c == 1 - core)
            def _():
                partner_copy(item).wait_send()

            @pl.when(jnp.logical_and(place.c == core, place.hop(which, direction) != 0))
            def _():
                ring_copy(item).wait_send()

    return begin, [step(j) for j in range(last + 1 + 3 * skew)], end


VMEM_SPEC = pl.BlockSpec(memory_space=pltpu.VMEM)
ANY_SPEC = pl.BlockSpec(memory_space=pl.ANY)


def dma(count):
    return pltpu.SemaphoreType.DMA((count,))


def comm_call(kernel, outs, ins, in_specs, out_specs, scratch, ident):
    return pl.pallas_call(
        kernel,
        out_shape=outs,
        in_specs=in_specs,
        out_specs=out_specs,
        scratch_shapes=scratch,
        compiler_params=pltpu.CompilerParams(
            collective_id=ident, has_side_effects=True, vmem_limit_bytes=60 * 2**20
        ),
    )(*ins)


def base_rows(counts, ks):
    base, at = {}, 0
    for which in ks:
        base[which] = at
        at += counts[which]
    return base, at


def own_rows_copy(place, counts, local_rows, ks, base, own_ref, out_ref, sem, act):
    for which in ks:
        for core in (0, 1):
            rows = min(counts[which] - core * local_rows, local_rows)
            if rows > 0:
                @pl.when(jnp.logical_and(place.c == core, place.f == which))
                def _():
                    act(pltpu.make_async_copy(
                        own_ref.at[pl.ds(0, rows)],
                        out_ref.at[pl.ds(base[which] + core * local_rows, rows)],
                        sem.at[0],
                    ))


class LineSum:
    def __init__(self, place, rows, own, early, mid, low, total, sems):
        self.place, self.rows = place, rows
        self.own, self.early, self.mid, self.low, self.total = own, early, mid, low, total
        self.sems = sems

    def cut(self, ref, i):
        return ref.at[pl.ds(pl.multiple_of(i * self.rows, self.rows), self.rows)]

    def from_end(self, i, mate):
        s1, r1 = self.sems[:2]
        return remote(self.cut(self.own, i), self.cut(self.early, i), s1.at[i], r1.at[i], self.place.chip_z(mate))

    def across(self, i):
        s2, r2 = self.sems[2:4]
        return remote(self.cut(self.mid, i), self.cut(self.low, i), s2.at[i], r2.at[i], self.place.chip_z(3 - self.place.t))

    def back(self, i, mate):
        s3, r3 = self.sems[4:6]
        return remote(self.cut(self.total, i), self.cut(self.total, i), s3.at[i], r3.at[i], self.place.chip_z(mate))

    def send(self, i):
        @pl.when(self.place.outer)
        def _():
            self.from_end(i, self.place.inner_mate).start()

    def pair_up(self, i):
        @pl.when(jnp.logical_not(self.place.outer))
        def _():
            self.from_end(i, self.place.outer_mate).wait_recv()
            pair = self.cut(self.own, i)[...].astype(jnp.float32) + self.cut(self.early, i)[...].astype(jnp.float32)
            self.cut(self.mid, i)[...] = pair.astype(self.mid.dtype)
            self.across(i).start()

    def join(self, i):
        @pl.when(jnp.logical_not(self.place.outer))
        def _():
            self.across(i).wait_recv()
            whole = self.cut(self.mid, i)[...].astype(jnp.float32) + self.cut(self.low, i)[...].astype(jnp.float32)
            self.cut(self.total, i)[...] = whole.astype(self.total.dtype)
            self.back(i, self.place.outer_mate).start()

    def receive(self, i):
        @pl.when(self.place.outer)
        def _():
            self.back(i, self.place.inner_mate).wait_recv()

    def finish(self, pieces):
        @pl.when(self.place.outer)
        def _():
            for i in range(pieces):
                self.from_end(i, self.place.inner_mate).wait_send()

        @pl.when(jnp.logical_not(self.place.outer))
        def _():
            for i in range(pieces):
                self.across(i).wait_send()
                self.back(i, self.place.outer_mate).wait_send()


def nt_dot(left, right):
    return lax.dot_general(left, right, (((1,), (1,)), ((), ())), preferred_element_type=jnp.float32)


def nn_dot(left, right):
    return jnp.dot(left, right, preferred_element_type=jnp.float32)


def tn_dot(left, right):
    return lax.dot_general(left, right, (((0,), (0,)), ((), ())), preferred_element_type=jnp.float32)


def centred(values):
    centre = values - jnp.mean(values, axis=-1, keepdims=True)
    spread = jnp.mean(centre * centre, axis=-1, keepdims=True)
    return centre, lax.rsqrt(spread + norm_eps)


def norm_back(values, gain_row, grads):
    centre, scale = centred(values)
    xhat = centre * scale
    e = grads * gain_row
    moved = scale * (e - jnp.mean(e, axis=-1, keepdims=True) - xhat * jnp.mean(e * xhat, axis=-1, keepdims=True))
    return moved, jnp.sum(grads * xhat, axis=0, keepdims=True)


def layer_both_ways(tokens, out_grad, own_block, norm_gains, cosine, sine, seg_column, seg_row, counts, ident):
    count, width = tokens.shape
    local_rows = own_block.shape[0]
    inner = counts[1]
    ff = counts[3]
    heads = inner // HEAD_DIM
    full = 2 * count
    rows = count // 4
    split = 4
    sub = rows // split
    pieces = 4 * split
    stack = heads * rows
    piece = 64
    score_scale = HEAD_DIM ** (-0.5)
    f32, low = jnp.float32, jnp.bfloat16
    first_plan, first_count = gather_plan(counts, local_rows, (0, 1), 64)
    last_plan, last_count = gather_plan(counts, local_rows, (2, 3), 64)
    first_base, first_rows = base_rows(counts, (0, 1))
    last_base, last_rows = base_rows(counts, (2, 3))

    def kernel(tok_ref, og_ref, own_ref, gain_ref, cos_ref, sin_ref, sc_ref, sr_ref,
               act_ref, attn_ref, resid_ref, mlp_ref, hid_ref, dm_ref, b2_ref, dres_ref, db_ref, dproj_ref, t3_ref, dg_ref,
               w1st, wlast, q_ref, kv_ref, kq_ref, p_ref, s_ref, pl_ref, do_ref, dp_ref, ds_ref,
               t1_ref, e1, m1, l1, sum1, t2_ref, e2, m2, l2, sum2, dq_ref, dkv_ref, dkv_tx, dkv_rx, cos_all, sin_all, *sems):
        place = Place()
        greet(place, True, True, True)
        begin1, steps1, ready1, end1 = gather_steps(place, first_plan, local_rows, first_base, own_ref, w1st, sems[0:4], 1)
        begin2, steps2, ready2, end2 = gather_steps(place, last_plan, local_rows, last_base, own_ref, wlast, sems[4:8])
        line1 = LineSum(place, sub, t1_ref, e1, m1, l1, sum1, sems[8:14])
        line2 = LineSum(place, sub, t2_ref, e2, m2, l2, sum2, sems[14:20])
        swap, local_sem = sems[20], sems[21]

        def each_piece(act, chunk):
            for part in range(split):
                act(split * chunk + part)

        begin1()
        own_rows_copy(place, counts, local_rows, (0, 1), first_base, own_ref, w1st, local_sem, lambda d: d.start())

        def at(i, size=rows):
            return pl.ds(pl.multiple_of(i * size, size), size)

        def norm_one(i, carry):
            centre, scale = centred(tok_ref[at(i)].astype(f32))
            act_ref[at(i)] = (centre * scale * gain_ref[0:1]).astype(low)
            cos_all[at(i)] = jnp.concatenate([cos_ref[at(i)]] * (2 * heads), axis=1)
            sin_all[at(i)] = jnp.concatenate([sin_ref[at(i)]] * (2 * heads), axis=1)
            return carry

        lax.fori_loop(0, 4, norm_one, 0)
        dg_ref[...] = jnp.zeros_like(dg_ref)
        begin2()
        run_steps(steps1)
        own_rows_copy(place, counts, local_rows, (0, 1), first_base, own_ref, w1st, local_sem, lambda d: d.wait())
        own_rows_copy(place, counts, local_rows, (2, 3), last_base, own_ref, wlast, local_sem, lambda d: d.start())
        ready1()
        waiting = list(steps2)

        def forward(number):
            for step in waiting[:number]:
                step()
            del waiting[:number]

        forward(1)

        lane = lax.broadcasted_iota(jnp.int32, (1, inner), 1)
        front = (lane % HEAD_DIM) < HEAD_DIM // 2

        def half_turn(value):
            return jnp.where(front, pltpu.roll(value, inner - HEAD_DIM // 2, 1), pltpu.roll(value, HEAD_DIM // 2, 1))

        sign = jnp.where(front, -1.0, 1.0).astype(f32)

        def rotated(value, i):
            return value * cos_all[at(i)] + half_turn(value) * (sin_all[at(i)] * sign)

        def rotated_back(value, i):
            return value * cos_all[at(i)] - half_turn(value * sin_all[at(i)]) * sign

        def project_rows(i, carry):
            value = nt_dot(act_ref[at(i)], w1st[0:3 * inner])
            q_ref[at(i)] = rotated(value[:, 0:inner], i).astype(low)
            kv_ref[at(i), 0:inner] = rotated(value[:, inner:2 * inner], i).astype(low)
            kv_ref[at(i), inner:2 * inner] = value[:, 2 * inner:3 * inner].astype(low)
            return carry

        lax.fori_loop(0, 4, project_rows, 0)
        kv_copy = remote(kv_ref.at[pl.ds(0, count)], kv_ref.at[pl.ds(count, count)], swap.at[0], swap.at[1], place.partner())
        kv_copy.start()
        forward(2)
        kv_copy.wait()

        def head_mask(h):
            return jnp.logical_and(lane >= h * HEAD_DIM, lane < (h + 1) * HEAD_DIM)

        def stacked(value):
            return jnp.concatenate([jnp.where(head_mask(h), value, jnp.zeros_like(value)) for h in range(heads)], axis=0)

        def unstacked(value):
            total = jnp.where(head_mask(0), value[0:rows], 0.0)
            for h in range(1, heads):
                total = total + jnp.where(head_mask(h), value[h * rows:(h + 1) * rows], 0.0)
            return total

        per = rows // piece

        def attend(i):
            kq_ref[...] = stacked(q_ref[at(i)])
            s_ref[...] = nt_dot(kq_ref[...], kv_ref[:, 0:inner])

            def soft(r, inside):
                seg = sc_ref[pl.ds(pl.multiple_of(i * rows + (r % per) * piece, piece), piece)]
                score = jnp.where(seg == sr_ref[...], s_ref[at(r, piece)] * score_scale, -jnp.inf)
                score = jnp.exp(score - jnp.max(score, axis=-1, keepdims=True))
                prob = score * (1.0 / jnp.sum(score, axis=-1, keepdims=True))
                p_ref[i, at(r, piece)] = prob
                pl_ref[at(r, piece)] = prob.astype(low)
                return inside

            lax.fori_loop(0, stack // piece, soft, 0)
            mixed = unstacked(nn_dot(pl_ref[...], kv_ref[:, inner:2 * inner]))
            keep = (sc_ref[at(i)] > 0).astype(f32)
            attn = (mixed * keep).astype(low)
            attn_ref[at(i)] = attn
            t1_ref[at(i)] = nn_dot(attn, w1st[3 * inner:4 * inner]).astype(low)
            each_piece(line1.send, i)

            if i >= 1:
                each_piece(line1.pair_up, i - 1)
            if i >= 2:
                each_piece(line1.join, i - 2)

        for i in range(4):
            attend(i)
            forward(2)
        forward(len(waiting))
        own_rows_copy(place, counts, local_rows, (2, 3), last_base, own_ref, wlast, local_sem, lambda d: d.wait())
        ready2()

        def feed(i, carry):
            each_piece(line1.receive, i)
            resid = tok_ref[at(i)].astype(f32) + sum1[at(i)].astype(f32)
            resid_ref[at(i)] = resid
            centre, scale = centred(resid)
            mlp = (centre * scale * gain_ref[1:2]).astype(low)
            mlp_ref[at(i)] = mlp
            gate = nt_dot(mlp, wlast[0:ff])
            up = nt_dot(mlp, wlast[ff:2 * ff])
            cdf = 0.5 * (1.0 + lax.erf(gate * (0.5 ** 0.5)))
            bell = jnp.exp(gate * gate * -0.5) * (1.0 / math.sqrt(2.0 * math.pi))
            gelu = gate * cdf
            hidden = (gelu * up).astype(low)
            hid_ref[at(i)] = hidden
            dhidden = nt_dot(og_ref[at(i)], wlast[2 * ff:3 * ff])
            dgate = (dhidden * up * (cdf + gate * bell)).astype(low)
            dup = (dhidden * gelu).astype(low)
            dm_ref[0, at(i)] = dgate
            dm_ref[1, at(i)] = dup
            t2_ref[at(i)] = (nn_dot(dgate, wlast[0:ff]) + nn_dot(dup, wlast[ff:2 * ff])).astype(low)
            each_piece(line2.send, i)
            b2_ref[at(i)] = nn_dot(hidden, wlast[2 * ff:3 * ff]).astype(low)

            @pl.when(i == 0)
            def _():
                each_piece(line1.pair_up, 3)

            @pl.when(i <= 1)
            def _():
                each_piece(line1.join, i + 2)

            @pl.when(i >= 1)
            def _():
                each_piece(line2.pair_up, i - 1)

            @pl.when(i >= 2)
            def _():
                each_piece(line2.join, i - 2)
            return carry

        lax.fori_loop(0, 4, feed, 0)
        dkv_ref[...] = jnp.zeros_like(dkv_ref)

        def turn_back(i, carry):
            each_piece(line2.receive, i)
            moved, gain_part = norm_back(resid_ref[at(i)], gain_ref[1:2], sum2[at(i)].astype(f32))
            dg_ref[1:2] = dg_ref[1:2] + gain_part
            dresid = og_ref[at(i)].astype(f32) + moved
            dres_ref[at(i)] = dresid
            dbranch = dresid.astype(low)
            db_ref[at(i)] = dbranch
            keep = (sc_ref[at(i)] > 0).astype(low)
            dattn = nt_dot(dbranch, w1st[3 * inner:4 * inner]).astype(low) * keep
            do_ref[...] = stacked(dattn)
            kq_ref[...] = stacked(q_ref[at(i)])
            dp_ref[...] = nt_dot(do_ref[...], kv_ref[:, inner:2 * inner])

            def soft_back(r, inside):
                prob = p_ref[i, at(r, piece)]
                dprob = dp_ref[at(r, piece)]
                delta = jnp.sum(prob * dprob, axis=-1, keepdims=True)
                ds_ref[at(r, piece)] = (prob * (dprob - delta) * score_scale).astype(low)
                pl_ref[at(r, piece)] = prob.astype(low)
                return inside

            lax.fori_loop(0, stack // piece, soft_back, 0)
            dq_ref[at(i)] = unstacked(nn_dot(ds_ref[...], kv_ref[:, 0:inner]))
            dkv_ref[:, 0:inner] = dkv_ref[:, 0:inner] + tn_dot(ds_ref[...], kq_ref[...])
            dkv_ref[:, inner:2 * inner] = dkv_ref[:, inner:2 * inner] + tn_dot(pl_ref[...], do_ref[...])

            @pl.when(i == 0)
            def _():
                each_piece(line2.pair_up, 3)

            @pl.when(i <= 1)
            def _():
                each_piece(line2.join, i + 2)
            return carry

        lax.fori_loop(0, 4, turn_back, 0)
        dkv_tx[...] = dkv_ref[count:full].astype(low)
        dkv_copy = remote(dkv_tx, dkv_rx, swap.at[2], swap.at[3], place.partner())
        dkv_copy.start()

        def unproject_query(i, carry):
            dproj_ref[at(i), 0:inner] = rotated_back(dq_ref[at(i)], i).astype(low)
            return carry

        lax.fori_loop(0, 4, unproject_query, 0)
        dkv_copy.wait()

        def unproject(i, carry):
            both = dkv_ref[at(i)] + dkv_rx[at(i)].astype(f32)
            dproj_ref[at(i), inner:2 * inner] = rotated_back(both[:, 0:inner], i).astype(low)
            dproj_ref[at(i), 2 * inner:3 * inner] = both[:, inner:2 * inner].astype(low)
            t3_ref[at(i)] = nn_dot(dproj_ref[at(i)], w1st[0:3 * inner]).astype(low)
            return carry

        lax.fori_loop(0, 4, unproject, 0)
        line1.finish(pieces)
        line2.finish(pieces)
        end1()
        end2()

    def shape(*dims, dtype=low):
        return jax.ShapeDtypeStruct(dims, dtype)

    outs = (
        shape(count, width), shape(count, inner), shape(count, width, dtype=f32), shape(count, width), shape(count, ff),
        shape(2, count, ff), shape(count, width), shape(count, width, dtype=f32), shape(count, width),
        shape(count, 3 * inner), shape(count, width), shape(8, width, dtype=f32),
    )
    line = pltpu.VMEM((count, width), low)
    scratch = [
        pltpu.VMEM((first_rows, width), low), pltpu.VMEM((last_rows, width), low), pltpu.VMEM((count, inner), low),
        pltpu.VMEM((full, 2 * inner), low), pltpu.VMEM((stack, inner), low), pltpu.VMEM((4, stack, full), f32),
        pltpu.VMEM((stack, full), f32), pltpu.VMEM((stack, full), low), pltpu.VMEM((stack, inner), low),
        pltpu.VMEM((stack, full), f32), pltpu.VMEM((stack, full), low),
    ]
    scratch += [line] * 10
    scratch += [
        pltpu.VMEM((count, inner), f32), pltpu.VMEM((full, 2 * inner), f32),
        pltpu.VMEM((count, 2 * inner), low), pltpu.VMEM((count, 2 * inner), low),
        pltpu.VMEM((count, inner), f32), pltpu.VMEM((count, inner), f32),
    ]
    scratch += [dma(first_count)] * 4 + [dma(last_count)] * 4 + [dma(pieces)] * 12 + [dma(4), dma(1)]
    ins = (tokens, out_grad, own_block, norm_gains, cosine, sine, seg_column, seg_row)
    return pl.pallas_call(
        kernel,
        out_shape=outs,
        in_specs=[VMEM_SPEC] * len(ins),
        out_specs=(VMEM_SPEC,) * len(outs),
        scratch_shapes=scratch,
        compiler_params=pltpu.CompilerParams(
            collective_id=ident, has_side_effects=True, vmem_limit_bytes=67043328
        ),
    )(*ins)


def tail_grams(left_right, muon_rows, counts, ident):
    dproj, act_in, attn_in, dbranch, dmixed, mlp_in, hidden, out_low = left_right
    local_rows, width = muon_rows.shape
    ks = (0, 1, 2, 3)
    plan, count = gather_plan(counts, local_rows, ks, 96)
    base, total_rows = base_rows(counts, ks)
    ff = counts[3]
    tile = width // 4
    split = 4
    half = tile // split
    chunks = 5 * split
    f32, low16 = jnp.float32, jnp.bfloat16

    def kernel(dp_ref, act_ref, at_ref, db_ref, dm_ref, mlp_ref, hid_ref, og_ref, mu_ref,
               grad_ref, x_ref, g_ref, norm_ref,
               part, prx, rrx, mine, theirs, gprx, tot, other, early, mid, low, norm_own, *sems):
        place = Place()
        c = place.c
        greet(place, True, True, True)
        begin, steps, end = scatter_steps(place, plan, local_rows, base, part, grad_ref, prx, rrx, part, sems[:4])

        def terms(row, left, right):
            span = left.shape[1]

            def columns(j, carry):
                cols = pl.ds(pl.multiple_of(j * tile, tile), tile)
                part[pl.ds(row, span), cols] = tn_dot(left[...], right[:, cols]).astype(low16)
                return carry

            lax.fori_loop(0, 4, columns, 0)

        terms(base[2], dm_ref.at[0], mlp_ref)
        terms(base[2] + ff, dm_ref.at[1], mlp_ref)
        begin((2,))
        terms(base[3], hid_ref, og_ref)
        begin((3,))
        terms(base[0], dp_ref, act_ref)
        begin((0,))
        terms(base[1], at_ref, db_ref)
        begin((1,))
        grad_ref[...] = jnp.zeros_like(grad_ref)
        run_steps(steps)
        end()

        def momentum(i, carry):
            sl = pl.ds(pl.multiple_of(i * 16, 16), 16)
            grad = grad_ref[sl]
            after = muon_beta * mu_ref[sl] + (1.0 - muon_beta) * grad
            direction = (1.0 - muon_beta) * grad + muon_beta * after
            x_ref[sl] = direction.astype(low16)
            square = direction * direction
            return carry + square[0:8] + square[8:16]

        square = lax.fori_loop(0, local_rows // 16, momentum, jnp.zeros((8, width), f32))
        own_square = jnp.broadcast_to(jnp.sum(jnp.sum(square, axis=1, keepdims=True), axis=0, keepdims=True), (8, tile))
        norm_own[...] = own_square

        sp, rp, st, rt = sems[10:14]

        def blocks(core):
            return [(3 * core, 3 * core), (2 * core, 2 * core + 1), (core + 1, core + 1), (core, core + 2), (core, 3 - core)]

        def at(k):
            return pl.ds(pl.multiple_of(k * tile, tile), tile)

        def gram(i, j):
            return tn_dot(x_ref[:, at(i)], x_ref[:, at(j)])

        def partner(n):
            sl = pl.ds(n * tile, tile)
            return remote(theirs.at[sl], gprx.at[sl], sp.at[n], rp.at[n], place.partner())

        def norm_row(ref):
            return ref.at[pl.ds(5 * tile, 8)]

        for n, (i, j) in enumerate(blocks(1 - c)):
            theirs[pl.ds(n * tile, tile)] = gram(i, j)
            partner(n).start()
        norm_row(theirs)[...] = norm_own[...]
        pn = remote(norm_row(theirs), norm_row(gprx), sp.at[5], rp.at[5], place.partner())
        pn.start()

        def span(i):
            return pl.ds(i * half, half) if i < chunks - 1 else pl.ds(i * half, half + 8)

        def cut(ref):
            return lambda i: ref.at[span(i)]

        def prep(i):
            if i % split == 0:
                n = i // split
                sl = pl.ds(n * tile, tile)
                block = gram(*blocks(c)[n])
                partner(n).wait_recv()
                mine[sl] = block + gprx[sl]
            if i == chunks - 1:
                pn.wait_recv()
                norm_row(mine)[...] = norm_row(gprx)[...] + norm_own[...]

        def share(i):
            return remote(cut(tot)(i), cut(other)(i), st.at[i], rt.at[i], place.partner())

        def place_block(ref, n, core):
            i, j = blocks(core)[n]
            block = ref[pl.ds(n * tile, tile)]
            g_ref[at(i), at(j)] = block
            g_ref[at(j), at(i)] = block.T

        def done(i):
            share(i).start()
            if i % split == split - 1:
                place_block(tot, i // split, c)
            if i >= 2:
                share(i - 2).wait_recv()
                if (i - 2) % split == split - 1:
                    place_block(other, (i - 2) // split, 1 - c)

        line, line_end = line_steps(place, chunks, cut(mine), cut(tot), cut(early), cut(mid), cut(low), sems[4:10],
                                    lag=3, back_lag=4, prep=prep, done=done)
        run_steps(line)
        for i in (chunks - 2, chunks - 1):
            share(i).wait_recv()
        place_block(other, 4, 1 - c)
        norm_ref[...] = jnp.broadcast_to(tot[5 * tile:5 * tile + 8, 0:128], (8, 128))
        line_end()
        for n in range(5):
            partner(n).wait_send()
        pn.wait_send()
        for i in range(chunks):
            share(i).wait_send()

    rows_low = pltpu.VMEM((total_rows, width), low16)
    packed = pltpu.VMEM((5 * tile + 8, tile), f32)
    outs = (
        jax.ShapeDtypeStruct((local_rows, width), f32),
        jax.ShapeDtypeStruct((local_rows, width), low16), jax.ShapeDtypeStruct((width, width), f32),
        jax.ShapeDtypeStruct((8, 128), f32),
    )
    scratch = [rows_low] * 3 + [packed] * 8 + [pltpu.VMEM((8, tile), f32)]
    scratch += [dma(count)] * 4 + [dma(chunks)] * 6 + [dma(6), dma(6), dma(chunks), dma(chunks)]
    ins = tuple(left_right) + (muon_rows,)
    return comm_call(kernel, outs, ins, [VMEM_SPEC] * len(ins), (VMEM_SPEC,) * len(outs), scratch, ident)


def halves(value):
    high = value.astype(jnp.bfloat16)
    return high, (value - high.astype(jnp.float32)).astype(jnp.bfloat16)


def iterate(gram, norm, direction_low, normed_term, branch_term, tokens_in, resid, dresid, dgain_rows, norm_gains, adam_first,
            adam_second, ident):
    rows, width = direction_low.shape
    tile = 256
    parts = width // tile
    tokens = branch_term.shape[0]
    each = 8
    chunks = 2 * each
    step_rows = tokens // each
    aa = ns_first * ns_first
    ab = 2.0 * ns_first * ns_second
    bbac = ns_second * ns_second + 2.0 * ns_first * ns_third
    bc = 2.0 * ns_second * ns_third
    cc = ns_third * ns_third
    correction = 1.0 - adam_beta**STEP

    def kernel(g_ref, n_ref, d_ref, t3_ref, b2_ref, tok_ref, r_ref, dres_ref, dgr_ref, gain_ref, af_ref, as_ref,
               x_ref, lo_ref, tg_ref, gg_ref, afn_ref, asn_ref, gu_ref,
               p_ref, ph, pl_, hh, hl, uh, ul, mx, early, mid, low, total, held, dg_ref, *sems):
        place = Place()
        s1, r1, s2, r2, s3, r3, sg, rg = sems
        me = place.f * 2 + place.c
        barrier = pltpu.get_barrier_semaphore()

        def plane(shift):
            other = (me + shift) % 8
            return (other // 2, other % 2, place.t)

        for shift in range(1, 8):
            pl.semaphore_signal(barrier, inc=1, device_id=plane(shift), device_id_type=MESH_ID)

        @pl.when(place.outer)
        def _():
            pl.semaphore_signal(barrier, inc=1, device_id=place.chip_z(place.inner_mate), device_id_type=MESH_ID)
            pl.semaphore_wait(barrier, 8)

        @pl.when(jnp.logical_not(place.outer))
        def _():
            pl.semaphore_signal(barrier, inc=1, device_id=place.chip_z(place.outer_mate), device_id_type=MESH_ID)
            pl.semaphore_signal(barrier, inc=1, device_id=place.chip_z(3 - place.t), device_id_type=MESH_ID)
            pl.semaphore_wait(barrier, 9)

        def cut(ref, i):
            if isinstance(i, int):
                return ref.at[pl.ds(i * step_rows, step_rows)]
            return ref.at[pl.ds(pl.multiple_of(i * step_rows, step_rows), step_rows)]

        def from_end(i, device, own):
            local = i % each
            return remote(cut(own, local), cut(early, i), s1.at[i], r1.at[i], device)

        def across(i):
            return remote(cut(mid, i), cut(low, i), s2.at[i], r2.at[i], place.chip_z(3 - place.t))

        def back(i, device):
            return remote(cut(total, i), cut(total, i), s3.at[i], r3.at[i], device)

        dg_ref[...] = jnp.zeros_like(dg_ref)

        @pl.when(place.outer)
        def _():
            for i in range(each):
                from_end(i, place.chip_z(place.inner_mate), t3_ref).start()
            for i in range(each):
                from_end(each + i, place.chip_z(place.inner_mate), b2_ref).start()

        def pair_up(i, own):
            @pl.when(jnp.logical_not(place.outer))
            def _():
                from_end(i, place.chip_z(place.outer_mate), own).wait_recv()
                pair = cut(own, i % each)[...].astype(jnp.float32) + cut(early, i)[...].astype(jnp.float32)
                cut(mid, i)[...] = pair.astype(mid.dtype)
                across(i).start()

        def join(i):
            @pl.when(jnp.logical_not(place.outer))
            def _():
                across(i).wait_recv()
                whole = cut(mid, i)[...].astype(jnp.float32) + cut(low, i)[...].astype(jnp.float32)
                cut(total, i)[...] = whole.astype(total.dtype)
                back(i, place.chip_z(place.outer_mate)).start()

        plan = {
            "start": {4: ((), (13,))},
            "squares": {1: ((), (0,)), 2: ((), (3, 4, 5)), 3: ((), (8, 9, 10)), 4: ((), (14,))},
            "rows": {1: ((3, 4, 5), (1,)), 2: ((8, 9, 10), ()), 3: ((13, 14, 15), ()), 4: ((), (15,))},
            "cube": {0: ((0, 1, 2), ()), 1: ((6, 7), (2,)), 2: ((11, 12), (6, 7)), 3: ((), (11, 12))},
        }

        def travel(spot, sweep):
            for when, (pairs, joins) in plan[spot].items():
                @pl.when(sweep == when)
                def _():
                    for i in joins:
                        join(i)
                    for i in pairs:
                        pair_up(i, t3_ref if i < each else b2_ref)

        norm_size = jnp.sqrt(n_ref[0:1, 0:1])
        inverse = 1.0 / (norm_size + ortho_eps)
        scale = inverse * inverse

        for k in range(parts):
            sl = pl.ds(k * tile, tile)
            value = g_ref[sl] * scale
            p_ref[sl] = value
            high, rest = halves(value)
            ph[sl] = high
            pl_[sl] = rest
        x_ref[...] = d_ref[...].astype(jnp.float32) * inverse

        def product(lh, ll, rh, rl, k):
            sl, cols = pl.ds(k * tile, tile), pl.ds(k * tile, width - k * tile)

            def dot(left, right):
                return jnp.dot(left[sl], right[:, cols], preferred_element_type=jnp.float32)

            return dot(lh, rh) + dot(ll, rh) + dot(lh, rl)

        def spread_out(value, high_ref, low_ref, k):
            sl, cols = pl.ds(k * tile, tile), pl.ds(k * tile, width - k * tile)
            high, rest = halves(value)
            high_ref[sl, cols] = high
            low_ref[sl, cols] = rest
            for j in range(k + 1, parts):
                at = (j - k) * tile
                high_ref[pl.ds(j * tile, tile), sl] = high[:, at:at + tile].T
                low_ref[pl.ds(j * tile, tile), sl] = rest[:, at:at + tile].T

        def squares():
            for k in range(parts):
                sl, cols = pl.ds(k * tile, tile), pl.ds(k * tile, width - k * tile)
                value = product(ph, pl_, ph, pl_, k)
                spread_out(value, hh, hl, k)
                mix = (ns_second * p_ref[sl, cols] + ns_third * value).astype(mx.dtype)
                mx[sl, cols] = mix
                for j in range(k + 1, parts):
                    at = (j - k) * tile
                    mx[pl.ds(j * tile, tile), sl] = mix[:, at:at + tile].T

        def rotate_rows():
            for at, size in ((0, 336), (336, 320)):
                sl = pl.ds(at, size)
                old = x_ref[sl]
                x_ref[sl] = ns_first * old + jnp.dot(old.astype(jnp.bfloat16), mx[...], preferred_element_type=jnp.float32)

        def gains_copy(shift):
            return remote(dg_ref, held.at[me], sg.at[shift], rg.at[shift], plane(shift))

        def first_norm_back():
            @pl.when(place.outer)
            def _():
                for i in range(each):
                    back(i, place.chip_z(place.inner_mate)).wait_recv()

            def some(i, inside):
                sl = pl.ds(pl.multiple_of(i * 64, 64), 64)
                moved, gain_part = norm_back(tok_ref[sl].astype(jnp.float32), gain_ref[0:1], total[sl].astype(jnp.float32))
                dg_ref[0:1] = dg_ref[0:1] + gain_part
                tg_ref[sl] = (dres_ref[sl] + moved).astype(tg_ref.dtype)
                return inside

            lax.fori_loop(0, tokens // 64, some, 0)
            dg_ref[1:2] = dgr_ref[1:2]
            held[pl.ds(me, 1)] = dg_ref[...][None]
            for shift in range(1, 8):
                gains_copy(shift).start()

        def body(sweep, carry):
            travel("start", sweep)
            squares()
            travel("squares", sweep)
            rotate_rows()
            travel("rows", sweep)

            @pl.when(sweep < ITERS - 1)
            def _():
                for k in range(parts):
                    sl, cols = pl.ds(k * tile, tile), pl.ds(k * tile, width - k * tile)
                    cube = product(ph, pl_, hh, hl, k)
                    square = hh[sl, cols].astype(jnp.float32) + hl[sl, cols].astype(jnp.float32)
                    spread_out(bc * square + cc * cube, uh, ul, k)
                    p_ref[sl, cols] = aa * p_ref[sl, cols] + ab * square + bbac * cube
                travel("cube", sweep)
                for k in range(parts):
                    sl, cols = pl.ds(k * tile, tile), pl.ds(k * tile, width - k * tile)
                    value = p_ref[sl, cols] + product(hh, hl, uh, ul, k)
                    p_ref[sl, cols] = value
                    spread_out(value, ph, pl_, k)

            @pl.when(sweep == ITERS - 2)
            def _():
                first_norm_back()
            return carry

        lax.fori_loop(0, ITERS, body, 0)
        for shift in range(1, 8):
            gains_copy(shift).wait()
        grads = held[0]
        for k in range(1, 8):
            grads = grads + held[k]
        grads = grads[0:2]
        gg_ref[...] = grads
        first = adam_beta * af_ref[...] + (1.0 - adam_beta) * grads
        second = adam_beta * as_ref[...] + (1.0 - adam_beta) * grads * grads
        afn_ref[...] = first
        asn_ref[...] = second
        gu_ref[...] = -adam_rate * (
            first / correction / (jnp.sqrt(second / correction) + adam_eps) + decay_rate * gain_ref[...]
        )

        @pl.when(place.outer)
        def _():
            for i in range(each, chunks):
                back(i, place.chip_z(place.inner_mate)).wait_recv()
            for i in range(each):
                from_end(i, place.chip_z(place.inner_mate), t3_ref).wait_send()
                from_end(each + i, place.chip_z(place.inner_mate), b2_ref).wait_send()
        lo_ref[...] = (r_ref[...] + total[tokens:2 * tokens].astype(jnp.float32)).astype(lo_ref.dtype)

        @pl.when(jnp.logical_not(place.outer))
        def _():
            for i in range(chunks):
                across(i).wait_send()
                back(i, place.chip_z(place.outer_mate)).wait_send()

    f32, low16 = jnp.float32, jnp.bfloat16
    small = jax.ShapeDtypeStruct(norm_gains.shape, f32)
    narrow = jax.ShapeDtypeStruct((tokens, width), low16)
    outs = (jax.ShapeDtypeStruct((rows, width), f32), narrow, narrow, small, small, small, small)
    full = pltpu.VMEM((width, width), low16)
    line = pltpu.VMEM((2 * tokens, width), low16)
    scratch = [pltpu.VMEM((width, width), f32)] + [full] * 7 + [line] * 4
    scratch += [pltpu.VMEM((8, 8, width), f32), pltpu.VMEM((8, width), f32)] + [dma(chunks)] * 6 + [dma(8)] * 2
    ins = (gram, norm, direction_low, normed_term, branch_term, tokens_in, resid, dresid, dgain_rows, norm_gains,
           adam_first, adam_second)
    return comm_call(kernel, outs, ins, [VMEM_SPEC] * len(ins), (VMEM_SPEC,) * len(outs), scratch, ident)


def per_device_block(tokens, out_grad, weight_stack, muon_state, norm_gains, adam_first, adam_second, segment_ids,
                     position_ids):
    token_count, _, model_width = tokens.shape
    groups, contexts = 4, 2
    full_len = token_count * contexts
    local_rows = weight_stack.shape[2]
    heads_dev = HEADS // groups
    ff_dev = FF // groups
    inner_width = heads_dev * HEAD_DIM
    counts = (3 * inner_width, inner_width, 2 * ff_dev, ff_dev)
    own_block = weight_stack.reshape(local_rows, model_width)
    context = lax.axis_index("context")

    cosine, sine_table = rope_tables(position_ids.reshape(token_count), HEAD_DIM)
    segments = segment_ids.reshape(full_len)
    seg_query = lax.dynamic_slice_in_dim(segments, context * token_count, token_count, 0)
    seg_other = lax.dynamic_slice_in_dim(segments, (1 - context) * token_count, token_count, 0)
    (act_in, attn_in, resid, mlp_in, hidden, dmixed, branch_two_term, dresid, dbranch_one, dprojected, dnormed_one_term,
     dgain_rows) = layer_both_ways(
        tokens.reshape(token_count, model_width), out_grad.reshape(token_count, model_width), own_block, norm_gains,
        cosine[:, : HEAD_DIM // 2], sine_table[:, : HEAD_DIM // 2],
        seg_query.reshape(token_count, 1), jnp.concatenate([seg_query, seg_other]).reshape(1, full_len), counts, 0,
    )
    momentum = muon_state.reshape(local_rows, model_width)
    grad_block, direction_low, gram, norm_total = tail_grams(
        (dprojected, act_in, attn_in, dbranch_one, dmixed, mlp_in, hidden, out_grad.reshape(token_count, model_width)),
        momentum, counts, 1,
    )
    direction_scale = jnp.log(jnp.sqrt(norm_total[0, 0])).reshape(1)
    ortho, layer_out, tokens_grad, gain_grads, adam_first_next, adam_second_next, gain_update = iterate(
        gram, norm_total, direction_low, dnormed_one_term, branch_two_term,
        tokens.reshape(token_count, model_width), resid, dresid, dgain_rows, norm_gains, adam_first, adam_second, 2,
    )
    muon_next = muon_beta * momentum + (1.0 - muon_beta) * grad_block
    owner_index = lax.axis_index("fsdp")
    spreads = [0.2 * math.sqrt(3 * D), 0.2 * math.sqrt(D), 0.2 * math.sqrt(2 * FF), 0.2 * math.sqrt(FF)]
    spread = jnp.sum(jnp.where(jnp.arange(4) == owner_index, jnp.array(spreads, jnp.float32), 0.0))
    weight_update = -muon_rate * (spread * ortho + decay_rate * own_block.astype(jnp.float32))
    layer_out = layer_out.reshape(tokens.shape)
    tokens_grad = tokens_grad.reshape(tokens.shape)
    block_shape = (1, 1, local_rows, model_width)
    return (
        layer_out,
        tokens_grad,
        grad_block.reshape(block_shape),
        muon_next.reshape(block_shape),
        weight_update.reshape(block_shape),
        direction_scale,
        gain_grads,
        adam_first_next,
        adam_second_next,
        gain_update,
    )


def solution(mesh):
    sizes = dict(mesh.shape)
    block = (sizes["fsdp"], sizes["context"], sizes["tensor"]) == (4, 2, 4)
    return jax.shard_map(
        per_device_block if block else per_device,
        mesh=mesh,
        in_specs=(
            P("context", "fsdp", None),
            P("context", "fsdp", None),
            P("fsdp", "tensor", "context", None),
            P("fsdp", "tensor", "context", None),
            P(),
            P(),
            P(),
            P(None, "fsdp"),
            P("context", "fsdp"),
        ),
        out_specs=(
            P("context", "fsdp", None),
            P("context", "fsdp", None),
            P("fsdp", "tensor", "context", None),
            P("fsdp", "tensor", "context", None),
            P("fsdp", "tensor", "context", None),
            P("fsdp"),
            P(),
            P(),
            P(),
            P(),
        ),
        check_vma=False,
    )
```

```python
import math

import jax
import jax.numpy as jnp
from jax import lax
from jax.experimental import pallas as pl
from jax.experimental.pallas import tpu as pltpu
from jax.sharding import PartitionSpec as P

D = 1024
HEADS = 16
HEAD_DIM = 64
FF = 2624
ITERS = 5
STEP = 8


rope_base = 160000.0
norm_eps = 1e-05
ns_first = 3.4445
ns_second = -4.775
ns_third = 2.0315
muon_beta = 0.5
muon_rate = 0.15
decay_rate = 0.1
adam_beta = 0.5
adam_rate = 0.05
ortho_eps = 1e-07
adam_eps = 1e-08
precision_highest = lax.Precision.HIGHEST


def layer_norm(values, gain_row):
    centre = values - jnp.mean(values, axis=-1, keepdims=True)
    spread = jnp.mean(centre * centre, axis=-1, keepdims=True)
    return centre * lax.rsqrt(spread + norm_eps) * gain_row


def rope_tables(positions, head_width):
    half_width = head_width // 2
    freqs = rope_base ** (-(jnp.arange(half_width, dtype=jnp.float32) * 2.0 / head_width))
    angle = positions.astype(jnp.float32)[..., None] * freqs
    angle = jnp.concatenate([angle, angle], axis=-1)
    return (jnp.cos(angle), jnp.sin(angle))


def rotate(values, cosine, sine_table):
    half_width = values.shape[-1] // 2
    turned = jnp.concatenate([-values[..., half_width:], values[..., :half_width]], axis=-1)
    return values * cosine + turned * sine_table


def rotate_back(grads_in, cosine, sine_table):
    half_width = grads_in.shape[-1] // 2
    scaled = grads_in * sine_table
    turned = jnp.concatenate([scaled[..., half_width:], -scaled[..., :half_width]], axis=-1)
    return grads_in * cosine + turned


def project(left_rows, right_rows):
    return lax.dot_general(
        left_rows, right_rows, (((1,), (1,)), ((), ())), preferred_element_type=jnp.float32
    )


def contract_exact(left_rows, right_rows):
    return lax.dot_general(
        left_rows,
        right_rows,
        (((0,), (0,)), ((), ())),
        precision=precision_highest,
        preferred_element_type=jnp.float32,
    )


def geglu_gate(gate_part, up_part):
    return jax.nn.gelu(gate_part, approximate=False) * up_part


def per_device(
    tokens,
    out_grad,
    weight_stack,
    muon_state,
    norm_gains,
    adam_first,
    adam_second,
    segment_ids,
    position_ids,
):
    local_len, seq_count, model_width = tokens.shape
    token_count = local_len * seq_count
    groups = lax.axis_size("tensor")
    contexts = lax.axis_size("context")
    full_len = local_len * contexts
    local_rows = weight_stack.shape[2]
    pad_rows = local_rows * contexts
    heads_dev = HEADS // groups
    ff_dev = FF // groups
    inner_width = heads_dev * HEAD_DIM
    counts = (3 * inner_width, inner_width, 2 * ff_dev, ff_dev)
    score_scale = HEAD_DIM ** (-0.5)
    own_block = weight_stack.reshape(local_rows, model_width)
    gathered = lax.all_gather(own_block, ("fsdp", "context"), axis=0, tiled=True).reshape(
        4, pad_rows, model_width
    )
    w_qkv = gathered[0, : counts[0]]
    w_out = gathered[1, : counts[1]]
    w_in = gathered[2, : counts[2]]
    w_down = gathered[3, : counts[3]]
    inputs = tokens.astype(jnp.float32).reshape(token_count, model_width)
    act_in = layer_norm(inputs, norm_gains[0]).astype(jnp.bfloat16)
    projected = project(act_in, w_qkv).reshape(local_len, seq_count, 3, heads_dev, HEAD_DIM)
    cosine, sine_table = rope_tables(position_ids, HEAD_DIM)
    rot_cos = cosine[:, :, None, :]
    rot_sin = sine_table[:, :, None, :]
    query_matrix = rotate(projected[:, :, 0], rot_cos, rot_sin).astype(jnp.bfloat16)
    key_matrix_rows = rotate(projected[:, :, 1], rot_cos, rot_sin).astype(jnp.bfloat16)
    value_matrix_rows = projected[:, :, 2].astype(jnp.bfloat16)
    key_value = jnp.concatenate(
        [
            key_matrix_rows.reshape(local_len, seq_count, inner_width),
            value_matrix_rows.reshape(local_len, seq_count, inner_width),
        ],
        axis=-1,
    )
    key_value_all = lax.all_gather(key_value, "context", axis=0, tiled=True)
    keys_all = key_value_all[..., :inner_width].reshape(full_len, seq_count, heads_dev, HEAD_DIM)
    values_all = key_value_all[..., inner_width:].reshape(full_len, seq_count, heads_dev, HEAD_DIM)
    offset = lax.axis_index("context") * local_len
    seg_query = lax.dynamic_slice_in_dim(segment_ids, offset, local_len, 0)
    same_doc = seg_query.T[:, :, None] == segment_ids.T[:, None, :]
    keep_mask = (seg_query > 0).astype(jnp.float32)
    unscaled_score = jnp.einsum(
        "lshd,mshd->shlm", query_matrix, keys_all, preferred_element_type=jnp.float32
    )
    scores = jnp.where(same_doc[:, None], unscaled_score * score_scale, -jnp.inf)
    row_max = jnp.max(scores, axis=-1, keepdims=True)
    log_total = row_max + jnp.log(jnp.sum(jnp.exp(scores - row_max), axis=-1, keepdims=True))
    probs_low = jnp.exp(scores - log_total).astype(jnp.bfloat16)
    attended = jnp.einsum(
        "shlm,mshd->lshd", probs_low, values_all, preferred_element_type=jnp.float32
    )
    attn_in = (
        (attended * keep_mask[:, :, None, None])
        .astype(jnp.bfloat16)
        .reshape(token_count, inner_width)
    )
    branch_one = lax.psum(
        jnp.dot(attn_in, w_out, preferred_element_type=jnp.float32).astype(jnp.bfloat16), "tensor"
    ).astype(jnp.float32)
    resid = inputs + branch_one
    mlp_in = layer_norm(resid, norm_gains[1]).astype(jnp.bfloat16)
    mixed_rows = project(mlp_in, w_in)
    hidden_full, geglu_pull = jax.vjp(geglu_gate, mixed_rows[:, :ff_dev], mixed_rows[:, ff_dev:])
    hidden = hidden_full.astype(jnp.bfloat16)
    branch_two = lax.psum(
        jnp.dot(hidden, w_down, preferred_element_type=jnp.float32).astype(jnp.bfloat16), "tensor"
    ).astype(jnp.float32)
    layer_out = (resid + branch_two).astype(jnp.bfloat16).reshape(local_len, seq_count, model_width)
    out_cot = out_grad.astype(jnp.float32).reshape(token_count, model_width)
    dbranch_two = out_cot.astype(jnp.bfloat16)
    dhidden = project(dbranch_two, w_down)
    dgate, dup_part = geglu_pull(dhidden)
    dmixed = jnp.concatenate([dgate, dup_part], axis=1).astype(jnp.bfloat16)
    dnormed_two = lax.psum(
        jnp.dot(dmixed, w_in, preferred_element_type=jnp.float32).astype(jnp.bfloat16), "tensor"
    ).astype(jnp.float32)
    norm_two_out, norm_two_pull = jax.vjp(layer_norm, resid, norm_gains[1])
    dresid_norm, dgain_two = norm_two_pull(dnormed_two)
    dresid = out_cot + dresid_norm
    dbranch_one = dresid.astype(jnp.bfloat16)
    keep_low = keep_mask.reshape(token_count, 1).astype(jnp.bfloat16)
    dattended = project(dbranch_one, w_out).astype(jnp.bfloat16) * keep_low
    dattn = dattended.reshape(local_len, seq_count, heads_dev, HEAD_DIM)
    dquery_list = []
    dkey_list = []
    dvalue_list = []
    for head_index in range(heads_dev):
        query_head = query_matrix[:, :, head_index]
        key_head = keys_all[:, :, head_index]
        value_head = values_all[:, :, head_index]
        dout_head = dattn[:, :, head_index]
        raw_head = jnp.einsum(
            "lsd,msd->slm", query_head, key_head, preferred_element_type=jnp.float32
        )
        prob_head = jnp.exp(
            jnp.where(same_doc, raw_head * score_scale, -jnp.inf) - log_total[:, head_index]
        )
        dprob = jnp.einsum(
            "lsd,msd->slm", dout_head, value_head, preferred_element_type=jnp.float32
        )
        delta = jnp.sum(prob_head * dprob, axis=-1, keepdims=True)
        dscore = (prob_head * (dprob - delta) * score_scale).astype(jnp.bfloat16)
        dquery_list.append(
            jnp.einsum("slm,msd->lsd", dscore, key_head, preferred_element_type=jnp.float32)
        )
        dkey_head = jnp.einsum(
            "slm,lsd->msd", dscore, query_head, preferred_element_type=jnp.float32
        )
        dvalue_head = jnp.einsum(
            "slm,lsd->msd",
            prob_head.astype(jnp.bfloat16),
            dout_head,
            preferred_element_type=jnp.float32,
        )
        summed = lax.psum_scatter(
            jnp.concatenate([dkey_head, dvalue_head], axis=-1).astype(jnp.bfloat16),
            "context",
            scatter_dimension=0,
            tiled=True,
        ).astype(jnp.float32)
        dkey_list.append(summed[..., :HEAD_DIM])
        dvalue_list.append(summed[..., HEAD_DIM:])
    dqueries = jnp.stack(dquery_list, axis=2)
    dkeys = jnp.stack(dkey_list, axis=2)
    dvalues = jnp.stack(dvalue_list, axis=2)
    dprojected = (
        jnp.stack(
            [
                rotate_back(dqueries, rot_cos, rot_sin),
                rotate_back(dkeys, rot_cos, rot_sin),
                dvalues,
            ],
            axis=2,
        )
        .astype(jnp.bfloat16)
        .reshape(token_count, 3 * inner_width)
    )
    dnormed_one = lax.psum(
        jnp.dot(dprojected, w_qkv, preferred_element_type=jnp.float32).astype(jnp.bfloat16),
        "tensor",
    ).astype(jnp.float32)
    norm_one_out, norm_one_pull = jax.vjp(layer_norm, inputs, norm_gains[0])
    dinput_norm, dgain_one = norm_one_pull(dnormed_one)
    tokens_grad = (
        (dresid + dinput_norm).astype(jnp.bfloat16).reshape(local_len, seq_count, model_width)
    )
    gain_grads = lax.psum(jnp.stack([dgain_one, dgain_two]), ("fsdp", "context"))

    def padded(block, used_rows):
        return jnp.pad(block, ((0, 0), (0, pad_rows - used_rows)))

    left_rows = jnp.concatenate(
        [
            padded(dprojected, counts[0]),
            padded(attn_in, counts[1]),
            padded(dmixed, counts[2]),
            padded(hidden, counts[3]),
        ],
        axis=1,
    )
    right_rows = jnp.stack([act_in, dbranch_one, mlp_in, dbranch_two])
    blocks = local_rows * lax.axis_size(("fsdp", "context")) // pad_rows
    col_block = left_rows.reshape(token_count, blocks, pad_rows)
    grad_block = lax.psum_scatter(
        jnp.einsum(
            "nbp,bnd->bpd", col_block, right_rows, preferred_element_type=jnp.float32
        ).reshape(local_rows * lax.axis_size(("fsdp", "context")), model_width),
        ("fsdp", "context"),
        scatter_dimension=0,
        tiled=True,
    )
    momentum = muon_state.reshape(local_rows, model_width)
    muon_next = muon_beta * momentum + (1.0 - muon_beta) * grad_block
    direction = (1.0 - muon_beta) * grad_block + muon_beta * muon_next
    norm_total = lax.psum(jnp.sum(direction * direction), ("context", "tensor"))
    norm_size = jnp.sqrt(norm_total)
    direction_scale = jnp.log(norm_size).reshape(1)
    ortho_local = direction / (norm_size + ortho_eps)
    ortho_block = lax.all_gather(
        ortho_local.astype(jnp.bfloat16), "context", axis=0, tiled=True
    ).astype(ortho_local.dtype)
    for sweep_index in range(ITERS):
        gram_sum = lax.psum(
            contract_exact(ortho_block, ortho_block).astype(jnp.bfloat16), "tensor"
        ).astype(jnp.float32)
        square = jnp.dot(
            gram_sum, gram_sum, precision=precision_highest, preferred_element_type=jnp.float32
        )
        mix_matrix = ns_second * gram_sum + ns_third * square
        ortho_block = ns_first * ortho_block + jnp.dot(
            ortho_block, mix_matrix, precision=precision_highest, preferred_element_type=jnp.float32
        )
    own_rows = lax.dynamic_slice_in_dim(
        ortho_block, lax.axis_index("context") * local_rows, local_rows, 0
    )
    owner_index = lax.axis_index("fsdp")
    spreads = jnp.array(
        [0.2 * math.sqrt(3 * D), 0.2 * math.sqrt(D), 0.2 * math.sqrt(2 * FF), 0.2 * math.sqrt(FF)],
        jnp.float32,
    )
    spread = jnp.sum(jnp.where(jnp.arange(4) == owner_index, spreads, 0.0))
    old_weight = own_block.astype(jnp.float32)
    weight_update = -muon_rate * (spread * own_rows + decay_rate * old_weight)
    adam_first_next = adam_beta * adam_first + (1.0 - adam_beta) * gain_grads
    adam_second_next = adam_beta * adam_second + (1.0 - adam_beta) * gain_grads * gain_grads
    correction = 1.0 - adam_beta**STEP
    gain_update = -adam_rate * (
        adam_first_next / correction / (jnp.sqrt(adam_second_next / correction) + adam_eps)
        + decay_rate * norm_gains
    )
    block_shape = (1, 1, local_rows, model_width)
    return (
        layer_out,
        tokens_grad,
        grad_block.reshape(block_shape),
        muon_next.reshape(block_shape),
        weight_update.reshape(block_shape),
        direction_scale,
        gain_grads,
        adam_first_next,
        adam_second_next,
        gain_update,
    )


MESH_ID = pl.DeviceIdType.MESH
ANY = pl.ANY


def ring_place(index):
    return index + index // 2 - 2 * (index // 3)


def split_units(rows, parts, unit=16):
    units = rows // unit
    sizes = [(units // parts + (1 if i < units % parts else 0)) * unit for i in range(parts)]
    return [s for s in sizes if s]


def ring_chunks(counts, local_rows, which, core, target):
    first = core * local_rows
    rows = min(counts[which], first + local_rows) - first
    if rows <= 0:
        return [[], []]
    halves = split_units(rows, 2)
    if len(halves) == 1:
        halves = halves + [0]
    out, at = [], first
    for half in halves:
        pieces = []
        if half:
            for size in split_units(half, max(1, round(half / target))):
                pieces.append((at, size))
                at += size
        out.append(pieces)
    return out


class Place:
    def __init__(self):
        self.f = lax.axis_index("fsdp")
        self.c = lax.axis_index("context")
        self.t = lax.axis_index("tensor")
        self.pos = ring_place(self.f)
        self.next = ring_place((self.pos + 1) % 4)
        self.prev = ring_place((self.pos + 3) % 4)
        homes = (0, 1, 3, 2)
        self.hops = [[(self.pos + 4 - home) % 4, (home + 4 - self.pos) % 4] for home in homes]
        self.outer = jnp.logical_or(self.t == 0, self.t == 3)
        self.inner_mate = jnp.where(self.t == 0, 1, 2)
        self.outer_mate = jnp.where(self.t == 1, 0, 3)

    def ring(self, direction):
        return (self.next if direction == 0 else self.prev, self.c, self.t)

    def partner(self):
        return (self.f, 1 - self.c, self.t)

    def chip_z(self, z):
        return (self.f, self.c, z)

    def hop(self, which, direction):
        return self.hops[which][direction]


def greet(place, ring, partner, line):
    barrier = pltpu.get_barrier_semaphore()

    def signal(device):
        pl.semaphore_signal(barrier, inc=1, device_id=device, device_id_type=MESH_ID)

    count = 0
    if ring:
        signal(place.ring(0))
        signal(place.ring(1))
        count += 2
    if partner:
        signal(place.partner())
        count += 1
    if line:
        @pl.when(place.outer)
        def _():
            signal(place.chip_z(place.inner_mate))
            pl.semaphore_wait(barrier, count + 1)

        @pl.when(jnp.logical_not(place.outer))
        def _():
            signal(place.chip_z(place.outer_mate))
            signal(place.chip_z(3 - place.t))
            pl.semaphore_wait(barrier, count + 2)
    else:
        pl.semaphore_wait(barrier, count)


def remote(src, dst, send, recv, device):
    return pltpu.make_async_remote_copy(
        src_ref=src, dst_ref=dst, send_sem=send, recv_sem=recv, device_id=device, device_id_type=MESH_ID
    )


def run_steps(*tracks):
    total = max(len(track) for track in tracks)
    done = [0] * len(tracks)
    for index in range(total):
        for number, track in enumerate(tracks):
            upto = -(-len(track) * (index + 1) // total)
            while done[number] < upto:
                track[done[number]]()
                done[number] += 1


def gather_plan(counts, local_rows, ks, target=96):
    plan = []
    for core in (0, 1):
        ident = 0
        for which in ks:
            for direction, pieces in enumerate(ring_chunks(counts, local_rows, which, core, target)):
                for order, (row, rows) in enumerate(pieces):
                    plan.append((ident, which, core, direction, order, row, rows))
                    ident += 1
    return plan, max(p[0] for p in plan) + 1


def gather_steps(place, plan, local_rows, base, own_ref, out_ref, sems, skew=2):
    ss, rs, sp, rp = sems

    def dst(which, row, rows):
        return out_ref.at[pl.ds(base[which] + row, rows)]

    def src(core, row, rows):
        return own_ref.at[pl.ds(row - core * local_rows, rows)]

    def begin():
        for ident, which, core, direction, order, row, rows in plan:
            @pl.when(jnp.logical_and(place.c == core, place.f == which))
            def _():
                remote(src(core, row, rows), dst(which, row, rows), ss.at[ident], rs.at[ident],
                       place.ring(direction)).start()
        for ident, which, core, direction, order, row, rows in plan:
            @pl.when(jnp.logical_and(place.c == core, place.f == which))
            def _():
                remote(src(core, row, rows), dst(which, row, rows), sp.at[ident], rp.at[ident],
                       place.partner()).start()

    ordered = sorted(plan, key=lambda p: (p[4], p[1]))
    last = max(p[4] for p in plan)

    def visit(item, role):
        ident, which, core, direction, order, row, rows = item
        mine = dst(which, row, rows)

        @pl.when(jnp.logical_and(place.c == core, place.hop(which, direction) == role))
        def _():
            remote(mine, mine, ss.at[ident], rs.at[ident], place.ring(direction)).wait_recv()
            if role <= 2:
                remote(mine, mine, ss.at[ident], rs.at[ident], place.ring(direction)).start()
            remote(mine, mine, sp.at[ident], rp.at[ident], place.partner()).start()

    def step(j):
        def run():
            for role in (1, 2, 3):
                for item in ordered:
                    if item[4] == j - skew * (role - 1):
                        visit(item, role)
        return run

    def ready():
        for ident, which, core, direction, order, row, rows in plan:
            mine = dst(which, row, rows)

            @pl.when(place.c == 1 - core)
            def _():
                remote(mine, mine, sp.at[ident], rp.at[ident], place.partner()).wait_recv()

    def end():
        for ident, which, core, direction, order, row, rows in plan:
            hop = place.hop(which, direction)
            mine = dst(which, row, rows)

            @pl.when(jnp.logical_and(place.c == core, hop <= 2))
            def _():
                remote(mine, mine, ss.at[ident], rs.at[ident], place.ring(direction)).wait_send()

            @pl.when(place.c == core)
            def _():
                remote(mine, mine, sp.at[ident], rp.at[ident], place.partner()).wait_send()

    return begin, [step(j) for j in range(last + 1 + 2 * skew)], ready, end


def line_steps(place, chunks, own, out, early, mid, low, sems, lag=2, back_lag=3, prep=None, done=None):
    s1, r1, s2, r2, s3, r3 = sems

    def from_end(i, device):
        return remote(own(i), early(i), s1.at[i], r1.at[i], device)

    def across(i):
        return remote(mid(i), low(i), s2.at[i], r2.at[i], place.chip_z(3 - place.t))

    def back(i, device):
        return remote(out(i), out(i), s3.at[i], r3.at[i], device)

    def step(i):
        def run():
            if i < chunks and prep is not None:
                prep(i)

            @pl.when(place.outer)
            def _():
                if i < chunks:
                    from_end(i, place.chip_z(place.inner_mate)).start()
                if 0 <= i - lag - back_lag < chunks:
                    back(i - lag - back_lag, place.chip_z(place.inner_mate)).wait_recv()

            @pl.when(jnp.logical_not(place.outer))
            def _():
                if i < chunks:
                    from_end(i, place.chip_z(place.outer_mate)).wait_recv()
                    pair = own(i)[...].astype(jnp.float32) + early(i)[...].astype(jnp.float32)
                    mid(i)[...] = pair.astype(mid(i).dtype)
                    across(i).start()
                j = i - lag
                if 0 <= j < chunks:
                    across(j).wait_recv()
                    total = mid(j)[...].astype(jnp.float32) + low(j)[...].astype(jnp.float32)
                    out(j)[...] = total.astype(out(j).dtype)
                    back(j, place.chip_z(place.outer_mate)).start()
            if done is not None:
                if 0 <= i - lag - back_lag < chunks:
                    done(i - lag - back_lag)
        return run

    def end():
        @pl.when(place.outer)
        def _():
            for i in range(chunks):
                from_end(i, place.chip_z(place.inner_mate)).wait_send()

        @pl.when(jnp.logical_not(place.outer))
        def _():
            for i in range(chunks):
                across(i).wait_send()
                back(i, place.chip_z(place.outer_mate)).wait_send()

    return [step(i) for i in range(chunks + lag + back_lag)], end


def scatter_steps(place, plan, local_rows, base, part_ref, grad_ref, prx, rrx, tx, sems, skew=2):
    ss, rs, sp, rp = sems

    def rows_of(ref, which, row, rows):
        return ref.at[pl.ds(base[which] + row, rows)]

    def partner_copy(item):
        ident, which, core, direction, order, row, rows = item
        return remote(rows_of(part_ref, which, row, rows), rows_of(prx, which, row, rows),
                      sp.at[ident], rp.at[ident], place.partner())

    def ring_copy(item):
        ident, which, core, direction, order, row, rows = item
        return remote(rows_of(tx, which, row, rows), rows_of(rrx, which, row, rows),
                      ss.at[ident], rs.at[ident], place.ring(direction))

    ordered = sorted(plan, key=lambda p: (p[4], p[1]))
    last = max(p[4] for p in plan)

    def begin(ks):
        for item in ordered:
            if item[1] in ks:
                @pl.when(place.c == 1 - item[2])
                def _():
                    partner_copy(item).start()

    def visit(item, late):
        ident, which, core, direction, order, row, rows = item
        hop = place.hop(which, direction)
        role = (late + 1) % 4

        @pl.when(jnp.logical_and(place.c == core, hop == role))
        def _():
            partner_copy(item).wait_recv()
            total = (rows_of(part_ref, which, row, rows)[...].astype(jnp.float32)
                     + rows_of(prx, which, row, rows)[...].astype(jnp.float32))
            if role != 1:
                ring_copy(item).wait_recv()
                total = total + rows_of(rrx, which, row, rows)[...].astype(jnp.float32)
            if role == 0:
                grad_ref[pl.ds(row - core * local_rows, rows)] = total
            else:
                rows_of(tx, which, row, rows)[...] = total.astype(tx.dtype)
                ring_copy(item).start()

    def step(j):
        def run():
            for late in range(4):
                for item in ordered:
                    if item[4] == j - skew * late:
                        visit(item, late)
        return run

    def end():
        for item in plan:
            ident, which, core, direction, order, row, rows = item

            @pl.when(place.c == 1 - core)
            def _():
                partner_copy(item).wait_send()

            @pl.when(jnp.logical_and(place.c == core, place.hop(which, direction) != 0))
            def _():
                ring_copy(item).wait_send()

    return begin, [step(j) for j in range(last + 1 + 3 * skew)], end


VMEM_SPEC = pl.BlockSpec(memory_space=pltpu.VMEM)
ANY_SPEC = pl.BlockSpec(memory_space=pl.ANY)


def dma(count):
    return pltpu.SemaphoreType.DMA((count,))


def comm_call(kernel, outs, ins, in_specs, out_specs, scratch, ident):
    return pl.pallas_call(
        kernel,
        out_shape=outs,
        in_specs=in_specs,
        out_specs=out_specs,
        scratch_shapes=scratch,
        compiler_params=pltpu.CompilerParams(
            collective_id=ident, has_side_effects=True, vmem_limit_bytes=60 * 2**20
        ),
    )(*ins)


def base_rows(counts, ks):
    base, at = {}, 0
    for which in ks:
        base[which] = at
        at += counts[which]
    return base, at


def own_rows_copy(place, counts, local_rows, ks, base, own_ref, out_ref, sem, act):
    for which in ks:
        for core in (0, 1):
            rows = min(counts[which] - core * local_rows, local_rows)
            if rows > 0:
                @pl.when(jnp.logical_and(place.c == core, place.f == which))
                def _():
                    act(pltpu.make_async_copy(
                        own_ref.at[pl.ds(0, rows)],
                        out_ref.at[pl.ds(base[which] + core * local_rows, rows)],
                        sem.at[0],
                    ))


class LineSum:
    def __init__(self, place, rows, own, early, mid, low, total, sems):
        self.place, self.rows = place, rows
        self.own, self.early, self.mid, self.low, self.total = own, early, mid, low, total
        self.sems = sems

    def cut(self, ref, i):
        return ref.at[pl.ds(pl.multiple_of(i * self.rows, self.rows), self.rows)]

    def from_end(self, i, mate):
        s1, r1 = self.sems[:2]
        return remote(self.cut(self.own, i), self.cut(self.early, i), s1.at[i], r1.at[i], self.place.chip_z(mate))

    def across(self, i):
        s2, r2 = self.sems[2:4]
        return remote(self.cut(self.mid, i), self.cut(self.low, i), s2.at[i], r2.at[i], self.place.chip_z(3 - self.place.t))

    def back(self, i, mate):
        s3, r3 = self.sems[4:6]
        return remote(self.cut(self.total, i), self.cut(self.total, i), s3.at[i], r3.at[i], self.place.chip_z(mate))

    def send(self, i):
        @pl.when(self.place.outer)
        def _():
            self.from_end(i, self.place.inner_mate).start()

    def pair_up(self, i):
        @pl.when(jnp.logical_not(self.place.outer))
        def _():
            self.from_end(i, self.place.outer_mate).wait_recv()
            pair = self.cut(self.own, i)[...].astype(jnp.float32) + self.cut(self.early, i)[...].astype(jnp.float32)
            self.cut(self.mid, i)[...] = pair.astype(self.mid.dtype)
            self.across(i).start()

    def join(self, i):
        @pl.when(jnp.logical_not(self.place.outer))
        def _():
            self.across(i).wait_recv()
            whole = self.cut(self.mid, i)[...].astype(jnp.float32) + self.cut(self.low, i)[...].astype(jnp.float32)
            self.cut(self.total, i)[...] = whole.astype(self.total.dtype)
            self.back(i, self.place.outer_mate).start()

    def receive(self, i):
        @pl.when(self.place.outer)
        def _():
            self.back(i, self.place.inner_mate).wait_recv()

    def finish(self, pieces):
        @pl.when(self.place.outer)
        def _():
            for i in range(pieces):
                self.from_end(i, self.place.inner_mate).wait_send()

        @pl.when(jnp.logical_not(self.place.outer))
        def _():
            for i in range(pieces):
                self.across(i).wait_send()
                self.back(i, self.place.outer_mate).wait_send()


def nt_dot(left, right):
    return lax.dot_general(left, right, (((1,), (1,)), ((), ())), preferred_element_type=jnp.float32)


def nn_dot(left, right):
    return jnp.dot(left, right, preferred_element_type=jnp.float32)


def tn_dot(left, right):
    return lax.dot_general(left, right, (((0,), (0,)), ((), ())), preferred_element_type=jnp.float32)


def centred(values):
    centre = values - jnp.mean(values, axis=-1, keepdims=True)
    spread = jnp.mean(centre * centre, axis=-1, keepdims=True)
    return centre, lax.rsqrt(spread + norm_eps)


def norm_back(values, gain_row, grads):
    centre, scale = centred(values)
    xhat = centre * scale
    e = grads * gain_row
    moved = scale * (e - jnp.mean(e, axis=-1, keepdims=True) - xhat * jnp.mean(e * xhat, axis=-1, keepdims=True))
    return moved, jnp.sum(grads * xhat, axis=0, keepdims=True)


def layer_both_ways(tokens, out_grad, own_block, norm_gains, cosine, sine, seg_column, seg_row, counts, ident):
    count, width = tokens.shape
    local_rows = own_block.shape[0]
    inner = counts[1]
    ff = counts[3]
    heads = inner // HEAD_DIM
    full = 2 * count
    rows = count // 4
    split = 4
    sub = rows // split
    pieces = 4 * split
    stack = heads * rows
    piece = 64
    score_scale = HEAD_DIM ** (-0.5)
    f32, low = jnp.float32, jnp.bfloat16
    first_plan, first_count = gather_plan(counts, local_rows, (0, 1), 64)
    last_plan, last_count = gather_plan(counts, local_rows, (2, 3), 64)
    first_base, first_rows = base_rows(counts, (0, 1))
    last_base, last_rows = base_rows(counts, (2, 3))

    def kernel(tok_ref, og_ref, own_ref, gain_ref, cos_ref, sin_ref, sc_ref, sr_ref,
               act_ref, attn_ref, resid_ref, mlp_ref, hid_ref, dm_ref, b2_ref, dres_ref, db_ref, dproj_ref, t3_ref, dg_ref,
               w1st, wlast, q_ref, kv_ref, kq_ref, p_ref, s_ref, pl_ref, do_ref, dp_ref, ds_ref,
               t1_ref, e1, m1, l1, sum1, t2_ref, e2, m2, l2, sum2, dq_ref, dkv_ref, dkv_tx, dkv_rx, cos_all, sin_all, *sems):
        place = Place()
        greet(place, True, True, True)
        begin1, steps1, ready1, end1 = gather_steps(place, first_plan, local_rows, first_base, own_ref, w1st, sems[0:4], 1)
        begin2, steps2, ready2, end2 = gather_steps(place, last_plan, local_rows, last_base, own_ref, wlast, sems[4:8])
        line1 = LineSum(place, sub, t1_ref, e1, m1, l1, sum1, sems[8:14])
        line2 = LineSum(place, sub, t2_ref, e2, m2, l2, sum2, sems[14:20])
        swap, local_sem = sems[20], sems[21]

        def each_piece(act, chunk):
            for part in range(split):
                act(split * chunk + part)

        begin1()
        own_rows_copy(place, counts, local_rows, (0, 1), first_base, own_ref, w1st, local_sem, lambda d: d.start())

        def at(i, size=rows):
            return pl.ds(pl.multiple_of(i * size, size), size)

        def norm_one(i, carry):
            centre, scale = centred(tok_ref[at(i)].astype(f32))
            act_ref[at(i)] = (centre * scale * gain_ref[0:1]).astype(low)
            cos_all[at(i)] = jnp.concatenate([cos_ref[at(i)]] * (2 * heads), axis=1)
            sin_all[at(i)] = jnp.concatenate([sin_ref[at(i)]] * (2 * heads), axis=1)
            return carry

        lax.fori_loop(0, 4, norm_one, 0)
        dg_ref[...] = jnp.zeros_like(dg_ref)
        begin2()
        run_steps(steps1)
        own_rows_copy(place, counts, local_rows, (0, 1), first_base, own_ref, w1st, local_sem, lambda d: d.wait())
        own_rows_copy(place, counts, local_rows, (2, 3), last_base, own_ref, wlast, local_sem, lambda d: d.start())
        ready1()
        waiting = list(steps2)

        def forward(number):
            for step in waiting[:number]:
                step()
            del waiting[:number]

        forward(1)

        lane = lax.broadcasted_iota(jnp.int32, (1, inner), 1)
        front = (lane % HEAD_DIM) < HEAD_DIM // 2

        def half_turn(value):
            return jnp.where(front, pltpu.roll(value, inner - HEAD_DIM // 2, 1), pltpu.roll(value, HEAD_DIM // 2, 1))

        sign = jnp.where(front, -1.0, 1.0).astype(f32)

        def rotated(value, i):
            return value * cos_all[at(i)] + half_turn(value) * (sin_all[at(i)] * sign)

        def rotated_back(value, i):
            return value * cos_all[at(i)] - half_turn(value * sin_all[at(i)]) * sign

        def project_rows(i, carry):
            value = nt_dot(act_ref[at(i)], w1st[0:3 * inner])
            q_ref[at(i)] = rotated(value[:, 0:inner], i).astype(low)
            kv_ref[at(i), 0:inner] = rotated(value[:, inner:2 * inner], i).astype(low)
            kv_ref[at(i), inner:2 * inner] = value[:, 2 * inner:3 * inner].astype(low)
            return carry

        lax.fori_loop(0, 4, project_rows, 0)
        kv_copy = remote(kv_ref.at[pl.ds(0, count)], kv_ref.at[pl.ds(count, count)], swap.at[0], swap.at[1], place.partner())
        kv_copy.start()
        forward(2)
        kv_copy.wait()

        def head_mask(h):
            return jnp.logical_and(lane >= h * HEAD_DIM, lane < (h + 1) * HEAD_DIM)

        def stacked(value):
            return jnp.concatenate([jnp.where(head_mask(h), value, jnp.zeros_like(value)) for h in range(heads)], axis=0)

        def unstacked(value):
            total = jnp.where(head_mask(0), value[0:rows], 0.0)
            for h in range(1, heads):
                total = total + jnp.where(head_mask(h), value[h * rows:(h + 1) * rows], 0.0)
            return total

        per = rows // piece

        def attend(i):
            kq_ref[...] = stacked(q_ref[at(i)])
            s_ref[...] = nt_dot(kq_ref[...], kv_ref[:, 0:inner])

            def soft(r, inside):
                seg = sc_ref[pl.ds(pl.multiple_of(i * rows + (r % per) * piece, piece), piece)]
                score = jnp.where(seg == sr_ref[...], s_ref[at(r, piece)] * score_scale, -jnp.inf)
                score = jnp.exp(score - jnp.max(score, axis=-1, keepdims=True))
                prob = score * (1.0 / jnp.sum(score, axis=-1, keepdims=True))
                p_ref[i, at(r, piece)] = prob
                pl_ref[at(r, piece)] = prob.astype(low)
                return inside

            lax.fori_loop(0, stack // piece, soft, 0)
            mixed = unstacked(nn_dot(pl_ref[...], kv_ref[:, inner:2 * inner]))
            keep = (sc_ref[at(i)] > 0).astype(f32)
            attn = (mixed * keep).astype(low)
            attn_ref[at(i)] = attn
            t1_ref[at(i)] = nn_dot(attn, w1st[3 * inner:4 * inner]).astype(low)
            each_piece(line1.send, i)

            if i >= 1:
                each_piece(line1.pair_up, i - 1)
            if i >= 2:
                each_piece(line1.join, i - 2)

        for i in range(4):
            attend(i)
            forward(2)
        forward(len(waiting))
        own_rows_copy(place, counts, local_rows, (2, 3), last_base, own_ref, wlast, local_sem, lambda d: d.wait())
        ready2()

        def feed(i, carry):
            each_piece(line1.receive, i)
            resid = tok_ref[at(i)].astype(f32) + sum1[at(i)].astype(f32)
            resid_ref[at(i)] = resid
            centre, scale = centred(resid)
            mlp = (centre * scale * gain_ref[1:2]).astype(low)
            mlp_ref[at(i)] = mlp
            gate = nt_dot(mlp, wlast[0:ff])
            up = nt_dot(mlp, wlast[ff:2 * ff])
            cdf = 0.5 * (1.0 + lax.erf(gate * (0.5 ** 0.5)))
            bell = jnp.exp(gate * gate * -0.5) * (1.0 / math.sqrt(2.0 * math.pi))
            gelu = gate * cdf
            hidden = (gelu * up).astype(low)
            hid_ref[at(i)] = hidden
            dhidden = nt_dot(og_ref[at(i)], wlast[2 * ff:3 * ff])
            dgate = (dhidden * up * (cdf + gate * bell)).astype(low)
            dup = (dhidden * gelu).astype(low)
            dm_ref[0, at(i)] = dgate
            dm_ref[1, at(i)] = dup
            t2_ref[at(i)] = (nn_dot(dgate, wlast[0:ff]) + nn_dot(dup, wlast[ff:2 * ff])).astype(low)
            each_piece(line2.send, i)
            b2_ref[at(i)] = nn_dot(hidden, wlast[2 * ff:3 * ff]).astype(low)

            @pl.when(i == 0)
            def _():
                each_piece(line1.pair_up, 3)

            @pl.when(i <= 1)
            def _():
                each_piece(line1.join, i + 2)

            @pl.when(i >= 1)
            def _():
                each_piece(line2.pair_up, i - 1)

            @pl.when(i >= 2)
            def _():
                each_piece(line2.join, i - 2)
            return carry

        lax.fori_loop(0, 4, feed, 0)
        dkv_ref[...] = jnp.zeros_like(dkv_ref)

        def turn_back(i, carry):
            each_piece(line2.receive, i)
            moved, gain_part = norm_back(resid_ref[at(i)], gain_ref[1:2], sum2[at(i)].astype(f32))
            dg_ref[1:2] = dg_ref[1:2] + gain_part
            dresid = og_ref[at(i)].astype(f32) + moved
            dres_ref[at(i)] = dresid
            dbranch = dresid.astype(low)
            db_ref[at(i)] = dbranch
            keep = (sc_ref[at(i)] > 0).astype(low)
            dattn = nt_dot(dbranch, w1st[3 * inner:4 * inner]).astype(low) * keep
            do_ref[...] = stacked(dattn)
            kq_ref[...] = stacked(q_ref[at(i)])
            dp_ref[...] = nt_dot(do_ref[...], kv_ref[:, inner:2 * inner])

            def soft_back(r, inside):
                prob = p_ref[i, at(r, piece)]
                dprob = dp_ref[at(r, piece)]
                delta = jnp.sum(prob * dprob, axis=-1, keepdims=True)
                ds_ref[at(r, piece)] = (prob * (dprob - delta) * score_scale).astype(low)
                pl_ref[at(r, piece)] = prob.astype(low)
                return inside

            lax.fori_loop(0, stack // piece, soft_back, 0)
            dq_ref[at(i)] = unstacked(nn_dot(ds_ref[...], kv_ref[:, 0:inner]))
            dkv_ref[:, 0:inner] = dkv_ref[:, 0:inner] + tn_dot(ds_ref[...], kq_ref[...])
            dkv_ref[:, inner:2 * inner] = dkv_ref[:, inner:2 * inner] + tn_dot(pl_ref[...], do_ref[...])

            @pl.when(i == 0)
            def _():
                each_piece(line2.pair_up, 3)

            @pl.when(i <= 1)
            def _():
                each_piece(line2.join, i + 2)
            return carry

        lax.fori_loop(0, 4, turn_back, 0)
        dkv_tx[...] = dkv_ref[count:full].astype(low)
        dkv_copy = remote(dkv_tx, dkv_rx, swap.at[2], swap.at[3], place.partner())
        dkv_copy.start()

        def unproject_query(i, carry):
            dproj_ref[at(i), 0:inner] = rotated_back(dq_ref[at(i)], i).astype(low)
            return carry

        lax.fori_loop(0, 4, unproject_query, 0)
        dkv_copy.wait()

        def unproject(i, carry):
            both = dkv_ref[at(i)] + dkv_rx[at(i)].astype(f32)
            dproj_ref[at(i), inner:2 * inner] = rotated_back(both[:, 0:inner], i).astype(low)
            dproj_ref[at(i), 2 * inner:3 * inner] = both[:, inner:2 * inner].astype(low)
            t3_ref[at(i)] = nn_dot(dproj_ref[at(i)], w1st[0:3 * inner]).astype(low)
            return carry

        lax.fori_loop(0, 4, unproject, 0)
        line1.finish(pieces)
        line2.finish(pieces)
        end1()
        end2()

    def shape(*dims, dtype=low):
        return jax.ShapeDtypeStruct(dims, dtype)

    outs = (
        shape(count, width), shape(count, inner), shape(count, width, dtype=f32), shape(count, width), shape(count, ff),
        shape(2, count, ff), shape(count, width), shape(count, width, dtype=f32), shape(count, width),
        shape(count, 3 * inner), shape(count, width), shape(8, width, dtype=f32),
    )
    line = pltpu.VMEM((count, width), low)
    scratch = [
        pltpu.VMEM((first_rows, width), low), pltpu.VMEM((last_rows, width), low), pltpu.VMEM((count, inner), low),
        pltpu.VMEM((full, 2 * inner), low), pltpu.VMEM((stack, inner), low), pltpu.VMEM((4, stack, full), f32),
        pltpu.VMEM((stack, full), f32), pltpu.VMEM((stack, full), low), pltpu.VMEM((stack, inner), low),
        pltpu.VMEM((stack, full), f32), pltpu.VMEM((stack, full), low),
    ]
    scratch += [line] * 10
    scratch += [
        pltpu.VMEM((count, inner), f32), pltpu.VMEM((full, 2 * inner), f32),
        pltpu.VMEM((count, 2 * inner), low), pltpu.VMEM((count, 2 * inner), low),
        pltpu.VMEM((count, inner), f32), pltpu.VMEM((count, inner), f32),
    ]
    scratch += [dma(first_count)] * 4 + [dma(last_count)] * 4 + [dma(pieces)] * 12 + [dma(4), dma(1)]
    ins = (tokens, out_grad, own_block, norm_gains, cosine, sine, seg_column, seg_row)
    return pl.pallas_call(
        kernel,
        out_shape=outs,
        in_specs=[VMEM_SPEC] * len(ins),
        out_specs=(VMEM_SPEC,) * len(outs),
        scratch_shapes=scratch,
        compiler_params=pltpu.CompilerParams(
            collective_id=ident, has_side_effects=True, vmem_limit_bytes=67043328
        ),
    )(*ins)


def tail_grams(left_right, muon_rows, counts, ident):
    dproj, act_in, attn_in, dbranch, dmixed, mlp_in, hidden, out_low = left_right
    local_rows, width = muon_rows.shape
    ks = (0, 1, 2, 3)
    plan, count = gather_plan(counts, local_rows, ks, 96)
    base, total_rows = base_rows(counts, ks)
    ff = counts[3]
    tile = width // 4
    split = 4
    half = tile // split
    chunks = 5 * split
    f32, low16 = jnp.float32, jnp.bfloat16

    def kernel(dp_ref, act_ref, at_ref, db_ref, dm_ref, mlp_ref, hid_ref, og_ref, mu_ref,
               grad_ref, x_ref, g_ref, norm_ref,
               part, prx, rrx, mine, theirs, gprx, tot, other, early, mid, low, norm_own, *sems):
        place = Place()
        c = place.c
        greet(place, True, True, True)
        begin, steps, end = scatter_steps(place, plan, local_rows, base, part, grad_ref, prx, rrx, part, sems[:4])

        def terms(row, left, right):
            span = left.shape[1]

            def columns(j, carry):
                cols = pl.ds(pl.multiple_of(j * tile, tile), tile)
                part[pl.ds(row, span), cols] = tn_dot(left[...], right[:, cols]).astype(low16)
                return carry

            lax.fori_loop(0, 4, columns, 0)

        terms(base[2], dm_ref.at[0], mlp_ref)
        terms(base[2] + ff, dm_ref.at[1], mlp_ref)
        begin((2,))
        terms(base[3], hid_ref, og_ref)
        begin((3,))
        terms(base[0], dp_ref, act_ref)
        begin((0,))
        terms(base[1], at_ref, db_ref)
        begin((1,))
        grad_ref[...] = jnp.zeros_like(grad_ref)
        run_steps(steps)
        end()

        def momentum(i, carry):
            sl = pl.ds(pl.multiple_of(i * 16, 16), 16)
            grad = grad_ref[sl]
            after = muon_beta * mu_ref[sl] + (1.0 - muon_beta) * grad
            direction = (1.0 - muon_beta) * grad + muon_beta * after
            x_ref[sl] = direction.astype(low16)
            square = direction * direction
            return carry + square[0:8] + square[8:16]

        square = lax.fori_loop(0, local_rows // 16, momentum, jnp.zeros((8, width), f32))
        own_square = jnp.broadcast_to(jnp.sum(jnp.sum(square, axis=1, keepdims=True), axis=0, keepdims=True), (8, tile))
        norm_own[...] = own_square

        sp, rp, st, rt = sems[10:14]

        def blocks(core):
            return [(3 * core, 3 * core), (2 * core, 2 * core + 1), (core + 1, core + 1), (core, core + 2), (core, 3 - core)]

        def at(k):
            return pl.ds(pl.multiple_of(k * tile, tile), tile)

        def gram(i, j):
            return tn_dot(x_ref[:, at(i)], x_ref[:, at(j)])

        def partner(n):
            sl = pl.ds(n * tile, tile)
            return remote(theirs.at[sl], gprx.at[sl], sp.at[n], rp.at[n], place.partner())

        def norm_row(ref):
            return ref.at[pl.ds(5 * tile, 8)]

        for n, (i, j) in enumerate(blocks(1 - c)):
            theirs[pl.ds(n * tile, tile)] = gram(i, j)
            partner(n).start()
        norm_row(theirs)[...] = norm_own[...]
        pn = remote(norm_row(theirs), norm_row(gprx), sp.at[5], rp.at[5], place.partner())
        pn.start()

        def span(i):
            return pl.ds(i * half, half) if i < chunks - 1 else pl.ds(i * half, half + 8)

        def cut(ref):
            return lambda i: ref.at[span(i)]

        def prep(i):
            if i % split == 0:
                n = i // split
                sl = pl.ds(n * tile, tile)
                block = gram(*blocks(c)[n])
                partner(n).wait_recv()
                mine[sl] = block + gprx[sl]
            if i == chunks - 1:
                pn.wait_recv()
                norm_row(mine)[...] = norm_row(gprx)[...] + norm_own[...]

        def share(i):
            return remote(cut(tot)(i), cut(other)(i), st.at[i], rt.at[i], place.partner())

        def place_block(ref, n, core):
            i, j = blocks(core)[n]
            block = ref[pl.ds(n * tile, tile)]
            g_ref[at(i), at(j)] = block
            g_ref[at(j), at(i)] = block.T

        def done(i):
            share(i).start()
            if i % split == split - 1:
                place_block(tot, i // split, c)
            if i >= 2:
                share(i - 2).wait_recv()
                if (i - 2) % split == split - 1:
                    place_block(other, (i - 2) // split, 1 - c)

        line, line_end = line_steps(place, chunks, cut(mine), cut(tot), cut(early), cut(mid), cut(low), sems[4:10],
                                    lag=3, back_lag=4, prep=prep, done=done)
        run_steps(line)
        for i in (chunks - 2, chunks - 1):
            share(i).wait_recv()
        place_block(other, 4, 1 - c)
        norm_ref[...] = jnp.broadcast_to(tot[5 * tile:5 * tile + 8, 0:128], (8, 128))
        line_end()
        for n in range(5):
            partner(n).wait_send()
        pn.wait_send()
        for i in range(chunks):
            share(i).wait_send()

    rows_low = pltpu.VMEM((total_rows, width), low16)
    packed = pltpu.VMEM((5 * tile + 8, tile), f32)
    outs = (
        jax.ShapeDtypeStruct((local_rows, width), f32),
        jax.ShapeDtypeStruct((local_rows, width), low16), jax.ShapeDtypeStruct((width, width), f32),
        jax.ShapeDtypeStruct((8, 128), f32),
    )
    scratch = [rows_low] * 3 + [packed] * 8 + [pltpu.VMEM((8, tile), f32)]
    scratch += [dma(count)] * 4 + [dma(chunks)] * 6 + [dma(6), dma(6), dma(chunks), dma(chunks)]
    ins = tuple(left_right) + (muon_rows,)
    return comm_call(kernel, outs, ins, [VMEM_SPEC] * len(ins), (VMEM_SPEC,) * len(outs), scratch, ident)


def halves(value):
    high = value.astype(jnp.bfloat16)
    return high, (value - high.astype(jnp.float32)).astype(jnp.bfloat16)


def iterate(gram, norm, direction_low, normed_term, branch_term, tokens_in, resid, dresid, dgain_rows, norm_gains, adam_first,
            adam_second, ident):
    rows, width = direction_low.shape
    tile = 256
    parts = width // tile
    tokens = branch_term.shape[0]
    each = 8
    chunks = 2 * each
    step_rows = tokens // each
    aa = ns_first * ns_first
    ab = 2.0 * ns_first * ns_second
    bbac = ns_second * ns_second + 2.0 * ns_first * ns_third
    bc = 2.0 * ns_second * ns_third
    cc = ns_third * ns_third
    correction = 1.0 - adam_beta**STEP

    def kernel(g_ref, n_ref, d_ref, t3_ref, b2_ref, tok_ref, r_ref, dres_ref, dgr_ref, gain_ref, af_ref, as_ref,
               x_ref, lo_ref, tg_ref, gg_ref, afn_ref, asn_ref, gu_ref,
               p_ref, ph, pl_, hh, hl, uh, ul, mx, early, mid, low, total, held, dg_ref, acc, *sems):
        place = Place()
        s1, r1, s2, r2, s3, r3, sg, rg = sems
        me = place.f * 2 + place.c
        barrier = pltpu.get_barrier_semaphore()

        def plane(shift):
            other = (me + shift) % 8
            return (other // 2, other % 2, place.t)

        for shift in range(1, 8):
            pl.semaphore_signal(barrier, inc=1, device_id=plane(shift), device_id_type=MESH_ID)

        @pl.when(place.outer)
        def _():
            pl.semaphore_signal(barrier, inc=1, device_id=place.chip_z(place.inner_mate), device_id_type=MESH_ID)
            pl.semaphore_wait(barrier, 8)

        @pl.when(jnp.logical_not(place.outer))
        def _():
            pl.semaphore_signal(barrier, inc=1, device_id=place.chip_z(place.outer_mate), device_id_type=MESH_ID)
            pl.semaphore_signal(barrier, inc=1, device_id=place.chip_z(3 - place.t), device_id_type=MESH_ID)
            pl.semaphore_wait(barrier, 9)

        def cut(ref, i):
            if isinstance(i, int):
                return ref.at[pl.ds(i * step_rows, step_rows)]
            return ref.at[pl.ds(pl.multiple_of(i * step_rows, step_rows), step_rows)]

        def from_end(i, device, own):
            local = i % each
            return remote(cut(own, local), cut(early, i), s1.at[i], r1.at[i], device)

        def across(i):
            return remote(cut(mid, i), cut(low, i), s2.at[i], r2.at[i], place.chip_z(3 - place.t))

        def back(i, device):
            return remote(cut(total, i), cut(total, i), s3.at[i], r3.at[i], device)

        dg_ref[...] = jnp.zeros_like(dg_ref)

        @pl.when(place.outer)
        def _():
            for i in range(each):
                from_end(i, place.chip_z(place.inner_mate), t3_ref).start()
            for i in range(each):
                from_end(each + i, place.chip_z(place.inner_mate), b2_ref).start()

        def pair_up(i, own):
            @pl.when(jnp.logical_not(place.outer))
            def _():
                from_end(i, place.chip_z(place.outer_mate), own).wait_recv()
                pair = cut(own, i % each)[...].astype(jnp.float32) + cut(early, i)[...].astype(jnp.float32)
                cut(mid, i)[...] = pair.astype(mid.dtype)
                across(i).start()

        def join(i):
            @pl.when(jnp.logical_not(place.outer))
            def _():
                across(i).wait_recv()
                whole = cut(mid, i)[...].astype(jnp.float32) + cut(low, i)[...].astype(jnp.float32)
                cut(total, i)[...] = whole.astype(total.dtype)
                back(i, place.chip_z(place.outer_mate)).start()

        plan = {
            "start": {4: ((), (13,))},
            "squares": {1: ((), (0,)), 2: ((), (3, 4, 5)), 3: ((), (8, 9, 10)), 4: ((), (14,))},
            "rows": {1: ((3, 4, 5), (1,)), 2: ((8, 9, 10), ()), 3: ((13, 14, 15), ()), 4: ((), (15,))},
            "cube": {0: ((0, 1, 2), ()), 1: ((6, 7), (2,)), 2: ((11, 12), (6, 7)), 3: ((), (11, 12))},
        }

        def travel(spot, sweep):
            for when, (pairs, joins) in plan[spot].items():
                @pl.when(sweep == when)
                def _():
                    for i in joins:
                        join(i)
                    for i in pairs:
                        pair_up(i, t3_ref if i < each else b2_ref)

        norm_size = jnp.sqrt(n_ref[0:1, 0:1])
        inverse = 1.0 / (norm_size + ortho_eps)
        scale = inverse * inverse

        for k in range(parts):
            sl = pl.ds(k * tile, tile)
            value = g_ref[sl] * scale
            p_ref[sl] = value
            high, rest = halves(value)
            ph[sl] = high
            pl_[sl] = rest
        x_ref[...] = d_ref[...].astype(jnp.float32) * inverse

        def product(lh, ll, rh, rl, k):
            sl, cols = pl.ds(k * tile, tile), pl.ds(k * tile, width - k * tile)

            def dot(left, right):
                return jnp.dot(left[sl], right[:, cols], preferred_element_type=jnp.float32)

            return dot(lh, rh) + dot(ll, rh) + dot(lh, rl)

        def spread_out(value, high_ref, low_ref, k):
            sl, cols = pl.ds(k * tile, tile), pl.ds(k * tile, width - k * tile)
            high, rest = halves(value)
            high_ref[sl, cols] = high
            low_ref[sl, cols] = rest
            for j in range(k + 1, parts):
                at = (j - k) * tile
                high_ref[pl.ds(j * tile, tile), sl] = high[:, at:at + tile].T
                low_ref[pl.ds(j * tile, tile), sl] = rest[:, at:at + tile].T

        def squares(sweep):
            for k in range(parts):
                sl, cols = pl.ds(k * tile, tile), pl.ds(k * tile, width - k * tile)
                room = width - k * tile
                acc[:, 0:room] = nn_dot(ph[sl], ph[:, cols])

                @pl.when(sweep < ITERS - 1)
                def _():
                    acc[:, 0:room] = acc[:, 0:room] + nn_dot(pl_[sl], ph[:, cols]) + nn_dot(ph[sl], pl_[:, cols])
                value = acc[:, 0:room]
                spread_out(value, hh, hl, k)
                mix = (ns_second * p_ref[sl, cols] + ns_third * value).astype(mx.dtype)
                mx[sl, cols] = mix
                for j in range(k + 1, parts):
                    at = (j - k) * tile
                    mx[pl.ds(j * tile, tile), sl] = mix[:, at:at + tile].T

        def rotate_rows():
            for at, size in ((0, 336), (336, 320)):
                sl = pl.ds(at, size)
                old = x_ref[sl]
                x_ref[sl] = ns_first * old + jnp.dot(old.astype(jnp.bfloat16), mx[...], preferred_element_type=jnp.float32)

        def gains_copy(shift):
            return remote(dg_ref, held.at[me], sg.at[shift], rg.at[shift], plane(shift))

        def first_norm_back():
            @pl.when(place.outer)
            def _():
                for i in range(each):
                    back(i, place.chip_z(place.inner_mate)).wait_recv()

            def some(i, inside):
                sl = pl.ds(pl.multiple_of(i * 64, 64), 64)
                moved, gain_part = norm_back(tok_ref[sl].astype(jnp.float32), gain_ref[0:1], total[sl].astype(jnp.float32))
                dg_ref[0:1] = dg_ref[0:1] + gain_part
                tg_ref[sl] = (dres_ref[sl] + moved).astype(tg_ref.dtype)
                return inside

            lax.fori_loop(0, tokens // 64, some, 0)
            dg_ref[1:2] = dgr_ref[1:2]
            held[pl.ds(me, 1)] = dg_ref[...][None]
            for shift in range(1, 8):
                gains_copy(shift).start()

        def body(sweep, carry):
            travel("start", sweep)
            squares(sweep)
            travel("squares", sweep)
            rotate_rows()
            travel("rows", sweep)

            @pl.when(sweep < ITERS - 1)
            def _():
                for k in range(parts):
                    sl, cols = pl.ds(k * tile, tile), pl.ds(k * tile, width - k * tile)
                    cube = product(ph, pl_, hh, hl, k)
                    square = hh[sl, cols].astype(jnp.float32) + hl[sl, cols].astype(jnp.float32)
                    spread_out(bc * square + cc * cube, uh, ul, k)
                    p_ref[sl, cols] = aa * p_ref[sl, cols] + ab * square + bbac * cube
                travel("cube", sweep)
                for k in range(parts):
                    sl, cols = pl.ds(k * tile, tile), pl.ds(k * tile, width - k * tile)
                    value = p_ref[sl, cols] + product(hh, hl, uh, ul, k)
                    p_ref[sl, cols] = value
                    spread_out(value, ph, pl_, k)

            @pl.when(sweep == ITERS - 2)
            def _():
                first_norm_back()
            return carry

        lax.fori_loop(0, ITERS, body, 0)
        for shift in range(1, 8):
            gains_copy(shift).wait()
        grads = held[0]
        for k in range(1, 8):
            grads = grads + held[k]
        grads = grads[0:2]
        gg_ref[...] = grads
        first = adam_beta * af_ref[...] + (1.0 - adam_beta) * grads
        second = adam_beta * as_ref[...] + (1.0 - adam_beta) * grads * grads
        afn_ref[...] = first
        asn_ref[...] = second
        gu_ref[...] = -adam_rate * (
            first / correction / (jnp.sqrt(second / correction) + adam_eps) + decay_rate * gain_ref[...]
        )

        @pl.when(place.outer)
        def _():
            for i in range(each, chunks):
                back(i, place.chip_z(place.inner_mate)).wait_recv()
            for i in range(each):
                from_end(i, place.chip_z(place.inner_mate), t3_ref).wait_send()
                from_end(each + i, place.chip_z(place.inner_mate), b2_ref).wait_send()
        lo_ref[...] = (r_ref[...] + total[tokens:2 * tokens].astype(jnp.float32)).astype(lo_ref.dtype)

        @pl.when(jnp.logical_not(place.outer))
        def _():
            for i in range(chunks):
                across(i).wait_send()
                back(i, place.chip_z(place.outer_mate)).wait_send()

    f32, low16 = jnp.float32, jnp.bfloat16
    small = jax.ShapeDtypeStruct(norm_gains.shape, f32)
    narrow = jax.ShapeDtypeStruct((tokens, width), low16)
    outs = (jax.ShapeDtypeStruct((rows, width), f32), narrow, narrow, small, small, small, small)
    full = pltpu.VMEM((width, width), low16)
    line = pltpu.VMEM((2 * tokens, width), low16)
    scratch = [pltpu.VMEM((width, width), f32)] + [full] * 7 + [line] * 4
    scratch += [pltpu.VMEM((8, 8, width), f32), pltpu.VMEM((8, width), f32), pltpu.VMEM((tile, width), f32)] + [dma(chunks)] * 6 + [dma(8)] * 2
    ins = (gram, norm, direction_low, normed_term, branch_term, tokens_in, resid, dresid, dgain_rows, norm_gains,
           adam_first, adam_second)
    return comm_call(kernel, outs, ins, [VMEM_SPEC] * len(ins), (VMEM_SPEC,) * len(outs), scratch, ident)


def per_device_block(tokens, out_grad, weight_stack, muon_state, norm_gains, adam_first, adam_second, segment_ids,
                     position_ids):
    token_count, _, model_width = tokens.shape
    groups, contexts = 4, 2
    full_len = token_count * contexts
    local_rows = weight_stack.shape[2]
    heads_dev = HEADS // groups
    ff_dev = FF // groups
    inner_width = heads_dev * HEAD_DIM
    counts = (3 * inner_width, inner_width, 2 * ff_dev, ff_dev)
    own_block = weight_stack.reshape(local_rows, model_width)
    context = lax.axis_index("context")

    cosine, sine_table = rope_tables(position_ids.reshape(token_count), HEAD_DIM)
    segments = segment_ids.reshape(full_len)
    seg_query = lax.dynamic_slice_in_dim(segments, context * token_count, token_count, 0)
    seg_other = lax.dynamic_slice_in_dim(segments, (1 - context) * token_count, token_count, 0)
    (act_in, attn_in, resid, mlp_in, hidden, dmixed, branch_two_term, dresid, dbranch_one, dprojected, dnormed_one_term,
     dgain_rows) = layer_both_ways(
        tokens.reshape(token_count, model_width), out_grad.reshape(token_count, model_width), own_block, norm_gains,
        cosine[:, : HEAD_DIM // 2], sine_table[:, : HEAD_DIM // 2],
        seg_query.reshape(token_count, 1), jnp.concatenate([seg_query, seg_other]).reshape(1, full_len), counts, 0,
    )
    momentum = muon_state.reshape(local_rows, model_width)
    grad_block, direction_low, gram, norm_total = tail_grams(
        (dprojected, act_in, attn_in, dbranch_one, dmixed, mlp_in, hidden, out_grad.reshape(token_count, model_width)),
        momentum, counts, 1,
    )
    direction_scale = jnp.log(jnp.sqrt(norm_total[0, 0])).reshape(1)
    ortho, layer_out, tokens_grad, gain_grads, adam_first_next, adam_second_next, gain_update = iterate(
        gram, norm_total, direction_low, dnormed_one_term, branch_two_term,
        tokens.reshape(token_count, model_width), resid, dresid, dgain_rows, norm_gains, adam_first, adam_second, 2,
    )
    muon_next = muon_beta * momentum + (1.0 - muon_beta) * grad_block
    owner_index = lax.axis_index("fsdp")
    spreads = [0.2 * math.sqrt(3 * D), 0.2 * math.sqrt(D), 0.2 * math.sqrt(2 * FF), 0.2 * math.sqrt(FF)]
    spread = jnp.sum(jnp.where(jnp.arange(4) == owner_index, jnp.array(spreads, jnp.float32), 0.0))
    weight_update = -muon_rate * (spread * ortho + decay_rate * own_block.astype(jnp.float32))
    layer_out = layer_out.reshape(tokens.shape)
    tokens_grad = tokens_grad.reshape(tokens.shape)
    block_shape = (1, 1, local_rows, model_width)
    return (
        layer_out,
        tokens_grad,
        grad_block.reshape(block_shape),
        muon_next.reshape(block_shape),
        weight_update.reshape(block_shape),
        direction_scale,
        gain_grads,
        adam_first_next,
        adam_second_next,
        gain_update,
    )


def solution(mesh):
    sizes = dict(mesh.shape)
    block = (sizes["fsdp"], sizes["context"], sizes["tensor"]) == (4, 2, 4)
    return jax.shard_map(
        per_device_block if block else per_device,
        mesh=mesh,
        in_specs=(
            P("context", "fsdp", None),
            P("context", "fsdp", None),
            P("fsdp", "tensor", "context", None),
            P("fsdp", "tensor", "context", None),
            P(),
            P(),
            P(),
            P(None, "fsdp"),
            P("context", "fsdp"),
        ),
        out_specs=(
            P("context", "fsdp", None),
            P("context", "fsdp", None),
            P("fsdp", "tensor", "context", None),
            P("fsdp", "tensor", "context", None),
            P("fsdp", "tensor", "context", None),
            P("fsdp"),
            P(),
            P(),
            P(),
            P(),
        ),
        check_vma=False,
    )
```
